32 devices in a mesh: seq: 8 (over y, x, core), fsdp: 4 (over z).
Axes of the slice: x: 2, y: 2, z: 4, core: 2. Of those that a mesh axis runs over, the one named last changes fastest.
Arguments:
- tokens: bfloat16 [4, 1024, 2048], P('fsdp', 'seq'), may hold values from -6 to 6
- query_weight: bfloat16 [2048, 2048], P(('seq', 'fsdp')), may hold values from -0.125 to 0.125
- key_weight: bfloat16 [2048, 2048], P(('seq', 'fsdp')), may hold values from -0.125 to 0.125
- value_weight: bfloat16 [2048, 2048], P(('seq', 'fsdp')), may hold values from -0.125 to 0.125
- out_weight: bfloat16 [2048, 2048], P(('seq', 'fsdp')), may hold values from -0.125 to 0.125
- query_gain: bfloat16 [2048], P(('seq', 'fsdp')), may hold values from 0.25 to 1.75
- key_gain: bfloat16 [2048], P(('seq', 'fsdp')), may hold values from 0.25 to 1.75
- attention_gain: bfloat16 [2048], P(('seq', 'fsdp')), may hold values from 0.25 to 1.75
- gate_weight: bfloat16 [2048, 8192], P('fsdp', 'seq'), may hold values from -0.125 to 0.125
- up_weight: bfloat16 [2048, 8192], P('fsdp', 'seq'), may hold values from -0.125 to 0.125
- down_weight: bfloat16 [8192, 2048], P('seq', 'fsdp'), may hold values from -0.0625 to 0.0625
- feedforward_gain: bfloat16 [2048], P(('seq', 'fsdp')), may hold values from 0.25 to 1.75
- cotangent: bfloat16 [4, 1024, 2048], P('fsdp', 'seq'), may hold values from -6 to 6
Outputs:
- layer_out: bfloat16 [4, 1024, 2048], P('fsdp', 'seq')
- tokens_grad: float32 [4, 1024, 2048], P('fsdp', 'seq')
- query_weight_grad: float32 [2048, 2048], P(('seq', 'fsdp'))
- key_weight_grad: float32 [2048, 2048], P(('seq', 'fsdp'))
- value_weight_grad: float32 [2048, 2048], P(('seq', 'fsdp'))
- out_weight_grad: float32 [2048, 2048], P(('seq', 'fsdp'))
- query_gain_grad: float32 [2048], P(('seq', 'fsdp'))
- key_gain_grad: float32 [2048], P(('seq', 'fsdp'))
- attention_gain_grad: float32 [2048], P(('seq', 'fsdp'))
- gate_weight_grad: float32 [2048, 8192], P('fsdp', 'seq')
- up_weight_grad: float32 [2048, 8192], P('fsdp', 'seq')
- down_weight_grad: float32 [8192, 2048], P('seq', 'fsdp')
- feedforward_gain_grad: float32 [2048], P(('seq', 'fsdp'))
The draws below stay inside these ranges and needn't reach their ends.
All inputs are finite; a program needn't handle non-finite values.
Results may differ from the reference program's by a relative error of at most 0.02.
Values may be sent and summed in bfloat16 or wider, within the bound.
A program may use at most 256 MiB of HBM per device.

```python
import math
import jax
import jax.numpy as jnp
from jax import lax

D = 2048
H = 16
HD = 128
FF = 8192
LENGTH = 1024
SEQS = 4


def spiked(entries, own_key, source, target, shards_of, factor):
    def block_of(position):
        return (jnp.arange(entries.shape[position]) // (entries.shape[position] // shards_of)).reshape((-1,) + (1,) * (entries.ndim - 1 - position))

    near = jax.random.permutation(own_key, shards_of)[block_of(target)]
    second = (block_of(target) + shards_of // 2) % shards_of
    return jnp.where((block_of(source) == near) | (block_of(source) == second), factor * entries, entries)


def block_levels(own_key, shape, cuts, least, largest):
    loudness = 1.0
    for position, parts in cuts:
        heights = jax.random.uniform(jax.random.fold_in(jax.random.fold_in(own_key, 6), position), (parts,), jnp.float32, least / len(cuts), largest / len(cuts))
        loudness = loudness * jnp.repeat(jnp.exp(heights), shape[position] // parts).reshape((-1,) + (1,) * (len(shape) - 1 - position))
    return loudness


def noise(rng, extent, spread, limit, split=(), kind=jnp.bfloat16):
    entries = spread * jax.random.normal(rng, extent, jnp.float32)
    if split:
        entries = entries * block_levels(rng, extent, split, -0.22, 0.18)
    return jnp.clip(entries, -limit, limit).astype(kind)


def heavy_noise(stream_key, dims, scale, most, shards, heavy, kind=jnp.bfloat16):
    array = scale * jax.random.normal(stream_key, dims, jnp.float32)
    if shards:
        array = array * block_levels(stream_key, dims, shards, -0.22, 0.18)
    return jnp.clip(spiked(array, jax.random.fold_in(stream_key, 3), *heavy), -most, most).astype(kind)


def setup_inputs(seed: int = 0) -> dict:
    streams_of = jax.random.split(jax.random.key(seed), 14)
    tokens = noise(streams_of[0], (SEQS, LENGTH, D), 1.0, 6.0, ((0, 4), (1, 8)))
    query_weight = noise(streams_of[1], (D, D), D ** -0.5, 0.125, ((0, 32),))
    key_weight = noise(streams_of[2], (D, D), D ** -0.5, 0.125, ((0, 32),))
    value_weight = noise(streams_of[3], (D, D), D ** -0.5, 0.125, ((0, 32),))
    out_weight = noise(streams_of[4], (D, D), D ** -0.5, 0.125, ((0, 32),))
    query_gain = jnp.clip(1.0 + 0.15 * jax.random.normal(streams_of[5], (D,), jnp.float32), 0.25, 1.75).astype(jnp.bfloat16)
    key_gain = jnp.clip(1.0 + 0.15 * jax.random.normal(streams_of[6], (D,), jnp.float32), 0.25, 1.75).astype(jnp.bfloat16)
    attention_gain = jnp.clip(1.0 + 0.15 * jax.random.normal(streams_of[7], (D,), jnp.float32), 0.25, 1.75).astype(jnp.bfloat16)
    gate_weight = noise(streams_of[8], (D, FF), D ** -0.5, 0.125, ((0, 4), (1, 8)))
    up_weight = noise(streams_of[9], (D, FF), D ** -0.5, 0.125, ((0, 4), (1, 8)))
    down_weight = noise(streams_of[10], (FF, D), FF ** -0.5, 0.0625, ((0, 8), (1, 4)))
    feedforward_gain = jnp.clip(1.0 + 0.15 * jax.random.normal(streams_of[11], (D,), jnp.float32), 0.25, 1.75).astype(jnp.bfloat16)
    cotangent = heavy_noise(streams_of[12], (SEQS, LENGTH, D), 1.0, 6.0, ((0, 4), (1, 8)), (1, 2, 8, 2.0))
    return {"tokens": tokens, "query_weight": query_weight, "key_weight": key_weight, "value_weight": value_weight, "out_weight": out_weight, "query_gain": query_gain, "key_gain": key_gain, "attention_gain": attention_gain, "gate_weight": gate_weight, "up_weight": up_weight, "down_weight": down_weight, "feedforward_gain": feedforward_gain, "cotangent": cotangent}


EPSILON = 1e-06
THETA = 500000.0
HIGH = lax.Precision.HIGHEST

@jax.custom_vjp
def low(v):
    return lax.optimization_barrier(v.astype(jnp.bfloat16)).astype(jnp.float32)

@jax.custom_vjp
def low_back(v):
    return v

def low_keep(v):
    return (low(v), None)

def low_pass(kept, grad):
    return (grad,)

def back_keep(v):
    return (v, None)

def back_low(kept, grad):
    return (low(grad),)
low.defvjp(low_keep, low_pass)
low_back.defvjp(back_keep, back_low)

def rms_scale(value, gain):
    return value * lax.rsqrt(lax.optimization_barrier(jnp.mean(value * value, axis=-1, keepdims=True)) + EPSILON) * gain

def rotate(value, positions):
    half = HD // 2
    frequency = jnp.exp(jnp.arange(half, dtype=jnp.float32) * (-2.0 * math.log(THETA) / HD))
    angles = positions[:, None] * frequency[None, :]
    cosine = jnp.cos(angles)[:, None, :]
    sine = jnp.sin(angles)[:, None, :]
    first = value[..., :half]
    second = value[..., half:]
    return jnp.concatenate([first * cosine - second * sine, second * cosine + first * sine], axis=-1)

def attend(queries, keys, values):
    length = queries.shape[0]
    block = min(512, length)
    blocks = length // block
    scale = HD ** (-0.5)
    columns = jnp.arange(length, dtype=jnp.int32)

    def one_block(index):
        query_rows = lax.dynamic_slice_in_dim(queries, index * block, block, 0)
        scores = low_back(jnp.einsum('qhd,khd->hqk', query_rows, keys, precision=HIGH) * scale)
        positions = index * block + jnp.arange(block, dtype=jnp.int32)
        allowed = columns[None, :] <= positions[:, None]
        scores = jnp.where(allowed[None], scores, -jnp.inf)
        weights = jax.nn.softmax(scores, axis=-1)
        return jnp.einsum('hqk,khd->qhd', low(weights), values, precision=HIGH)
    results = lax.map(jax.checkpoint(one_block), jnp.arange(blocks, dtype=jnp.int32))
    return results.reshape(length, H, HD)

def layer(tokens, query_weight, key_weight, value_weight, out_weight, query_gain, key_gain, attention_gain, gate_weight, up_weight, down_weight, feedforward_gain):
    length = tokens.shape[0]
    positions = jnp.arange(length, dtype=jnp.int32).astype(jnp.float32)
    query_raw = low_back(jnp.dot(tokens, query_weight, precision=HIGH))
    key_raw = low_back(jnp.dot(tokens, key_weight, precision=HIGH))
    value_raw = jnp.dot(tokens, value_weight, precision=HIGH)
    queries = low_back(low(rotate(rms_scale(query_raw, query_gain).reshape(length, H, HD), positions)))
    keys = low_back(low(rotate(rms_scale(key_raw, key_gain).reshape(length, H, HD), positions)))
    values = low_back(low(value_raw.reshape(length, H, HD)))
    attended = low_back(low(attend(queries, keys, values))).reshape(length, D)
    branch = low_back(jnp.dot(attended, out_weight, precision=HIGH))
    hidden = tokens + rms_scale(branch, attention_gain)
    hidden_low = low(hidden)
    gate = low_back(jnp.dot(hidden_low, gate_weight, precision=HIGH))
    upward = low_back(jnp.dot(hidden_low, up_weight, precision=HIGH))
    inner = low(jax.nn.silu(gate) * upward)
    feedforward = low_back(jnp.dot(inner, down_weight, precision=HIGH))
    return hidden + rms_scale(feedforward, feedforward_gain)

def reference(tokens, query_weight, key_weight, value_weight, out_weight, query_gain, key_gain, attention_gain, gate_weight, up_weight, down_weight, feedforward_gain, cotangent):
    params = tuple((w.astype(jnp.float32) for w in (query_weight, key_weight, value_weight, out_weight, query_gain, key_gain, attention_gain, gate_weight, up_weight, down_weight, feedforward_gain)))

    def per_sequence(totals, pair):
        seq_tokens, seq_cotangent = pair
        result, pullback = jax.vjp(layer, seq_tokens.astype(jnp.float32), *params)
        grads = pullback(seq_cotangent.astype(jnp.float32))
        totals = tuple((t + g for t, g in zip(totals, grads[1:])))
        return (totals, (result.astype(jnp.bfloat16), grads[0]))
    zeros = tuple((jnp.zeros(w.shape, jnp.float32) for w in params))
    totals, (outputs, tokens_grad) = lax.scan(per_sequence, zeros, (tokens, cotangent))
    return (outputs, tokens_grad, totals[0], totals[1], totals[2], totals[3], totals[4], totals[5], totals[6], totals[7], totals[8], totals[9], totals[10])
```

```python
import functools
import math

import jax
import jax.numpy as jnp
from jax import lax
from jax.experimental import pallas as pl
from jax.experimental.pallas import tpu as pltpu
from jax.sharding import PartitionSpec as P

EPSILON = 1e-06
THETA = 500000.0
HD = 128
F32 = jnp.float32
BF16 = jnp.bfloat16


def dot(a, b, dims):
    return lax.dot_general(a, b, (dims, ((), ())), preferred_element_type=F32)


NN = ((1,), (0,))
NT = ((1,), (1,))
TN = ((0,), (0,))


def angles_of(length):
    half = HD // 2
    frequency = jnp.exp(jnp.arange(half, dtype=F32) * (-2.0 * math.log(THETA) / HD))
    angle = jnp.arange(length, dtype=F32)[:, None] * frequency[None, :]
    return jnp.cos(angle), jnp.sin(angle)


def rotate(value, cosine, sine, sign):
    length, width = value.shape
    value = value.reshape(length, width // HD, 2, HD // 2)
    first, second = value[:, :, 0], value[:, :, 1]
    c, s = cosine[:, None, :], sign * sine[:, None, :]
    return jnp.stack([first * c - second * s, second * c + first * s], axis=2).reshape(length, width)


def attention_forward_kernel(block, q_ref, k_ref, v_ref, out_ref, low_ref, log_ref):
    length = q_ref.shape[0]
    scale = HD ** (-0.5)
    for i in range(length // block):
        rows = pl.ds(i * block, block)
        width = (i + 1) * block
        s = dot(q_ref[rows, :], k_ref[pl.ds(0, width), :], NT) * scale
        column = lax.broadcasted_iota(jnp.int32, (block, width), 1)
        row = lax.broadcasted_iota(jnp.int32, (block, width), 0) + i * block
        s = jnp.where(column <= row, s, -jnp.inf)
        top = jnp.max(s, axis=-1, keepdims=True)
        p = jnp.exp(s - top)
        total = jnp.sum(p, axis=-1, keepdims=True)
        weights = (p * (1.0 / total)).astype(BF16)
        out = dot(weights, v_ref[pl.ds(0, width), :], NN)
        out_ref[rows, :] = out
        low_ref[rows, :] = out.astype(BF16)
        log_ref[0, rows, :] = top + jnp.log(total)


def attention_forward(q, k, v):
    length, width = q.shape
    heads = width // HD
    block = min(256, length)
    column = pl.BlockSpec((length, HD), lambda h: (0, h))
    return pl.pallas_call(
        functools.partial(attention_forward_kernel, block),
        grid=(heads,),
        in_specs=[column] * 3,
        out_specs=[column, column, pl.BlockSpec((1, length, 1), lambda h: (h, 0, 0))],
        out_shape=[
            jax.ShapeDtypeStruct((length, width), F32),
            jax.ShapeDtypeStruct((length, width), BF16),
            jax.ShapeDtypeStruct((heads, length, 1), F32),
        ],
        cost_estimate=pl.CostEstimate(
            flops=2 * heads * length * length * HD, bytes_accessed=10 * length * width, transcendentals=0
        ),
    )(q, k, v)


def attention_backward_kernel(block, q_ref, k_ref, v_ref, out_ref, log_ref, g_ref, dq_ref, dk_ref, dv_ref, dk, dv):
    length = q_ref.shape[0]
    scale = HD ** (-0.5)
    dk[...] = jnp.zeros_like(dk)
    dv[...] = jnp.zeros_like(dv)
    for i in range(length // block):
        rows = pl.ds(i * block, block)
        width = (i + 1) * block
        wide = pl.ds(0, width)
        q = q_ref[rows, :]
        g = g_ref[rows, :]
        s = dot(q, k_ref[wide, :], NT) * scale
        column = lax.broadcasted_iota(jnp.int32, (block, width), 1)
        row = lax.broadcasted_iota(jnp.int32, (block, width), 0) + i * block
        s = jnp.where(column <= row, s, -jnp.inf)
        weights = jnp.exp(s - log_ref[0, rows, :])
        correction = jnp.sum(g.astype(F32) * out_ref[rows, :], axis=-1, keepdims=True)
        gw = dot(g, v_ref[wide, :], NT)
        gs = (weights * (gw - correction)).astype(BF16)
        dq_ref[rows, :] = (dot(gs, k_ref[wide, :], NN) * scale).astype(BF16)
        dk[wide, :] += dot(gs, q, TN)
        dv[wide, :] += dot(weights.astype(BF16), g, TN)
    dk_ref[...] = (dk[...] * scale).astype(BF16)
    dv_ref[...] = dv[...].astype(BF16)


def attention_backward(q, k, v, out, log_total, g):
    length, width = q.shape
    heads = width // HD
    block = min(256, length)
    column = pl.BlockSpec((length, HD), lambda h: (0, h))
    return pl.pallas_call(
        functools.partial(attention_backward_kernel, block),
        grid=(heads,),
        in_specs=[column] * 4 + [pl.BlockSpec((1, length, 1), lambda h: (h, 0, 0)), column],
        out_specs=[column] * 3,
        out_shape=[jax.ShapeDtypeStruct((length, width), BF16)] * 3,
        scratch_shapes=[pltpu.VMEM((length, HD), F32)] * 2,
        cost_estimate=pl.CostEstimate(
            flops=5 * heads * length * length * HD, bytes_accessed=16 * length * width, transcendentals=0
        ),
    )(q, k, v, out, log_total, g)


def on_device(n, m, pair, *args):
    (
        tokens,
        query_weight,
        key_weight,
        value_weight,
        out_weight,
        query_gain,
        key_gain,
        attention_gain,
        gate_weight,
        up_weight,
        down_weight,
        feedforward_gain,
        cotangent,
    ) = args
    rows, width = tokens.shape[1], tokens.shape[2]
    length = rows * n
    part = query_weight.shape[0]
    cols = width // n
    depth, units = gate_weight.shape
    share = units // pair
    x = tokens.reshape(rows, width)
    groups = [[g * pair + u for u in range(pair)] for g in range(m // pair)]

    def gather_plane(v):
        return lax.all_gather(v, "seq", axis=0, tiled=True)

    def scatter_plane(v):
        return lax.psum_scatter(v.astype(BF16), "seq", scatter_dimension=0, tiled=True).astype(F32)

    def gather_pair(v):
        if pair > 1:
            v = lax.all_gather(v, "fsdp", axis=0, axis_index_groups=groups)
        v = lax.all_gather(v.reshape(pair, rows, width), "seq", axis=1, tiled=True)
        return v.reshape(pair * length, width)

    def scatter_pair(v):
        v = lax.psum_scatter(v.astype(BF16).reshape(pair, length, width), "seq", scatter_dimension=1, tiled=True)
        if pair > 1:
            v = lax.psum_scatter(v, "fsdp", scatter_dimension=0, axis_index_groups=groups)
        return v.reshape(rows, width).astype(F32)

    def spread(halves):
        return lax.all_to_all(jnp.tile(halves, (m // pair, 1, 1)), "fsdp", 0, 0, tiled=False)

    def settle(blocks):
        back = lax.all_to_all(blocks.astype(BF16), "fsdp", 0, 0, tiled=False)
        return jnp.sum(back.reshape((m // pair, pair) + back.shape[1:]).astype(F32), axis=0)

    stacked = jnp.stack([query_weight, key_weight, value_weight], axis=1).reshape(part, 3, n, cols)
    mine = lax.all_to_all(stacked.transpose(2, 0, 1, 3), "seq", 0, 0)
    qkv = lax.all_gather(mine, "fsdp", axis=1).reshape(width, 3 * cols)
    out_rows = lax.all_gather(out_weight, "fsdp", axis=0, tiled=True)
    gains = jnp.stack([query_gain, key_gain])
    own_gain = lax.all_gather(gains, "fsdp", axis=1).reshape(2, cols).astype(F32)
    full_gain = (
        lax.all_gather(jnp.stack([attention_gain, feedforward_gain]), ("seq", "fsdp"), axis=1)
        .reshape(2, width)
        .astype(F32)
    )
    q_gain, k_gain = own_gain[0], own_gain[1]
    branch_gain, feed_gain = full_gain[0], full_gain[1]

    xs = gather_plane(x)
    raw = dot(xs, qkv, NN)
    q_raw, k_raw, v = raw[:, :cols], raw[:, cols : 2 * cols], raw[:, 2 * cols :].astype(BF16)
    squares = jnp.stack([jnp.sum(q_raw * q_raw, axis=1), jnp.sum(k_raw * k_raw, axis=1)])
    squares = lax.psum(squares, "seq") / width
    inverse = lax.rsqrt(squares + EPSILON)
    q_inv, k_inv = inverse[0][:, None], inverse[1][:, None]
    cosine, sine = angles_of(length)
    q = rotate(q_raw * q_inv * q_gain, cosine, sine, 1.0).astype(BF16)
    k = rotate(k_raw * k_inv * k_gain, cosine, sine, 1.0).astype(BF16)
    attended, attended_low, log_total = attention_forward(q, k, v)
    branch = scatter_plane(dot(attended_low, out_rows, NN))
    branch_inv = lax.rsqrt(jnp.mean(branch * branch, axis=1, keepdims=True) + EPSILON)
    hidden = x.astype(F32) + branch * branch_inv * branch_gain
    hs = gather_pair(hidden.astype(BF16))

    gate_cols = spread(gate_weight.reshape(depth, pair, share).transpose(1, 0, 2)).reshape(width, share)
    up_cols = spread(up_weight.reshape(depth, pair, share).transpose(1, 0, 2)).reshape(width, share)
    down_rows = spread(down_weight.reshape(pair, share, depth)).transpose(1, 0, 2).reshape(share, width)

    gate = dot(hs, gate_cols, NN)
    up = dot(hs, up_cols, NN)
    sig = jax.nn.sigmoid(gate)
    inner = (gate * sig * up).astype(BF16)
    feed = scatter_pair(dot(inner, down_rows, NN))
    feed_inv = lax.rsqrt(jnp.mean(feed * feed, axis=1, keepdims=True) + EPSILON)
    normal = feed * feed_inv
    layer_out = (hidden + normal * feed_gain).astype(BF16)

    grad_out = cotangent.reshape(rows, width).astype(F32)
    u = grad_out * feed_gain
    grad_feed = feed_inv * (u - normal * jnp.mean(u * normal, axis=1, keepdims=True))
    feed_gain_term = jnp.sum(grad_out * normal, axis=0)
    gs = gather_pair(grad_feed.astype(BF16))
    grad_inner = dot(gs, down_rows, NT)
    grad_gate = (grad_inner * up * sig * (1.0 + gate * (1.0 - sig))).astype(BF16)
    grad_up = (grad_inner * gate * sig).astype(BF16)
    grad_hidden = grad_out + scatter_pair(dot(grad_gate, gate_cols, NT) + dot(grad_up, up_cols, NT))
    down_grad = settle(dot(inner, gs, TN).reshape(share, m, depth).transpose(1, 0, 2)).reshape(units, depth)
    gate_grad = settle(dot(hs, grad_gate, TN).reshape(m, depth, share)).transpose(1, 0, 2).reshape(depth, units)
    up_grad = settle(dot(hs, grad_up, TN).reshape(m, depth, share)).transpose(1, 0, 2).reshape(depth, units)

    normal = branch * branch_inv
    u = grad_hidden * branch_gain
    grad_branch = branch_inv * (u - normal * jnp.mean(u * normal, axis=1, keepdims=True))
    branch_gain_term = jnp.sum(grad_hidden * normal, axis=0)
    bs = gather_plane(grad_branch.astype(BF16))
    out_grad = lax.psum_scatter(
        dot(attended_low, bs, TN).astype(BF16), "fsdp", scatter_dimension=0, tiled=True
    ).astype(F32)
    grad_attended = dot(bs, out_rows, NT).astype(BF16)
    dq, dk, dv = attention_backward(q, k, v, attended, log_total, grad_attended)
    dq = rotate(dq.astype(F32), cosine, sine, -1.0)
    dk = rotate(dk.astype(F32), cosine, sine, -1.0)
    q_normal, k_normal = q_raw * q_inv, k_raw * k_inv
    q_gain_term = jnp.sum(dq * q_normal, axis=0)
    k_gain_term = jnp.sum(dk * k_normal, axis=0)
    dq, dk = dq * q_gain, dk * k_gain
    means = lax.psum(jnp.stack([jnp.sum(dq * q_normal, axis=1), jnp.sum(dk * k_normal, axis=1)]), "seq") / width
    dq = (q_inv * (dq - q_normal * means[0][:, None])).astype(BF16)
    dk = (k_inv * (dk - k_normal * means[1][:, None])).astype(BF16)
    d3 = jnp.concatenate([dq, dk, dv], axis=1)
    tokens_grad = grad_hidden + scatter_plane(dot(d3, qkv, NT))
    term = dot(xs, d3, TN).astype(BF16).reshape(n, m, part, 3 * cols)
    term = lax.psum_scatter(term, "fsdp", scatter_dimension=1)
    term = lax.all_to_all(term, "seq", 0, 0)
    term = term.reshape(n, part, 3, cols).transpose(2, 1, 0, 3).reshape(3, part, width).astype(F32)
    gain_own = lax.psum_scatter(jnp.stack([q_gain_term, k_gain_term]), "fsdp", scatter_dimension=1, tiled=True)
    gain_full = lax.psum_scatter(
        jnp.stack([branch_gain_term, feed_gain_term]), ("seq", "fsdp"), scatter_dimension=1, tiled=True
    )
    return (
        layer_out.reshape(tokens.shape),
        tokens_grad.reshape(tokens.shape),
        term[0],
        term[1],
        term[2],
        out_grad,
        gain_own[0],
        gain_own[1],
        gain_full[0],
        gate_grad,
        up_grad,
        down_grad,
        gain_full[1],
    )


def solution(mesh):
    n, m = mesh.shape["seq"], mesh.shape["fsdp"]
    tall, flat, act = P(("seq", "fsdp"), None), P(("seq", "fsdp")), P("fsdp", "seq", None)
    wide, deep = P("fsdp", "seq"), P("seq", "fsdp")
    return jax.shard_map(
        functools.partial(on_device, n, m, 2),
        mesh=mesh,
        in_specs=(act, tall, tall, tall, tall, flat, flat, flat, wide, wide, deep, flat, act),
        out_specs=(act, act, tall, tall, tall, tall, flat, flat, flat, wide, wide, deep, flat),
        check_vma=False,
    )
```

```python
import functools
import math

import jax
import jax.numpy as jnp
from jax import lax
from jax.experimental import pallas as pl
from jax.experimental.pallas import tpu as pltpu
from jax.sharding import PartitionSpec as P

EPSILON = 1e-06
THETA = 500000.0
HD = 128
F32 = jnp.float32
BF16 = jnp.bfloat16


def dot(a, b, dims):
    return lax.dot_general(a, b, (dims, ((), ())), preferred_element_type=F32)


NN = ((1,), (0,))
NT = ((1,), (1,))
TN = ((0,), (0,))


def angles_of(length):
    half = HD // 2
    frequency = jnp.exp(jnp.arange(half, dtype=F32) * (-2.0 * math.log(THETA) / HD))
    angle = jnp.arange(length, dtype=F32)[:, None] * frequency[None, :]
    return jnp.cos(angle), jnp.sin(angle)


def rotate(value, cosine, sine, sign):
    length, width = value.shape
    value = value.reshape(length, width // HD, 2, HD // 2)
    first, second = value[:, :, 0], value[:, :, 1]
    c, s = cosine[:, None, :], sign * sine[:, None, :]
    return jnp.stack([first * c - second * s, second * c + first * s], axis=2).reshape(length, width)


MESH = pl.DeviceIdType.MESH


def flip(index, bit):
    return index + bit - 2 * bit * ((index // bit) % 2)


class Place:
    def __init__(self, pair):
        self.s, self.f = lax.axis_index("seq"), lax.axis_index("fsdp")
        self.pair = pair
        s, f = self.s, self.f
        self.sx, self.sy = flip(s, 2), flip(s, 4)
        self.sd, self.sc = flip(self.sx, 4), flip(s, 1)
        self.q = f % pair
        self.x, self.y, self.core = (self.sx, f), (self.sy, f), (self.sc, f)
        self.z = (s, flip(f, 1)) if pair > 1 else None
        self.peers = [self.x, self.y, self.core] + ([self.z] if pair > 1 else [])

    def barrier(self):
        sem = pltpu.get_barrier_semaphore()
        for peer in self.peers:
            pl.semaphore_signal(sem, inc=1, device_id=peer, device_id_type=MESH)
        pl.semaphore_wait(sem, len(self.peers))


class Wires:
    def __init__(self, send, recv):
        self.send, self.recv, self.count, self.open = send, recv, 0, {}

    def new(self, key):
        self.open[key] = self.count
        self.count += 1

    def go(self, key, src, dst, device):
        i = self.open[key]
        copy = pltpu.make_async_remote_copy(
            src, dst, self.send.at[i], self.recv.at[i], device_id=device, device_id_type=MESH
        )
        copy.start()
        return copy


def gather_steps(place, wires, own, out, ready):
    pair, rows = place.pair, own.shape[0]
    half = rows // 2
    top, low = pl.ds(0, half), pl.ds(half, half)
    p = place
    qs = [p.q] + ([1 - p.q] if pair > 1 else [])
    kinds = ["xa", "xb", "ya", "yb", "xd", "yd", "c0", "cxa", "cxb", "cya", "cyb", "cda", "cdb"]
    for t in range(pair):
        for kind in kinds:
            wires.new((t, kind))
    if pair > 1:
        wires.new("z")
    live = {}

    def go(key, src, dst, device):
        live[key] = wires.go(key, src, dst, device)

    def begin(t, src):
        q = qs[t]
        go((t, "xa"), src.at[top], out.at[q, p.s, top], p.x)
        go((t, "yb"), src.at[low], out.at[q, p.s, low], p.y)
        go((t, "xb"), src.at[low], out.at[q, p.s, low], p.x)
        go((t, "ya"), src.at[top], out.at[q, p.s, top], p.y)
        go((t, "c0"), src, out.at[q, p.s], p.core)

    def arrived(key):
        live[key].wait_recv()

    if pair > 1:
        go("z", own, out.at[qs[0], p.s], p.z)
    begin(0, own)
    ready(qs[0], p.s, None)

    def first(t):
        q = qs[t]
        arrived((t, "xa"))
        go((t, "xd"), out.at[q, p.sx, top], out.at[q, p.sx, top], p.y)
        go((t, "cxa"), out.at[q, p.sx, top], out.at[q, p.sx, top], p.core)
        arrived((t, "yb"))
        go((t, "yd"), out.at[q, p.sy, low], out.at[q, p.sy, low], p.x)
        go((t, "cyb"), out.at[q, p.sy, low], out.at[q, p.sy, low], p.core)
        arrived((t, "c0"))
        ready(q, p.sc, None)

    def second(t):
        q = qs[t]
        arrived((t, "xb"))
        go((t, "cxb"), out.at[q, p.sx, low], out.at[q, p.sx, low], p.core)
        ready(q, p.sx, None)
        arrived((t, "ya"))
        go((t, "cya"), out.at[q, p.sy, top], out.at[q, p.sy, top], p.core)
        ready(q, p.sy, None)
        arrived((t, "xd"))
        go((t, "cda"), out.at[q, p.sd, top], out.at[q, p.sd, top], p.core)
        arrived((t, "yd"))
        go((t, "cdb"), out.at[q, p.sd, low], out.at[q, p.sd, low], p.core)

    def third(t):
        q = qs[t]
        arrived((t, "cxa"))
        arrived((t, "cxb"))
        ready(q, flip(p.sx, 1), None)
        arrived((t, "cya"))
        arrived((t, "cyb"))
        ready(q, flip(p.sy, 1), None)
        ready(q, p.sd, None)
        arrived((t, "cda"))
        arrived((t, "cdb"))
        ready(q, flip(p.sd, 1), None)

    first(0)
    if pair > 1:
        arrived("z")
        begin(1, out.at[qs[1], p.s])
        ready(qs[1], p.s, None)
    second(0)
    if pair > 1:
        first(1)
    third(0)
    if pair > 1:
        second(1)
        third(1)
    for copy in live.values():
        copy.wait_send()


def gather_wires(pair):
    return 13 * pair + (1 if pair > 1 else 0)


def gather_kernel(pair, own, out, send, recv, local):
    place = Place(pair)
    keep = pltpu.make_async_copy(own, out.at[place.q, place.s], local)
    keep.start()
    place.barrier()
    gather_steps(place, Wires(send, recv), own, out, lambda q, slot, half: None)
    keep.wait()


def plane_gather(v, n, pair, ident):
    rows, width = v.shape
    return pl.pallas_call(
        functools.partial(gather_kernel, pair),
        in_specs=[pl.BlockSpec(memory_space=pltpu.VMEM)],
        out_specs=pl.BlockSpec(memory_space=pl.ANY),
        out_shape=jax.ShapeDtypeStruct((pair, n, rows, width), v.dtype),
        scratch_shapes=[pltpu.SemaphoreType.DMA((gather_wires(pair),))] * 2 + [pltpu.SemaphoreType.DMA],
        compiler_params=pltpu.CompilerParams(collective_id=ident, has_side_effects=True),
        cost_estimate=pl.CostEstimate(flops=0, bytes_accessed=pair * n * rows * width * 20, transcendentals=0),
        name=f"gather_{ident}",
    )(v).reshape(pair * n * rows, width)


def add(a, b):
    return (a.astype(F32) + b.astype(F32)).astype(BF16)


def scatter_steps(place, wires, part, rc, rd, rx, ry, qbuf, zbuf, make, finish):
    p, pair = place, place.pair
    rows = rx.shape[1]
    half = rows // 2
    top, low = pl.ds(0, half), pl.ds(half, half)
    slots = {"d": p.sd, "x": p.sx, "y": p.sy, "o": p.s}
    order = ["d", "x", "y", "o"]
    names = ["c" + k for k in order] + ["da", "db", "xa", "xb", "ya", "yb"]
    for t in range(pair):
        for name in names:
            wires.new((t, name))
    if pair > 1:
        wires.new("z")
    live = {}

    def go(key, src, dst, device):
        live[key] = wires.go(key, src, dst, device)

    def arrived(key):
        live[key].wait_recv()

    for t in range(pair):
        for i, k in enumerate(order):
            make(t, k, 1)
            go((t, "c" + k), part(t, flip(slots[k], 1)), rc.at[t, i], p.core)

    def start(t):
        make(t, "d", 0)
        arrived((t, "cd"))
        qbuf[t, 0] = add(part(t, p.sd)[...], rc[t, 0])
        go((t, "da"), qbuf.at[t, 0, top], rd.at[t, top], p.x)
        go((t, "db"), qbuf.at[t, 0, low], rd.at[t, low], p.y)
        make(t, "x", 0)
        arrived((t, "cx"))
        qbuf[t, 1, top] = add(part(t, p.sx)[top], rc[t, 1, top])
        go((t, "xa"), qbuf.at[t, 1, top], rx.at[t, top], p.x)
        make(t, "y", 0)
        arrived((t, "cy"))
        qbuf[t, 2, low] = add(part(t, p.sy)[low], rc[t, 2, low])
        go((t, "yb"), qbuf.at[t, 2, low], ry.at[t, low], p.y)

    def relay(t):
        held = part(t, p.sx)[low].astype(F32) + rc[t, 1, low].astype(F32)
        arrived((t, "db"))
        qbuf[t, 1, low] = (held + rd[t, low].astype(F32)).astype(BF16)
        go((t, "xb"), qbuf.at[t, 1, low], rx.at[t, low], p.x)
        held = part(t, p.sy)[top].astype(F32) + rc[t, 2, top].astype(F32)
        arrived((t, "da"))
        qbuf[t, 2, top] = (held + rd[t, top].astype(F32)).astype(BF16)
        go((t, "ya"), qbuf.at[t, 2, top], ry.at[t, top], p.y)

    def total(t):
        make(t, "o", 0)
        arrived((t, "co"))
        value = part(t, p.s)[...].astype(F32) + rc[t, 3].astype(F32)
        for key in ("xa", "yb", "xb", "ya"):
            arrived((t, key))
        return value + rx[t].astype(F32) + ry[t].astype(F32)

    if pair > 1:
        start(0)
        start(1)
        relay(0)
        relay(1)
        zbuf[0] = total(0).astype(BF16)
        go("z", zbuf.at[0], zbuf.at[1], p.z)
        value = total(1)
        arrived("z")
        value = value + zbuf[1].astype(F32)
    else:
        start(0)
        relay(0)
        value = total(0)
    finish(value)
    for copy in live.values():
        copy.wait_send()


def scatter_wires(pair):
    return 10 * pair + (1 if pair > 1 else 0)


def scatter_scratch(pair, rows, width):
    block = lambda *lead: pltpu.VMEM(lead + (rows, width), BF16)
    return [
        block(pair, 4),
        block(pair),
        block(pair),
        block(pair),
        block(pair, 3),
        block(2) if pair > 1 else pltpu.VMEM((2, 16, 128), BF16),
        pltpu.SemaphoreType.DMA((scatter_wires(pair),)),
        pltpu.SemaphoreType.DMA((scatter_wires(pair),)),
    ]


def scatter_kernel(pair, value, out, rc, rd, rx, ry, qbuf, zbuf, send, recv):
    place = Place(pair)
    place.barrier()
    planes = [1 - place.q, place.q] if pair > 1 else [0]

    def part(t, slot):
        return value.at[planes[t], slot]

    def finish(total):
        out[...] = total

    scatter_steps(
        place, Wires(send, recv), part, rc, rd, rx, ry, qbuf, zbuf, lambda *_: None, finish
    )


def plane_scatter(v, n, pair, ident):
    width = v.shape[1]
    rows = v.shape[0] // (pair * n)
    return pl.pallas_call(
        functools.partial(scatter_kernel, pair),
        in_specs=[pl.BlockSpec(memory_space=pltpu.VMEM)],
        out_specs=pl.BlockSpec(memory_space=pltpu.VMEM),
        out_shape=jax.ShapeDtypeStruct((rows, width), F32),
        scratch_shapes=scatter_scratch(pair, rows, width),
        compiler_params=pltpu.CompilerParams(
            collective_id=ident, has_side_effects=True, vmem_limit_bytes=40 * 2**20
        ),
        cost_estimate=pl.CostEstimate(flops=0, bytes_accessed=pair * n * rows * width * 20, transcendentals=0),
        name=f"scatter_{ident}",
    )(v.astype(BF16).reshape(pair, n, rows, width))


def sum_kernel(n, own, out, held, send, recv):
    s, f = lax.axis_index("seq"), lax.axis_index("fsdp")
    sem = pltpu.get_barrier_semaphore()
    for d in range(1, n):
        pl.semaphore_signal(sem, inc=1, device_id=((s + d) % n, f), device_id_type=MESH)
    pl.semaphore_wait(sem, n - 1)
    copies = []
    for d in range(1, n):
        copy = pltpu.make_async_remote_copy(
            own,
            held.at[d - 1],
            send.at[d - 1],
            recv.at[d - 1],
            device_id=((s + d) % n, f),
            device_id_type=MESH,
        )
        copy.start()
        copies.append(copy)
    total = own[...]
    for d in range(1, n):
        copies[d - 1].wait_recv()
        total = total + held[d - 1]
    out[...] = total
    for copy in copies:
        copy.wait_send()


def plane_sum(v, n, ident):
    return pl.pallas_call(
        functools.partial(sum_kernel, n),
        in_specs=[pl.BlockSpec(memory_space=pltpu.VMEM)],
        out_specs=pl.BlockSpec(memory_space=pltpu.VMEM),
        out_shape=jax.ShapeDtypeStruct(v.shape, v.dtype),
        scratch_shapes=[pltpu.VMEM((n - 1,) + v.shape, v.dtype)]
        + [pltpu.SemaphoreType.DMA((n - 1,))] * 2,
        compiler_params=pltpu.CompilerParams(collective_id=ident, has_side_effects=True),
        name=f"sum_{ident}",
    )(v)


def when(condition, body):
    pl.when(condition)(body)


def line_barrier(n, m):
    s, f = lax.axis_index("seq"), lax.axis_index("fsdp")
    sem = pltpu.get_barrier_semaphore()
    for d in range(1, n):
        pl.semaphore_signal(sem, inc=1, device_id=((s + d) % n, f), device_id_type=MESH)
    for d in range(1, m):
        pl.semaphore_signal(sem, inc=1, device_id=(s, (f + d) % m), device_id_type=MESH)
    pl.semaphore_wait(sem, n + m - 2)


def entry_kernel(
    n, m, x, wq, wk, wv, gains, xs, qkv, full, send, recv, asend, arecv, zsend, zrecv, gsend, grecv, local
):
    place = Place(1)
    s, f = place.s, place.f
    cols = qkv.shape[-1]
    weights = (wq, wk, wv)
    kept = [pltpu.make_async_copy(x, xs.at[0, s], local.at[0]), pltpu.make_async_copy(gains, full.at[f, s], local.at[1])]
    for j, w in enumerate(weights):
        own = w.at[:, pl.ds(pl.multiple_of(s * cols, cols), cols)]
        kept.append(pltpu.make_async_copy(own, qkv.at[j, f, s], local.at[2 + j]))
    for copy in kept:
        copy.start()
    line_barrier(n, m)
    sent = []

    def remote(src, dst, a, b, device):
        copy = pltpu.make_async_remote_copy(src, dst, a, b, device_id=device, device_id_type=MESH)
        copy.start()
        sent.append(copy)
        return copy

    first = []
    for d in range(1, n):
        first.append(remote(gains, full.at[f, s], gsend.at[d], grecv.at[d], ((s + d) % n, f)))
    second = []
    for j, w in enumerate(weights):
        row = []
        for d in range(1, n):
            t = (s + d) % n
            src = w.at[:, pl.ds(pl.multiple_of(t * cols, cols), cols)]
            row.append(remote(src, qkv.at[j, f, s], asend.at[j, d], arecv.at[j, d], (t, f)))
        second.append(row)

    def piece(j, o):
        return full.at[o] if j == 3 else qkv.at[j, o]

    def hop(way, h, j):
        o = f - h if way == 0 else f + h
        there = f + 1 if way == 0 else f - 1
        place_ = piece(j, o)
        return pltpu.make_async_remote_copy(
            place_, place_, zsend.at[way, h, j], zrecv.at[way, h, j], device_id=(s, there), device_id_type=MESH
        )

    def sends(way, h):
        return ((f - h >= 0) & (f < m - 1)) if way == 0 else ((f + h <= m - 1) & (f > 0))

    def receives(way, h):
        return (f - h - 1 >= 0) if way == 0 else (f + h + 1 <= m - 1)

    def start(h, j):
        for way in (0, 1):
            when(sends(way, h), lambda: hop(way, h, j).start())

    def landed(h, j):
        for way in (0, 1):
            o = f - h - 1 if way == 0 else f + h + 1

            def wait():
                there = f - 1 if way == 0 else f + 1
                place_ = piece(j, o)
                pltpu.make_async_remote_copy(
                    place_, place_, zsend.at[way, h, j], zrecv.at[way, h, j], device_id=(s, there), device_id_type=MESH
                ).wait_recv()

            when(receives(way, h), wait)

    for copy in kept:
        copy.wait()
    for copy in first:
        copy.wait_recv()
    start(0, 3)
    for j in range(3):
        for copy in second[j]:
            copy.wait_recv()
        start(0, j)
    gather_steps(place, Wires(send, recv), x, xs, lambda *_: None)
    for h in range(m - 1):
        for j in (3, 0, 1, 2):
            landed(h, j)
            if h + 1 < m - 1:
                start(h + 1, j)
    for copy in sent:
        copy.wait_send()
    for h in range(m - 1):
        for j in range(4):
            for way in (0, 1):
                when(sends(way, h), lambda: hop(way, h, j).wait_send())


def entry(x, wq, wk, wv, gains, n, m, ident):
    rows, width = x.shape
    part = wq.shape[0]
    cols = width // n
    vmem, any_ = pl.BlockSpec(memory_space=pltpu.VMEM), pl.BlockSpec(memory_space=pl.ANY)
    dma = pltpu.SemaphoreType.DMA
    xs, qkv, full = pl.pallas_call(
        functools.partial(entry_kernel, n, m),
        in_specs=[vmem] * 5,
        out_specs=[any_] * 3,
        out_shape=[
            jax.ShapeDtypeStruct((1, n, rows, width), x.dtype),
            jax.ShapeDtypeStruct((3, m, n, part, cols), wq.dtype),
            jax.ShapeDtypeStruct((m, n) + gains.shape, gains.dtype),
        ],
        scratch_shapes=[dma((gather_wires(1),))] * 2
        + [dma((3, n))] * 2
        + [dma((2, m, 4))] * 2
        + [dma((n,))] * 2
        + [dma((5,))],
        compiler_params=pltpu.CompilerParams(collective_id=ident, has_side_effects=True),
        cost_estimate=pl.CostEstimate(flops=0, bytes_accessed=200 * 2**20, transcendentals=0),
        name=f"entry_{ident}",
    )(x, wq, wk, wv, gains)
    qkv = qkv.transpose(0, 2, 1, 3, 4).reshape(3, width, cols)
    return xs.reshape(n * rows, width), qkv, full


def exit_kernel(
    n,
    m,
    value,
    term,
    gains,
    grad_hidden,
    tokens_grad,
    weight_grad,
    gain_grad,
    rc,
    rd,
    rx,
    ry,
    qbuf,
    zbuf,
    send,
    recv,
    line,
    sums,
    done,
    got,
    gplane,
    gsum,
    gline,
    zsend,
    zrecv,
    asend,
    arecv,
    gsend,
    grecv,
    lsend,
    lrecv,
):
    place = Place(1)
    s, f = place.s, place.f
    line_barrier(n, m)
    last = m - 1
    cols = term.shape[-1]

    def remote(src, dst, a, b, device):
        return pltpu.make_async_remote_copy(src, dst, a, b, device_id=device, device_id_type=MESH)

    def target(way, r):
        return last - r if way == 0 else r

    def hop(way, r, j, fresh):
        there = f + 1 if way == 0 else f - 1
        src = term.at[j, :, target(way, r)] if fresh else sums.at[way, r, j]
        return remote(src, line.at[way, r, j], zsend.at[way, r, j], zrecv.at[way, r, j], (s, there))

    ends = (f == 0, f == last)
    inner = (f > 0, f < last)

    def beyond(way, r):
        return target(way, r) > f if way == 0 else target(way, r) < f

    for r in range(last):
        for j in range(3):
            for way in (0, 1):
                when(ends[way], lambda: hop(way, r, j, True).start())

    gain_copies = []
    for d in range(1, n):
        t = (s + d) % n
        copy = remote(gains.at[t], gplane.at[d - 1], gsend.at[d], grecv.at[d], (t, f))
        copy.start()
        gain_copies.append(copy)

    def part(t, slot):
        return value.at[0, slot]

    def finish(total):
        tokens_grad[...] = total + grad_hidden[...]

    scatter_steps(place, Wires(send, recv), part, rc, rd, rx, ry, qbuf, zbuf, lambda *_: None, finish)

    total = gains[s]
    for d in range(1, n):
        gain_copies[d - 1].wait_recv()
        total = total + gplane[d - 1]
    gsum[...] = total
    line_copies = []
    for d in range(1, m):
        t = (f + d) % m
        copy = remote(gsum.at[t], gline.at[d - 1], lsend.at[d], lrecv.at[d], (s, t))
        copy.start()
        line_copies.append(copy)

    for r in range(last):
        for j in range(3):
            for way in (0, 1):

                def relay():
                    hop(way, r, j, False).wait_recv()
                    sums[way, r, j] = add(term[j, :, target(way, r)], line[way, r, j])
                    hop(way, r, j, False).start()

                when(inner[way] & beyond(way, r), relay)

    for j in range(3):
        own = term[j, :, f].astype(F32)
        done[j] = own
        for way in (0, 1):
            r = last - f if way == 0 else f

            def take():
                pltpu.make_async_remote_copy(
                    sums.at[way, 0, j],
                    line.at[way, r, j],
                    zsend.at[way, r, j],
                    zrecv.at[way, r, j],
                    device_id=(s, f - 1 if way == 0 else f + 1),
                    device_id_type=MESH,
                ).wait_recv()
                done[j] += line[way, r, j].astype(F32)

            when(inner[way], take)
        got[0, j] = done[j].astype(BF16)

    copies = []
    for j in range(3):
        for d in range(1, n):
            t = (s + d) % n
            copy = remote(got.at[0, j, t], got.at[1, j, s], asend.at[j, d], arecv.at[j, d], (t, f))
            copy.start()
            copies.append(copy)
        weight_grad[j, s] = done[j, s]
    total = gsum[f]
    for d in range(1, m):
        line_copies[d - 1].wait_recv()
        total = total + gline[d - 1]
    gain_grad[...] = total
    for copy in copies:
        copy.wait_recv()
    for j in range(3):
        for d in range(1, n):
            t = (s + d) % n
            weight_grad[j, t] = got[1, j, t].astype(F32)
    for copy in copies + gain_copies + line_copies:
        copy.wait_send()
    for r in range(last):
        for j in range(3):
            for way in (0, 1):
                when(ends[way] | (inner[way] & beyond(way, r)), lambda: hop(way, r, j, False).wait_send())


def leave(value, term, gains, grad_hidden, n, m, ident):
    rows, width = grad_hidden.shape
    part, cols = term.shape[-2:]
    vmem = pl.BlockSpec(memory_space=pltpu.VMEM)
    dma = pltpu.SemaphoreType.DMA
    block = pltpu.VMEM((2, m - 1, 3, n, part, cols), BF16)
    return pl.pallas_call(
        functools.partial(exit_kernel, n, m),
        in_specs=[vmem] * 4,
        out_specs=[vmem] * 3,
        out_shape=[
            jax.ShapeDtypeStruct((rows, width), F32),
            jax.ShapeDtypeStruct((3, n, part, cols), F32),
            jax.ShapeDtypeStruct(gains.shape[2:], F32),
        ],
        scratch_shapes=scatter_scratch(1, rows, width)
        + [
            block,
            block,
            pltpu.VMEM((3, n, part, cols), F32),
            pltpu.VMEM((2, 3, n, part, cols), BF16),
            pltpu.VMEM((n - 1,) + gains.shape[1:], F32),
            pltpu.VMEM(gains.shape[1:], F32),
            pltpu.VMEM((m - 1,) + gains.shape[2:], F32),
        ]
        + [dma((2, m, 3))] * 2
        + [dma((3, n))] * 2
        + [dma((n,))] * 2
        + [dma((m,))] * 2,
        compiler_params=pltpu.CompilerParams(
            collective_id=ident, has_side_effects=True, vmem_limit_bytes=48 * 2**20
        ),
        cost_estimate=pl.CostEstimate(flops=0, bytes_accessed=200 * 2**20, transcendentals=0),
        name=f"leave_{ident}",
    )(value.astype(BF16).reshape(1, n, rows, width), term.astype(BF16), gains, grad_hidden)


def attention_forward_kernel(block, q_ref, k_ref, v_ref, out_ref, low_ref, log_ref):
    length = q_ref.shape[0]
    scale = HD ** (-0.5)
    for i in range(length // block):
        rows = pl.ds(i * block, block)
        width = (i + 1) * block
        s = dot(q_ref[rows, :], k_ref[pl.ds(0, width), :], NT) * scale
        column = lax.broadcasted_iota(jnp.int32, (block, width), 1)
        row = lax.broadcasted_iota(jnp.int32, (block, width), 0) + i * block
        s = jnp.where(column <= row, s, -jnp.inf)
        top = jnp.max(s, axis=-1, keepdims=True)
        p = jnp.exp(s - top)
        total = jnp.sum(p, axis=-1, keepdims=True)
        weights = (p * (1.0 / total)).astype(BF16)
        out = dot(weights, v_ref[pl.ds(0, width), :], NN)
        out_ref[rows, :] = out
        low_ref[rows, :] = out.astype(BF16)
        log_ref[0, rows, :] = top + jnp.log(total)


def attention_forward(q, k, v):
    length, width = q.shape
    heads = width // HD
    block = min(256, length)
    column = pl.BlockSpec((length, HD), lambda h: (0, h))
    return pl.pallas_call(
        functools.partial(attention_forward_kernel, block),
        grid=(heads,),
        in_specs=[column] * 3,
        out_specs=[column, column, pl.BlockSpec((1, length, 1), lambda h: (h, 0, 0))],
        out_shape=[
            jax.ShapeDtypeStruct((length, width), F32),
            jax.ShapeDtypeStruct((length, width), BF16),
            jax.ShapeDtypeStruct((heads, length, 1), F32),
        ],
        cost_estimate=pl.CostEstimate(
            flops=2 * heads * length * length * HD, bytes_accessed=10 * length * width, transcendentals=0
        ),
    )(q, k, v)


def attention_backward_kernel(block, q_ref, k_ref, v_ref, out_ref, log_ref, g_ref, dq_ref, dk_ref, dv_ref, dk, dv):
    length = q_ref.shape[0]
    scale = HD ** (-0.5)
    dk[...] = jnp.zeros_like(dk)
    dv[...] = jnp.zeros_like(dv)
    for i in range(length // block):
        rows = pl.ds(i * block, block)
        width = (i + 1) * block
        wide = pl.ds(0, width)
        q = q_ref[rows, :]
        g = g_ref[rows, :]
        s = dot(q, k_ref[wide, :], NT) * scale
        column = lax.broadcasted_iota(jnp.int32, (block, width), 1)
        row = lax.broadcasted_iota(jnp.int32, (block, width), 0) + i * block
        s = jnp.where(column <= row, s, -jnp.inf)
        weights = jnp.exp(s - log_ref[0, rows, :])
        correction = jnp.sum(g.astype(F32) * out_ref[rows, :], axis=-1, keepdims=True)
        gw = dot(g, v_ref[wide, :], NT)
        gs = (weights * (gw - correction)).astype(BF16)
        dq_ref[rows, :] = (dot(gs, k_ref[wide, :], NN) * scale).astype(BF16)
        dk[wide, :] += dot(gs, q, TN)
        dv[wide, :] += dot(weights.astype(BF16), g, TN)
    dk_ref[...] = (dk[...] * scale).astype(BF16)
    dv_ref[...] = dv[...].astype(BF16)


def attention_backward(q, k, v, out, log_total, g):
    length, width = q.shape
    heads = width // HD
    block = min(256, length)
    column = pl.BlockSpec((length, HD), lambda h: (0, h))
    return pl.pallas_call(
        functools.partial(attention_backward_kernel, block),
        grid=(heads,),
        in_specs=[column] * 4 + [pl.BlockSpec((1, length, 1), lambda h: (h, 0, 0)), column],
        out_specs=[column] * 3,
        out_shape=[jax.ShapeDtypeStruct((length, width), BF16)] * 3,
        scratch_shapes=[pltpu.VMEM((length, HD), F32)] * 2,
        cost_estimate=pl.CostEstimate(
            flops=5 * heads * length * length * HD, bytes_accessed=16 * length * width, transcendentals=0
        ),
    )(q, k, v, out, log_total, g)


def on_device(n, m, pair, *args):
    (
        tokens,
        query_weight,
        key_weight,
        value_weight,
        out_weight,
        query_gain,
        key_gain,
        attention_gain,
        gate_weight,
        up_weight,
        down_weight,
        feedforward_gain,
        cotangent,
    ) = args
    rows, width = tokens.shape[1], tokens.shape[2]
    length = rows * n
    part = query_weight.shape[0]
    cols = width // n
    depth, units = gate_weight.shape
    share = units // pair
    x = tokens.reshape(rows, width)
    groups = [[g * pair + u for u in range(pair)] for g in range(m // pair)]

    native = n == 8

    def gather_plane(v, ident):
        if native:
            return plane_gather(v, n, 1, ident)
        return lax.all_gather(v, "seq", axis=0, tiled=True)

    def scatter_plane(v, ident):
        if native:
            return plane_scatter(v, n, 1, ident)
        return lax.psum_scatter(v.astype(BF16), "seq", scatter_dimension=0, tiled=True).astype(F32)

    def gather_pair(v, ident):
        if native:
            return plane_gather(v, n, pair, ident)
        if pair > 1:
            v = lax.all_gather(v, "fsdp", axis=0, axis_index_groups=groups)
        v = lax.all_gather(v.reshape(pair, rows, width), "seq", axis=1, tiled=True)
        return v.reshape(pair * length, width)

    def scatter_pair(v, ident):
        if native:
            return plane_scatter(v, n, pair, ident)
        v = lax.psum_scatter(v.astype(BF16).reshape(pair, length, width), "seq", scatter_dimension=1, tiled=True)
        if pair > 1:
            v = lax.psum_scatter(v, "fsdp", scatter_dimension=0, axis_index_groups=groups)
        return v.reshape(rows, width).astype(F32)

    def total_plane(v, ident):
        return plane_sum(v, n, ident) if native else lax.psum(v, "seq")

    def spread(halves):
        return lax.all_to_all(jnp.tile(halves, (m // pair, 1, 1)), "fsdp", 0, 0, tiled=False)

    def settle(blocks):
        back = lax.all_to_all(blocks.astype(BF16), "fsdp", 0, 0, tiled=False)
        return jnp.sum(back.reshape((m // pair, pair) + back.shape[1:]).astype(F32), axis=0)

    gains = jnp.stack([query_gain, key_gain, attention_gain, feedforward_gain]).astype(F32)
    seq = lax.axis_index("seq")
    if native:
        xs, qkv, full = entry(
            x, query_weight, key_weight, value_weight, jnp.pad(gains, ((0, 4), (0, 128 - part))), n, m, 1
        )
        full_gain = full[:, :, :4, :part].transpose(2, 1, 0, 3).reshape(4, width)
    else:
        stacked = jnp.stack([query_weight, key_weight, value_weight]).reshape(3, part, n, cols)
        mine = lax.all_to_all(stacked.transpose(2, 0, 1, 3), "seq", 0, 0)
        qkv = lax.all_gather(mine, "fsdp", axis=1).transpose(2, 0, 1, 3, 4).reshape(3, width, cols)
        full_gain = lax.all_gather(gains, ("seq", "fsdp"), axis=1).reshape(4, width)
        xs = gather_plane(x, 1)
    out_rows = lax.all_gather(out_weight, "fsdp", axis=0, tiled=True)
    own_gain = lax.dynamic_slice_in_dim(full_gain[:2], seq * cols, cols, 1)
    full_gain = full_gain[2:]
    q_gain, k_gain = own_gain[0], own_gain[1]
    branch_gain, feed_gain = full_gain[0], full_gain[1]

    q_raw, k_raw, v = dot(xs, qkv[0], NN), dot(xs, qkv[1], NN), dot(xs, qkv[2], NN).astype(BF16)
    squares = jnp.stack([jnp.sum(q_raw * q_raw, axis=1), jnp.sum(k_raw * k_raw, axis=1)])
    squares = total_plane(squares, 9) / width
    inverse = lax.rsqrt(squares + EPSILON)
    q_inv, k_inv = inverse[0][:, None], inverse[1][:, None]
    cosine, sine = angles_of(length)
    q = rotate(q_raw * q_inv * q_gain, cosine, sine, 1.0).astype(BF16)
    k = rotate(k_raw * k_inv * k_gain, cosine, sine, 1.0).astype(BF16)
    attended, attended_low, log_total = attention_forward(q, k, v)
    branch = scatter_plane(dot(attended_low, out_rows, NN), 3)
    branch_inv = lax.rsqrt(jnp.mean(branch * branch, axis=1, keepdims=True) + EPSILON)
    hidden = x.astype(F32) + branch * branch_inv * branch_gain
    hs = gather_pair(hidden.astype(BF16), 5)

    gate_cols = spread(gate_weight.reshape(depth, pair, share).transpose(1, 0, 2)).reshape(width, share)
    up_cols = spread(up_weight.reshape(depth, pair, share).transpose(1, 0, 2)).reshape(width, share)
    down_rows = spread(down_weight.reshape(pair, share, depth)).transpose(1, 0, 2).reshape(share, width)

    gate = dot(hs, gate_cols, NN)
    up = dot(hs, up_cols, NN)
    sig = jax.nn.sigmoid(gate)
    inner = (gate * sig * up).astype(BF16)
    feed = scatter_pair(dot(inner, down_rows, NN), 7)
    feed_inv = lax.rsqrt(jnp.mean(feed * feed, axis=1, keepdims=True) + EPSILON)
    normal = feed * feed_inv
    layer_out = (hidden + normal * feed_gain).astype(BF16)

    grad_out = cotangent.reshape(rows, width).astype(F32)
    u = grad_out * feed_gain
    grad_feed = feed_inv * (u - normal * jnp.mean(u * normal, axis=1, keepdims=True))
    feed_gain_term = jnp.sum(grad_out * normal, axis=0)
    gs = gather_pair(grad_feed.astype(BF16), 6)
    grad_inner = dot(gs, down_rows, NT)
    grad_gate = (grad_inner * up * sig * (1.0 + gate * (1.0 - sig))).astype(BF16)
    grad_up = (grad_inner * gate * sig).astype(BF16)
    grad_hidden = grad_out + scatter_pair(dot(grad_gate, gate_cols, NT) + dot(grad_up, up_cols, NT), 8)
    down_grad = settle(dot(inner, gs, TN).reshape(share, m, depth).transpose(1, 0, 2)).reshape(units, depth)
    gate_grad = settle(dot(hs, grad_gate, TN).reshape(m, depth, share)).transpose(1, 0, 2).reshape(depth, units)
    up_grad = settle(dot(hs, grad_up, TN).reshape(m, depth, share)).transpose(1, 0, 2).reshape(depth, units)

    normal = branch * branch_inv
    u = grad_hidden * branch_gain
    grad_branch = branch_inv * (u - normal * jnp.mean(u * normal, axis=1, keepdims=True))
    branch_gain_term = jnp.sum(grad_hidden * normal, axis=0)
    bs = gather_plane(grad_branch.astype(BF16), 2)
    out_grad = lax.psum_scatter(
        dot(attended_low, bs, TN).astype(BF16), "fsdp", scatter_dimension=0, tiled=True
    ).astype(F32)
    grad_attended = dot(bs, out_rows, NT).astype(BF16)
    dq, dk, dv = attention_backward(q, k, v, attended, log_total, grad_attended)
    dq = rotate(dq.astype(F32), cosine, sine, -1.0)
    dk = rotate(dk.astype(F32), cosine, sine, -1.0)
    q_normal, k_normal = q_raw * q_inv, k_raw * k_inv
    q_gain_term = jnp.sum(dq * q_normal, axis=0)
    k_gain_term = jnp.sum(dk * k_normal, axis=0)
    dq, dk = dq * q_gain, dk * k_gain
    means = total_plane(jnp.stack([jnp.sum(dq * q_normal, axis=1), jnp.sum(dk * k_normal, axis=1)]), 10) / width
    dq = (q_inv * (dq - q_normal * means[0][:, None])).astype(BF16)
    dk = (k_inv * (dk - k_normal * means[1][:, None])).astype(BF16)
    value = dot(dq, qkv[0], NT) + dot(dk, qkv[1], NT) + dot(dv, qkv[2], NT)
    term = jnp.stack([dot(xs, d, TN).astype(BF16) for d in (dq, dk, dv)]).reshape(3, n, m, part, cols)
    gain_own = jnp.stack([q_gain_term, k_gain_term])
    gain_own = lax.dynamic_update_slice(jnp.zeros((2, width), F32), gain_own, (0, seq * cols))
    gain_terms = jnp.concatenate([gain_own, jnp.stack([branch_gain_term, feed_gain_term])]).reshape(4, n, m, part)
    if native:
        gain_terms = jnp.pad(gain_terms.transpose(1, 2, 0, 3), ((0, 0), (0, 0), (0, 4), (0, 128 - part)))
        tokens_grad, term, gain_grads = leave(value, term, gain_terms, grad_hidden, n, m, 4)
        term = term.transpose(0, 2, 1, 3)
        gain_grads = gain_grads[:4, :part]
    else:
        tokens_grad = grad_hidden + scatter_plane(value, 4)
        term = lax.psum_scatter(term, "fsdp", scatter_dimension=2)
        term = lax.all_to_all(term, "seq", 1, 1).astype(F32).transpose(0, 2, 1, 3)
        gain_grads = lax.psum_scatter(
            gain_terms.reshape(4, width), ("seq", "fsdp"), scatter_dimension=1, tiled=True
        )
    term = term.reshape(3, part, width)
    return (
        layer_out.reshape(tokens.shape),
        tokens_grad.reshape(tokens.shape),
        term[0],
        term[1],
        term[2],
        out_grad,
        gain_grads[0],
        gain_grads[1],
        gain_grads[2],
        gate_grad,
        up_grad,
        down_grad,
        gain_grads[3],
    )


def solution(mesh):
    n, m = mesh.shape["seq"], mesh.shape["fsdp"]
    tall, flat, act = P(("seq", "fsdp"), None), P(("seq", "fsdp")), P("fsdp", "seq", None)
    wide, deep = P("fsdp", "seq"), P("seq", "fsdp")
    return jax.shard_map(
        functools.partial(on_device, n, m, 2),
        mesh=mesh,
        in_specs=(act, tall, tall, tall, tall, flat, flat, flat, wide, wide, deep, flat, act),
        out_specs=(act, act, tall, tall, tall, tall, flat, flat, flat, wide, wide, deep, flat),
        check_vma=False,
    )
```

```python
import functools
import math

import jax
import jax.numpy as jnp
from jax import lax
from jax.experimental import pallas as pl
from jax.experimental.pallas import tpu as pltpu
from jax.sharding import PartitionSpec as P

EPSILON = 1e-06
THETA = 500000.0
HD = 128
F32 = jnp.float32
BF16 = jnp.bfloat16


def dot(a, b, dims):
    return lax.dot_general(a, b, (dims, ((), ())), preferred_element_type=F32)


NN = ((1,), (0,))
NT = ((1,), (1,))
TN = ((0,), (0,))


def angles_of(length):
    half = HD // 2
    frequency = jnp.exp(jnp.arange(half, dtype=F32) * (-2.0 * math.log(THETA) / HD))
    angle = jnp.arange(length, dtype=F32)[:, None] * frequency[None, :]
    return jnp.cos(angle), jnp.sin(angle)


def rotate(value, cosine, sine, sign):
    length, width = value.shape
    value = value.reshape(length, width // HD, 2, HD // 2)
    first, second = value[:, :, 0], value[:, :, 1]
    c, s = cosine[:, None, :], sign * sine[:, None, :]
    return jnp.stack([first * c - second * s, second * c + first * s], axis=2).reshape(length, width)


MESH = pl.DeviceIdType.MESH


def flip(index, bit):
    return index + bit - 2 * bit * ((index // bit) % 2)


class Place:
    def __init__(self, pair):
        self.s, self.f = lax.axis_index("seq"), lax.axis_index("fsdp")
        self.pair = pair
        s, f = self.s, self.f
        self.sx, self.sy = flip(s, 2), flip(s, 4)
        self.sd, self.sc = flip(self.sx, 4), flip(s, 1)
        self.q = f // 2 if pair > 1 else 0
        self.x, self.y, self.core = (self.sx, f), (self.sy, f), (self.sc, f)
        self.z = (s, opposite(f)) if pair > 1 else None
        self.peers = [self.x, self.y, self.core] + ([self.z] if pair > 1 else [])

    def barrier(self):
        sem = pltpu.get_barrier_semaphore()
        for peer in self.peers:
            pl.semaphore_signal(sem, inc=1, device_id=peer, device_id_type=MESH)
        pl.semaphore_wait(sem, len(self.peers))


class Wires:
    def __init__(self, send, recv):
        self.send, self.recv, self.count, self.open = send, recv, 0, {}

    def new(self, key):
        self.open[key] = self.count
        self.count += 1

    def go(self, key, src, dst, device):
        i = self.open[key]
        copy = pltpu.make_async_remote_copy(
            src, dst, self.send.at[i], self.recv.at[i], device_id=device, device_id_type=MESH
        )
        copy.start()
        return copy


def gather_steps(place, wires, own, out, ready):
    pair, rows = place.pair, own.shape[0]
    half = rows // 2
    top, low = pl.ds(0, half), pl.ds(half, half)
    p = place
    qs = [p.q] + ([1 - p.q] if pair > 1 else [])
    kinds = ["xa", "xb", "ya", "yb", "xd", "yd", "c0", "cxa", "cxb", "cya", "cyb", "cda", "cdb"]
    for t in range(pair):
        for kind in kinds:
            wires.new((t, kind))
    if pair > 1:
        wires.new("z")
    live = {}

    def go(key, src, dst, device):
        live[key] = wires.go(key, src, dst, device)

    def begin(t, src):
        q = qs[t]
        go((t, "xa"), src.at[top], out.at[q, p.s, top], p.x)
        go((t, "yb"), src.at[low], out.at[q, p.s, low], p.y)
        go((t, "xb"), src.at[low], out.at[q, p.s, low], p.x)
        go((t, "ya"), src.at[top], out.at[q, p.s, top], p.y)
        go((t, "c0"), src, out.at[q, p.s], p.core)

    def arrived(key):
        live[key].wait_recv()

    if pair > 1:
        go("z", own, out.at[qs[0], p.s], p.z)
    begin(0, own)
    ready(qs[0], p.s, None)

    def first(t):
        q = qs[t]
        arrived((t, "xa"))
        go((t, "xd"), out.at[q, p.sx, top], out.at[q, p.sx, top], p.y)
        go((t, "cxa"), out.at[q, p.sx, top], out.at[q, p.sx, top], p.core)
        arrived((t, "yb"))
        go((t, "yd"), out.at[q, p.sy, low], out.at[q, p.sy, low], p.x)
        go((t, "cyb"), out.at[q, p.sy, low], out.at[q, p.sy, low], p.core)
        arrived((t, "c0"))
        ready(q, p.sc, None)

    def second(t):
        q = qs[t]
        arrived((t, "xb"))
        go((t, "cxb"), out.at[q, p.sx, low], out.at[q, p.sx, low], p.core)
        ready(q, p.sx, None)
        arrived((t, "ya"))
        go((t, "cya"), out.at[q, p.sy, top], out.at[q, p.sy, top], p.core)
        ready(q, p.sy, None)
        arrived((t, "xd"))
        go((t, "cda"), out.at[q, p.sd, top], out.at[q, p.sd, top], p.core)
        arrived((t, "yd"))
        go((t, "cdb"), out.at[q, p.sd, low], out.at[q, p.sd, low], p.core)

    def third(t):
        q = qs[t]
        arrived((t, "cxa"))
        arrived((t, "cxb"))
        ready(q, flip(p.sx, 1), None)
        arrived((t, "cya"))
        arrived((t, "cyb"))
        ready(q, flip(p.sy, 1), None)
        ready(q, p.sd, None)
        arrived((t, "cda"))
        arrived((t, "cdb"))
        ready(q, flip(p.sd, 1), None)

    first(0)
    if pair > 1:
        arrived("z")
        begin(1, out.at[qs[1], p.s])
        ready(qs[1], p.s, None)
    second(0)
    if pair > 1:
        first(1)
    third(0)
    if pair > 1:
        second(1)
        third(1)
    for copy in live.values():
        copy.wait_send()


def gather_wires(pair):
    return 13 * pair + (1 if pair > 1 else 0)


def gather_kernel(pair, own, out, send, recv, local):
    place = Place(pair)
    keep = pltpu.make_async_copy(own, out.at[place.q, place.s], local)
    keep.start()
    place.barrier()
    gather_steps(place, Wires(send, recv), own, out, lambda q, slot, half: None)
    keep.wait()


def plane_gather(v, n, pair, ident):
    rows, width = v.shape
    return pl.pallas_call(
        functools.partial(gather_kernel, pair),
        in_specs=[pl.BlockSpec(memory_space=pltpu.VMEM)],
        out_specs=pl.BlockSpec(memory_space=pl.ANY),
        out_shape=jax.ShapeDtypeStruct((pair, n, rows, width), v.dtype),
        scratch_shapes=[pltpu.SemaphoreType.DMA((gather_wires(pair),))] * 2 + [pltpu.SemaphoreType.DMA],
        compiler_params=pltpu.CompilerParams(collective_id=ident, has_side_effects=True),
        cost_estimate=pl.CostEstimate(flops=0, bytes_accessed=pair * n * rows * width * 20, transcendentals=0),
        name=f"gather_{ident}",
    )(v).reshape(pair * n * rows, width)


def add(a, b):
    return (a.astype(F32) + b.astype(F32)).astype(BF16)


def scatter_steps(place, wires, part, rc, rd, rx, ry, qbuf, zbuf, make, finish):
    p, pair = place, place.pair
    rows = rx.shape[1]
    half = rows // 2
    top, low = pl.ds(0, half), pl.ds(half, half)
    slots = {"d": p.sd, "x": p.sx, "y": p.sy, "o": p.s}
    order = ["d", "x", "y", "o"]
    names = ["c" + k for k in order] + ["da", "db", "xa", "xb", "ya", "yb"]
    for t in range(pair):
        for name in names:
            wires.new((t, name))
    if pair > 1:
        wires.new("z")
    live = {}

    def go(key, src, dst, device):
        live[key] = wires.go(key, src, dst, device)

    def arrived(key):
        live[key].wait_recv()

    for t in range(pair):
        for i, k in enumerate(order):
            make(t, k, 1)
            go((t, "c" + k), part(t, flip(slots[k], 1)), rc.at[t, i], p.core)

    def start(t):
        make(t, "d", 0)
        arrived((t, "cd"))
        qbuf[t, 0] = add(part(t, p.sd)[...], rc[t, 0])
        go((t, "da"), qbuf.at[t, 0, top], rd.at[t, top], p.x)
        go((t, "db"), qbuf.at[t, 0, low], rd.at[t, low], p.y)
        make(t, "x", 0)
        arrived((t, "cx"))
        qbuf[t, 1, top] = add(part(t, p.sx)[top], rc[t, 1, top])
        go((t, "xa"), qbuf.at[t, 1, top], rx.at[t, top], p.x)
        make(t, "y", 0)
        arrived((t, "cy"))
        qbuf[t, 2, low] = add(part(t, p.sy)[low], rc[t, 2, low])
        go((t, "yb"), qbuf.at[t, 2, low], ry.at[t, low], p.y)

    def relay(t):
        held = part(t, p.sx)[low].astype(F32) + rc[t, 1, low].astype(F32)
        arrived((t, "db"))
        qbuf[t, 1, low] = (held + rd[t, low].astype(F32)).astype(BF16)
        go((t, "xb"), qbuf.at[t, 1, low], rx.at[t, low], p.x)
        held = part(t, p.sy)[top].astype(F32) + rc[t, 2, top].astype(F32)
        arrived((t, "da"))
        qbuf[t, 2, top] = (held + rd[t, top].astype(F32)).astype(BF16)
        go((t, "ya"), qbuf.at[t, 2, top], ry.at[t, top], p.y)

    def total(t):
        make(t, "o", 0)
        arrived((t, "co"))
        value = part(t, p.s)[...].astype(F32) + rc[t, 3].astype(F32)
        for key in ("xa", "yb", "xb", "ya"):
            arrived((t, key))
        return value + rx[t].astype(F32) + ry[t].astype(F32)

    if pair > 1:
        start(0)
        start(1)
        relay(0)
        relay(1)
        zbuf[0] = total(0).astype(BF16)
        go("z", zbuf.at[0], zbuf.at[1], p.z)
        value = total(1)
        arrived("z")
        value = value + zbuf[1].astype(F32)
    else:
        start(0)
        relay(0)
        value = total(0)
    finish(value)
    for copy in live.values():
        copy.wait_send()


def scatter_wires(pair):
    return 10 * pair + (1 if pair > 1 else 0)


def scatter_scratch(pair, rows, width):
    block = lambda *lead: pltpu.VMEM(lead + (rows, width), BF16)
    return [
        block(pair, 4),
        block(pair),
        block(pair),
        block(pair),
        block(pair, 3),
        block(2) if pair > 1 else pltpu.VMEM((2, 16, 128), BF16),
        pltpu.SemaphoreType.DMA((scatter_wires(pair),)),
        pltpu.SemaphoreType.DMA((scatter_wires(pair),)),
    ]


def scatter_kernel(pair, value, out, rc, rd, rx, ry, qbuf, zbuf, send, recv):
    place = Place(pair)
    place.barrier()
    planes = [1 - place.q, place.q] if pair > 1 else [0]

    def part(t, slot):
        return value.at[planes[t], slot]

    def finish(total):
        out[...] = total

    scatter_steps(
        place, Wires(send, recv), part, rc, rd, rx, ry, qbuf, zbuf, lambda *_: None, finish
    )


def plane_scatter(v, n, pair, ident):
    width = v.shape[1]
    rows = v.shape[0] // (pair * n)
    return pl.pallas_call(
        functools.partial(scatter_kernel, pair),
        in_specs=[pl.BlockSpec(memory_space=pltpu.VMEM)],
        out_specs=pl.BlockSpec(memory_space=pltpu.VMEM),
        out_shape=jax.ShapeDtypeStruct((rows, width), F32),
        scratch_shapes=scatter_scratch(pair, rows, width),
        compiler_params=pltpu.CompilerParams(
            collective_id=ident, has_side_effects=True, vmem_limit_bytes=40 * 2**20
        ),
        cost_estimate=pl.CostEstimate(flops=0, bytes_accessed=pair * n * rows * width * 20, transcendentals=0),
        name=f"scatter_{ident}",
    )(v.astype(BF16).reshape(pair, n, rows, width))


def sum_kernel(n, own, out, held, send, recv):
    s, f = lax.axis_index("seq"), lax.axis_index("fsdp")
    sem = pltpu.get_barrier_semaphore()
    for d in range(1, n):
        pl.semaphore_signal(sem, inc=1, device_id=((s + d) % n, f), device_id_type=MESH)
    pl.semaphore_wait(sem, n - 1)
    copies = []
    for d in range(1, n):
        copy = pltpu.make_async_remote_copy(
            own,
            held.at[d - 1],
            send.at[d - 1],
            recv.at[d - 1],
            device_id=((s + d) % n, f),
            device_id_type=MESH,
        )
        copy.start()
        copies.append(copy)
    total = own[...]
    for d in range(1, n):
        copies[d - 1].wait_recv()
        total = total + held[d - 1]
    out[...] = total
    for copy in copies:
        copy.wait_send()


def plane_sum(v, n, ident):
    return pl.pallas_call(
        functools.partial(sum_kernel, n),
        in_specs=[pl.BlockSpec(memory_space=pltpu.VMEM)],
        out_specs=pl.BlockSpec(memory_space=pltpu.VMEM),
        out_shape=jax.ShapeDtypeStruct(v.shape, v.dtype),
        scratch_shapes=[pltpu.VMEM((n - 1,) + v.shape, v.dtype)]
        + [pltpu.SemaphoreType.DMA((n - 1,))] * 2,
        compiler_params=pltpu.CompilerParams(collective_id=ident, has_side_effects=True),
        name=f"sum_{ident}",
    )(v)


def when(condition, body):
    pl.when(condition)(body)


def line_barrier(n, m):
    s, f = lax.axis_index("seq"), lax.axis_index("fsdp")
    sem = pltpu.get_barrier_semaphore()
    for d in range(1, n):
        pl.semaphore_signal(sem, inc=1, device_id=((s + d) % n, f), device_id_type=MESH)
    for d in range(1, m):
        pl.semaphore_signal(sem, inc=1, device_id=(s, (f + d) % m), device_id_type=MESH)
    pl.semaphore_wait(sem, n + m - 2)


def entry_kernel(
    n, m, x, wq, wk, wv, wo, gains, xs, qkv, out, full, send, recv, asend, arecv, zsend, zrecv, gsend, grecv, local
):
    place = Place(1)
    s, f = place.s, place.f
    cols = qkv.shape[-1]
    weights = (wq, wk, wv)
    kept = [pltpu.make_async_copy(x, xs.at[0, s], local.at[0]), pltpu.make_async_copy(gains, full.at[f, s], local.at[1])]
    for j, w in enumerate(weights):
        own = w.at[:, pl.ds(pl.multiple_of(s * cols, cols), cols)]
        kept.append(pltpu.make_async_copy(own, qkv.at[j, f, s], local.at[2 + j]))
    kept.append(pltpu.make_async_copy(wo, out.at[f], local.at[5]))
    for copy in kept:
        copy.start()
    line_barrier(n, m)
    sent = []

    def remote(src, dst, a, b, device):
        copy = pltpu.make_async_remote_copy(src, dst, a, b, device_id=device, device_id_type=MESH)
        copy.start()
        sent.append(copy)
        return copy

    first = []
    for d in range(1, n):
        first.append(remote(gains, full.at[f, s], gsend.at[d], grecv.at[d], ((s + d) % n, f)))
    second = []
    for j, w in enumerate(weights):
        row = []
        for d in range(1, n):
            t = (s + d) % n
            src = w.at[:, pl.ds(pl.multiple_of(t * cols, cols), cols)]
            row.append(remote(src, qkv.at[j, f, s], asend.at[j, d], arecv.at[j, d], (t, f)))
        second.append(row)

    def piece(j, o):
        return full.at[o] if j == 3 else out.at[o] if j == 4 else qkv.at[j, o]

    def hop(way, h, j):
        o = f - h if way == 0 else f + h
        there = f + 1 if way == 0 else f - 1
        place_ = piece(j, o)
        return pltpu.make_async_remote_copy(
            place_, place_, zsend.at[way, h, j], zrecv.at[way, h, j], device_id=(s, there), device_id_type=MESH
        )

    def sends(way, h):
        return ((f - h >= 0) & (f < m - 1)) if way == 0 else ((f + h <= m - 1) & (f > 0))

    def receives(way, h):
        return (f - h - 1 >= 0) if way == 0 else (f + h + 1 <= m - 1)

    def start(h, j):
        for way in (0, 1):
            when(sends(way, h), lambda: hop(way, h, j).start())

    def landed(h, j):
        for way in (0, 1):
            o = f - h - 1 if way == 0 else f + h + 1

            def wait():
                there = f - 1 if way == 0 else f + 1
                place_ = piece(j, o)
                pltpu.make_async_remote_copy(
                    place_, place_, zsend.at[way, h, j], zrecv.at[way, h, j], device_id=(s, there), device_id_type=MESH
                ).wait_recv()

            when(receives(way, h), wait)

    for copy in kept:
        copy.wait()
    for copy in first:
        copy.wait_recv()
    start(0, 3)
    for j in range(3):
        for copy in second[j]:
            copy.wait_recv()
        start(0, j)
    start(0, 4)
    gather_steps(place, Wires(send, recv), x, xs, lambda *_: None)
    for h in range(m - 1):
        for j in (3, 0, 1, 2, 4):
            landed(h, j)
            if h + 1 < m - 1:
                start(h + 1, j)
    for copy in sent:
        copy.wait_send()
    for h in range(m - 1):
        for j in range(5):
            for way in (0, 1):
                when(sends(way, h), lambda: hop(way, h, j).wait_send())


def entry(x, wq, wk, wv, wo, gains, n, m, ident):
    rows, width = x.shape
    part = wq.shape[0]
    cols = width // n
    vmem, any_ = pl.BlockSpec(memory_space=pltpu.VMEM), pl.BlockSpec(memory_space=pl.ANY)
    dma = pltpu.SemaphoreType.DMA
    return pl.pallas_call(
        functools.partial(entry_kernel, n, m),
        in_specs=[vmem] * 6,
        out_specs=[any_] * 4,
        out_shape=[
            jax.ShapeDtypeStruct((1, n, rows, width), x.dtype),
            jax.ShapeDtypeStruct((3, m, n, part, cols), wq.dtype),
            jax.ShapeDtypeStruct((m,) + wo.shape, wo.dtype),
            jax.ShapeDtypeStruct((m, n) + gains.shape, gains.dtype),
        ],
        scratch_shapes=[dma((gather_wires(1),))] * 2
        + [dma((3, n))] * 2
        + [dma((2, m, 5))] * 2
        + [dma((n,))] * 2
        + [dma((6,))],
        compiler_params=pltpu.CompilerParams(collective_id=ident, has_side_effects=True),
        cost_estimate=pl.CostEstimate(flops=0, bytes_accessed=200 * 2**20, transcendentals=0),
        name=f"entry_{ident}",
    )(x, wq, wk, wv, wo, gains)


def exit_kernel(
    n,
    m,
    value,
    term,
    gains,
    grad_hidden,
    tokens_grad,
    weight_grad,
    gain_grad,
    rc,
    rd,
    rx,
    ry,
    qbuf,
    zbuf,
    send,
    recv,
    line,
    sums,
    done,
    got,
    gplane,
    gsum,
    gline,
    zsend,
    zrecv,
    asend,
    arecv,
    gsend,
    grecv,
    lsend,
    lrecv,
):
    place = Place(1)
    s, f = place.s, place.f
    line_barrier(n, m)
    last = m - 1
    cols = term.shape[-1]

    def remote(src, dst, a, b, device):
        return pltpu.make_async_remote_copy(src, dst, a, b, device_id=device, device_id_type=MESH)

    def target(way, r):
        return last - r if way == 0 else r

    def hop(way, r, j, fresh):
        there = f + 1 if way == 0 else f - 1
        src = term.at[j, :, target(way, r)] if fresh else sums.at[way, r, j]
        return remote(src, line.at[way, r, j], zsend.at[way, r, j], zrecv.at[way, r, j], (s, there))

    ends = (f == 0, f == last)
    inner = (f > 0, f < last)

    def beyond(way, r):
        return target(way, r) > f if way == 0 else target(way, r) < f

    for r in range(last):
        for j in range(3):
            for way in (0, 1):
                when(ends[way], lambda: hop(way, r, j, True).start())

    gain_copies = []
    for d in range(1, n):
        t = (s + d) % n
        copy = remote(gains.at[t], gplane.at[d - 1], gsend.at[d], grecv.at[d], (t, f))
        copy.start()
        gain_copies.append(copy)

    def part(t, slot):
        return value.at[0, slot]

    def finish(total):
        tokens_grad[...] = total + grad_hidden[...]

    scatter_steps(place, Wires(send, recv), part, rc, rd, rx, ry, qbuf, zbuf, lambda *_: None, finish)

    total = gains[s]
    for d in range(1, n):
        gain_copies[d - 1].wait_recv()
        total = total + gplane[d - 1]
    gsum[...] = total
    line_copies = []
    for d in range(1, m):
        t = (f + d) % m
        copy = remote(gsum.at[t], gline.at[d - 1], lsend.at[d], lrecv.at[d], (s, t))
        copy.start()
        line_copies.append(copy)

    for r in range(last):
        for j in range(3):
            for way in (0, 1):

                def relay():
                    hop(way, r, j, False).wait_recv()
                    sums[way, r, j] = add(term[j, :, target(way, r)], line[way, r, j])
                    hop(way, r, j, False).start()

                when(inner[way] & beyond(way, r), relay)

    for j in range(3):
        own = term[j, :, f].astype(F32)
        done[j] = own
        for way in (0, 1):
            r = last - f if way == 0 else f

            def take():
                pltpu.make_async_remote_copy(
                    sums.at[way, 0, j],
                    line.at[way, r, j],
                    zsend.at[way, r, j],
                    zrecv.at[way, r, j],
                    device_id=(s, f - 1 if way == 0 else f + 1),
                    device_id_type=MESH,
                ).wait_recv()
                done[j] += line[way, r, j].astype(F32)

            when(inner[way], take)
        got[0, j] = done[j].astype(BF16)

    copies = []
    for j in range(3):
        for d in range(1, n):
            t = (s + d) % n
            copy = remote(got.at[0, j, t], got.at[1, j, s], asend.at[j, d], arecv.at[j, d], (t, f))
            copy.start()
            copies.append(copy)
        weight_grad[j, s] = done[j, s]
    total = gsum[f]
    for d in range(1, m):
        line_copies[d - 1].wait_recv()
        total = total + gline[d - 1]
    gain_grad[...] = total
    for copy in copies:
        copy.wait_recv()
    for j in range(3):
        for d in range(1, n):
            t = (s + d) % n
            weight_grad[j, t] = got[1, j, t].astype(F32)
    for copy in copies + gain_copies + line_copies:
        copy.wait_send()
    for r in range(last):
        for j in range(3):
            for way in (0, 1):
                when(ends[way] | (inner[way] & beyond(way, r)), lambda: hop(way, r, j, False).wait_send())


def leave(value, term, gains, grad_hidden, n, m, ident):
    rows, width = grad_hidden.shape
    part, cols = term.shape[-2:]
    vmem = pl.BlockSpec(memory_space=pltpu.VMEM)
    dma = pltpu.SemaphoreType.DMA
    block = pltpu.VMEM((2, m - 1, 3, n, part, cols), BF16)
    return pl.pallas_call(
        functools.partial(exit_kernel, n, m),
        in_specs=[vmem] * 4,
        out_specs=[vmem] * 3,
        out_shape=[
            jax.ShapeDtypeStruct((rows, width), F32),
            jax.ShapeDtypeStruct((3, n, part, cols), F32),
            jax.ShapeDtypeStruct(gains.shape[2:], F32),
        ],
        scratch_shapes=scatter_scratch(1, rows, width)
        + [
            block,
            block,
            pltpu.VMEM((3, n, part, cols), F32),
            pltpu.VMEM((2, 3, n, part, cols), BF16),
            pltpu.VMEM((n - 1,) + gains.shape[1:], F32),
            pltpu.VMEM(gains.shape[1:], F32),
            pltpu.VMEM((m - 1,) + gains.shape[2:], F32),
        ]
        + [dma((2, m, 3))] * 2
        + [dma((3, n))] * 2
        + [dma((n,))] * 2
        + [dma((m,))] * 2,
        compiler_params=pltpu.CompilerParams(
            collective_id=ident, has_side_effects=True, vmem_limit_bytes=48 * 2**20
        ),
        cost_estimate=pl.CostEstimate(flops=0, bytes_accessed=200 * 2**20, transcendentals=0),
        name=f"leave_{ident}",
    )(value.astype(BF16).reshape(1, n, rows, width), term.astype(BF16), gains, grad_hidden)


class Moves:
    def __init__(self, sems):
        self.sems, self.count, self.open = sems, 0, []

    def start(self, src, dst):
        copy = pltpu.make_async_copy(src, dst, self.sems.at[self.count])
        self.count += 1
        copy.start()
        self.open.append(copy)
        return copy

    def finish(self):
        for copy in self.open:
            copy.wait()
        self.open = []

    def wait(self, copies):
        for copy in copies:
            copy.wait()
        self.open = [copy for copy in self.open if all(copy is not other for other in copies)]


def gather_pairs(place, wires, own, out, ready, hook=lambda: None):
    p, pair = place, place.pair
    half = own.shape[0] // 2
    top, low = pl.ds(0, half), pl.ds(half, half)
    qs = [p.q] + ([1 - p.q] if pair > 1 else [])
    kinds = ["xa", "xb", "ya", "yb", "xd", "yd", "c0", "cxa", "cxb", "cya", "cyb", "cda", "cdb"]
    for t in range(pair):
        for kind in kinds:
            wires.new((t, kind))
    if pair > 1:
        wires.new("z")
    live = {}

    def go(key, src, dst, device):
        live[key] = wires.go(key, src, dst, device)

    def arrived(*keys):
        for key in keys:
            live[key].wait_recv()

    def begin(t, src):
        q = qs[t]
        go((t, "xa"), src.at[top], out.at[q, p.s, top], p.x)
        go((t, "yb"), src.at[low], out.at[q, p.s, low], p.y)
        go((t, "xb"), src.at[low], out.at[q, p.s, low], p.x)
        go((t, "ya"), src.at[top], out.at[q, p.s, top], p.y)
        go((t, "c0"), src, out.at[q, p.s], p.core)

    def pass_on(t, key, name, slot, rows, device):
        ref = out.at[qs[t], slot, rows]
        go((t, name), ref, ref, device)

    def first(t):
        arrived((t, "xa"))
        pass_on(t, "xa", "xd", p.sx, top, p.y)
        pass_on(t, "xa", "cxa", p.sx, top, p.core)
        arrived((t, "yb"))
        pass_on(t, "yb", "yd", p.sy, low, p.x)
        pass_on(t, "yb", "cyb", p.sy, low, p.core)

    def second(t):
        arrived((t, "xb"))
        pass_on(t, "xb", "cxb", p.sx, low, p.core)
        arrived((t, "ya"))
        pass_on(t, "ya", "cya", p.sy, top, p.core)

    def third(t):
        arrived((t, "xd"))
        pass_on(t, "xd", "cda", p.sd, top, p.core)
        arrived((t, "yd"))
        pass_on(t, "yd", "cdb", p.sd, low, p.core)

    def use(t, slot, *keys):
        arrived(*[(t, key) for key in keys])
        ready(qs[t], slot // 2)

    if pair > 1:
        go("z", own, out.at[qs[0], p.s], p.z)
    begin(0, own)
    use(0, p.s, "c0")
    first(0)
    if pair > 1:
        arrived("z")
        begin(1, out.at[qs[1], p.s])
    second(0)
    if pair > 1:
        use(1, p.s, "c0")
    use(0, p.sx, "cxa", "cxb")
    third(0)
    use(0, p.sy, "cya", "cyb")
    if pair > 1:
        first(1)
    hook()
    use(0, p.sd, "cda", "cdb")
    if pair > 1:
        second(1)
        use(1, p.sx, "cxa", "cxb")
        third(1)
        use(1, p.sy, "cya", "cyb")
        use(1, p.sd, "cda", "cdb")
    return live


def scatter_pairs(place, wires, value, rc, rd, rx, ry, qbuf, zbuf, make, hook=lambda: None):
    p, pair = place, place.pair
    rows = rx.shape[1]
    half = rows // 2
    top, low = pl.ds(0, half), pl.ds(half, half)
    slots = {"d": p.sd, "x": p.sx, "y": p.sy, "o": p.s}
    order = ["d", "x", "y", "o"]
    planes = [1 - p.q, p.q] if pair > 1 else [p.q]
    for t in range(pair):
        for name in ["c" + k for k in order] + ["da", "db", "xa", "xb", "ya", "yb"]:
            wires.new((t, name))
    if pair > 1:
        wires.new("z")
    live = {}

    def go(key, src, dst, device):
        live[key] = wires.go(key, src, dst, device)

    def arrived(*keys):
        for key in keys:
            live[key].wait_recv()

    def part(t, slot):
        return value.at[planes[t], slot]

    def share(t, k):
        make(planes[t], slots[k] // 2)
        go((t, "c" + k), part(t, flip(slots[k], 1)), rc.at[t, order.index(k)], p.core)

    def diag(t):
        arrived((t, "cd"))
        qbuf[t, 0] = add(part(t, p.sd)[...], rc[t, 0])
        go((t, "da"), qbuf.at[t, 0, top], rd.at[t, top], p.x)
        go((t, "db"), qbuf.at[t, 0, low], rd.at[t, low], p.y)

    def ahead(t):
        arrived((t, "cx"))
        qbuf[t, 1, top] = add(part(t, p.sx)[top], rc[t, 1, top])
        go((t, "xa"), qbuf.at[t, 1, top], rx.at[t, top], p.x)
        arrived((t, "cy"))
        qbuf[t, 2, low] = add(part(t, p.sy)[low], rc[t, 2, low])
        go((t, "yb"), qbuf.at[t, 2, low], ry.at[t, low], p.y)

    def relay(t):
        arrived((t, "db"))
        held = part(t, p.sx)[low].astype(F32) + rc[t, 1, low].astype(F32)
        qbuf[t, 1, low] = (held + rd[t, low].astype(F32)).astype(BF16)
        go((t, "xb"), qbuf.at[t, 1, low], rx.at[t, low], p.x)
        arrived((t, "da"))
        held = part(t, p.sy)[top].astype(F32) + rc[t, 2, top].astype(F32)
        qbuf[t, 2, top] = (held + rd[t, top].astype(F32)).astype(BF16)
        go((t, "ya"), qbuf.at[t, 2, top], ry.at[t, top], p.y)

    def total(t):
        arrived((t, "co"), (t, "xa"), (t, "yb"), (t, "xb"), (t, "ya"))
        result = part(t, p.s)[...].astype(F32) + rc[t, 3].astype(F32)
        return result + rx[t].astype(F32) + ry[t].astype(F32)

    share(0, "d")
    share(0, "x")
    diag(0)
    share(0, "y")
    if pair > 1:
        ahead(0)
        share(1, "d")
        share(0, "o")
        diag(1)
        relay(0)
        share(1, "x")
        share(1, "y")
        ahead(1)
        share(1, "o")
        zbuf[0] = total(0).astype(BF16)
        go("z", zbuf.at[0], zbuf.at[1], p.z)
        relay(1)
        result = total(1)
        arrived("z")
        result = result + zbuf[1].astype(F32)
    else:
        ahead(0)
        share(0, "o")
        hook()
        relay(0)
        result = total(0)
    return result, live


def rms_back(value, gain, grad):
    inverse = lax.rsqrt(jnp.mean(value * value, axis=-1, keepdims=True) + EPSILON)
    normal = value * inverse
    u = grad * gain
    return inverse * (u - normal * jnp.mean(u * normal, axis=-1, keepdims=True)), grad * normal


def up_kernel(
    pair, h, wg, wu, down_w, hs, gate, up, inner, inner_t, wd, hs_v, w_v, g_v, u_v, i_v, t_v, send, recv, zsem, sems
):
    place = Place(pair)
    place.peers.append((place.s, flip(place.f, 1)))
    moves = Moves(sems)
    loads = [moves.start(wg, w_v.at[0]), moves.start(wu, w_v.at[1])]
    rows, width = h.shape
    block, share = 2 * rows, wg.shape[1]
    hs_v[place.q, place.s] = h[...]
    place.barrier()
    stream, view = Stream(place, zsem), half_rows(down_w, share)
    stream.start_far(0, view, wd)
    stream.start_near(0, view, wd)
    n = hs.shape[1]
    step = min(256, share)
    waited = []

    def ready(q, chip):
        if not waited:
            moves.wait(loads)
            waited.append(True)
        slots = pl.ds(2 * chip, 2)
        moves.start(hs_v.at[q, slots], hs.at[q, slots])
        at = pl.multiple_of(q * n * rows + chip * block, block)
        here = pl.ds(at, block)

        @pl.loop(0, share // step)
        def _(j):
            cols = pl.ds(pl.multiple_of(j * step, step), step)
            a = hs_v[q, slots].reshape(block, width)
            g = dot(a, w_v[0, :, cols], NN)
            u = dot(a, w_v[1, :, cols], NN)
            g_v[here, cols] = g
            u_v[here, cols] = u
            value = (g * (1.0 / (1.0 + jnp.exp(-g))) * u)
            i_v[here, cols] = value.astype(BF16)
            t_v[cols, here] = value.T.astype(BF16)

        moves.start(g_v.at[here], gate.at[here])
        moves.start(u_v.at[here], up.at[here])
        moves.start(i_v.at[here], inner.at[here])

    live = gather_pairs(
        place, Wires(send, recv), h, hs_v, ready, lambda: stream.relay(0, view, wd)
    )
    moves.start(t_v, inner_t)
    stream.finish(0, view, wd)
    for copy in live.values():
        copy.wait_send()
    moves.finish()


def any_specs(count):
    return [pl.BlockSpec(memory_space=pl.ANY)] * count


def vmem_specs(count):
    return [pl.BlockSpec(memory_space=pltpu.VMEM)] * count


def kernel_params(ident, mib=60):
    return pltpu.CompilerParams(collective_id=ident, has_side_effects=True, vmem_limit_bytes=mib * 2**20)


def shape(dims, kind):
    return jax.ShapeDtypeStruct(dims, kind)


def ffn_up(h, wg, wu, down_w, n, pair, ident):
    rows, width = h.shape
    share, long = wg.shape[1], pair * n * rows
    dma = pltpu.SemaphoreType.DMA
    outs = [
        shape((pair, n, rows, width), BF16),
        shape((long, share), F32),
        shape((long, share), F32),
        shape((long, share), BF16),
        shape((share, long), BF16),
        shape((width // down_w.shape[1], share, down_w.shape[1]), BF16),
    ]
    return pl.pallas_call(
        functools.partial(up_kernel, pair),
        in_specs=vmem_specs(1) + any_specs(3),
        out_specs=any_specs(6),
        out_shape=outs,
        scratch_shapes=[
            pltpu.VMEM((pair, n, rows, width), BF16),
            pltpu.VMEM((2, width, share), BF16),
            pltpu.VMEM((long, share), F32),
            pltpu.VMEM((long, share), F32),
            pltpu.VMEM((long, share), BF16),
            pltpu.VMEM((share, long), BF16),
            dma((gather_wires(pair),)),
            dma((gather_wires(pair),)),
            dma((1, 4, 2)),
            dma((3 + 4 * pair * n // 2,)),
        ],
        compiler_params=kernel_params(ident),
        cost_estimate=pl.CostEstimate(
            flops=4 * long * width * share, bytes_accessed=long * width * 40, transcendentals=0
        ),
        name=f"up_{ident}",
    )(h, wg, wu, down_w)


def down_kernel(
    pair, inner, wd, hidden, gain, cotangent, layer_out, grad_low, gain_term, i_v, w_v, value, rc, rd, rx, ry, qbuf, zbuf, send, recv, sems
):
    place = Place(pair)
    moves = Moves(sems)
    deep = wd.shape[2]
    for j in range(wd.shape[0]):
        moves.start(wd.at[j], w_v.at[:, pl.ds(j * deep, deep)])
    moves.start(inner, i_v)
    rows, width = hidden.shape
    block = 2 * rows
    n = value.shape[1]
    step = min(512, width)
    place.barrier()
    moves.finish()

    def make(q, chip):
        here = pl.ds(pl.multiple_of(q * n * rows + chip * block, block), block)

        @pl.loop(0, width // step)
        def _(j):
            cols = pl.ds(pl.multiple_of(j * step, step), step)
            part = dot(i_v[here, :], w_v[:, cols], NN).astype(BF16)
            value[q, pl.ds(2 * chip, 2), :, cols] = part.reshape(2, rows, step)

    feed, live = scatter_pairs(place, Wires(send, recv), value, rc, rd, rx, ry, qbuf, zbuf, make)
    grad = cotangent[...].astype(F32)
    inverse = lax.rsqrt(jnp.mean(feed * feed, axis=-1, keepdims=True) + EPSILON)
    normal = feed * inverse
    layer_out[...] = (hidden[...] + normal * gain[...]).astype(BF16)
    u = grad * gain[...]
    grad_low[...] = (inverse * (u - normal * jnp.mean(u * normal, axis=-1, keepdims=True))).astype(BF16)
    gain_term[...] = jnp.sum(grad * normal, axis=0, keepdims=True)
    for copy in live.values():
        copy.wait_send()


def ffn_down(inner, wd, hidden, gain, cotangent, n, pair, ident):
    rows, width = hidden.shape
    dma = pltpu.SemaphoreType.DMA
    return pl.pallas_call(
        functools.partial(down_kernel, pair),
        in_specs=any_specs(2) + vmem_specs(3),
        out_specs=vmem_specs(3),
        out_shape=[shape((rows, width), BF16), shape((rows, width), BF16), shape((1, width), F32)],
        scratch_shapes=[
            pltpu.VMEM(inner.shape, BF16),
            pltpu.VMEM((wd.shape[1], width), BF16),
            pltpu.VMEM((pair, n, rows, width), BF16),
        ]
        + scatter_scratch(pair, rows, width)
        + [dma((1 + wd.shape[0],))],
        compiler_params=kernel_params(ident),
        cost_estimate=pl.CostEstimate(
            flops=2 * inner.shape[0] * inner.shape[1] * width, bytes_accessed=pair * n * rows * width * 40, transcendentals=0
        ),
        name=f"down_{ident}",
    )(inner, wd, hidden, gain.reshape(1, width), cotangent)


def grad_kernel(
    pair, g, wd, gate, up, gs, grad_gate, grad_up, gate_t, up_t, gs_v, w_v, g_v, u_v, gg_v, gu_v, gt_v, ut_v, send, recv, sems
):
    place = Place(pair)
    moves = Moves(sems)
    deep = wd.shape[2]
    loads = [moves.start(wd.at[j], w_v.at[:, pl.ds(j * deep, deep)]) for j in range(wd.shape[0])]
    loads += [moves.start(gate, g_v), moves.start(up, u_v)]
    rows, width = g.shape
    block, share = 2 * rows, wd.shape[1]
    gs_v[place.q, place.s] = g[...]
    place.barrier()
    n = gs.shape[1]
    step = min(256, share)
    waited = []

    def ready(q, chip):
        if not waited:
            moves.wait(loads)
            waited.append(True)
        slots = pl.ds(2 * chip, 2)
        moves.start(gs_v.at[q, slots], gs.at[q, slots])
        here = pl.ds(pl.multiple_of(q * n * rows + chip * block, block), block)

        @pl.loop(0, share // step)
        def _(j):
            cols = pl.ds(pl.multiple_of(j * step, step), step)
            a = gs_v[q, slots].reshape(block, width)
            e = dot(a, w_v[cols, :], NT)
            v, u = g_v[here, cols], u_v[here, cols]
            s = 1.0 / (1.0 + jnp.exp(-v))
            dg = e * u * s * (1.0 + v * (1.0 - s))
            du = e * v * s
            gg_v[here, cols] = dg.astype(BF16)
            gu_v[here, cols] = du.astype(BF16)
            gt_v[cols, here] = dg.T.astype(BF16)
            ut_v[cols, here] = du.T.astype(BF16)

        moves.start(gg_v.at[here], grad_gate.at[here])
        moves.start(gu_v.at[here], grad_up.at[here])

    live = gather_pairs(place, Wires(send, recv), g, gs_v, ready)
    moves.start(gt_v, gate_t)
    moves.start(ut_v, up_t)
    for copy in live.values():
        copy.wait_send()
    moves.finish()


def ffn_grad(g, wd, gate, up, n, pair, ident):
    rows, width = g.shape
    share, long = wd.shape[1], pair * n * rows
    dma = pltpu.SemaphoreType.DMA
    flat, tall = pltpu.VMEM((long, share), BF16), pltpu.VMEM((share, long), BF16)
    return pl.pallas_call(
        functools.partial(grad_kernel, pair),
        in_specs=vmem_specs(1) + any_specs(3),
        out_specs=any_specs(5),
        out_shape=[shape((pair, n, rows, width), BF16)]
        + [shape((long, share), BF16)] * 2
        + [shape((share, long), BF16)] * 2,
        scratch_shapes=[
            pltpu.VMEM((pair, n, rows, width), BF16),
            pltpu.VMEM((share, width), BF16),
            pltpu.VMEM((long, share), F32),
            pltpu.VMEM((long, share), F32),
            flat,
            flat,
            tall,
            tall,
            dma((gather_wires(pair),)),
            dma((gather_wires(pair),)),
            dma((4 + wd.shape[0] + 3 * pair * n // 2,)),
        ],
        compiler_params=kernel_params(ident),
        cost_estimate=pl.CostEstimate(
            flops=2 * long * width * share, bytes_accessed=long * width * 40, transcendentals=0
        ),
        name=f"grad_{ident}",
    )(g, wd, gate, up)


def back_kernel(
    pair, gg, gu, wg, wu, branch, gain, cotangent, grad_hidden, grad_low, gain_term, a_v, w_v, value, rc, rd, rx, ry, qbuf, zbuf, send, recv, sems
):
    place = Place(pair)
    moves = Moves(sems)
    moves.start(wg, w_v.at[0])
    moves.start(wu, w_v.at[1])
    moves.start(gg, a_v.at[0])
    moves.start(gu, a_v.at[1])
    rows, width = branch.shape
    block = 2 * rows
    n = value.shape[1]
    step = min(256, width)
    place.barrier()
    moves.finish()

    def make(q, chip):
        here = pl.ds(pl.multiple_of(q * n * rows + chip * block, block), block)

        @pl.loop(0, width // step)
        def _(j):
            cols = pl.ds(pl.multiple_of(j * step, step), step)
            part = dot(a_v[0, here, :], w_v[0, cols, :], NT) + dot(a_v[1, here, :], w_v[1, cols, :], NT)
            value[q, pl.ds(2 * chip, 2), :, cols] = part.astype(BF16).reshape(2, rows, step)

    total, live = scatter_pairs(place, Wires(send, recv), value, rc, rd, rx, ry, qbuf, zbuf, make)
    grad = cotangent[...].astype(F32) + total
    grad_hidden[...] = grad
    back, term = rms_back(branch[...], gain[...], grad)
    grad_low[...] = back.astype(BF16)
    gain_term[...] = jnp.sum(term, axis=0, keepdims=True)
    for copy in live.values():
        copy.wait_send()


def ffn_back(gg, gu, wg, wu, branch, gain, cotangent, n, pair, ident):
    rows, width = branch.shape
    dma = pltpu.SemaphoreType.DMA
    return pl.pallas_call(
        functools.partial(back_kernel, pair),
        in_specs=any_specs(4) + vmem_specs(3),
        out_specs=vmem_specs(3),
        out_shape=[shape((rows, width), F32), shape((rows, width), BF16), shape((1, width), F32)],
        scratch_shapes=[
            pltpu.VMEM((2,) + gg.shape, BF16),
            pltpu.VMEM((2,) + wg.shape, BF16),
            pltpu.VMEM((pair, n, rows, width), BF16),
        ]
        + scatter_scratch(pair, rows, width)
        + [dma((4,))],
        compiler_params=kernel_params(ident),
        cost_estimate=pl.CostEstimate(
            flops=4 * gg.shape[0] * gg.shape[1] * width, bytes_accessed=pair * n * rows * width * 40, transcendentals=0
        ),
        name=f"back_{ident}",
    )(gg, gu, wg, wu, branch, gain.reshape(1, width), cotangent)


def opposite(f):
    return (f + 2) % 4


class Stream:
    def __init__(self, place, sems):
        self.place, self.sems = place, sems
        f = place.f
        self.half, self.far_f, self.near_f = f // 2, opposite(f), flip(f, 1)
        self.far, self.near = (place.s, self.far_f), (place.s, self.near_f)

    def remote(self, k, step, src, dst, device):
        return pltpu.make_async_remote_copy(
            src, dst, self.sems.at[k, step, 0], self.sems.at[k, step, 1], device_id=device, device_id_type=MESH
        )

    def far_copy(self, k, view, full):
        return self.remote(k, 0, view(1 - self.half), full.at[self.place.f], self.far)

    def near_copy(self, k, view, full):
        return self.remote(k, 1, view(self.half), full.at[self.place.f], self.near)

    def own_copy(self, k, view, full):
        return pltpu.make_async_copy(view(self.half), full.at[self.place.f], self.sems.at[k, 3, 0])

    def relay_copy(self, k, full):
        return self.remote(k, 2, full.at[self.far_f], full.at[self.far_f], self.near)

    def start_far(self, k, view, full):
        self.far_copy(k, view, full).start()

    def start_near(self, k, view, full):
        self.near_copy(k, view, full).start()
        self.own_copy(k, view, full).start()

    def relay(self, k, view, full):
        self.far_copy(k, view, full).wait_recv()
        self.relay_copy(k, full).start()

    def finish(self, k, view, full):
        self.near_copy(k, view, full).wait_recv()
        self.relay_copy(k, full).wait_recv()
        self.own_copy(k, view, full).wait()
        self.far_copy(k, view, full).wait_send()
        self.near_copy(k, view, full).wait_send()
        self.relay_copy(k, full).wait_send()


def half_columns(ref, share):
    return lambda u: ref.at[:, pl.ds(pl.multiple_of(u * share, share), share)]


def half_rows(ref, share):
    return lambda u: ref.at[pl.ds(pl.multiple_of(u * share, share), share), :]


def full_barrier(place, n, near):
    sem = pltpu.get_barrier_semaphore()
    s, f = place.s, place.f
    for d in range(1, n):
        pl.semaphore_signal(sem, inc=1, device_id=((s + d) % n, f), device_id_type=MESH)
    for other in near:
        pl.semaphore_signal(sem, inc=1, device_id=(s, other), device_id_type=MESH)
    pl.semaphore_wait(sem, n - 1 + len(near))


def swap_halves(v):
    return pltpu.roll(v, HD // 2, axis=1)


def to_rows(first, second):
    rows = first.shape[0]
    lane = lax.broadcasted_iota(jnp.int32, (rows, 128), 1)
    wide = jnp.where(lane == 0, first, jnp.where(lane == 1, second, 0.0))
    return wide.T[:8]


def to_columns(v):
    return jnp.concatenate([v, jnp.zeros((120, v.shape[1]), F32)], axis=0).T


def exchange(place, n, own, held, send, recv):
    copies = []
    for d in range(1, n):
        copy = pltpu.make_async_remote_copy(
            own,
            held.at[d - 1],
            send.at[d - 1],
            recv.at[d - 1],
            device_id=((place.s + d) % n, place.f),
            device_id_type=MESH,
        )
        copy.start()
        copies.append(copy)
    total = own[...]
    for d in range(1, n):
        copies[d - 1].wait_recv()
        total = total + held[d - 1]
    return total, copies


def attend(block, q_v, k_v, v_v, out_v, low_v, log_v):
    length = q_v.shape[0]
    scale = HD ** (-0.5)

    @pl.loop(0, q_v.shape[1] // HD)
    def _(h):
        cols = pl.ds(pl.multiple_of(h * HD, HD), HD)
        for i in range(length // block):
            rows, wide = pl.ds(i * block, block), pl.ds(0, (i + 1) * block)
            s = dot(q_v[rows, cols], k_v[wide, cols], NT) * scale
            column = lax.broadcasted_iota(jnp.int32, s.shape, 1)
            row = lax.broadcasted_iota(jnp.int32, s.shape, 0) + i * block
            s = jnp.where(column <= row, s, -jnp.inf)
            top = jnp.max(s, axis=-1, keepdims=True)
            p = jnp.exp(s - top)
            total = jnp.sum(p, axis=-1, keepdims=True)
            out = dot((p * (1.0 / total)).astype(BF16), v_v[wide, cols], NN)
            out_v[rows, cols] = out
            low_v[rows, cols] = out.astype(BF16)
            log_v[h, rows, :] = top + jnp.log(total)


def attention_kernel(
    x, gain, tables, branch_gain, xs, qkv, wo, gate_w, up_w,
    raw, heads, attended, low, log_total, inverse, branch, hidden, hidden_low, wg, wu,
    xs_v, w_v, wo_v, raw_v, heads_v, out_v, low_v, log_v, small, held, value,
    rc, rd, rx, ry, qbuf, zbuf, send, recv, ssend, srecv, zsem, sems,
):
    place = Place(1)
    n, m = xs.shape[1], qkv.shape[1]
    rows, width = x.shape
    length, cols = raw.shape[1], raw.shape[2]
    share = wg.shape[2]
    moves = Moves(sems)
    loads = [moves.start(xs.at[0], xs_v)]
    for j in range(3):
        for f in range(m):
            loads.append(moves.start(qkv.at[j, f], w_v.at[j, :, f]))
    late = [moves.start(wo, wo_v)]
    near = [opposite(place.f), flip(place.f, 1)]
    full_barrier(place, n, near)
    stream = Stream(place, zsem)
    views = [half_columns(gate_w, share), half_columns(up_w, share)]
    fulls = [wg, wu]
    for k in range(2):
        stream.start_far(k, views[k], fulls[k])
    for k in range(2):
        stream.start_near(k, views[k], fulls[k])
    moves.wait(loads)
    block = min(256, length)
    per = block // rows

    @pl.loop(0, length // block)
    def _(i):
        here = pl.ds(pl.multiple_of(i * block, block), block)
        a = xs_v[pl.ds(i * per, per)].reshape(block, width)
        q = dot(a, w_v[0].reshape(width, cols), NN)
        k = dot(a, w_v[1].reshape(width, cols), NN)
        raw_v[0, here, :] = q
        raw_v[1, here, :] = k
        heads_v[2, here, :] = dot(a, w_v[2].reshape(width, cols), NN).astype(BF16)
        small[0, :, here] = to_rows(
            jnp.sum(q * q, axis=1, keepdims=True), jnp.sum(k * k, axis=1, keepdims=True)
        )

    moves.start(raw_v, raw)
    total, stat_copies = exchange(place, n, small.at[0], held, ssend, srecv)
    small[1] = lax.rsqrt(total * (1.0 / width) + EPSILON)
    moves.start(small.at[1], inverse)

    @pl.loop(0, length // block)
    def _(i):
        here = pl.ds(pl.multiple_of(i * block, block), block)
        inv = to_columns(small[1, :, here])
        cosine, sine = tables[0, here, :], tables[1, here, :]
        for j in range(2):
            for h in range(cols // HD):
                part = pl.ds(h * HD, HD)
                v = raw_v[j, here, part] * inv[:, j : j + 1] * gain[j, :, part]
                heads_v[j, here, part] = (v * cosine + swap_halves(v) * sine).astype(BF16)

    moves.start(heads_v, heads)
    attend(block, heads_v.at[0], heads_v.at[1], heads_v.at[2], out_v, low_v, log_v)
    moves.start(out_v, attended)
    moves.start(low_v, low)
    moves.start(log_v, log_total)
    moves.wait(late)
    step = min(512, width)

    def make(q, chip):
        here = pl.ds(pl.multiple_of(chip * 2 * rows, 2 * rows), 2 * rows)

        @pl.loop(0, width // step)
        def _(j):
            at = pl.ds(pl.multiple_of(j * step, step), step)
            part = dot(low_v[here, :], wo_v[:, :, at].reshape(cols, step), NN).astype(BF16)
            value[q, pl.ds(2 * chip, 2), :, at] = part.reshape(2, rows, step)

    total, live = scatter_pairs(
        place, Wires(send, recv), value, rc, rd, rx, ry, qbuf, zbuf, make,
        lambda: stream.relay(0, views[0], fulls[0]),
    )
    branch[...] = total
    inv = lax.rsqrt(jnp.mean(total * total, axis=-1, keepdims=True) + EPSILON)
    h = x[...].astype(F32) + total * inv * branch_gain[...]
    hidden[...] = h
    hidden_low[...] = h.astype(BF16)
    stream.relay(1, views[1], fulls[1])
    for copy in list(live.values()) + stat_copies:
        copy.wait_send()
    moves.finish()
    for k in range(2):
        stream.finish(k, views[k], fulls[k])


def attention_half(x, gain, tables, branch_gain, xs, qkv, wo, gate_w, up_w, ident):
    rows, width = x.shape
    n, m, part, cols = xs.shape[1], qkv.shape[1], qkv.shape[3], qkv.shape[4]
    length, share = n * rows, gate_w.shape[1] // 2
    dma = pltpu.SemaphoreType.DMA
    heads = cols // HD
    outs = [
        shape((2, length, cols), F32),
        shape((3, length, cols), BF16),
        shape((length, cols), F32),
        shape((length, cols), BF16),
        shape((heads, length, 1), F32),
        shape((8, length), F32),
        shape((rows, width), F32),
        shape((rows, width), F32),
        shape((rows, width), BF16),
        shape((m,) + (gate_w.shape[0], share), BF16),
        shape((m,) + (gate_w.shape[0], share), BF16),
    ]
    return pl.pallas_call(
        attention_kernel,
        in_specs=vmem_specs(4) + any_specs(5),
        out_specs=any_specs(6) + vmem_specs(3) + any_specs(2),
        out_shape=outs,
        scratch_shapes=[
            pltpu.VMEM((n, rows, width), BF16),
            pltpu.VMEM((3, n, m, part, cols), BF16),
            pltpu.VMEM(wo.shape, BF16),
            pltpu.VMEM((2, length, cols), F32),
            pltpu.VMEM((3, length, cols), BF16),
            pltpu.VMEM((length, cols), F32),
            pltpu.VMEM((length, cols), BF16),
            pltpu.VMEM((heads, length, 1), F32),
            pltpu.VMEM((2, 8, length), F32),
            pltpu.VMEM((n - 1, 8, length), F32),
            pltpu.VMEM((1, n, rows, width), BF16),
        ]
        + scatter_scratch(1, rows, width)
        + [dma((n - 1,)), dma((n - 1,)), dma((2, 4, 2)), dma((20 + 3 * m,))],
        compiler_params=kernel_params(ident),
        cost_estimate=pl.CostEstimate(flops=10**10, bytes_accessed=200 * 2**20, transcendentals=0),
        name=f"attention_{ident}",
    )(x, gain, tables, branch_gain, xs, qkv, wo, gate_w, up_w)


def attention_forward_kernel(block, q_ref, k_ref, v_ref, out_ref, low_ref, log_ref):
    length = q_ref.shape[0]
    scale = HD ** (-0.5)
    for i in range(length // block):
        rows = pl.ds(i * block, block)
        width = (i + 1) * block
        s = dot(q_ref[rows, :], k_ref[pl.ds(0, width), :], NT) * scale
        column = lax.broadcasted_iota(jnp.int32, (block, width), 1)
        row = lax.broadcasted_iota(jnp.int32, (block, width), 0) + i * block
        s = jnp.where(column <= row, s, -jnp.inf)
        top = jnp.max(s, axis=-1, keepdims=True)
        p = jnp.exp(s - top)
        total = jnp.sum(p, axis=-1, keepdims=True)
        weights = (p * (1.0 / total)).astype(BF16)
        out = dot(weights, v_ref[pl.ds(0, width), :], NN)
        out_ref[rows, :] = out
        low_ref[rows, :] = out.astype(BF16)
        log_ref[0, rows, :] = top + jnp.log(total)


def attention_forward(q, k, v):
    length, width = q.shape
    heads = width // HD
    block = min(256, length)
    column = pl.BlockSpec((length, HD), lambda h: (0, h))
    return pl.pallas_call(
        functools.partial(attention_forward_kernel, block),
        grid=(heads,),
        in_specs=[column] * 3,
        out_specs=[column, column, pl.BlockSpec((1, length, 1), lambda h: (h, 0, 0))],
        out_shape=[
            jax.ShapeDtypeStruct((length, width), F32),
            jax.ShapeDtypeStruct((length, width), BF16),
            jax.ShapeDtypeStruct((heads, length, 1), F32),
        ],
        cost_estimate=pl.CostEstimate(
            flops=2 * heads * length * length * HD, bytes_accessed=10 * length * width, transcendentals=0
        ),
    )(q, k, v)


def attention_backward_kernel(block, q_ref, k_ref, v_ref, out_ref, log_ref, g_ref, dq_ref, dk_ref, dv_ref, dk, dv):
    length = q_ref.shape[0]
    scale = HD ** (-0.5)
    dk[...] = jnp.zeros_like(dk)
    dv[...] = jnp.zeros_like(dv)
    for i in range(length // block):
        rows = pl.ds(i * block, block)
        width = (i + 1) * block
        wide = pl.ds(0, width)
        q = q_ref[rows, :]
        g = g_ref[rows, :]
        s = dot(q, k_ref[wide, :], NT) * scale
        column = lax.broadcasted_iota(jnp.int32, (block, width), 1)
        row = lax.broadcasted_iota(jnp.int32, (block, width), 0) + i * block
        s = jnp.where(column <= row, s, -jnp.inf)
        weights = jnp.exp(s - log_ref[0, rows, :])
        correction = jnp.sum(g.astype(F32) * out_ref[rows, :], axis=-1, keepdims=True)
        gw = dot(g, v_ref[wide, :], NT)
        gs = (weights * (gw - correction)).astype(BF16)
        dq_ref[rows, :] = (dot(gs, k_ref[wide, :], NN) * scale).astype(BF16)
        dk[wide, :] += dot(gs, q, TN)
        dv[wide, :] += dot(weights.astype(BF16), g, TN)
    dk_ref[...] = (dk[...] * scale).astype(BF16)
    dv_ref[...] = dv[...].astype(BF16)


def attention_backward(q, k, v, out, log_total, g):
    length, width = q.shape
    heads = width // HD
    block = min(256, length)
    column = pl.BlockSpec((length, HD), lambda h: (0, h))
    return pl.pallas_call(
        functools.partial(attention_backward_kernel, block),
        grid=(heads,),
        in_specs=[column] * 4 + [pl.BlockSpec((1, length, 1), lambda h: (h, 0, 0)), column],
        out_specs=[column] * 3,
        out_shape=[jax.ShapeDtypeStruct((length, width), BF16)] * 3,
        scratch_shapes=[pltpu.VMEM((length, HD), F32)] * 2,
        cost_estimate=pl.CostEstimate(
            flops=5 * heads * length * length * HD, bytes_accessed=16 * length * width, transcendentals=0
        ),
    )(q, k, v, out, log_total, g)


def on_device(n, m, pair, *args):
    (
        tokens,
        query_weight,
        key_weight,
        value_weight,
        out_weight,
        query_gain,
        key_gain,
        attention_gain,
        gate_weight,
        up_weight,
        down_weight,
        feedforward_gain,
        cotangent,
    ) = args
    rows, width = tokens.shape[1], tokens.shape[2]
    length = rows * n
    part = query_weight.shape[0]
    cols = width // n
    depth, units = gate_weight.shape
    share = units // pair
    x = tokens.reshape(rows, width)
    groups = [[g * pair + u for u in range(pair)] for g in range(m // pair)]

    native = n == 8 and m == 4

    def gather_plane(v, ident):
        if native:
            return plane_gather(v, n, 1, ident)
        return lax.all_gather(v, "seq", axis=0, tiled=True)

    def scatter_plane(v, ident):
        if native:
            return plane_scatter(v, n, 1, ident)
        return lax.psum_scatter(v.astype(BF16), "seq", scatter_dimension=0, tiled=True).astype(F32)

    def gather_pair(v, ident):
        if native:
            return plane_gather(v, n, pair, ident)
        if pair > 1:
            v = lax.all_gather(v, "fsdp", axis=0, axis_index_groups=groups)
        v = lax.all_gather(v.reshape(pair, rows, width), "seq", axis=1, tiled=True)
        return v.reshape(pair * length, width)

    def scatter_pair(v, ident):
        if native:
            return plane_scatter(v, n, pair, ident)
        v = lax.psum_scatter(v.astype(BF16).reshape(pair, length, width), "seq", scatter_dimension=1, tiled=True)
        if pair > 1:
            v = lax.psum_scatter(v, "fsdp", scatter_dimension=0, axis_index_groups=groups)
        return v.reshape(rows, width).astype(F32)

    def total_plane(v, ident):
        return plane_sum(v, n, ident) if native else lax.psum(v, "seq")

    def spread(halves):
        return lax.all_to_all(jnp.tile(halves, (m // pair, 1, 1)), "fsdp", 0, 0, tiled=False)

    def settle(blocks):
        back = lax.all_to_all(blocks.astype(BF16), "fsdp", 0, 0, tiled=False)
        if native:
            return jnp.sum(back.reshape((pair, m // pair) + back.shape[1:]).astype(F32), axis=1)
        return jnp.sum(back.reshape((m // pair, pair) + back.shape[1:]).astype(F32), axis=0)

    gains = jnp.stack([query_gain, key_gain, attention_gain, feedforward_gain]).astype(F32)
    seq = lax.axis_index("seq")
    cosine, sine = angles_of(length)
    grad_out = cotangent.reshape(rows, width)
    if native:
        xs, qkv, out_rows, full = entry(
            x, query_weight, key_weight, value_weight, out_weight, jnp.pad(gains, ((0, 4), (0, 128 - part))), n, m, 1
        )
        full_gain = full[:, :, :4, :part].transpose(2, 1, 0, 3).reshape(4, width)
    else:
        stacked = jnp.stack([query_weight, key_weight, value_weight]).reshape(3, part, n, cols)
        mine = lax.all_to_all(stacked.transpose(2, 0, 1, 3), "seq", 0, 0)
        qkv = lax.all_gather(mine, "fsdp", axis=1).transpose(2, 0, 1, 3, 4).reshape(3, width, cols)
        full_gain = lax.all_gather(gains, ("seq", "fsdp"), axis=1).reshape(4, width)
        xs = gather_plane(x, 1)
        out_rows = lax.all_gather(out_weight, "fsdp", axis=0, tiled=True)
    own_gain = lax.dynamic_slice_in_dim(full_gain[:2], seq * cols, cols, 1)
    q_gain, k_gain, branch_gain, feed_gain = own_gain[0], own_gain[1], full_gain[2], full_gain[3]

    if native:
        tables = jnp.stack([jnp.tile(cosine, (1, 2)), jnp.concatenate([-sine, sine], axis=1)])
        raw, heads, attended, attended_low, log_total, inverse, branch, hidden, hidden_low, gate_cols, up_cols = (
            attention_half(
                x, own_gain[:, None, :], tables, branch_gain[None, :], xs, qkv, out_rows, gate_weight, up_weight, 3
            )
        )
        gate_cols, up_cols = gate_cols.reshape(width, share), up_cols.reshape(width, share)
        q_raw, k_raw, q, k, v = raw[0], raw[1], heads[0], heads[1], heads[2]
        q_inv, k_inv = inverse[0][:, None], inverse[1][:, None]
        xs = xs.reshape(length, width)
        qkv = qkv.transpose(0, 2, 1, 3, 4).reshape(3, width, cols)
        out_rows = out_rows.reshape(cols, width)
        hs, gate, up, inner, inner_t, down_rows = ffn_up(hidden_low, gate_cols, up_cols, down_weight, n, pair, 5)
        layer_out, grad_low, feed_gain_term = ffn_down(inner, down_rows, hidden, feed_gain, grad_out, n, pair, 7)
        gs, grad_gate, grad_up, gate_t, up_t = ffn_grad(grad_low, down_rows, gate, up, n, pair, 6)
        grad_hidden, branch_low, branch_gain_term = ffn_back(
            grad_gate, grad_up, gate_cols, up_cols, branch, branch_gain, grad_out, n, pair, 8
        )
        feed_gain_term, branch_gain_term = feed_gain_term[0], branch_gain_term[0]
        hs, gs = hs.reshape(pair * length, width), gs.reshape(pair * length, width)
    else:
        q_raw, k_raw, v = dot(xs, qkv[0], NN), dot(xs, qkv[1], NN), dot(xs, qkv[2], NN).astype(BF16)
        squares = jnp.stack([jnp.sum(q_raw * q_raw, axis=1), jnp.sum(k_raw * k_raw, axis=1)])
        inverse = lax.rsqrt(lax.psum(squares, "seq") / width + EPSILON)
        q_inv, k_inv = inverse[0][:, None], inverse[1][:, None]
        q = rotate(q_raw * q_inv * q_gain, cosine, sine, 1.0).astype(BF16)
        k = rotate(k_raw * k_inv * k_gain, cosine, sine, 1.0).astype(BF16)
        attended, attended_low, log_total = attention_forward(q, k, v)
        branch = scatter_plane(dot(attended_low, out_rows, NN), 3)
        branch_inv = lax.rsqrt(jnp.mean(branch * branch, axis=1, keepdims=True) + EPSILON)
        hidden = x.astype(F32) + branch * branch_inv * branch_gain
        hidden_low = hidden.astype(BF16)
        gate_cols = spread(gate_weight.reshape(depth, pair, share).transpose(1, 0, 2)).reshape(width, share)
        up_cols = spread(up_weight.reshape(depth, pair, share).transpose(1, 0, 2)).reshape(width, share)
        down_rows = spread(down_weight.reshape(pair, share, depth)).transpose(1, 0, 2).reshape(share, width)
        grad_out = grad_out.astype(F32)
        hs = gather_pair(hidden_low, 5)
        gate = dot(hs, gate_cols, NN)
        up = dot(hs, up_cols, NN)
        sig = jax.nn.sigmoid(gate)
        inner = (gate * sig * up).astype(BF16)
        feed = scatter_pair(dot(inner, down_rows, NN), 7)
        feed_inv = lax.rsqrt(jnp.mean(feed * feed, axis=1, keepdims=True) + EPSILON)
        layer_out = (hidden + feed * feed_inv * feed_gain).astype(BF16)
        grad_feed, term = rms_back(feed, feed_gain, grad_out)
        feed_gain_term = jnp.sum(term, axis=0)
        gs = gather_pair(grad_feed.astype(BF16), 6)
        grad_inner = dot(gs, down_rows, NT)
        grad_gate = (grad_inner * up * sig * (1.0 + gate * (1.0 - sig))).astype(BF16)
        grad_up = (grad_inner * gate * sig).astype(BF16)
        grad_hidden = grad_out + scatter_pair(dot(grad_gate, gate_cols, NT) + dot(grad_up, up_cols, NT), 8)
        grad_branch, term = rms_back(branch, branch_gain, grad_hidden)
        branch_low = grad_branch.astype(BF16)
        branch_gain_term = jnp.sum(term, axis=0)
        inner_t, gate_t, up_t = inner.T, grad_gate.T, grad_up.T

    def cut(v):
        return v.reshape(share, m, depth).transpose(1, 0, 2)

    down_grad = settle(cut(dot(inner_t, gs, NN))).reshape(units, depth)
    gate_grad = settle(cut(dot(gate_t, hs, NN))).transpose(2, 0, 1).reshape(depth, units)
    up_grad = settle(cut(dot(up_t, hs, NN))).transpose(2, 0, 1).reshape(depth, units)
    bs = gather_plane(branch_low, 2)
    out_grad = lax.psum_scatter(
        dot(attended_low, bs, TN).astype(BF16), "fsdp", scatter_dimension=0, tiled=True
    ).astype(F32)
    grad_attended = dot(bs, out_rows, NT).astype(BF16)
    dq, dk, dv = attention_backward(q, k, v, attended, log_total, grad_attended)
    dq = rotate(dq.astype(F32), cosine, sine, -1.0)
    dk = rotate(dk.astype(F32), cosine, sine, -1.0)
    q_normal, k_normal = q_raw * q_inv, k_raw * k_inv
    q_gain_term = jnp.sum(dq * q_normal, axis=0)
    k_gain_term = jnp.sum(dk * k_normal, axis=0)
    dq, dk = dq * q_gain, dk * k_gain
    means = total_plane(jnp.stack([jnp.sum(dq * q_normal, axis=1), jnp.sum(dk * k_normal, axis=1)]), 10) / width
    dq = (q_inv * (dq - q_normal * means[0][:, None])).astype(BF16)
    dk = (k_inv * (dk - k_normal * means[1][:, None])).astype(BF16)
    value = dot(dq, qkv[0], NT) + dot(dk, qkv[1], NT) + dot(dv, qkv[2], NT)
    term = jnp.stack([dot(xs, d, TN).astype(BF16) for d in (dq, dk, dv)]).reshape(3, n, m, part, cols)
    gain_own = jnp.stack([q_gain_term, k_gain_term])
    gain_own = lax.dynamic_update_slice(jnp.zeros((2, width), F32), gain_own, (0, seq * cols))
    gain_terms = jnp.concatenate([gain_own, jnp.stack([branch_gain_term, feed_gain_term])]).reshape(4, n, m, part)
    if native:
        gain_terms = jnp.pad(gain_terms.transpose(1, 2, 0, 3), ((0, 0), (0, 0), (0, 4), (0, 128 - part)))
        tokens_grad, term, gain_grads = leave(value, term, gain_terms, grad_hidden, n, m, 4)
        term = term.transpose(0, 2, 1, 3)
        gain_grads = gain_grads[:4, :part]
    else:
        tokens_grad = grad_hidden + scatter_plane(value, 4)
        term = lax.psum_scatter(term, "fsdp", scatter_dimension=2)
        term = lax.all_to_all(term, "seq", 1, 1).astype(F32).transpose(0, 2, 1, 3)
        gain_grads = lax.psum_scatter(
            gain_terms.reshape(4, width), ("seq", "fsdp"), scatter_dimension=1, tiled=True
        )
    term = term.reshape(3, part, width)
    return (
        layer_out.reshape(tokens.shape),
        tokens_grad.reshape(tokens.shape),
        term[0],
        term[1],
        term[2],
        out_grad,
        gain_grads[0],
        gain_grads[1],
        gain_grads[2],
        gate_grad,
        up_grad,
        down_grad,
        gain_grads[3],
    )


def solution(mesh):
    n, m = mesh.shape["seq"], mesh.shape["fsdp"]
    tall, flat, act = P(("seq", "fsdp"), None), P(("seq", "fsdp")), P("fsdp", "seq", None)
    wide, deep = P("fsdp", "seq"), P("seq", "fsdp")
    return jax.shard_map(
        functools.partial(on_device, n, m, 2),
        mesh=mesh,
        in_specs=(act, tall, tall, tall, tall, flat, flat, flat, wide, wide, deep, flat, act),
        out_specs=(act, act, tall, tall, tall, tall, flat, flat, flat, wide, wide, deep, flat),
        check_vma=False,
    )
```

```python
import functools
import math

import jax
import jax.numpy as jnp
from jax import lax
from jax.experimental import pallas as pl
from jax.experimental.pallas import tpu as pltpu
from jax.sharding import PartitionSpec as P

EPSILON = 1e-06
THETA = 500000.0
HD = 128
F32 = jnp.float32
BF16 = jnp.bfloat16


def dot(a, b, dims):
    return lax.dot_general(a, b, (dims, ((), ())), preferred_element_type=F32)


NN = ((1,), (0,))
NT = ((1,), (1,))
TN = ((0,), (0,))


def angles_of(length):
    half = HD // 2
    frequency = jnp.exp(jnp.arange(half, dtype=F32) * (-2.0 * math.log(THETA) / HD))
    angle = jnp.arange(length, dtype=F32)[:, None] * frequency[None, :]
    return jnp.cos(angle), jnp.sin(angle)


def rotate(value, cosine, sine, sign):
    length, width = value.shape
    value = value.reshape(length, width // HD, 2, HD // 2)
    first, second = value[:, :, 0], value[:, :, 1]
    c, s = cosine[:, None, :], sign * sine[:, None, :]
    return jnp.stack([first * c - second * s, second * c + first * s], axis=2).reshape(length, width)


MESH = pl.DeviceIdType.MESH


def flip(index, bit):
    return index + bit - 2 * bit * ((index // bit) % 2)


class Place:
    def __init__(self, pair):
        self.s, self.f = lax.axis_index("seq"), lax.axis_index("fsdp")
        self.pair = pair
        s, f = self.s, self.f
        self.sx, self.sy = flip(s, 2), flip(s, 4)
        self.sd, self.sc = flip(self.sx, 4), flip(s, 1)
        self.q = f // 2 if pair > 1 else 0
        self.x, self.y, self.core = (self.sx, f), (self.sy, f), (self.sc, f)
        self.z = (s, opposite(f)) if pair > 1 else None
        self.peers = [self.x, self.y, self.core] + ([self.z] if pair > 1 else [])

    def barrier(self):
        sem = pltpu.get_barrier_semaphore()
        for peer in self.peers:
            pl.semaphore_signal(sem, inc=1, device_id=peer, device_id_type=MESH)
        pl.semaphore_wait(sem, len(self.peers))


class Wires:
    def __init__(self, send, recv):
        self.send, self.recv, self.count, self.open = send, recv, 0, {}

    def new(self, key):
        self.open[key] = self.count
        self.count += 1

    def go(self, key, src, dst, device):
        i = self.open[key]
        copy = pltpu.make_async_remote_copy(
            src, dst, self.send.at[i], self.recv.at[i], device_id=device, device_id_type=MESH
        )
        copy.start()
        return copy


def gather_steps(place, wires, own, out, ready):
    pair, rows = place.pair, own.shape[0]
    half = rows // 2
    top, low = pl.ds(0, half), pl.ds(half, half)
    p = place
    qs = [p.q] + ([1 - p.q] if pair > 1 else [])
    kinds = ["xa", "xb", "ya", "yb", "xd", "yd", "c0", "cxa", "cxb", "cya", "cyb", "cda", "cdb"]
    for t in range(pair):
        for kind in kinds:
            wires.new((t, kind))
    if pair > 1:
        wires.new("z")
    live = {}

    def go(key, src, dst, device):
        live[key] = wires.go(key, src, dst, device)

    def begin(t, src):
        q = qs[t]
        go((t, "xa"), src.at[top], out.at[q, p.s, top], p.x)
        go((t, "yb"), src.at[low], out.at[q, p.s, low], p.y)
        go((t, "xb"), src.at[low], out.at[q, p.s, low], p.x)
        go((t, "ya"), src.at[top], out.at[q, p.s, top], p.y)
        go((t, "c0"), src, out.at[q, p.s], p.core)

    def arrived(key):
        live[key].wait_recv()

    if pair > 1:
        go("z", own, out.at[qs[0], p.s], p.z)
    begin(0, own)
    ready(qs[0], p.s, None)

    def first(t):
        q = qs[t]
        arrived((t, "xa"))
        go((t, "xd"), out.at[q, p.sx, top], out.at[q, p.sx, top], p.y)
        go((t, "cxa"), out.at[q, p.sx, top], out.at[q, p.sx, top], p.core)
        arrived((t, "yb"))
        go((t, "yd"), out.at[q, p.sy, low], out.at[q, p.sy, low], p.x)
        go((t, "cyb"), out.at[q, p.sy, low], out.at[q, p.sy, low], p.core)
        arrived((t, "c0"))
        ready(q, p.sc, None)

    def second(t):
        q = qs[t]
        arrived((t, "xb"))
        go((t, "cxb"), out.at[q, p.sx, low], out.at[q, p.sx, low], p.core)
        ready(q, p.sx, None)
        arrived((t, "ya"))
        go((t, "cya"), out.at[q, p.sy, top], out.at[q, p.sy, top], p.core)
        ready(q, p.sy, None)
        arrived((t, "xd"))
        go((t, "cda"), out.at[q, p.sd, top], out.at[q, p.sd, top], p.core)
        arrived((t, "yd"))
        go((t, "cdb"), out.at[q, p.sd, low], out.at[q, p.sd, low], p.core)

    def third(t):
        q = qs[t]
        arrived((t, "cxa"))
        arrived((t, "cxb"))
        ready(q, flip(p.sx, 1), None)
        arrived((t, "cya"))
        arrived((t, "cyb"))
        ready(q, flip(p.sy, 1), None)
        ready(q, p.sd, None)
        arrived((t, "cda"))
        arrived((t, "cdb"))
        ready(q, flip(p.sd, 1), None)

    first(0)
    if pair > 1:
        arrived("z")
        begin(1, out.at[qs[1], p.s])
        ready(qs[1], p.s, None)
    second(0)
    if pair > 1:
        first(1)
    third(0)
    if pair > 1:
        second(1)
        third(1)
    for copy in live.values():
        copy.wait_send()


def gather_wires(pair):
    return 14 * pair + (2 if pair > 1 else 0)


def gather_kernel(pair, own, out, send, recv, local):
    place = Place(pair)
    keep = pltpu.make_async_copy(own, out.at[place.q, place.s], local)
    keep.start()
    place.barrier()
    gather_steps(place, Wires(send, recv), own, out, lambda q, slot, half: None)
    keep.wait()


def plane_gather(v, n, pair, ident):
    rows, width = v.shape
    return pl.pallas_call(
        functools.partial(gather_kernel, pair),
        in_specs=[pl.BlockSpec(memory_space=pltpu.VMEM)],
        out_specs=pl.BlockSpec(memory_space=pl.ANY),
        out_shape=jax.ShapeDtypeStruct((pair, n, rows, width), v.dtype),
        scratch_shapes=[pltpu.SemaphoreType.DMA((gather_wires(pair),))] * 2 + [pltpu.SemaphoreType.DMA],
        compiler_params=pltpu.CompilerParams(collective_id=ident, has_side_effects=True),
        cost_estimate=pl.CostEstimate(flops=0, bytes_accessed=pair * n * rows * width * 20, transcendentals=0),
        name=f"gather_{ident}",
    )(v).reshape(pair * n * rows, width)


def add(a, b):
    return (a.astype(F32) + b.astype(F32)).astype(BF16)


def scatter_steps(place, wires, part, rc, rd, rx, ry, qbuf, zbuf, make, finish):
    p, pair = place, place.pair
    rows = rx.shape[1]
    half = rows // 2
    top, low = pl.ds(0, half), pl.ds(half, half)
    slots = {"d": p.sd, "x": p.sx, "y": p.sy, "o": p.s}
    order = ["d", "x", "y", "o"]
    names = ["c" + k for k in order] + ["da", "db", "xa", "xb", "ya", "yb"]
    for t in range(pair):
        for name in names:
            wires.new((t, name))
    if pair > 1:
        wires.new("z")
    live = {}

    def go(key, src, dst, device):
        live[key] = wires.go(key, src, dst, device)

    def arrived(key):
        live[key].wait_recv()

    for t in range(pair):
        for i, k in enumerate(order):
            make(t, k, 1)
            go((t, "c" + k), part(t, flip(slots[k], 1)), rc.at[t, i], p.core)

    def start(t):
        make(t, "d", 0)
        arrived((t, "cd"))
        qbuf[t, 0] = add(part(t, p.sd)[...], rc[t, 0])
        go((t, "da"), qbuf.at[t, 0, top], rd.at[t, top], p.x)
        go((t, "db"), qbuf.at[t, 0, low], rd.at[t, low], p.y)
        make(t, "x", 0)
        arrived((t, "cx"))
        qbuf[t, 1, top] = add(part(t, p.sx)[top], rc[t, 1, top])
        go((t, "xa"), qbuf.at[t, 1, top], rx.at[t, top], p.x)
        make(t, "y", 0)
        arrived((t, "cy"))
        qbuf[t, 2, low] = add(part(t, p.sy)[low], rc[t, 2, low])
        go((t, "yb"), qbuf.at[t, 2, low], ry.at[t, low], p.y)

    def relay(t):
        held = part(t, p.sx)[low].astype(F32) + rc[t, 1, low].astype(F32)
        arrived((t, "db"))
        qbuf[t, 1, low] = (held + rd[t, low].astype(F32)).astype(BF16)
        go((t, "xb"), qbuf.at[t, 1, low], rx.at[t, low], p.x)
        held = part(t, p.sy)[top].astype(F32) + rc[t, 2, top].astype(F32)
        arrived((t, "da"))
        qbuf[t, 2, top] = (held + rd[t, top].astype(F32)).astype(BF16)
        go((t, "ya"), qbuf.at[t, 2, top], ry.at[t, top], p.y)

    def total(t):
        make(t, "o", 0)
        arrived((t, "co"))
        value = part(t, p.s)[...].astype(F32) + rc[t, 3].astype(F32)
        for key in ("xa", "yb", "xb", "ya"):
            arrived((t, key))
        return value + rx[t].astype(F32) + ry[t].astype(F32)

    if pair > 1:
        start(0)
        start(1)
        relay(0)
        relay(1)
        zbuf[0] = total(0).astype(BF16)
        go("z", zbuf.at[0], zbuf.at[1], p.z)
        value = total(1)
        arrived("z")
        value = value + zbuf[1].astype(F32)
    else:
        start(0)
        relay(0)
        value = total(0)
    finish(value)
    for copy in live.values():
        copy.wait_send()


def scatter_wires(pair):
    return 20 * pair + (2 if pair > 1 else 0)


def scatter_scratch(pair, rows, width):
    block = lambda *lead: pltpu.VMEM(lead + (rows, width), BF16)
    return [
        block(pair, 4),
        block(pair),
        block(pair),
        block(pair),
        block(pair, 3),
        block(2) if pair > 1 else pltpu.VMEM((2, 16, 128), BF16),
        pltpu.SemaphoreType.DMA((scatter_wires(pair),)),
        pltpu.SemaphoreType.DMA((scatter_wires(pair),)),
    ]


def scatter_kernel(pair, value, out, rc, rd, rx, ry, qbuf, zbuf, send, recv):
    place = Place(pair)
    place.barrier()
    planes = [1 - place.q, place.q] if pair > 1 else [0]

    def part(t, slot):
        return value.at[planes[t], slot]

    def finish(total):
        out[...] = total

    scatter_steps(
        place, Wires(send, recv), part, rc, rd, rx, ry, qbuf, zbuf, lambda *_: None, finish
    )


def plane_scatter(v, n, pair, ident):
    width = v.shape[1]
    rows = v.shape[0] // (pair * n)
    return pl.pallas_call(
        functools.partial(scatter_kernel, pair),
        in_specs=[pl.BlockSpec(memory_space=pltpu.VMEM)],
        out_specs=pl.BlockSpec(memory_space=pltpu.VMEM),
        out_shape=jax.ShapeDtypeStruct((rows, width), F32),
        scratch_shapes=scatter_scratch(pair, rows, width),
        compiler_params=pltpu.CompilerParams(
            collective_id=ident, has_side_effects=True, vmem_limit_bytes=40 * 2**20
        ),
        cost_estimate=pl.CostEstimate(flops=0, bytes_accessed=pair * n * rows * width * 20, transcendentals=0),
        name=f"scatter_{ident}",
    )(v.astype(BF16).reshape(pair, n, rows, width))


def sum_kernel(n, own, out, held, send, recv):
    s, f = lax.axis_index("seq"), lax.axis_index("fsdp")
    sem = pltpu.get_barrier_semaphore()
    for d in range(1, n):
        pl.semaphore_signal(sem, inc=1, device_id=((s + d) % n, f), device_id_type=MESH)
    pl.semaphore_wait(sem, n - 1)
    copies = []
    for d in range(1, n):
        copy = pltpu.make_async_remote_copy(
            own,
            held.at[d - 1],
            send.at[d - 1],
            recv.at[d - 1],
            device_id=((s + d) % n, f),
            device_id_type=MESH,
        )
        copy.start()
        copies.append(copy)
    total = own[...]
    for d in range(1, n):
        copies[d - 1].wait_recv()
        total = total + held[d - 1]
    out[...] = total
    for copy in copies:
        copy.wait_send()


def plane_sum(v, n, ident):
    return pl.pallas_call(
        functools.partial(sum_kernel, n),
        in_specs=[pl.BlockSpec(memory_space=pltpu.VMEM)],
        out_specs=pl.BlockSpec(memory_space=pltpu.VMEM),
        out_shape=jax.ShapeDtypeStruct(v.shape, v.dtype),
        scratch_shapes=[pltpu.VMEM((n - 1,) + v.shape, v.dtype)]
        + [pltpu.SemaphoreType.DMA((n - 1,))] * 2,
        compiler_params=pltpu.CompilerParams(collective_id=ident, has_side_effects=True),
        name=f"sum_{ident}",
    )(v)


def when(condition, body):
    pl.when(condition)(body)


def line_barrier(n, m):
    s, f = lax.axis_index("seq"), lax.axis_index("fsdp")
    sem = pltpu.get_barrier_semaphore()
    for d in range(1, n):
        pl.semaphore_signal(sem, inc=1, device_id=((s + d) % n, f), device_id_type=MESH)
    for d in range(1, m):
        pl.semaphore_signal(sem, inc=1, device_id=(s, (f + d) % m), device_id_type=MESH)
    pl.semaphore_wait(sem, n + m - 2)


def entry_kernel(
    n, m, x, wq, wk, wv, wo, gains, xs, qkv, out, full, send, recv, asend, arecv, zsend, zrecv, gsend, grecv, local
):
    place = Place(1)
    s, f = place.s, place.f
    cols = qkv.shape[-1]
    weights = (wq, wk, wv)
    kept = [pltpu.make_async_copy(x, xs.at[0, s], local.at[0]), pltpu.make_async_copy(gains, full.at[f, s], local.at[1])]
    for j, w in enumerate(weights):
        own = w.at[:, pl.ds(pl.multiple_of(s * cols, cols), cols)]
        kept.append(pltpu.make_async_copy(own, qkv.at[j, f, s], local.at[2 + j]))
    kept.append(pltpu.make_async_copy(wo, out.at[f], local.at[5]))
    for copy in kept:
        copy.start()
    line_barrier(n, m)
    sent = []

    def remote(src, dst, a, b, device):
        copy = pltpu.make_async_remote_copy(src, dst, a, b, device_id=device, device_id_type=MESH)
        copy.start()
        sent.append(copy)
        return copy

    first = []
    for d in range(1, n):
        first.append(remote(gains, full.at[f, s], gsend.at[d], grecv.at[d], ((s + d) % n, f)))
    second = []
    for j, w in enumerate(weights):
        row = []
        for d in range(1, n):
            t = (s + d) % n
            src = w.at[:, pl.ds(pl.multiple_of(t * cols, cols), cols)]
            row.append(remote(src, qkv.at[j, f, s], asend.at[j, d], arecv.at[j, d], (t, f)))
        second.append(row)

    def piece(j, o):
        return out.at[o] if j == 3 else full.at[o] if j == 4 else qkv.at[j, o]

    def hop(way, h, j):
        o = f - h if way == 0 else f + h
        there = f + 1 if way == 0 else f - 1
        place_ = piece(j, o)
        return pltpu.make_async_remote_copy(
            place_, place_, zsend.at[way, h, j], zrecv.at[way, h, j], device_id=(s, there), device_id_type=MESH
        )

    def sends(way, h):
        return ((f - h >= 0) & (f < m - 1)) if way == 0 else ((f + h <= m - 1) & (f > 0))

    def receives(way, h):
        return (f - h - 1 >= 0) if way == 0 else (f + h + 1 <= m - 1)

    def start(h, j):
        for way in (0, 1):
            when(sends(way, h), lambda: hop(way, h, j).start())

    def landed(h, j):
        for way in (0, 1):
            o = f - h - 1 if way == 0 else f + h + 1

            def wait():
                there = f - 1 if way == 0 else f + 1
                place_ = piece(j, o)
                pltpu.make_async_remote_copy(
                    place_, place_, zsend.at[way, h, j], zrecv.at[way, h, j], device_id=(s, there), device_id_type=MESH
                ).wait_recv()

            when(receives(way, h), wait)

    for copy in kept:
        copy.wait()
    start(0, 3)
    for j in range(3):
        for copy in second[j]:
            copy.wait_recv()
        start(0, j)
    for copy in first:
        copy.wait_recv()
    start(0, 4)
    gather_steps(place, Wires(send, recv), x, xs, lambda *_: None)
    for h in range(m - 1):
        for j in range(5) if h else (3, 0, 1, 2, 4):
            landed(h, j)
            if h + 1 < m - 1:
                start(h + 1, j)
    for copy in sent:
        copy.wait_send()
    for h in range(m - 1):
        for j in range(5):
            for way in (0, 1):
                when(sends(way, h), lambda: hop(way, h, j).wait_send())


def entry(x, wq, wk, wv, wo, gains, n, m, ident):
    rows, width = x.shape
    part = wq.shape[0]
    cols = width // n
    vmem, any_ = pl.BlockSpec(memory_space=pltpu.VMEM), pl.BlockSpec(memory_space=pl.ANY)
    dma = pltpu.SemaphoreType.DMA
    return pl.pallas_call(
        functools.partial(entry_kernel, n, m),
        in_specs=[vmem] * 6,
        out_specs=[any_] * 4,
        out_shape=[
            jax.ShapeDtypeStruct((1, n, rows, width), x.dtype),
            jax.ShapeDtypeStruct((3, m, n, part, cols), wq.dtype),
            jax.ShapeDtypeStruct((m,) + wo.shape, wo.dtype),
            jax.ShapeDtypeStruct((m, n) + gains.shape, gains.dtype),
        ],
        scratch_shapes=[dma((gather_wires(1),))] * 2
        + [dma((3, n))] * 2
        + [dma((2, m, 5))] * 2
        + [dma((n,))] * 2
        + [dma((6,))],
        compiler_params=pltpu.CompilerParams(collective_id=ident, has_side_effects=True),
        cost_estimate=pl.CostEstimate(flops=0, bytes_accessed=200 * 2**20, transcendentals=0),
        name=f"entry_{ident}",
    )(x, wq, wk, wv, wo, gains)


def exit_kernel(
    n,
    m,
    d3,
    qkv,
    term,
    gains,
    grad_hidden,
    tokens_grad,
    weight_grad,
    gain_grad,
    w_v,
    value,
    rc,
    rd,
    rx,
    ry,
    qbuf,
    zbuf,
    send,
    recv,
    line,
    sums,
    done,
    got,
    gplane,
    gsum,
    gline,
    zsend,
    zrecv,
    asend,
    arecv,
    gsend,
    grecv,
    lsend,
    lrecv,
    sems,
):
    place = Place(1)
    s, f = place.s, place.f
    moves = Moves(sems)
    for j in range(3):
        for plane in range(m):
            moves.start(qkv.at[j, plane], w_v.at[j, :, plane])
    line_barrier(n, m)
    last = m - 1
    cols = term.shape[-1]

    def remote(src, dst, a, b, device):
        return pltpu.make_async_remote_copy(src, dst, a, b, device_id=device, device_id_type=MESH)

    def target(way, r):
        return last - r if way == 0 else r

    def hop(way, r, j, fresh):
        there = f + 1 if way == 0 else f - 1
        src = term.at[j, :, target(way, r)] if fresh else sums.at[way, r, j]
        return remote(src, line.at[way, r, j], zsend.at[way, r, j], zrecv.at[way, r, j], (s, there))

    ends = (f == 0, f == last)
    inner = (f > 0, f < last)

    def beyond(way, r):
        return target(way, r) > f if way == 0 else target(way, r) < f

    for r in range(last):
        for j in range(4):
            for way in (0, 1):
                when(ends[way], lambda: hop(way, r, j, True).start())

    gain_copies = []
    for d in range(1, n):
        t = (s + d) % n
        copy = remote(gains.at[t], gplane.at[d - 1], gsend.at[d], grecv.at[d], (t, f))
        copy.start()
        gain_copies.append(copy)

    moves.finish()
    rows, width = grad_hidden.shape
    block, step = 2 * rows, min(512, width)
    per = step // (m * qkv.shape[3])

    def make(q, chip, c):
        here = pl.ds(pl.multiple_of(chip * block, block), block)

        @pl.loop(c * (width // 2) // step, (c + 1) * (width // 2) // step)
        def _(i):
            at = pl.ds(pl.multiple_of(i * step, step), step)
            total = jnp.zeros((block, step), F32)
            for j in range(3):
                w = w_v[j, pl.ds(i * per, per)].reshape(step, cols)
                total = total + dot(d3[j, here, :], w, NT)
            value[q, pl.ds(2 * chip, 2), :, at] = total.astype(BF16).reshape(2, rows, step)

    def relays(r, j):
        for way in (0, 1):

            def relay():
                hop(way, r, j, False).wait_recv()
                sums[way, r, j] = add(term[j, :, target(way, r)], line[way, r, j])
                hop(way, r, j, False).start()

            when(inner[way] & beyond(way, r), relay)

    live = scatter_pairs(place, Wires(send, recv), value, rc, rd, rx, ry, qbuf, zbuf, make, tokens_grad)
    tokens_grad[...] += grad_hidden[...]

    total = gains[s]
    for d in range(1, n):
        gain_copies[d - 1].wait_recv()
        total = total + gplane[d - 1]
    gsum[...] = total
    line_copies = []
    for d in range(1, m):
        t = (f + d) % m
        copy = remote(gsum.at[t], gline.at[d - 1], lsend.at[d], lrecv.at[d], (s, t))
        copy.start()
        line_copies.append(copy)

    for r in range(last):
        for j in range(4):
            relays(r, j)

    copies = []
    for j in range(4):
        own = term[j, :, f].astype(F32)
        done[j] = own
        for way in (0, 1):
            r = last - f if way == 0 else f

            def take():
                pltpu.make_async_remote_copy(
                    sums.at[way, 0, j],
                    line.at[way, r, j],
                    zsend.at[way, r, j],
                    zrecv.at[way, r, j],
                    device_id=(s, f - 1 if way == 0 else f + 1),
                    device_id_type=MESH,
                ).wait_recv()
                done[j] += line[way, r, j].astype(F32)

            when(inner[way], take)
        weight_grad[j, s] = done[j, s]
        if j == 3:
            weight_grad[j] = done[j]
            continue
        got[0, j] = done[j].astype(BF16)
        for d in range(1, n):
            t = (s + d) % n
            copy = remote(got.at[0, j, t], got.at[1, j, s], asend.at[j, d], arecv.at[j, d], (t, f))
            copy.start()
            copies.append(copy)
    total = gsum[f]
    for d in range(1, m):
        line_copies[d - 1].wait_recv()
        total = total + gline[d - 1]
    gain_grad[...] = total
    for copy in copies:
        copy.wait_recv()
    for j in range(3):
        for d in range(1, n):
            t = (s + d) % n
            weight_grad[j, t] = got[1, j, t].astype(F32)
    for copy in copies + gain_copies + line_copies + list(live.values()):
        copy.wait_send()
    for r in range(last):
        for j in range(4):
            for way in (0, 1):
                when(ends[way] | (inner[way] & beyond(way, r)), lambda: hop(way, r, j, False).wait_send())


def leave(d3, qkv, term, gains, grad_hidden, n, m, ident):
    rows, width = grad_hidden.shape
    part, cols = term.shape[-2:]
    vmem = pl.BlockSpec(memory_space=pltpu.VMEM)
    dma = pltpu.SemaphoreType.DMA
    block = pltpu.VMEM((2, m - 1, 4, n, part, cols), BF16)
    return pl.pallas_call(
        functools.partial(exit_kernel, n, m),
        in_specs=[vmem, pl.BlockSpec(memory_space=pl.ANY)] + [vmem] * 3,
        out_specs=[vmem] * 3,
        out_shape=[
            jax.ShapeDtypeStruct((rows, width), F32),
            jax.ShapeDtypeStruct((4, n, part, cols), F32),
            jax.ShapeDtypeStruct(gains.shape[2:], F32),
        ],
        scratch_shapes=[pltpu.VMEM((3, n, m, part, cols), BF16), pltpu.VMEM((1, n, rows, width), BF16)]
        + scatter_scratch(1, rows, width)
        + [
            block,
            block,
            pltpu.VMEM((4, n, part, cols), F32),
            pltpu.VMEM((2, 3, n, part, cols), BF16),
            pltpu.VMEM((n - 1,) + gains.shape[1:], F32),
            pltpu.VMEM(gains.shape[1:], F32),
            pltpu.VMEM((m - 1,) + gains.shape[2:], F32),
        ]
        + [dma((2, m, 4))] * 2
        + [dma((3, n))] * 2
        + [dma((n,))] * 2
        + [dma((m,))] * 2
        + [dma((3 * m,))],
        compiler_params=pltpu.CompilerParams(
            collective_id=ident, has_side_effects=True, vmem_limit_bytes=60 * 2**20
        ),
        cost_estimate=pl.CostEstimate(flops=0, bytes_accessed=200 * 2**20, transcendentals=0),
        name=f"leave_{ident}",
    )(d3, qkv, term, gains, grad_hidden)


class Moves:
    def __init__(self, sems):
        self.sems, self.count, self.open = sems, 0, []

    def start(self, src, dst):
        copy = pltpu.make_async_copy(src, dst, self.sems.at[self.count])
        self.count += 1
        copy.start()
        self.open.append(copy)
        return copy

    def finish(self):
        for copy in self.open:
            copy.wait()
        self.open = []

    def wait(self, copies):
        for copy in copies:
            copy.wait()
        self.open = [copy for copy in self.open if all(copy is not other for other in copies)]


def gather_pairs(place, wires, own, out, ready, hook=lambda: None):
    p, pair = place, place.pair
    half = own.shape[0] // 2
    top, low = pl.ds(0, half), pl.ds(half, half)
    qs = [p.q] + ([1 - p.q] if pair > 1 else [])
    for t in range(pair):
        for kind in ["xa", "xb", "ya", "yb", "xd", "yd", "ca", "cb", "cxa", "cxb", "cya", "cyb", "cda", "cdb"]:
            wires.new((t, kind))
    if pair > 1:
        wires.new("za")
        wires.new("zb")
    live = {}

    def go(key, src, dst, device):
        live[key] = wires.go(key, src, dst, device)

    def arrived(*keys):
        for key in keys:
            live[key].wait_recv()

    def begin(t, src, tops):
        q = qs[t]
        rows = top if tops else low
        go((t, "xa" if tops else "xb"), src.at[rows], out.at[q, p.s, rows], p.x)
        go((t, "ya" if tops else "yb"), src.at[rows], out.at[q, p.s, rows], p.y)
        go((t, "ca" if tops else "cb"), src.at[rows], out.at[q, p.s, rows], p.core)

    def pass_on(t, name, slot, rows, device):
        ref = out.at[qs[t], slot, rows]
        go((t, name), ref, ref, device)

    def first(t):
        arrived((t, "xa"))
        pass_on(t, "xd", p.sx, top, p.y)
        pass_on(t, "cxa", p.sx, top, p.core)
        arrived((t, "ya"))
        pass_on(t, "cya", p.sy, top, p.core)

    def second(t):
        arrived((t, "yb"))
        pass_on(t, "yd", p.sy, low, p.x)
        pass_on(t, "cyb", p.sy, low, p.core)
        arrived((t, "xb"))
        pass_on(t, "cxb", p.sx, low, p.core)

    def third(t):
        arrived((t, "xd"))
        pass_on(t, "cda", p.sd, top, p.core)
        arrived((t, "yd"))
        pass_on(t, "cdb", p.sd, low, p.core)

    def use(t, slot, *keys):
        arrived(*[(t, key) for key in keys])
        ready(qs[t], slot // 2)

    if pair > 1:
        go("za", own.at[top], out.at[qs[0], p.s, top], p.z)
        go("zb", own.at[low], out.at[qs[0], p.s, low], p.z)
    begin(0, own, True)
    begin(0, own, False)
    use(0, p.s, "ca", "cb")
    hook()
    first(0)
    if pair > 1:
        second(0)
        use(0, p.sx, "cxa", "cxb")
        arrived("za")
        begin(1, out.at[qs[1], p.s], True)
        use(0, p.sy, "cya", "cyb")
        third(0)
        hook()
        arrived("zb")
        begin(1, out.at[qs[1], p.s], False)
        use(0, p.sd, "cda", "cdb")
        first(1)
        use(1, p.s, "ca", "cb")
        second(1)
        hook()
        use(1, p.sx, "cxa", "cxb")
        use(1, p.sy, "cya", "cyb")
        third(1)
        use(1, p.sd, "cda", "cdb")
    else:
        hook()
        second(0)
        use(0, p.sx, "cxa", "cxb")
        use(0, p.sy, "cya", "cyb")
        hook()
        third(0)
        use(0, p.sd, "cda", "cdb")
    return live


def scatter_pairs(place, wires, value, rc, rd, rx, ry, qbuf, zbuf, make, result, hook=lambda: None):
    p, pair = place, place.pair
    rows, width = rx.shape[1], rx.shape[2]
    half, wide = rows // 2, width // 2
    top, low = pl.ds(0, half), pl.ds(half, half)
    slots = {"d": p.sd, "x": p.sx, "y": p.sy, "o": p.s}
    order = ["d", "x", "y", "o"]
    planes = [1 - p.q, p.q] if pair > 1 else [p.q]
    jobs = [(t, c) for t in range(pair) for c in range(2)]
    for job in jobs:
        for name in ["c" + k for k in order] + ["da", "db", "xa", "xb", "ya", "yb"]:
            wires.new((job, name))
    if pair > 1:
        wires.new("z0")
        wires.new("z1")
    live = {}

    def go(key, src, dst, device):
        live[key] = wires.go(key, src, dst, device)

    def arrived(*keys):
        for key in keys:
            live[key].wait_recv()

    def at(c):
        return pl.ds(c * wide, wide)

    def part(job, slot, rows_):
        return value.at[planes[job[0]], slot, rows_, at(job[1])]

    every = pl.ds(0, rows)

    def share(job, k):
        t, c = job
        make(planes[t], slots[k] // 2, c)
        go((job, "c" + k), part(job, flip(slots[k], 1), every), rc.at[t, order.index(k), :, at(c)], p.core)

    def begin(job):
        share(job, "d")
        share(job, "x")

    def rest(job):
        t, c = job
        arrived((job, "cd"))
        qbuf[t, 0, :, at(c)] = add(part(job, p.sd, every)[...], rc[t, 0, :, at(c)])
        go((job, "da"), qbuf.at[t, 0, top, at(c)], rd.at[t, top, at(c)], p.x)
        go((job, "db"), qbuf.at[t, 0, low, at(c)], rd.at[t, low, at(c)], p.y)
        share(job, "y")
        arrived((job, "cx"))
        qbuf[t, 1, top, at(c)] = add(part(job, p.sx, top)[...], rc[t, 1, top, at(c)])
        go((job, "xa"), qbuf.at[t, 1, top, at(c)], rx.at[t, top, at(c)], p.x)
        share(job, "o")
        arrived((job, "cy"))
        qbuf[t, 2, low, at(c)] = add(part(job, p.sy, low)[...], rc[t, 2, low, at(c)])
        go((job, "yb"), qbuf.at[t, 2, low, at(c)], ry.at[t, low, at(c)], p.y)

    def relay(job):
        t, c = job
        arrived((job, "db"))
        held = part(job, p.sx, low)[...].astype(F32) + rc[t, 1, low, at(c)].astype(F32)
        qbuf[t, 1, low, at(c)] = (held + rd[t, low, at(c)].astype(F32)).astype(BF16)
        go((job, "xb"), qbuf.at[t, 1, low, at(c)], rx.at[t, low, at(c)], p.x)
        arrived((job, "da"))
        held = part(job, p.sy, top)[...].astype(F32) + rc[t, 2, top, at(c)].astype(F32)
        qbuf[t, 2, top, at(c)] = (held + rd[t, top, at(c)].astype(F32)).astype(BF16)
        go((job, "ya"), qbuf.at[t, 2, top, at(c)], ry.at[t, top, at(c)], p.y)

    def total(job):
        t, c = job
        arrived((job, "co"), (job, "xa"), (job, "yb"), (job, "xb"), (job, "ya"))
        value_ = part(job, p.s, every)[...].astype(F32) + rc[t, 3, :, at(c)].astype(F32)
        value_ = value_ + rx[t, :, at(c)].astype(F32) + ry[t, :, at(c)].astype(F32)
        if pair > 1 and t == 0:
            zbuf[0, :, at(c)] = value_.astype(BF16)
            go(f"z{c}", zbuf.at[0, :, at(c)], zbuf.at[1, :, at(c)], p.z)
        else:
            result[:, at(c)] = value_

    begin(jobs[0])
    rest(jobs[0])
    for i, job in enumerate(jobs):
        after = jobs[i + 1] if i + 1 < len(jobs) else None
        if after:
            begin(after)
        hook()
        relay(job)
        if after:
            rest(after)
        hook()
        total(job)
    if pair > 1:
        for c in range(2):
            arrived(f"z{c}")
            result[:, at(c)] += zbuf[1, :, at(c)].astype(F32)
    return live


def rms_back(value, gain, grad):
    inverse = lax.rsqrt(jnp.mean(value * value, axis=-1, keepdims=True) + EPSILON)
    normal = value * inverse
    u = grad * gain
    return inverse * (u - normal * jnp.mean(u * normal, axis=-1, keepdims=True)), grad * normal


def up_kernel(
    pair, h, wg, wu, down_w, wd_far, hs, gate, up, inner, inner_t, wd, hs_v, w_v, g_v, u_v, i_v, t_v, send, recv, zsem, sems
):
    place = Place(pair)
    place.peers.append((place.s, flip(place.f, 1)))
    moves = Moves(sems)
    loads = [moves.start(wg, w_v.at[0]), moves.start(wu, w_v.at[1])]
    rows, width = h.shape
    block, share = 2 * rows, wg.shape[1]
    hs_v[place.q, place.s] = h[...]
    place.barrier()
    stream, view = Stream(place, zsem), half_rows(down_w, share)
    stream_copies = [
        stream.remote(0, 1, view(stream.half), wd.at[place.f], stream.near),
        stream.remote(0, 2, wd_far, wd.at[stream.far_f], stream.near),
    ]
    local = [
        pltpu.make_async_copy(view(stream.half), wd.at[place.f], zsem.at[0, 3, 0]),
        pltpu.make_async_copy(wd_far, wd.at[stream.far_f], zsem.at[0, 3, 1]),
    ]

    def pass_down():
        for copy in stream_copies + local:
            copy.start()
    n = hs.shape[1]
    step = min(256, share)
    waited = []

    def ready(q, chip):
        if not waited:
            moves.wait(loads)
            waited.append(True)
        slots = pl.ds(2 * chip, 2)
        moves.start(hs_v.at[q, slots], hs.at[q, slots])
        at = pl.multiple_of(q * n * rows + chip * block, block)
        here = pl.ds(at, block)

        @pl.loop(0, share // step)
        def _(j):
            cols = pl.ds(pl.multiple_of(j * step, step), step)
            a = hs_v[q, slots].reshape(block, width)
            g = dot(a, w_v[0, :, cols], NN)
            u = dot(a, w_v[1, :, cols], NN)
            g_v[here, cols] = g
            u_v[here, cols] = u
            value = (g * (1.0 / (1.0 + jnp.exp(-g))) * u)
            i_v[here, cols] = value.astype(BF16)
            t_v[cols, here] = value.T.astype(BF16)

        moves.start(g_v.at[here], gate.at[here])
        moves.start(u_v.at[here], up.at[here])
        moves.start(i_v.at[here], inner.at[here])

    live = gather_pairs(place, Wires(send, recv), h, hs_v, ready, Work([lambda: None, pass_down]))
    moves.start(t_v, inner_t)
    for copy in stream_copies + local:
        copy.wait()
    for copy in live.values():
        copy.wait_send()
    moves.finish()


def any_specs(count):
    return [pl.BlockSpec(memory_space=pl.ANY)] * count


def vmem_specs(count):
    return [pl.BlockSpec(memory_space=pltpu.VMEM)] * count


def kernel_params(ident, mib=60):
    return pltpu.CompilerParams(collective_id=ident, has_side_effects=True, vmem_limit_bytes=mib * 2**20)


def shape(dims, kind):
    return jax.ShapeDtypeStruct(dims, kind)


def ffn_up(h, wg, wu, down_w, wd_far, n, pair, ident):
    rows, width = h.shape
    share, long = wg.shape[1], pair * n * rows
    dma = pltpu.SemaphoreType.DMA
    outs = [
        shape((pair, n, rows, width), BF16),
        shape((long, share), F32),
        shape((long, share), F32),
        shape((long, share), BF16),
        shape((share, long), BF16),
        shape((width // down_w.shape[1], share, down_w.shape[1]), BF16),
    ]
    return pl.pallas_call(
        functools.partial(up_kernel, pair),
        in_specs=vmem_specs(1) + any_specs(4),
        out_specs=any_specs(6),
        out_shape=outs,
        scratch_shapes=[
            pltpu.VMEM((pair, n, rows, width), BF16),
            pltpu.VMEM((2, width, share), BF16),
            pltpu.VMEM((long, share), F32),
            pltpu.VMEM((long, share), F32),
            pltpu.VMEM((long, share), BF16),
            pltpu.VMEM((share, long), BF16),
            dma((gather_wires(pair),)),
            dma((gather_wires(pair),)),
            dma((1, 4, 2)),
            dma((3 + 4 * pair * n // 2,)),
        ],
        compiler_params=kernel_params(ident),
        cost_estimate=pl.CostEstimate(
            flops=4 * long * width * share, bytes_accessed=long * width * 40, transcendentals=0
        ),
        name=f"up_{ident}",
    )(h, wg, wu, down_w, wd_far)


def down_kernel(
    pair, inner, wd, hidden, gain, cotangent, layer_out, grad_low, gain_term, i_v, w_v, sum_v, value, rc, rd, rx, ry, qbuf, zbuf, send, recv, sems
):
    place = Place(pair)
    moves = Moves(sems)
    deep = wd.shape[2]
    for j in range(wd.shape[0]):
        moves.start(wd.at[j], w_v.at[:, pl.ds(j * deep, deep)])
    moves.start(inner, i_v)
    rows, width = hidden.shape
    block = 2 * rows
    n = value.shape[1]
    step = min(512, width)
    place.barrier()
    moves.finish()

    def make(q, chip, c):
        here = pl.ds(pl.multiple_of(q * n * rows + chip * block, block), block)

        @pl.loop(c * (width // 2) // step, (c + 1) * (width // 2) // step)
        def _(j):
            cols = pl.ds(pl.multiple_of(j * step, step), step)
            part = dot(i_v[here, :], w_v[:, cols], NN).astype(BF16)
            value[q, pl.ds(2 * chip, 2), :, cols] = part.reshape(2, rows, step)

    live = scatter_pairs(place, Wires(send, recv), value, rc, rd, rx, ry, qbuf, zbuf, make, sum_v)
    feed = sum_v[...]
    grad = cotangent[...].astype(F32)
    inverse = lax.rsqrt(jnp.mean(feed * feed, axis=-1, keepdims=True) + EPSILON)
    normal = feed * inverse
    layer_out[...] = (hidden[...] + normal * gain[...]).astype(BF16)
    u = grad * gain[...]
    grad_low[...] = (inverse * (u - normal * jnp.mean(u * normal, axis=-1, keepdims=True))).astype(BF16)
    gain_term[...] = jnp.sum(grad * normal, axis=0, keepdims=True)
    for copy in live.values():
        copy.wait_send()


def ffn_down(inner, wd, hidden, gain, cotangent, n, pair, ident):
    rows, width = hidden.shape
    dma = pltpu.SemaphoreType.DMA
    return pl.pallas_call(
        functools.partial(down_kernel, pair),
        in_specs=any_specs(2) + vmem_specs(3),
        out_specs=vmem_specs(3),
        out_shape=[shape((rows, width), BF16), shape((rows, width), BF16), shape((1, width), F32)],
        scratch_shapes=[
            pltpu.VMEM(inner.shape, BF16),
            pltpu.VMEM((wd.shape[1], width), BF16),
            pltpu.VMEM((rows, width), F32),
            pltpu.VMEM((pair, n, rows, width), BF16),
        ]
        + scatter_scratch(pair, rows, width)
        + [dma((1 + wd.shape[0],))],
        compiler_params=kernel_params(ident),
        cost_estimate=pl.CostEstimate(
            flops=2 * inner.shape[0] * inner.shape[1] * width, bytes_accessed=pair * n * rows * width * 40, transcendentals=0
        ),
        name=f"down_{ident}",
    )(inner, wd, hidden, gain.reshape(1, width), cotangent)


def grad_kernel(
    pair, g, wd, gate, up, inner_t, grad_gate, grad_up, gate_t, up_t, down_term,
    gs_v, w_v, g_v, u_v, gg_v, gu_v, gt_v, ut_v, it_v, acc, low_v, send, recv, sems
):
    place = Place(pair)
    moves = Moves(sems)
    deep = wd.shape[2]
    loads = [moves.start(wd.at[j], w_v.at[:, pl.ds(j * deep, deep)]) for j in range(wd.shape[0])]
    loads += [moves.start(gate, g_v), moves.start(up, u_v), moves.start(inner_t, it_v)]
    rows, width = g.shape
    block, share = 2 * rows, wd.shape[1]
    gs_v[place.q, place.s] = g[...]
    place.barrier()
    n = gs_v.shape[1]
    step = min(256, share)
    waited = []

    def ready(q, chip):
        new = not waited
        if new:
            moves.wait(loads)
            waited.append(True)
        slots = pl.ds(2 * chip, 2)
        here = pl.ds(pl.multiple_of(q * n * rows + chip * block, block), block)

        @pl.loop(0, share // step)
        def _(j):
            cols = pl.ds(pl.multiple_of(j * step, step), step)
            a = gs_v[q, slots].reshape(block, width)
            e = dot(a, w_v[cols, :], NT)
            v, u = g_v[here, cols], u_v[here, cols]
            s = 1.0 / (1.0 + jnp.exp(-v))
            dg = e * u * s * (1.0 + v * (1.0 - s))
            du = e * v * s
            gg_v[here, cols] = dg.astype(BF16)
            gu_v[here, cols] = du.astype(BF16)
            gt_v[cols, here] = dg.T.astype(BF16)
            ut_v[cols, here] = du.T.astype(BF16)

        wide = min(512, width)

        @pl.loop(0, width // wide)
        def _(j):
            cols = pl.ds(pl.multiple_of(j * wide, wide), wide)
            part = dot(it_v[:, here], gs_v[q, slots, :, cols].reshape(block, wide), NN)
            if new:
                acc[:, cols] = part
            else:
                acc[:, cols] += part

        moves.start(gg_v.at[here], grad_gate.at[here])
        moves.start(gu_v.at[here], grad_up.at[here])

    live = gather_pairs(place, Wires(send, recv), g, gs_v, ready)
    for j in range(down_term.shape[0]):
        low_v[j] = acc[:, pl.ds(j * deep, deep)].astype(BF16)
    moves.start(low_v, down_term)
    moves.start(gt_v, gate_t)
    moves.start(ut_v, up_t)
    for copy in live.values():
        copy.wait_send()
    moves.finish()


def ffn_grad(g, wd, gate, up, inner_t, n, pair, ident):
    rows, width = g.shape
    share, long = wd.shape[1], pair * n * rows
    dma = pltpu.SemaphoreType.DMA
    flat, tall = pltpu.VMEM((long, share), BF16), pltpu.VMEM((share, long), BF16)
    return pl.pallas_call(
        functools.partial(grad_kernel, pair),
        in_specs=vmem_specs(1) + any_specs(4),
        out_specs=any_specs(5),
        out_shape=[shape((long, share), BF16)] * 2
        + [shape((share, long), BF16)] * 2
        + [shape((wd.shape[0], share, wd.shape[2]), BF16)],
        scratch_shapes=[
            pltpu.VMEM((pair, n, rows, width), BF16),
            pltpu.VMEM((share, width), BF16),
            pltpu.VMEM((long, share), F32),
            pltpu.VMEM((long, share), F32),
            flat,
            flat,
            tall,
            tall,
            tall,
            pltpu.VMEM((share, width), F32),
            pltpu.VMEM((wd.shape[0], share, wd.shape[2]), BF16),
            dma((gather_wires(pair),)),
            dma((gather_wires(pair),)),
            dma((8 + wd.shape[0] + 3 * pair * n // 2,)),
        ],
        compiler_params=kernel_params(ident, 63),
        cost_estimate=pl.CostEstimate(
            flops=2 * long * width * share, bytes_accessed=long * width * 40, transcendentals=0
        ),
        name=f"grad_{ident}",
    )(g, wd, gate, up, inner_t)


def back_kernel(
    pair, gg, gu, wg, wu, gate_t, up_t, hs, down_term, branch, gain, cotangent,
    grad_hidden, grad_low, gain_term, down_grad, gate_term, up_term,
    a_v, w_v, value, rc, rd, rx, ry, qbuf, zbuf, send, recv,
    gt_v, ut_v, hs_v, gterm, uterm, down_own, down_near, down_total, down_from, dsem, sems
):
    place = Place(pair)
    place.peers.append((place.s, flip(place.f, 1)))
    moves = Moves(sems)
    loads = [moves.start(wg, w_v.at[0]), moves.start(wu, w_v.at[1])]
    loads += [moves.start(gg, a_v.at[0]), moves.start(gu, a_v.at[1])]
    late = [moves.start(gate_t, gt_v)] + [moves.start(hs.at[q], hs_v.at[q]) for q in range(pair)]
    late += [moves.start(up_t, ut_v)]
    down = Settle(place, dsem, down_term, down_own, down_near, down_total, down_from)
    pieces = term_work(gterm, gt_v, hs_v, lambda: moves.wait(late), gate_term, moves)
    pieces += term_work(uterm, ut_v, hs_v, lambda: None, up_term, moves)
    work = Work(pieces[:4] + [lambda: (pieces[4](), down.middle())] + pieces[5:])
    rows, width = branch.shape
    block = 2 * rows
    n = value.shape[1]
    step = min(256, width)
    place.barrier()
    down.start()
    moves.wait(loads)

    def make(q, chip, c):
        here = pl.ds(pl.multiple_of(q * n * rows + chip * block, block), block)

        @pl.loop(c * (width // 2) // step, (c + 1) * (width // 2) // step)
        def _(j):
            cols = pl.ds(pl.multiple_of(j * step, step), step)
            part = dot(a_v[0, here, :], w_v[0, cols, :], NT) + dot(a_v[1, here, :], w_v[1, cols, :], NT)
            value[q, pl.ds(2 * chip, 2), :, cols] = part.astype(BF16).reshape(2, rows, step)

    live = scatter_pairs(place, Wires(send, recv), value, rc, rd, rx, ry, qbuf, zbuf, make, grad_hidden, work)
    work.rest()
    grad = cotangent[...].astype(F32) + grad_hidden[...]
    grad_hidden[...] = grad
    back, term = rms_back(branch[...], gain[...], grad)
    grad_low[...] = back.astype(BF16)
    gain_term[...] = jnp.sum(term, axis=0, keepdims=True)
    share = down_grad.shape[0] // 2

    def store(u, value):
        down_grad[pl.ds(pl.multiple_of(u * share, share), share), :] = value

    down.finish(store)
    for copy in live.values():
        copy.wait_send()
    moves.finish()


def ffn_back(gg, gu, wg, wu, gate_t, up_t, hs, down_term, branch, gain, cotangent, n, m, pair, ident):
    rows, width = branch.shape
    share, deep = gate_t.shape[0], width // m
    term = down_term.shape
    dma = pltpu.SemaphoreType.DMA
    return pl.pallas_call(
        functools.partial(back_kernel, pair),
        in_specs=any_specs(8) + vmem_specs(3),
        out_specs=vmem_specs(4) + any_specs(2),
        out_shape=[
            shape((rows, width), F32),
            shape((rows, width), BF16),
            shape((1, width), F32),
            shape((2 * share, deep), F32),
            shape(term, BF16),
            shape(term, BF16),
        ],
        scratch_shapes=[
            pltpu.VMEM((2,) + gg.shape, BF16),
            pltpu.VMEM((2,) + wg.shape, BF16),
            pltpu.VMEM((pair, n, rows, width), BF16),
        ]
        + scatter_scratch(pair, rows, width)
        + [pltpu.VMEM(v.shape, BF16) for v in (gate_t, up_t, hs)]
        + [pltpu.VMEM(term, BF16)] * 2
        + settle_scratch(share, deep)
        + [dma((20,))],
        compiler_params=kernel_params(ident, 63),
        cost_estimate=pl.CostEstimate(
            flops=4 * gg.shape[0] * gg.shape[1] * width, bytes_accessed=pair * n * rows * width * 40, transcendentals=0
        ),
        name=f"back_{ident}",
    )(gg, gu, wg, wu, gate_t, up_t, hs, down_term, branch, gain.reshape(1, width), cotangent)


def opposite(f):
    return (f + 2) % 4


class Stream:
    def __init__(self, place, sems):
        self.place, self.sems = place, sems
        f = place.f
        self.half, self.far_f, self.near_f = f // 2, opposite(f), flip(f, 1)
        self.far, self.near = (place.s, self.far_f), (place.s, self.near_f)

    def remote(self, k, step, src, dst, device):
        return pltpu.make_async_remote_copy(
            src, dst, self.sems.at[k, step, 0], self.sems.at[k, step, 1], device_id=device, device_id_type=MESH
        )

    def far_copy(self, k, view, full):
        return self.remote(k, 0, view(1 - self.half), full.at[self.place.f], self.far)

    def near_copy(self, k, view, full):
        return self.remote(k, 1, view(self.half), full.at[self.place.f], self.near)

    def own_copy(self, k, view, full):
        return pltpu.make_async_copy(view(self.half), full.at[self.place.f], self.sems.at[k, 3, 0])

    def relay_copy(self, k, full):
        return self.remote(k, 2, full.at[self.far_f], full.at[self.far_f], self.near)

    def start_far(self, k, view, full):
        self.far_copy(k, view, full).start()

    def start_near(self, k, view, full):
        self.near_copy(k, view, full).start()
        self.own_copy(k, view, full).start()

    def relay(self, k, view, full):
        self.far_copy(k, view, full).wait_recv()
        self.relay_copy(k, full).start()

    def finish(self, k, view, full):
        self.near_copy(k, view, full).wait_recv()
        self.relay_copy(k, full).wait_recv()
        self.own_copy(k, view, full).wait()
        self.far_copy(k, view, full).wait_send()
        self.near_copy(k, view, full).wait_send()
        self.relay_copy(k, full).wait_send()


def half_columns(ref, share):
    return lambda u: ref.at[:, pl.ds(pl.multiple_of(u * share, share), share)]


def half_rows(ref, share):
    return lambda u: ref.at[pl.ds(pl.multiple_of(u * share, share), share), :]


def full_barrier(place, n, near):
    sem = pltpu.get_barrier_semaphore()
    s, f = place.s, place.f
    for d in range(1, n):
        pl.semaphore_signal(sem, inc=1, device_id=((s + d) % n, f), device_id_type=MESH)
    for other in near:
        pl.semaphore_signal(sem, inc=1, device_id=(s, other), device_id_type=MESH)
    pl.semaphore_wait(sem, n - 1 + len(near))


def swap_halves(v):
    return pltpu.roll(v, HD // 2, axis=1)


def to_rows(first, second):
    rows = first.shape[0]
    lane = lax.broadcasted_iota(jnp.int32, (rows, 128), 1)
    wide = jnp.where(lane == 0, first, jnp.where(lane == 1, second, 0.0))
    return wide.T[:8]


def to_columns(v):
    return jnp.concatenate([v, jnp.zeros((120, v.shape[1]), F32)], axis=0).T


def exchange(place, n, own, held, send, recv):
    copies = []
    for d in range(1, n):
        copy = pltpu.make_async_remote_copy(
            own,
            held.at[d - 1],
            send.at[d - 1],
            recv.at[d - 1],
            device_id=((place.s + d) % n, place.f),
            device_id_type=MESH,
        )
        copy.start()
        copies.append(copy)
    total = own[...]
    for d in range(1, n):
        copies[d - 1].wait_recv()
        total = total + held[d - 1]
    return total, copies


def attend(block, q_v, k_v, v_v, out_v, low_v, lt_v, log_v):
    length = q_v.shape[0]
    scale = HD ** (-0.5)

    @pl.loop(0, q_v.shape[1] // HD)
    def _(h):
        cols = pl.ds(pl.multiple_of(h * HD, HD), HD)
        for i in range(length // block):
            rows, wide = pl.ds(i * block, block), pl.ds(0, (i + 1) * block)
            s = dot(q_v[rows, cols], k_v[wide, cols], NT) * scale
            column = lax.broadcasted_iota(jnp.int32, s.shape, 1)
            row = lax.broadcasted_iota(jnp.int32, s.shape, 0) + i * block
            s = jnp.where(column <= row, s, -jnp.inf)
            top = jnp.max(s, axis=-1, keepdims=True)
            p = jnp.exp(s - top)
            total = jnp.sum(p, axis=-1, keepdims=True)
            out = dot((p * (1.0 / total)).astype(BF16), v_v[wide, cols], NN)
            out_v[rows, cols] = out
            low_v[rows, cols] = out.astype(BF16)
            lt_v[cols, rows] = out.T.astype(BF16)
            log_v[h, rows, :] = top + jnp.log(total)


def attention_kernel(
    x, gain, tables, branch_gain, xs, qkv, wo, gate_w, up_w, down_w,
    raw, heads, attended, low_t, xs_t, log_total, inverse, branch, hidden, hidden_low, wg, wu, wd_far,
    xs_v, xt_v, lt_v, w_v, wo_v, raw_v, heads_v, out_v, low_v, log_v, small, held, value,
    rc, rd, rx, ry, qbuf, zbuf, send, recv, ssend, srecv, zsem, sems,
):
    place = Place(1)
    n, m = xs.shape[1], qkv.shape[1]
    rows, width = x.shape
    length, cols = raw.shape[1], raw.shape[2]
    share = wg.shape[2]
    moves = Moves(sems)
    loads = [moves.start(xs.at[0], xs_v)]
    for j in range(3):
        for f in range(m):
            loads.append(moves.start(qkv.at[j, f], w_v.at[j, :, f]))
    late = [moves.start(wo, wo_v)]
    near = [opposite(place.f), flip(place.f, 1)]
    full_barrier(place, n, near)
    stream = Stream(place, zsem)
    views = [half_columns(gate_w, share), half_columns(up_w, share)]
    fulls = [wg, wu]
    for k in range(2):
        stream.start_far(k, views[k], fulls[k])
    for k in range(2):
        stream.start_near(k, views[k], fulls[k])
    down_far = stream.remote(2, 0, half_rows(down_w, share)(1 - stream.half), wd_far, stream.far)
    down_far.start()
    moves.wait(loads)
    block = min(256, length)
    per = block // rows

    @pl.loop(0, length // block)
    def _(i):
        here = pl.ds(pl.multiple_of(i * block, block), block)
        a = xs_v[pl.ds(i * per, per)].reshape(block, width)
        q = dot(a, w_v[0].reshape(width, cols), NN)
        k = dot(a, w_v[1].reshape(width, cols), NN)
        raw_v[0, here, :] = q
        raw_v[1, here, :] = k
        heads_v[2, here, :] = dot(a, w_v[2].reshape(width, cols), NN).astype(BF16)
        xt_v[:, here] = a.T
        small[0, :, here] = to_rows(
            jnp.sum(q * q, axis=1, keepdims=True), jnp.sum(k * k, axis=1, keepdims=True)
        )

    moves.start(raw_v, raw)
    moves.start(xt_v, xs_t)
    total, stat_copies = exchange(place, n, small.at[0], held, ssend, srecv)
    small[1] = lax.rsqrt(total * (1.0 / width) + EPSILON)
    moves.start(small.at[1], inverse)

    @pl.loop(0, length // block)
    def _(i):
        here = pl.ds(pl.multiple_of(i * block, block), block)
        inv = to_columns(small[1, :, here])
        cosine, sine = tables[0, here, :], tables[1, here, :]
        for j in range(2):
            for h in range(cols // HD):
                part = pl.ds(h * HD, HD)
                v = raw_v[j, here, part] * inv[:, j : j + 1] * gain[j, :, part]
                heads_v[j, here, part] = (v * cosine + swap_halves(v) * sine).astype(BF16)

    moves.start(heads_v, heads)
    attend(block, heads_v.at[0], heads_v.at[1], heads_v.at[2], out_v, low_v, lt_v, log_v)
    moves.start(out_v, attended)
    moves.start(lt_v, low_t)
    moves.start(log_v, log_total)
    moves.wait(late)
    step = min(512, width)

    def make(q, chip, c):
        here = pl.ds(pl.multiple_of(chip * 2 * rows, 2 * rows), 2 * rows)

        @pl.loop(c * (width // 2) // step, (c + 1) * (width // 2) // step)
        def _(j):
            at = pl.ds(pl.multiple_of(j * step, step), step)
            part = dot(low_v[here, :], wo_v[:, :, at].reshape(cols, step), NN).astype(BF16)
            value[q, pl.ds(2 * chip, 2), :, at] = part.reshape(2, rows, step)

    live = scatter_pairs(
        place, Wires(send, recv), value, rc, rd, rx, ry, qbuf, zbuf, make, branch,
        Work([lambda: None, lambda: stream.relay(0, views[0], fulls[0])]),
    )
    total = branch[...]
    inv = lax.rsqrt(jnp.mean(total * total, axis=-1, keepdims=True) + EPSILON)
    h = x[...].astype(F32) + total * inv * branch_gain[...]
    hidden[...] = h
    hidden_low[...] = h.astype(BF16)
    stream.relay(1, views[1], fulls[1])
    for copy in list(live.values()) + stat_copies:
        copy.wait_send()
    moves.finish()
    for k in range(2):
        stream.finish(k, views[k], fulls[k])
    down_far.wait()


def attention_half(x, gain, tables, branch_gain, xs, qkv, wo, gate_w, up_w, down_w, ident):
    rows, width = x.shape
    n, m, part, cols = xs.shape[1], qkv.shape[1], qkv.shape[3], qkv.shape[4]
    length, share = n * rows, gate_w.shape[1] // 2
    dma = pltpu.SemaphoreType.DMA
    heads = cols // HD
    outs = [
        shape((2, length, cols), F32),
        shape((3, length, cols), BF16),
        shape((length, cols), F32),
        shape((cols, length), BF16),
        shape((width, length), BF16),
        shape((heads, length, 1), F32),
        shape((8, length), F32),
        shape((rows, width), F32),
        shape((rows, width), F32),
        shape((rows, width), BF16),
        shape((m,) + (gate_w.shape[0], share), BF16),
        shape((m,) + (gate_w.shape[0], share), BF16),
        shape((share, down_w.shape[1]), BF16),
    ]
    return pl.pallas_call(
        attention_kernel,
        in_specs=vmem_specs(4) + any_specs(6),
        out_specs=any_specs(7) + vmem_specs(3) + any_specs(3),
        out_shape=outs,
        scratch_shapes=[
            pltpu.VMEM((n, rows, width), BF16),
            pltpu.VMEM((width, length), BF16),
            pltpu.VMEM((cols, length), BF16),
            pltpu.VMEM((3, n, m, part, cols), BF16),
            pltpu.VMEM(wo.shape, BF16),
            pltpu.VMEM((2, length, cols), F32),
            pltpu.VMEM((3, length, cols), BF16),
            pltpu.VMEM((length, cols), F32),
            pltpu.VMEM((length, cols), BF16),
            pltpu.VMEM((heads, length, 1), F32),
            pltpu.VMEM((2, 8, length), F32),
            pltpu.VMEM((n - 1, 8, length), F32),
            pltpu.VMEM((1, n, rows, width), BF16),
        ]
        + scatter_scratch(1, rows, width)
        + [dma((n - 1,)), dma((n - 1,)), dma((3, 4, 2)), dma((20 + 3 * m,))],
        compiler_params=kernel_params(ident),
        cost_estimate=pl.CostEstimate(flops=10**10, bytes_accessed=200 * 2**20, transcendentals=0),
        name=f"attention_{ident}",
    )(x, gain, tables, branch_gain, xs, qkv, wo, gate_w, up_w, down_w)


class Settle:
    def __init__(self, place, sems, term, own, near, total, far):
        self.place, self.sems, self.term, self.own = place, sems, term, own
        self.near, self.total, self.far = near, total, far
        f = place.f
        self.f = f
        self.odd, self.half = f % 2, f // 2

    def remote(self, step, src, dst, plane):
        return pltpu.make_async_remote_copy(
            src, dst, self.sems.at[step, 0], self.sems.at[step, 1], device_id=(self.place.s, plane), device_id_type=MESH
        )

    def given(self, i):
        return 1 - self.odd + 2 * i

    def kept(self, i):
        return self.odd + 2 * i

    def near_copy(self, i):
        return self.remote(i, self.term.at[self.given(i)], self.near.at[i], flip(self.f, 1))

    def far_copy(self):
        return self.remote(2, self.total.at[0], self.far, opposite(self.f))

    def load(self, i):
        return pltpu.make_async_copy(self.term.at[self.kept(i)], self.own.at[i], self.sems.at[3, i])

    def start(self):
        for i in (0, 1):
            self.near_copy(i).start()
            self.load(i).start()

    def middle(self):
        for i in (0, 1):
            self.load(i).wait()
            self.near_copy(i).wait_recv()
        other = 1 - self.half
        self.total[0] = add(self.own[other], self.near[other])
        self.far_copy().start()

    def finish(self, store):
        half = self.half
        store(half, self.own[half].astype(F32) + self.near[half].astype(F32))
        self.far_copy().wait_recv()
        store(1 - half, self.far[...].astype(F32))
        for i in (0, 1):
            self.near_copy(i).wait_send()
        self.far_copy().wait_send()


def settle_scratch(share, depth):
    block = lambda *lead: pltpu.VMEM(lead + (share, depth), BF16)
    return [block(2), block(2), block(1), block(), pltpu.SemaphoreType.DMA((4, 2))]


def term_block(term, left, right, block):
    deep, long = term.shape[2], left.shape[1]
    step = min(256, deep)

    @pl.loop(0, deep // step)
    def _(j):
        at = pl.ds(pl.multiple_of(block * deep + j * step, step), step)
        to = pl.ds(pl.multiple_of(j * step, step), step)
        term[block, :, to] = dot(left[...], right[:, :, :, at].reshape(long, step), NN).astype(BF16)


class Work:
    def __init__(self, pieces):
        self.pieces = list(pieces)

    def __call__(self):
        if self.pieces:
            self.pieces.pop(0)()

    def rest(self):
        while self.pieces:
            self()


def term_work(term, left, right, prepare, out, moves):
    def piece(block):
        def run():
            if block == 0:
                prepare()
            term_block(term, left, right, block)
            moves.start(term.at[block], out.at[block])

        return run

    return [piece(block) for block in range(term.shape[0])]


def turn(v, cosine, sine):
    return v * cosine + swap_halves(v) * sine


def attend_back(block, q_v, k_v, v_v, out_v, log_v, g_v, dq, dk, dv):
    length = q_v.shape[0]
    scale = HD ** (-0.5)
    dk[...] = jnp.zeros_like(dk)
    dv[...] = jnp.zeros_like(dv)

    @pl.loop(0, q_v.shape[1] // HD)
    def _(h):
        cols = pl.ds(pl.multiple_of(h * HD, HD), HD)
        for i in range(length // block):
            rows, wide = pl.ds(i * block, block), pl.ds(0, (i + 1) * block)
            q, g = q_v[rows, cols], g_v[rows, cols]
            s = dot(q, k_v[wide, cols], NT) * scale
            column = lax.broadcasted_iota(jnp.int32, s.shape, 1)
            row = lax.broadcasted_iota(jnp.int32, s.shape, 0) + i * block
            s = jnp.where(column <= row, s, -jnp.inf)
            weights = jnp.exp(s - log_v[h, rows, :])
            correction = jnp.sum(g.astype(F32) * out_v[rows, cols], axis=-1, keepdims=True)
            gw = dot(g, v_v[wide, cols], NT)
            gs = (weights * (gw - correction)).astype(BF16)
            dq[rows, cols] = dot(gs, k_v[wide, cols], NN) * scale
            dk[wide, cols] += dot(gs, q, TN) * scale
            dv[wide, cols] += dot(weights.astype(BF16), g, TN)


def attention_back_kernel(
    g, gain, tables, inverse, wo, raw, heads, attended, low_t, log_total, xs_t, gate_term, up_term,
    d3, term, out_term, gain_term, gate_grad, up_grad,
    bs, wo_v, raw_v, heads_v, out_v, low_v, log_v, ga_v, dq, dk, dv, d_v, xs_v, term_v, ot_v, small, held,
    gown, gnear, gtotal, gfar, gsem, uown, unear, utotal, ufar, usem,
    send, recv, ssend, srecv, sems,
):
    place = Place(1)
    n, m = bs.shape[1], wo.shape[0]
    rows, width = g.shape
    length, cols = raw.shape[1], raw.shape[2]
    share = gate_term.shape[1]
    moves = Moves(sems)
    second = [moves.start(wo, wo_v)]
    fourth = [
        moves.start(heads, heads_v),
        moves.start(attended, out_v),
        moves.start(log_total, log_v),
        moves.start(low_t, low_v),
        moves.start(raw, raw_v),
        moves.start(xs_t, xs_v),
    ]
    bs[0, place.s] = g[...]
    full_barrier(place, n, [opposite(place.f), flip(place.f, 1)])
    gate = Settle(place, gsem, gate_term, gown, gnear, gtotal, gfar)
    up = Settle(place, usem, up_term, uown, unear, utotal, ufar)
    gate.start()
    up.start()
    block = min(256, length)
    waited = []

    def ready(q, chip):
        if not waited:
            moves.wait(second)
            waited.append(True)
        here = pl.ds(pl.multiple_of(chip * 2 * rows, 2 * rows), 2 * rows)
        a = bs[0, pl.ds(2 * chip, 2)].reshape(2 * rows, width)
        ga_v[here, :] = dot(a, wo_v[...].reshape(cols, width), NT).astype(BF16)

    live = gather_pairs(place, Wires(send, recv), g, bs, ready)
    moves.wait(fourth)
    attend_back(block, heads_v.at[0], heads_v.at[1], heads_v.at[2], out_v, log_v, ga_v, dq, dk, dv)
    gate.middle()

    @pl.loop(0, length // block)
    def _(i):
        here = pl.ds(pl.multiple_of(i * block, block), block)
        inv = to_columns(inverse[:, here])
        cosine, sine = tables[0, here, :], -tables[1, here, :]
        sums = []
        for j, d in enumerate((dq, dk)):
            total = jnp.zeros((block, 1), F32)
            for h in range(cols // HD):
                part = pl.ds(h * HD, HD)
                normal = raw_v[j, here, part] * inv[:, j : j + 1]
                v = turn(d[here, part].astype(BF16).astype(F32), cosine, sine)
                raw_v[j, here, part] = normal
                gained = v * gain[j, :, part]
                total = total + jnp.sum(gained * normal, axis=1, keepdims=True)
                term_sum = jnp.sum(v * normal, axis=0, keepdims=True)
                d[here, part] = gained

                @pl.when(i == 0)
                def _():
                    gain_term[j, :, part] = term_sum

                @pl.when(i > 0)
                def _():
                    gain_term[j, :, part] += term_sum

            sums.append(total)
        small[0, :, here] = to_rows(sums[0], sums[1])
        d_v[2, here, :] = dv[here, :].astype(BF16)

    total, stat_copies = exchange(place, n, small.at[0], held, ssend, srecv)
    small[1] = total * (1.0 / width)

    @pl.loop(0, length // block)
    def _(i):
        here = pl.ds(pl.multiple_of(i * block, block), block)
        inv = to_columns(inverse[:, here])
        mean = to_columns(small[1, :, here])
        for j, d in enumerate((dq, dk)):
            d_v[j, here, :] = (
                inv[:, j : j + 1] * (d[here, :] - raw_v[j, here, :] * mean[:, j : j + 1])
            ).astype(BF16)

    moves.start(d_v, d3)
    up.middle()
    step = min(512, width)

    @pl.loop(0, width // step)
    def _(i):
        at = pl.ds(pl.multiple_of(i * step, step), step)
        ot_v[:, at] = dot(low_v[...], bs[0, :, :, at].reshape(length, step), NN).astype(BF16)
        for j in range(3):
            term_v[j, at, :] = dot(xs_v[at, :], d_v[j], NN).astype(BF16)

    moves.start(ot_v, out_term)
    moves.start(term_v, term)

    def store(ref):
        def put(u, value):
            ref[:, pl.ds(pl.multiple_of(u * share, share), share)] = value.T

        return put

    gate.finish(store(gate_grad))
    up.finish(store(up_grad))
    for copy in list(live.values()) + stat_copies:
        copy.wait_send()
    moves.finish()


def attention_back(g, gain, tables, inverse, wo, raw, heads, attended, low_t, log_total, xs_t, gate_term, up_term, n, ident):
    rows, width = g.shape
    m = wo.shape[0]
    length, cols = raw.shape[1], raw.shape[2]
    share, deep = gate_term.shape[1], width // m
    dma = pltpu.SemaphoreType.DMA
    vmem = pltpu.VMEM
    outs = [
        shape((3, length, cols), BF16),
        shape((3, width, cols), BF16),
        shape((cols, width), BF16),
        shape((2, 1, cols), F32),
        shape((deep, 2 * share), F32),
        shape((deep, 2 * share), F32),
    ]
    return pl.pallas_call(
        attention_back_kernel,
        in_specs=vmem_specs(4) + any_specs(9),
        out_specs=any_specs(3) + vmem_specs(3),
        out_shape=outs,
        scratch_shapes=[
            vmem((1, n, rows, width), BF16),
            vmem(wo.shape, BF16),
            vmem(raw.shape, F32),
            vmem(heads.shape, BF16),
            vmem(attended.shape, F32),
            vmem(low_t.shape, BF16),
            vmem(log_total.shape, F32),
            vmem((length, cols), BF16),
            vmem((length, cols), F32),
            vmem((length, cols), F32),
            vmem((length, cols), F32),
            vmem((3, length, cols), BF16),
            vmem(xs_t.shape, BF16),
            vmem((3, width, cols), BF16),
            vmem((cols, width), BF16),
            vmem((2, 8, length), F32),
            vmem((n - 1, 8, length), F32),
        ]
        + settle_scratch(share, deep) * 2
        + [
            dma((gather_wires(1),)),
            dma((gather_wires(1),)),
            dma((n - 1,)),
            dma((n - 1,)),
            dma((20,)),
        ],
        compiler_params=kernel_params(ident, 63),
        cost_estimate=pl.CostEstimate(flops=10**10, bytes_accessed=200 * 2**20, transcendentals=0),
        name=f"attention_back_{ident}",
    )(g, gain, tables, inverse, wo, raw, heads, attended, low_t, log_total, xs_t, gate_term, up_term)


def attention_forward_kernel(block, q_ref, k_ref, v_ref, out_ref, low_ref, log_ref):
    length = q_ref.shape[0]
    scale = HD ** (-0.5)
    for i in range(length // block):
        rows = pl.ds(i * block, block)
        width = (i + 1) * block
        s = dot(q_ref[rows, :], k_ref[pl.ds(0, width), :], NT) * scale
        column = lax.broadcasted_iota(jnp.int32, (block, width), 1)
        row = lax.broadcasted_iota(jnp.int32, (block, width), 0) + i * block
        s = jnp.where(column <= row, s, -jnp.inf)
        top = jnp.max(s, axis=-1, keepdims=True)
        p = jnp.exp(s - top)
        total = jnp.sum(p, axis=-1, keepdims=True)
        weights = (p * (1.0 / total)).astype(BF16)
        out = dot(weights, v_ref[pl.ds(0, width), :], NN)
        out_ref[rows, :] = out
        low_ref[rows, :] = out.astype(BF16)
        log_ref[0, rows, :] = top + jnp.log(total)


def attention_forward(q, k, v):
    length, width = q.shape
    heads = width // HD
    block = min(256, length)
    column = pl.BlockSpec((length, HD), lambda h: (0, h))
    return pl.pallas_call(
        functools.partial(attention_forward_kernel, block),
        grid=(heads,),
        in_specs=[column] * 3,
        out_specs=[column, column, pl.BlockSpec((1, length, 1), lambda h: (h, 0, 0))],
        out_shape=[
            jax.ShapeDtypeStruct((length, width), F32),
            jax.ShapeDtypeStruct((length, width), BF16),
            jax.ShapeDtypeStruct((heads, length, 1), F32),
        ],
        cost_estimate=pl.CostEstimate(
            flops=2 * heads * length * length * HD, bytes_accessed=10 * length * width, transcendentals=0
        ),
    )(q, k, v)


def attention_backward_kernel(block, q_ref, k_ref, v_ref, out_ref, log_ref, g_ref, dq_ref, dk_ref, dv_ref, dk, dv):
    length = q_ref.shape[0]
    scale = HD ** (-0.5)
    dk[...] = jnp.zeros_like(dk)
    dv[...] = jnp.zeros_like(dv)
    for i in range(length // block):
        rows = pl.ds(i * block, block)
        width = (i + 1) * block
        wide = pl.ds(0, width)
        q = q_ref[rows, :]
        g = g_ref[rows, :]
        s = dot(q, k_ref[wide, :], NT) * scale
        column = lax.broadcasted_iota(jnp.int32, (block, width), 1)
        row = lax.broadcasted_iota(jnp.int32, (block, width), 0) + i * block
        s = jnp.where(column <= row, s, -jnp.inf)
        weights = jnp.exp(s - log_ref[0, rows, :])
        correction = jnp.sum(g.astype(F32) * out_ref[rows, :], axis=-1, keepdims=True)
        gw = dot(g, v_ref[wide, :], NT)
        gs = (weights * (gw - correction)).astype(BF16)
        dq_ref[rows, :] = (dot(gs, k_ref[wide, :], NN) * scale).astype(BF16)
        dk[wide, :] += dot(gs, q, TN)
        dv[wide, :] += dot(weights.astype(BF16), g, TN)
    dk_ref[...] = (dk[...] * scale).astype(BF16)
    dv_ref[...] = dv[...].astype(BF16)


def attention_backward(q, k, v, out, log_total, g):
    length, width = q.shape
    heads = width // HD
    block = min(256, length)
    column = pl.BlockSpec((length, HD), lambda h: (0, h))
    return pl.pallas_call(
        functools.partial(attention_backward_kernel, block),
        grid=(heads,),
        in_specs=[column] * 4 + [pl.BlockSpec((1, length, 1), lambda h: (h, 0, 0)), column],
        out_specs=[column] * 3,
        out_shape=[jax.ShapeDtypeStruct((length, width), BF16)] * 3,
        scratch_shapes=[pltpu.VMEM((length, HD), F32)] * 2,
        cost_estimate=pl.CostEstimate(
            flops=5 * heads * length * length * HD, bytes_accessed=16 * length * width, transcendentals=0
        ),
    )(q, k, v, out, log_total, g)


def on_device(n, m, pair, *args):
    (
        tokens,
        query_weight,
        key_weight,
        value_weight,
        out_weight,
        query_gain,
        key_gain,
        attention_gain,
        gate_weight,
        up_weight,
        down_weight,
        feedforward_gain,
        cotangent,
    ) = args
    rows, width = tokens.shape[1], tokens.shape[2]
    length = rows * n
    part = query_weight.shape[0]
    cols = width // n
    depth, units = gate_weight.shape
    share = units // pair
    x = tokens.reshape(rows, width)
    groups = [[g * pair + u for u in range(pair)] for g in range(m // pair)]

    native = n == 8 and m == 4

    def gather_plane(v, ident):
        if native:
            return plane_gather(v, n, 1, ident)
        return lax.all_gather(v, "seq", axis=0, tiled=True)

    def scatter_plane(v, ident):
        if native:
            return plane_scatter(v, n, 1, ident)
        return lax.psum_scatter(v.astype(BF16), "seq", scatter_dimension=0, tiled=True).astype(F32)

    def gather_pair(v, ident):
        if native:
            return plane_gather(v, n, pair, ident)
        if pair > 1:
            v = lax.all_gather(v, "fsdp", axis=0, axis_index_groups=groups)
        v = lax.all_gather(v.reshape(pair, rows, width), "seq", axis=1, tiled=True)
        return v.reshape(pair * length, width)

    def scatter_pair(v, ident):
        if native:
            return plane_scatter(v, n, pair, ident)
        v = lax.psum_scatter(v.astype(BF16).reshape(pair, length, width), "seq", scatter_dimension=1, tiled=True)
        if pair > 1:
            v = lax.psum_scatter(v, "fsdp", scatter_dimension=0, axis_index_groups=groups)
        return v.reshape(rows, width).astype(F32)

    def total_plane(v, ident):
        return plane_sum(v, n, ident) if native else lax.psum(v, "seq")

    def spread(halves):
        return lax.all_to_all(jnp.tile(halves, (m // pair, 1, 1)), "fsdp", 0, 0, tiled=False)

    def settle(blocks):
        back = lax.all_to_all(blocks.astype(BF16), "fsdp", 0, 0, tiled=False)
        if native:
            return jnp.sum(back.reshape((pair, m // pair) + back.shape[1:]).astype(F32), axis=1)
        return jnp.sum(back.reshape((m // pair, pair) + back.shape[1:]).astype(F32), axis=0)

    gains = jnp.stack([query_gain, key_gain, attention_gain, feedforward_gain]).astype(F32)
    seq = lax.axis_index("seq")
    cosine, sine = angles_of(length)
    grad_out = cotangent.reshape(rows, width)
    if native:
        xs, qkv, out_rows, full = entry(
            x, query_weight, key_weight, value_weight, out_weight, jnp.pad(gains, ((0, 4), (0, 128 - part))), n, m, 1
        )
        full_gain = full[:, :, :4, :part].transpose(2, 1, 0, 3).reshape(4, width)
    else:
        stacked = jnp.stack([query_weight, key_weight, value_weight]).reshape(3, part, n, cols)
        mine = lax.all_to_all(stacked.transpose(2, 0, 1, 3), "seq", 0, 0)
        qkv = lax.all_gather(mine, "fsdp", axis=1).transpose(2, 0, 1, 3, 4).reshape(3, width, cols)
        full_gain = lax.all_gather(gains, ("seq", "fsdp"), axis=1).reshape(4, width)
        xs = gather_plane(x, 1)
        out_rows = lax.all_gather(out_weight, "fsdp", axis=0, tiled=True)
    own_gain = lax.dynamic_slice_in_dim(full_gain[:2], seq * cols, cols, 1)
    q_gain, k_gain, branch_gain, feed_gain = own_gain[0], own_gain[1], full_gain[2], full_gain[3]

    if native:
        tables = jnp.stack([jnp.tile(cosine, (1, 2)), jnp.concatenate([-sine, sine], axis=1)])
        raw, heads, attended, low_t, xs_t, log_total, inverse, branch, hidden, hidden_low, gate_cols, up_cols, down_far = (
            attention_half(
                x, own_gain[:, None, :], tables, branch_gain[None, :], xs, qkv, out_rows, gate_weight, up_weight,
                down_weight, 3
            )
        )
        gate_cols, up_cols = gate_cols.reshape(width, share), up_cols.reshape(width, share)
        hs, gate, up, inner, inner_t, down_rows = ffn_up(hidden_low, gate_cols, up_cols, down_weight, down_far, n, pair, 5)
        layer_out, grad_low, feed_gain_term = ffn_down(inner, down_rows, hidden, feed_gain, grad_out, n, pair, 7)
        grad_gate, grad_up, gate_t, up_t, down_term = ffn_grad(grad_low, down_rows, gate, up, inner_t, n, pair, 6)
        grad_hidden, branch_low, branch_gain_term, down_grad, gate_term, up_term = ffn_back(
            grad_gate, grad_up, gate_cols, up_cols, gate_t, up_t, hs, down_term, branch, branch_gain, grad_out, n, m, pair, 8
        )
        d3, term, out_term, gain_own, gate_grad, up_grad = attention_back(
            branch_low, own_gain[:, None, :], tables, inverse, out_rows, raw, heads, attended, low_t, log_total,
            xs_t, gate_term, up_term, n, 2
        )
        gain_own = lax.dynamic_update_slice(jnp.zeros((2, width), F32), gain_own[:, 0], (0, seq * cols))
        gain_terms = jnp.concatenate([gain_own, branch_gain_term, feed_gain_term]).reshape(4, n, m, part)
        gain_terms = jnp.pad(gain_terms.transpose(1, 2, 0, 3), ((0, 0), (0, 0), (0, 4), (0, 128 - part)))
        out_term = out_term.reshape(m, part, n, cols).transpose(2, 0, 1, 3)
        term = jnp.concatenate([term.reshape(3, n, m, part, cols), out_term[None]])
        tokens_grad, term, gain_grads = leave(d3, qkv, term, gain_terms, grad_hidden, n, m, 4)
        term = term.transpose(0, 2, 1, 3).reshape(4, part, width)
        out_grad = term[3]
        gain_grads = gain_grads[:4, :part]
    else:
        q_raw, k_raw, v = dot(xs, qkv[0], NN), dot(xs, qkv[1], NN), dot(xs, qkv[2], NN).astype(BF16)
        squares = jnp.stack([jnp.sum(q_raw * q_raw, axis=1), jnp.sum(k_raw * k_raw, axis=1)])
        inverse = lax.rsqrt(lax.psum(squares, "seq") / width + EPSILON)
        q_inv, k_inv = inverse[0][:, None], inverse[1][:, None]
        q = rotate(q_raw * q_inv * q_gain, cosine, sine, 1.0).astype(BF16)
        k = rotate(k_raw * k_inv * k_gain, cosine, sine, 1.0).astype(BF16)
        attended, attended_low, log_total = attention_forward(q, k, v)
        branch = scatter_plane(dot(attended_low, out_rows, NN), 3)
        branch_inv = lax.rsqrt(jnp.mean(branch * branch, axis=1, keepdims=True) + EPSILON)
        hidden = x.astype(F32) + branch * branch_inv * branch_gain
        hidden_low = hidden.astype(BF16)
        gate_cols = spread(gate_weight.reshape(depth, pair, share).transpose(1, 0, 2)).reshape(width, share)
        up_cols = spread(up_weight.reshape(depth, pair, share).transpose(1, 0, 2)).reshape(width, share)
        down_rows = spread(down_weight.reshape(pair, share, depth)).transpose(1, 0, 2).reshape(share, width)
        grad_out = grad_out.astype(F32)
        hs = gather_pair(hidden_low, 5)
        gate = dot(hs, gate_cols, NN)
        up = dot(hs, up_cols, NN)
        sig = jax.nn.sigmoid(gate)
        inner = (gate * sig * up).astype(BF16)
        feed = scatter_pair(dot(inner, down_rows, NN), 7)
        feed_inv = lax.rsqrt(jnp.mean(feed * feed, axis=1, keepdims=True) + EPSILON)
        layer_out = (hidden + feed * feed_inv * feed_gain).astype(BF16)
        grad_feed, term = rms_back(feed, feed_gain, grad_out)
        feed_gain_term = jnp.sum(term, axis=0)
        gs = gather_pair(grad_feed.astype(BF16), 6)
        grad_inner = dot(gs, down_rows, NT)
        grad_gate = (grad_inner * up * sig * (1.0 + gate * (1.0 - sig))).astype(BF16)
        grad_up = (grad_inner * gate * sig).astype(BF16)
        grad_hidden = grad_out + scatter_pair(dot(grad_gate, gate_cols, NT) + dot(grad_up, up_cols, NT), 8)
        grad_branch, term = rms_back(branch, branch_gain, grad_hidden)
        branch_low = grad_branch.astype(BF16)
        branch_gain_term = jnp.sum(term, axis=0)
        inner_t, gate_t, up_t = inner.T, grad_gate.T, grad_up.T

        def cut(v):
            return v.reshape(share, m, depth).transpose(1, 0, 2)

        down_grad = settle(cut(dot(inner_t, gs, NN))).reshape(units, depth)
        gate_grad = settle(cut(dot(gate_t, hs, NN))).transpose(2, 0, 1).reshape(depth, units)
        up_grad = settle(cut(dot(up_t, hs, NN))).transpose(2, 0, 1).reshape(depth, units)
        bs = gather_plane(branch_low, 2)
        out_grad = lax.psum_scatter(
            dot(attended_low, bs, TN).astype(BF16), "fsdp", scatter_dimension=0, tiled=True
        ).astype(F32)
        grad_attended = dot(bs, out_rows, NT).astype(BF16)
        dq, dk, dv = attention_backward(q, k, v, attended, log_total, grad_attended)
        dq = rotate(dq.astype(F32), cosine, sine, -1.0)
        dk = rotate(dk.astype(F32), cosine, sine, -1.0)
        q_normal, k_normal = q_raw * q_inv, k_raw * k_inv
        q_gain_term = jnp.sum(dq * q_normal, axis=0)
        k_gain_term = jnp.sum(dk * k_normal, axis=0)
        dq, dk = dq * q_gain, dk * k_gain
        means = total_plane(jnp.stack([jnp.sum(dq * q_normal, axis=1), jnp.sum(dk * k_normal, axis=1)]), 10) / width
        dq = (q_inv * (dq - q_normal * means[0][:, None])).astype(BF16)
        dk = (k_inv * (dk - k_normal * means[1][:, None])).astype(BF16)
        value = dot(dq, qkv[0], NT) + dot(dk, qkv[1], NT) + dot(dv, qkv[2], NT)
        term = jnp.stack([dot(xs, d, TN).astype(BF16) for d in (dq, dk, dv)]).reshape(3, n, m, part, cols)
        gain_own = jnp.stack([q_gain_term, k_gain_term])
        gain_own = lax.dynamic_update_slice(jnp.zeros((2, width), F32), gain_own, (0, seq * cols))
        gain_terms = jnp.concatenate([gain_own, jnp.stack([branch_gain_term, feed_gain_term])]).reshape(4, n, m, part)
        tokens_grad = grad_hidden + scatter_plane(value, 4)
        term = lax.psum_scatter(term, "fsdp", scatter_dimension=2)
        term = lax.all_to_all(term, "seq", 1, 1).astype(F32).transpose(0, 2, 1, 3)
        gain_grads = lax.psum_scatter(
            gain_terms.reshape(4, width), ("seq", "fsdp"), scatter_dimension=1, tiled=True
        )
        term = term.reshape(3, part, width)

    return (
        layer_out.reshape(tokens.shape),
        tokens_grad.reshape(tokens.shape),
        term[0],
        term[1],
        term[2],
        out_grad,
        gain_grads[0],
        gain_grads[1],
        gain_grads[2],
        gate_grad,
        up_grad,
        down_grad,
        gain_grads[3],
    )


def solution(mesh):
    n, m = mesh.shape["seq"], mesh.shape["fsdp"]
    tall, flat, act = P(("seq", "fsdp"), None), P(("seq", "fsdp")), P("fsdp", "seq", None)
    wide, deep = P("fsdp", "seq"), P("seq", "fsdp")
    return jax.shard_map(
        functools.partial(on_device, n, m, 2),
        mesh=mesh,
        in_specs=(act, tall, tall, tall, tall, flat, flat, flat, wide, wide, deep, flat, act),
        out_specs=(act, act, tall, tall, tall, tall, flat, flat, flat, wide, wide, deep, flat),
        check_vma=False,
    )
```

```python
import functools
import math

import jax
import jax.numpy as jnp
from jax import lax
from jax.experimental import pallas as pl
from jax.experimental.pallas import tpu as pltpu
from jax.sharding import PartitionSpec as P

EPSILON = 1e-06
THETA = 500000.0
HD = 128
F32 = jnp.float32
BF16 = jnp.bfloat16


def dot(a, b, dims):
    return lax.dot_general(a, b, (dims, ((), ())), preferred_element_type=F32)


NN = ((1,), (0,))
NT = ((1,), (1,))
TN = ((0,), (0,))


def angles_of(length):
    half = HD // 2
    frequency = jnp.exp(jnp.arange(half, dtype=F32) * (-2.0 * math.log(THETA) / HD))
    angle = jnp.arange(length, dtype=F32)[:, None] * frequency[None, :]
    return jnp.cos(angle), jnp.sin(angle)


def rotate(value, cosine, sine, sign):
    length, width = value.shape
    value = value.reshape(length, width // HD, 2, HD // 2)
    first, second = value[:, :, 0], value[:, :, 1]
    c, s = cosine[:, None, :], sign * sine[:, None, :]
    return jnp.stack([first * c - second * s, second * c + first * s], axis=2).reshape(length, width)


MESH = pl.DeviceIdType.MESH


def flip(index, bit):
    return index + bit - 2 * bit * ((index // bit) % 2)


class Place:
    def __init__(self, pair):
        self.s, self.f = lax.axis_index("seq"), lax.axis_index("fsdp")
        self.pair = pair
        s, f = self.s, self.f
        self.sx, self.sy = flip(s, 2), flip(s, 4)
        self.sd, self.sc = flip(self.sx, 4), flip(s, 1)
        self.q = f // 2 if pair > 1 else 0
        self.x, self.y, self.core = (self.sx, f), (self.sy, f), (self.sc, f)
        self.z = (s, opposite(f)) if pair > 1 else None
        self.peers = [self.x, self.y, self.core] + ([self.z] if pair > 1 else [])

    def barrier(self):
        sem = pltpu.get_barrier_semaphore()
        for peer in self.peers:
            pl.semaphore_signal(sem, inc=1, device_id=peer, device_id_type=MESH)
        pl.semaphore_wait(sem, len(self.peers))


class Wires:
    def __init__(self, send, recv):
        self.send, self.recv, self.count, self.open = send, recv, 0, {}

    def new(self, key):
        self.open[key] = self.count
        self.count += 1

    def go(self, key, src, dst, device):
        i = self.open[key]
        copy = pltpu.make_async_remote_copy(
            src, dst, self.send.at[i], self.recv.at[i], device_id=device, device_id_type=MESH
        )
        copy.start()
        return copy


def gather_steps(place, wires, own, out, ready):
    pair, rows = place.pair, own.shape[0]
    half = rows // 2
    top, low = pl.ds(0, half), pl.ds(half, half)
    p = place
    qs = [p.q] + ([1 - p.q] if pair > 1 else [])
    kinds = ["xa", "xb", "ya", "yb", "xd", "yd", "c0", "cxa", "cxb", "cya", "cyb", "cda", "cdb"]
    for t in range(pair):
        for kind in kinds:
            wires.new((t, kind))
    if pair > 1:
        wires.new("z")
    live = {}

    def go(key, src, dst, device):
        live[key] = wires.go(key, src, dst, device)

    def begin(t, src):
        q = qs[t]
        go((t, "xa"), src.at[top], out.at[q, p.s, top], p.x)
        go((t, "yb"), src.at[low], out.at[q, p.s, low], p.y)
        go((t, "xb"), src.at[low], out.at[q, p.s, low], p.x)
        go((t, "ya"), src.at[top], out.at[q, p.s, top], p.y)
        go((t, "c0"), src, out.at[q, p.s], p.core)

    def arrived(key):
        live[key].wait_recv()

    if pair > 1:
        go("z", own, out.at[qs[0], p.s], p.z)
    begin(0, own)
    ready(qs[0], p.s, None)

    def first(t):
        q = qs[t]
        arrived((t, "xa"))
        go((t, "xd"), out.at[q, p.sx, top], out.at[q, p.sx, top], p.y)
        go((t, "cxa"), out.at[q, p.sx, top], out.at[q, p.sx, top], p.core)
        arrived((t, "yb"))
        go((t, "yd"), out.at[q, p.sy, low], out.at[q, p.sy, low], p.x)
        go((t, "cyb"), out.at[q, p.sy, low], out.at[q, p.sy, low], p.core)
        arrived((t, "c0"))
        ready(q, p.sc, None)

    def second(t):
        q = qs[t]
        arrived((t, "xb"))
        go((t, "cxb"), out.at[q, p.sx, low], out.at[q, p.sx, low], p.core)
        ready(q, p.sx, None)
        arrived((t, "ya"))
        go((t, "cya"), out.at[q, p.sy, top], out.at[q, p.sy, top], p.core)
        ready(q, p.sy, None)
        arrived((t, "xd"))
        go((t, "cda"), out.at[q, p.sd, top], out.at[q, p.sd, top], p.core)
        arrived((t, "yd"))
        go((t, "cdb"), out.at[q, p.sd, low], out.at[q, p.sd, low], p.core)

    def third(t):
        q = qs[t]
        arrived((t, "cxa"))
        arrived((t, "cxb"))
        ready(q, flip(p.sx, 1), None)
        arrived((t, "cya"))
        arrived((t, "cyb"))
        ready(q, flip(p.sy, 1), None)
        ready(q, p.sd, None)
        arrived((t, "cda"))
        arrived((t, "cdb"))
        ready(q, flip(p.sd, 1), None)

    first(0)
    if pair > 1:
        arrived("z")
        begin(1, out.at[qs[1], p.s])
        ready(qs[1], p.s, None)
    second(0)
    if pair > 1:
        first(1)
    third(0)
    if pair > 1:
        second(1)
        third(1)
    for copy in live.values():
        copy.wait_send()


def gather_wires(pair):
    return 14 * pair + (2 if pair > 1 else 0)


def gather_kernel(pair, own, out, send, recv, local):
    place = Place(pair)
    keep = pltpu.make_async_copy(own, out.at[place.q, place.s], local)
    keep.start()
    place.barrier()
    gather_steps(place, Wires(send, recv), own, out, lambda q, slot, half: None)
    keep.wait()


def plane_gather(v, n, pair, ident):
    rows, width = v.shape
    return pl.pallas_call(
        functools.partial(gather_kernel, pair),
        in_specs=[pl.BlockSpec(memory_space=pltpu.VMEM)],
        out_specs=pl.BlockSpec(memory_space=pl.ANY),
        out_shape=jax.ShapeDtypeStruct((pair, n, rows, width), v.dtype),
        scratch_shapes=[pltpu.SemaphoreType.DMA((gather_wires(pair),))] * 2 + [pltpu.SemaphoreType.DMA],
        compiler_params=pltpu.CompilerParams(collective_id=ident, has_side_effects=True),
        cost_estimate=pl.CostEstimate(flops=0, bytes_accessed=pair * n * rows * width * 20, transcendentals=0),
        name=f"gather_{ident}",
    )(v).reshape(pair * n * rows, width)


def add(a, b):
    return (a.astype(F32) + b.astype(F32)).astype(BF16)


def scatter_steps(place, wires, part, rc, rd, rx, ry, qbuf, zbuf, make, finish):
    p, pair = place, place.pair
    rows = rx.shape[1]
    half = rows // 2
    top, low = pl.ds(0, half), pl.ds(half, half)
    slots = {"d": p.sd, "x": p.sx, "y": p.sy, "o": p.s}
    order = ["d", "x", "y", "o"]
    names = ["c" + k for k in order] + ["da", "db", "xa", "xb", "ya", "yb"]
    for t in range(pair):
        for name in names:
            wires.new((t, name))
    if pair > 1:
        wires.new("z")
    live = {}

    def go(key, src, dst, device):
        live[key] = wires.go(key, src, dst, device)

    def arrived(key):
        live[key].wait_recv()

    for t in range(pair):
        for i, k in enumerate(order):
            make(t, k, 1)
            go((t, "c" + k), part(t, flip(slots[k], 1)), rc.at[t, i], p.core)

    def start(t):
        make(t, "d", 0)
        arrived((t, "cd"))
        qbuf[t, 0] = add(part(t, p.sd)[...], rc[t, 0])
        go((t, "da"), qbuf.at[t, 0, top], rd.at[t, top], p.x)
        go((t, "db"), qbuf.at[t, 0, low], rd.at[t, low], p.y)
        make(t, "x", 0)
        arrived((t, "cx"))
        qbuf[t, 1, top] = add(part(t, p.sx)[top], rc[t, 1, top])
        go((t, "xa"), qbuf.at[t, 1, top], rx.at[t, top], p.x)
        make(t, "y", 0)
        arrived((t, "cy"))
        qbuf[t, 2, low] = add(part(t, p.sy)[low], rc[t, 2, low])
        go((t, "yb"), qbuf.at[t, 2, low], ry.at[t, low], p.y)

    def relay(t):
        held = part(t, p.sx)[low].astype(F32) + rc[t, 1, low].astype(F32)
        arrived((t, "db"))
        qbuf[t, 1, low] = (held + rd[t, low].astype(F32)).astype(BF16)
        go((t, "xb"), qbuf.at[t, 1, low], rx.at[t, low], p.x)
        held = part(t, p.sy)[top].astype(F32) + rc[t, 2, top].astype(F32)
        arrived((t, "da"))
        qbuf[t, 2, top] = (held + rd[t, top].astype(F32)).astype(BF16)
        go((t, "ya"), qbuf.at[t, 2, top], ry.at[t, top], p.y)

    def total(t):
        make(t, "o", 0)
        arrived((t, "co"))
        value = part(t, p.s)[...].astype(F32) + rc[t, 3].astype(F32)
        for key in ("xa", "yb", "xb", "ya"):
            arrived((t, key))
        return value + rx[t].astype(F32) + ry[t].astype(F32)

    if pair > 1:
        start(0)
        start(1)
        relay(0)
        relay(1)
        zbuf[0] = total(0).astype(BF16)
        go("z", zbuf.at[0], zbuf.at[1], p.z)
        value = total(1)
        arrived("z")
        value = value + zbuf[1].astype(F32)
    else:
        start(0)
        relay(0)
        value = total(0)
    finish(value)
    for copy in live.values():
        copy.wait_send()


def scatter_wires(pair):
    return 20 * pair + (2 if pair > 1 else 0)


def scatter_scratch(pair, rows, width):
    block = lambda *lead: pltpu.VMEM(lead + (rows, width), BF16)
    return [
        block(pair, 4),
        block(pair),
        block(pair),
        block(pair),
        block(pair, 3),
        block(2) if pair > 1 else pltpu.VMEM((2, 16, 128), BF16),
        pltpu.SemaphoreType.DMA((scatter_wires(pair),)),
        pltpu.SemaphoreType.DMA((scatter_wires(pair),)),
    ]


def scatter_kernel(pair, value, out, rc, rd, rx, ry, qbuf, zbuf, send, recv):
    place = Place(pair)
    place.barrier()
    planes = [1 - place.q, place.q] if pair > 1 else [0]

    def part(t, slot):
        return value.at[planes[t], slot]

    def finish(total):
        out[...] = total

    scatter_steps(
        place, Wires(send, recv), part, rc, rd, rx, ry, qbuf, zbuf, lambda *_: None, finish
    )


def plane_scatter(v, n, pair, ident):
    width = v.shape[1]
    rows = v.shape[0] // (pair * n)
    return pl.pallas_call(
        functools.partial(scatter_kernel, pair),
        in_specs=[pl.BlockSpec(memory_space=pltpu.VMEM)],
        out_specs=pl.BlockSpec(memory_space=pltpu.VMEM),
        out_shape=jax.ShapeDtypeStruct((rows, width), F32),
        scratch_shapes=scatter_scratch(pair, rows, width),
        compiler_params=pltpu.CompilerParams(
            collective_id=ident, has_side_effects=True, vmem_limit_bytes=40 * 2**20
        ),
        cost_estimate=pl.CostEstimate(flops=0, bytes_accessed=pair * n * rows * width * 20, transcendentals=0),
        name=f"scatter_{ident}",
    )(v.astype(BF16).reshape(pair, n, rows, width))


def sum_kernel(n, own, out, held, send, recv):
    s, f = lax.axis_index("seq"), lax.axis_index("fsdp")
    sem = pltpu.get_barrier_semaphore()
    for d in range(1, n):
        pl.semaphore_signal(sem, inc=1, device_id=((s + d) % n, f), device_id_type=MESH)
    pl.semaphore_wait(sem, n - 1)
    copies = []
    for d in range(1, n):
        copy = pltpu.make_async_remote_copy(
            own,
            held.at[d - 1],
            send.at[d - 1],
            recv.at[d - 1],
            device_id=((s + d) % n, f),
            device_id_type=MESH,
        )
        copy.start()
        copies.append(copy)
    total = own[...]
    for d in range(1, n):
        copies[d - 1].wait_recv()
        total = total + held[d - 1]
    out[...] = total
    for copy in copies:
        copy.wait_send()


def plane_sum(v, n, ident):
    return pl.pallas_call(
        functools.partial(sum_kernel, n),
        in_specs=[pl.BlockSpec(memory_space=pltpu.VMEM)],
        out_specs=pl.BlockSpec(memory_space=pltpu.VMEM),
        out_shape=jax.ShapeDtypeStruct(v.shape, v.dtype),
        scratch_shapes=[pltpu.VMEM((n - 1,) + v.shape, v.dtype)]
        + [pltpu.SemaphoreType.DMA((n - 1,))] * 2,
        compiler_params=pltpu.CompilerParams(collective_id=ident, has_side_effects=True),
        name=f"sum_{ident}",
    )(v)


def when(condition, body):
    pl.when(condition)(body)


def line_barrier(n, m):
    s, f = lax.axis_index("seq"), lax.axis_index("fsdp")
    sem = pltpu.get_barrier_semaphore()
    for d in range(1, n):
        pl.semaphore_signal(sem, inc=1, device_id=((s + d) % n, f), device_id_type=MESH)
    for d in range(1, m):
        pl.semaphore_signal(sem, inc=1, device_id=(s, (f + d) % m), device_id_type=MESH)
    pl.semaphore_wait(sem, n + m - 2)


def entry_kernel(
    n, m, x, wq, wk, wv, gains, xs, qkv, all_gains, tables, full, send, recv, asend, arecv, zsend, zrecv, gsend, grecv, local
):
    place = Place(1)
    s, f = place.s, place.f
    cols, part = qkv.shape[-1], wq.shape[0]
    weights = (wq, wk, wv)
    kept = [pltpu.make_async_copy(x, xs.at[0, s], local.at[0])]
    for j, w in enumerate(weights):
        own = w.at[:, pl.ds(pl.multiple_of(s * cols, cols), cols)]
        kept.append(pltpu.make_async_copy(own, qkv.at[j, f, s], local.at[1 + j]))
    for copy in kept:
        copy.start()
    full[f, s] = gains[...]
    line_barrier(n, m)
    sent = []

    def remote(src, dst, a, b, device):
        copy = pltpu.make_async_remote_copy(src, dst, a, b, device_id=device, device_id_type=MESH)
        copy.start()
        sent.append(copy)
        return copy

    second = []
    for j, w in enumerate(weights):
        row = []
        for d in range(1, n):
            t = (s + d) % n
            src = w.at[:, pl.ds(pl.multiple_of(t * cols, cols), cols)]
            row.append(remote(src, qkv.at[j, f, s], asend.at[j, d], arecv.at[j, d], (t, f)))
        second.append(row)
    first = []
    for d in range(1, n):
        first.append(remote(gains, full.at[f, s], gsend.at[d], grecv.at[d], ((s + d) % n, f)))

    def piece(j, o):
        return full.at[o] if j == 3 else qkv.at[j, o]

    def hop(way, h, j):
        o = f - h if way == 0 else f + h
        there = f + 1 if way == 0 else f - 1
        place_ = piece(j, o)
        return pltpu.make_async_remote_copy(
            place_, place_, zsend.at[way, h, j], zrecv.at[way, h, j], device_id=(s, there), device_id_type=MESH
        )

    def sends(way, h):
        return ((f - h >= 0) & (f < m - 1)) if way == 0 else ((f + h <= m - 1) & (f > 0))

    def receives(way, h):
        return (f - h - 1 >= 0) if way == 0 else (f + h + 1 <= m - 1)

    def start(h, j):
        for way in (0, 1):
            when(sends(way, h), lambda: hop(way, h, j).start())

    def landed(h, j):
        for way in (0, 1):
            o = f - h - 1 if way == 0 else f + h + 1

            def wait():
                there = f - 1 if way == 0 else f + 1
                place_ = piece(j, o)
                pltpu.make_async_remote_copy(
                    place_, place_, zsend.at[way, h, j], zrecv.at[way, h, j], device_id=(s, there), device_id_type=MESH
                ).wait_recv()

            when(receives(way, h), wait)

    def step(h, j):
        landed(h, j)
        if h + 1 < m - 1:
            start(h + 1, j)

    for copy in kept:
        copy.wait()
    for j in range(3):
        for copy in second[j]:
            copy.wait_recv()
        start(0, j)
    for copy in first:
        copy.wait_recv()
    start(0, 3)
    live = gather_pairs(
        place, Wires(send, recv), x, xs, lambda *_: None, Work([lambda: None, lambda: step(0, 0), lambda: step(0, 1)])
    )
    step(0, 2)
    step(0, 3)
    length = tables.shape[1]
    half = HD // 2
    block = min(256, length)
    lane = lax.broadcasted_iota(jnp.int32, (block, HD), 1)
    row = lax.broadcasted_iota(jnp.int32, (block, HD), 0)
    frequency = jnp.exp((lane % half).astype(F32) * (-2.0 * math.log(THETA) / HD))

    @pl.loop(0, length // block)
    def _(i):
        angle = (row + i * block).astype(F32) * frequency
        here = pl.ds(pl.multiple_of(i * block, block), block)
        tables[0, here, :] = jnp.cos(angle)
        sine = jnp.sin(angle)
        tables[1, here, :] = jnp.where(lane < half, -sine, sine)

    for h in range(1, m - 1):
        for j in range(4):
            step(h, j)
    for t in range(n):
        for plane in range(m):
            at = (t * m + plane) * part
            all_gains[:, at : at + part] = full[plane, t, :, :part]
    for copy in sent + list(live.values()):
        copy.wait_send()
    for h in range(m - 1):
        for j in range(4):
            for way in (0, 1):
                when(sends(way, h), lambda: hop(way, h, j).wait_send())


def entry(x, wq, wk, wv, gains, n, m, ident):
    rows, width = x.shape
    part = wq.shape[0]
    cols = width // n
    vmem, any_ = pl.BlockSpec(memory_space=pltpu.VMEM), pl.BlockSpec(memory_space=pl.ANY)
    dma = pltpu.SemaphoreType.DMA
    return pl.pallas_call(
        functools.partial(entry_kernel, n, m),
        in_specs=[vmem] * 5,
        out_specs=[any_] * 2 + [vmem] * 2,
        out_shape=[
            jax.ShapeDtypeStruct((1, n, rows, width), x.dtype),
            jax.ShapeDtypeStruct((3, m, n, part, cols), wq.dtype),
            jax.ShapeDtypeStruct((gains.shape[0], width), F32),
            jax.ShapeDtypeStruct((2, n * rows, HD), F32),
        ],
        scratch_shapes=[pltpu.VMEM((m, n) + gains.shape, gains.dtype)]
        + [dma((gather_wires(1),))] * 2
        + [dma((3, n))] * 2
        + [dma((2, m, 4))] * 2
        + [dma((n,))] * 2
        + [dma((4,))],
        compiler_params=pltpu.CompilerParams(collective_id=ident, has_side_effects=True),
        cost_estimate=pl.CostEstimate(flops=0, bytes_accessed=200 * 2**20, transcendentals=0),
        name=f"entry_{ident}",
    )(x, wq, wk, wv, gains)


def exit_kernel(
    n,
    m,
    d3,
    term,
    own_gain,
    branch_gain,
    feed_gain,
    grad_hidden,
    qkv,
    tokens_grad,
    weight_grad,
    gain_grad,
    w_v,
    value,
    rc,
    rd,
    rx,
    ry,
    qbuf,
    zbuf,
    send,
    recv,
    line,
    sums,
    done,
    got,
    gains,
    gplane,
    gsum,
    gline,
    zsend,
    zrecv,
    asend,
    arecv,
    gsend,
    grecv,
    lsend,
    lrecv,
    sems,
):
    place = Place(1)
    s, f = place.s, place.f
    moves = Moves(sems)
    for j in range(3):
        for plane in range(m):
            moves.start(qkv.at[j, plane], w_v.at[j, :, plane])
    line_barrier(n, m)
    last = m - 1
    cols = term.shape[-1]

    def remote(src, dst, a, b, device):
        return pltpu.make_async_remote_copy(src, dst, a, b, device_id=device, device_id_type=MESH)

    def target(way, r):
        return last - r if way == 0 else r

    def hop(way, r, j, fresh):
        there = f + 1 if way == 0 else f - 1
        src = term.at[j, :, target(way, r)] if fresh else sums.at[way, r, j]
        return remote(src, line.at[way, r, j], zsend.at[way, r, j], zrecv.at[way, r, j], (s, there))

    ends = (f == 0, f == last)
    inner = (f > 0, f < last)

    def beyond(way, r):
        return target(way, r) > f if way == 0 else target(way, r) < f

    for group in ((0, 1, 2), (3,)):
        for r in range(last):
            for j in group:
                for way in (0, 1):
                    when(ends[way], lambda: hop(way, r, j, True).start())

    gain_copies = []
    for t in range(n):
        at = pl.ds(t * cols, cols)
        for j in range(2):
            gains[t, j : j + 1, :] = jnp.where(s == t, own_gain[j], 0.0)
        gains[t, 2:3, :] = branch_gain[:, at]
        gains[t, 3:4, :] = feed_gain[:, at]
        gains[t, 4:, :] = jnp.zeros((4, cols), F32)
    for d in range(1, n):
        t = (s + d) % n
        copy = remote(gains.at[t], gplane.at[d - 1], gsend.at[d], grecv.at[d], (t, f))
        copy.start()
        gain_copies.append(copy)

    moves.finish()
    rows, width = grad_hidden.shape
    block, step = 2 * rows, min(512, width)
    per = step // (m * qkv.shape[3])

    def make(q, chip, c):
        here = pl.ds(pl.multiple_of(chip * block, block), block)

        @pl.loop(c * (width // 2) // step, (c + 1) * (width // 2) // step)
        def _(i):
            at = pl.ds(pl.multiple_of(i * step, step), step)
            total = jnp.zeros((block, step), F32)
            for j in range(3):
                w = w_v[j, pl.ds(i * per, per)].reshape(step, cols)
                total = total + dot(d3[j, here, :], w, NT)
            value[q, pl.ds(2 * chip, 2), :, at] = total.astype(BF16).reshape(2, rows, step)

    side = f // (m // 2)
    middle = (f > 0) & (f < last)

    def relays(k, j, from_end):
        way = side if from_end else 1 - side
        o = way * k + (1 - way) * (last - k)

        def relay():
            there = f + 1 - 2 * way
            copy = remote(
                sums.at[way, k, j], line.at[way, k, j], zsend.at[way, k, j], zrecv.at[way, k, j], (s, there)
            )
            copy.wait_recv()
            sums[way, k, j] = add(term[j, :, o], line[way, k, j])
            copy.start()

        when(middle, relay)

    live = scatter_pairs(
        place, Wires(send, recv), value, rc, rd, rx, ry, qbuf, zbuf, make, tokens_grad,
        Work([lambda: None] + [lambda j=j: relays(0, j, True) for j in range(3)]),
    )
    tokens_grad[...] += grad_hidden[...]

    total = gains[s]
    for d in range(1, n):
        gain_copies[d - 1].wait_recv()
        total = total + gplane[d - 1]
    gsum[...] = total
    line_copies = []
    for d in range(1, m):
        t = (f + d) % m
        copy = remote(gsum, gline.at[d - 1], lsend.at[d], lrecv.at[d], (s, t))
        copy.start()
        line_copies.append(copy)

    copies = []
    plan = [(True, k, j) for k in range(1, m // 2) for j in range(3)]
    plan += [(False, k, j) for k in range(m // 2 - 1) for j in range(3)] + [(None, 0, j) for j in range(3)]
    plan += [(True, k, 3) for k in range(m // 2)] + [(False, k, 3) for k in range(m // 2 - 1)] + [(None, 0, 3)]
    for from_end, k, j in plan:
        if from_end is not None:
            relays(k, j, from_end)
            continue
        own = term[j, :, f].astype(F32)
        done[j] = own
        for way in (0, 1):
            r = last - f if way == 0 else f

            def take():
                pltpu.make_async_remote_copy(
                    sums.at[way, 0, j],
                    line.at[way, r, j],
                    zsend.at[way, r, j],
                    zrecv.at[way, r, j],
                    device_id=(s, f - 1 if way == 0 else f + 1),
                    device_id_type=MESH,
                ).wait_recv()
                done[j] += line[way, r, j].astype(F32)

            when(inner[way], take)
        if j == 3:
            for t in range(n):
                weight_grad[j, :, pl.ds(t * cols, cols)] = done[j, t]
            continue
        weight_grad[j, :, pl.ds(pl.multiple_of(s * cols, cols), cols)] = done[j, s]
        got[0, j] = done[j].astype(BF16)
        for d in range(1, n):
            t = (s + d) % n
            copy = remote(got.at[0, j, t], got.at[1, j, s], asend.at[j, d], arecv.at[j, d], (t, f))
            copy.start()
            copies.append(copy)
    total = gsum[...]
    for d in range(1, m):
        line_copies[d - 1].wait_recv()
        total = total + gline[d - 1]
    small = cols // m
    gain = jnp.zeros((8, small), F32)
    for plane in range(m):
        gain = gain + jnp.where(f == plane, total[:, plane * small : (plane + 1) * small], 0.0)
    gain_grad[...] = gain
    for copy in copies:
        copy.wait_recv()
    for j in range(3):
        for d in range(1, n):
            t = (s + d) % n
            weight_grad[j, :, pl.ds(pl.multiple_of(t * cols, cols), cols)] = got[1, j, t].astype(F32)
    for copy in copies + gain_copies + line_copies + list(live.values()):
        copy.wait_send()
    for r in range(last):
        for j in range(4):
            for way in (0, 1):
                when(ends[way] | (inner[way] & beyond(way, r)), lambda: hop(way, r, j, False).wait_send())


def leave(d3, term, own_gain, branch_gain, feed_gain, grad_hidden, qkv, n, m, ident):
    rows, width = grad_hidden.shape
    part, cols = term.shape[-2:]
    vmem = pl.BlockSpec(memory_space=pltpu.VMEM)
    dma = pltpu.SemaphoreType.DMA
    block = pltpu.VMEM((2, m - 1, 4, n, part, cols), BF16)
    return pl.pallas_call(
        functools.partial(exit_kernel, n, m),
        in_specs=[vmem] * 6 + [pl.BlockSpec(memory_space=pl.ANY)],
        out_specs=[vmem] * 3,
        out_shape=[
            jax.ShapeDtypeStruct((rows, width), F32),
            jax.ShapeDtypeStruct((4, part, width), F32),
            jax.ShapeDtypeStruct((8, cols // m), F32),
        ],
        scratch_shapes=[pltpu.VMEM((3, n, m, part, cols), BF16), pltpu.VMEM((1, n, rows, width), BF16)]
        + scatter_scratch(1, rows, width)
        + [
            block,
            block,
            pltpu.VMEM((4, n, part, cols), F32),
            pltpu.VMEM((2, 3, n, part, cols), BF16),
            pltpu.VMEM((n, 8, cols), F32),
            pltpu.VMEM((n - 1, 8, cols), F32),
            pltpu.VMEM((8, cols), F32),
            pltpu.VMEM((m - 1, 8, cols), F32),
        ]
        + [dma((2, m, 4))] * 2
        + [dma((3, n))] * 2
        + [dma((n,))] * 2
        + [dma((m,))] * 2
        + [dma((3 * m,))],
        compiler_params=pltpu.CompilerParams(
            collective_id=ident, has_side_effects=True, vmem_limit_bytes=60 * 2**20
        ),
        cost_estimate=pl.CostEstimate(flops=0, bytes_accessed=200 * 2**20, transcendentals=0),
        name=f"leave_{ident}",
    )(d3, term, own_gain, branch_gain, feed_gain, grad_hidden, qkv)


class Moves:
    def __init__(self, sems):
        self.sems, self.count, self.open = sems, 0, []

    def start(self, src, dst):
        copy = pltpu.make_async_copy(src, dst, self.sems.at[self.count])
        self.count += 1
        copy.start()
        self.open.append(copy)
        return copy

    def finish(self):
        for copy in self.open:
            copy.wait()
        self.open = []

    def wait(self, copies):
        for copy in copies:
            copy.wait()
        self.open = [copy for copy in self.open if all(copy is not other for other in copies)]


def place_kernel(parts, count, *refs):
    ins, outs = refs[:count], refs[count : count + len(parts)]
    held, sems = refs[count + len(parts) : -1], refs[-1]
    copies = []
    for i, (source, row) in enumerate(parts):
        src = ins[source] if row is None else ins[source].at[row]
        copies.append(pltpu.make_async_copy(src, held[i], sems.at[0, i]))
        copies[-1].start()
    back = []
    for i in range(len(parts)):
        copies[i].wait()
        back.append(pltpu.make_async_copy(held[i], outs[i], sems.at[1, i]))
        back[-1].start()
    for copy in back:
        copy.wait()


def place_outputs(arrays):
    parts, shapes = [], []
    for source, a in enumerate(arrays):
        for row in range(a.shape[0]) if a.ndim == 3 else [None]:
            parts.append((source, row))
            shapes.append(shape(a.shape[-2:], a.dtype))
    return pl.pallas_call(
        functools.partial(place_kernel, tuple(parts), len(arrays)),
        in_specs=[pl.BlockSpec(memory_space=pltpu.MemorySpace.HBM)] * len(arrays),
        out_specs=[pl.BlockSpec(memory_space=pltpu.MemorySpace.HBM)] * len(parts),
        out_shape=shapes,
        scratch_shapes=[pltpu.VMEM(a.shape, a.dtype) for a in shapes] + [pltpu.SemaphoreType.DMA((2, len(parts)))],
        compiler_params=pltpu.CompilerParams(vmem_limit_bytes=63 * 2**20),
        name="place",
    )(*arrays)


def gather_pairs(place, wires, own, out, ready, hook=lambda: None):
    p, pair = place, place.pair
    half = own.shape[0] // 2
    top, low = pl.ds(0, half), pl.ds(half, half)
    qs = [p.q] + ([1 - p.q] if pair > 1 else [])
    for t in range(pair):
        for kind in ["xa", "xb", "ya", "yb", "xd", "yd", "ca", "cb", "cxa", "cxb", "cya", "cyb", "cda", "cdb"]:
            wires.new((t, kind))
    if pair > 1:
        wires.new("za")
        wires.new("zb")
    live = {}

    def go(key, src, dst, device):
        live[key] = wires.go(key, src, dst, device)

    def arrived(*keys):
        for key in keys:
            live[key].wait_recv()

    def begin(t, src, tops):
        q = qs[t]
        rows = top if tops else low
        go((t, "xa" if tops else "xb"), src.at[rows], out.at[q, p.s, rows], p.x)
        go((t, "ya" if tops else "yb"), src.at[rows], out.at[q, p.s, rows], p.y)
        go((t, "ca" if tops else "cb"), src.at[rows], out.at[q, p.s, rows], p.core)

    def pass_on(t, name, slot, rows, device):
        ref = out.at[qs[t], slot, rows]
        go((t, name), ref, ref, device)

    def first(t):
        arrived((t, "xa"))
        pass_on(t, "xd", p.sx, top, p.y)
        pass_on(t, "cxa", p.sx, top, p.core)
        arrived((t, "ya"))
        pass_on(t, "cya", p.sy, top, p.core)

    def second(t):
        arrived((t, "yb"))
        pass_on(t, "yd", p.sy, low, p.x)
        pass_on(t, "cyb", p.sy, low, p.core)
        arrived((t, "xb"))
        pass_on(t, "cxb", p.sx, low, p.core)

    def third(t):
        arrived((t, "xd"))
        pass_on(t, "cda", p.sd, top, p.core)
        arrived((t, "yd"))
        pass_on(t, "cdb", p.sd, low, p.core)

    def use(t, slot, *keys):
        arrived(*[(t, key) for key in keys])
        ready(qs[t], slot // 2)

    if pair > 1:
        go("za", own.at[top], out.at[qs[0], p.s, top], p.z)
        go("zb", own.at[low], out.at[qs[0], p.s, low], p.z)
    begin(0, own, True)
    begin(0, own, False)
    use(0, p.s, "ca", "cb")
    hook()
    first(0)
    if pair > 1:
        second(0)
        use(0, p.sx, "cxa", "cxb")
        arrived("za")
        begin(1, out.at[qs[1], p.s], True)
        use(0, p.sy, "cya", "cyb")
        third(0)
        hook()
        arrived("zb")
        begin(1, out.at[qs[1], p.s], False)
        use(0, p.sd, "cda", "cdb")
        first(1)
        use(1, p.s, "ca", "cb")
        second(1)
        hook()
        use(1, p.sx, "cxa", "cxb")
        use(1, p.sy, "cya", "cyb")
        third(1)
        use(1, p.sd, "cda", "cdb")
    else:
        hook()
        second(0)
        use(0, p.sx, "cxa", "cxb")
        use(0, p.sy, "cya", "cyb")
        hook()
        third(0)
        use(0, p.sd, "cda", "cdb")
    return live


def scatter_pairs(place, wires, value, rc, rd, rx, ry, qbuf, zbuf, make, result, hook=lambda: None, first=0):
    p, pair = place, place.pair
    rows, width = rx.shape[1], rx.shape[2]
    half, wide = rows // 2, width // 2
    top, low = pl.ds(0, half), pl.ds(half, half)
    slots = {"d": p.sd, "x": p.sx, "y": p.sy, "o": p.s}
    order = ["d", "x", "y", "o"]
    planes = [1 - p.q, p.q] if pair > 1 else [p.q]
    jobs = [(t, c) for t in range(pair) for c in range(2)]
    if not isinstance(first, int):
        jobs = [(t, c) for c in range(2) for t in range(pair)]
    for job in jobs:
        for name in ["c" + k for k in order] + ["da", "db", "xa", "xb", "ya", "yb"]:
            wires.new((job, name))
    if pair > 1:
        wires.new("z0")
        wires.new("z1")
    live = {}

    def go(key, src, dst, device):
        live[key] = wires.go(key, src, dst, device)

    def arrived(*keys):
        for key in keys:
            live[key].wait_recv()

    def at(c, first=first):
        if isinstance(first, int):
            return pl.ds(c * wide, wide)
        return pl.ds(pl.multiple_of((c + first) % 2 * wide, wide), wide)

    def part(job, slot, rows_):
        return value.at[planes[job[0]], slot, rows_, at(job[1])]

    every = pl.ds(0, rows)

    def share(job, k):
        t, c = job
        make(planes[t], slots[k] // 2, c)
        go((job, "c" + k), part(job, flip(slots[k], 1), every), rc.at[t, order.index(k), :, at(c)], p.core)

    def begin(job):
        share(job, "d")
        share(job, "x")

    def rest(job):
        t, c = job
        arrived((job, "cd"))
        qbuf[t, 0, :, at(c)] = add(part(job, p.sd, every)[...], rc[t, 0, :, at(c)])
        go((job, "da"), qbuf.at[t, 0, top, at(c)], rd.at[t, top, at(c)], p.x)
        go((job, "db"), qbuf.at[t, 0, low, at(c)], rd.at[t, low, at(c)], p.y)
        share(job, "y")
        arrived((job, "cx"))
        qbuf[t, 1, top, at(c)] = add(part(job, p.sx, top)[...], rc[t, 1, top, at(c)])
        go((job, "xa"), qbuf.at[t, 1, top, at(c)], rx.at[t, top, at(c)], p.x)
        share(job, "o")
        arrived((job, "cy"))
        qbuf[t, 2, low, at(c)] = add(part(job, p.sy, low)[...], rc[t, 2, low, at(c)])
        go((job, "yb"), qbuf.at[t, 2, low, at(c)], ry.at[t, low, at(c)], p.y)

    def relay(job):
        t, c = job
        arrived((job, "db"))
        held = part(job, p.sx, low)[...].astype(F32) + rc[t, 1, low, at(c)].astype(F32)
        qbuf[t, 1, low, at(c)] = (held + rd[t, low, at(c)].astype(F32)).astype(BF16)
        go((job, "xb"), qbuf.at[t, 1, low, at(c)], rx.at[t, low, at(c)], p.x)
        arrived((job, "da"))
        held = part(job, p.sy, top)[...].astype(F32) + rc[t, 2, top, at(c)].astype(F32)
        qbuf[t, 2, top, at(c)] = (held + rd[t, top, at(c)].astype(F32)).astype(BF16)
        go((job, "ya"), qbuf.at[t, 2, top, at(c)], ry.at[t, top, at(c)], p.y)

    def total(job):
        t, c = job
        arrived((job, "co"), (job, "xa"), (job, "yb"), (job, "xb"), (job, "ya"))
        value_ = part(job, p.s, every)[...].astype(F32) + rc[t, 3, :, at(c)].astype(F32)
        value_ = value_ + rx[t, :, at(c)].astype(F32) + ry[t, :, at(c)].astype(F32)
        if pair > 1 and t == 0:
            zbuf[0, :, at(c)] = value_.astype(BF16)
            go(f"z{c}", zbuf.at[0, :, at(c)], zbuf.at[1, :, at(c)], p.z)
        else:
            result[:, at(c)] = value_

    begin(jobs[0])
    rest(jobs[0])
    for i, job in enumerate(jobs):
        after = jobs[i + 1] if i + 1 < len(jobs) else None
        if after:
            begin(after)
        hook()
        relay(job)
        if after:
            rest(after)
        hook()
        total(job)
    if pair > 1:
        for c in range(2):
            here = at(c) if isinstance(first, int) else at(1 - c)
            arrived(f"z{c}")
            result[:, here] += zbuf[1, :, here].astype(F32)
    return live


def rms_back(value, gain, grad):
    inverse = lax.rsqrt(jnp.mean(value * value, axis=-1, keepdims=True) + EPSILON)
    normal = value * inverse
    u = grad * gain
    return inverse * (u - normal * jnp.mean(u * normal, axis=-1, keepdims=True)), grad * normal


def up_kernel(
    pair, h, wg, wu, down_w, hs, gate, up, inner, inner_t, wd, hs_v, w_v, g_v, u_v, i_v, t_v, send, recv, zsem, sems
):
    place = Place(pair)
    place.peers.append((place.s, flip(place.f, 1)))
    moves = Moves(sems)
    loads = [moves.start(wg, w_v.at[0]), moves.start(wu, w_v.at[1])]
    rows, width = h.shape
    block, share = 2 * rows, wg.shape[1]
    hs_v[place.q, place.s] = h[...]
    place.barrier()
    stream, view = Stream(place, zsem), half_rows(down_w, share)
    down_copies = [stream.near_copy(0, view, wd), stream.own_copy(0, view, wd), stream.far_copy(0, view, wd)]

    def pass_down():
        for copy in down_copies:
            copy.start()

    n = hs.shape[1]
    step = min(256, share)
    waited = []

    def ready(q, chip):
        if not waited:
            moves.wait(loads)
            waited.append(True)
        slots = pl.ds(2 * chip, 2)
        moves.start(hs_v.at[q, slots], hs.at[q, slots])
        at = pl.multiple_of(q * n * rows + chip * block, block)
        here = pl.ds(at, block)

        @pl.loop(0, share // step)
        def _(j):
            cols = pl.ds(pl.multiple_of(j * step, step), step)
            a = hs_v[q, slots].reshape(block, width)
            g = dot(a, w_v[0, :, cols], NN)
            u = dot(a, w_v[1, :, cols], NN)
            g_v[here, cols] = g
            u_v[here, cols] = u
            value = (g * (1.0 / (1.0 + jnp.exp(-g))) * u)
            i_v[here, cols] = value.astype(BF16)
            t_v[cols, here] = value.T.astype(BF16)

        moves.start(g_v.at[here], gate.at[here])
        moves.start(u_v.at[here], up.at[here])
        moves.start(i_v.at[here], inner.at[here])

    live = gather_pairs(place, Wires(send, recv), h, hs_v, ready, Work([lambda: None, pass_down]))
    moves.start(t_v, inner_t)
    for copy in down_copies:
        copy.wait()
    for copy in live.values():
        copy.wait_send()
    moves.finish()


def any_specs(count):
    return [pl.BlockSpec(memory_space=pl.ANY)] * count


def vmem_specs(count):
    return [pl.BlockSpec(memory_space=pltpu.VMEM)] * count


def kernel_params(ident, mib=60):
    return pltpu.CompilerParams(collective_id=ident, has_side_effects=True, vmem_limit_bytes=mib * 2**20)


def shape(dims, kind):
    return jax.ShapeDtypeStruct(dims, kind)


def ffn_up(h, wg, wu, down_w, n, pair, ident):
    rows, width = h.shape
    share, long = wg.shape[1], pair * n * rows
    dma = pltpu.SemaphoreType.DMA
    outs = [
        shape((pair, n, rows, width), BF16),
        shape((long, share), F32),
        shape((long, share), F32),
        shape((long, share), BF16),
        shape((share, long), BF16),
        shape((width // down_w.shape[1], share, down_w.shape[1]), BF16),
    ]
    return pl.pallas_call(
        functools.partial(up_kernel, pair),
        in_specs=vmem_specs(1) + any_specs(3),
        out_specs=any_specs(6),
        out_shape=outs,
        scratch_shapes=[
            pltpu.VMEM((pair, n, rows, width), BF16),
            pltpu.VMEM((2, width, share), BF16),
            pltpu.VMEM((long, share), F32),
            pltpu.VMEM((long, share), F32),
            pltpu.VMEM((long, share), BF16),
            pltpu.VMEM((share, long), BF16),
            dma((gather_wires(pair),)),
            dma((gather_wires(pair),)),
            dma((1, 4, 2)),
            dma((3 + 4 * pair * n // 2,)),
        ],
        compiler_params=kernel_params(ident),
        cost_estimate=pl.CostEstimate(
            flops=4 * long * width * share, bytes_accessed=long * width * 40, transcendentals=0
        ),
        name=f"up_{ident}",
    )(h, wg, wu, down_w)


def down_kernel(
    pair, inner, wd, hidden, gains, cotangent, layer_out, grad_low, gain_term, wd_all,
    i_v, w_v, sum_v, value, rc, rd, rx, ry, qbuf, zbuf, send, recv, wsem, sems
):
    place = Place(pair)
    place.peers.append((place.s, flip(place.f, 1)))
    moves = Moves(sems)
    gain = gains[3:4, :]
    f, far_f, near_f = place.f, opposite(place.f), flip(place.f, 1)
    deep = wd.shape[2]

    def columns(plane):
        return w_v.at[:, pl.ds(pl.multiple_of(plane * deep, deep), deep)]

    for plane in (f, near_f, far_f):
        moves.start(wd.at[plane], columns(plane))
    moves.start(inner, i_v)
    rows, width = hidden.shape
    block = 2 * rows
    n = value.shape[1]
    step = min(512, width)
    place.barrier()
    relay = pltpu.make_async_remote_copy(
        wd.at[far_f], columns(far_f), wsem.at[0], wsem.at[1], device_id=(place.s, near_f), device_id_type=MESH
    )
    relay.start()
    moves.finish()
    loaded = []

    def make(q, chip, c):
        if c == 1 and not loaded:
            relay.wait_recv()
            loaded.append(True)
        c = (c + f // 2) % 2
        here = pl.ds(pl.multiple_of(q * n * rows + chip * block, block), block)

        @pl.loop(c * (width // 2) // step, (c + 1) * (width // 2) // step)
        def _(j):
            cols = pl.ds(pl.multiple_of(j * step, step), step)
            part = dot(i_v[here, :], w_v[:, cols], NN).astype(BF16)
            value[q, pl.ds(2 * chip, 2), :, cols] = part.reshape(2, rows, step)

    live = scatter_pairs(place, Wires(send, recv), value, rc, rd, rx, ry, qbuf, zbuf, make, sum_v, first=f // 2)
    moves.start(w_v, wd_all)
    feed = sum_v[...]
    grad = cotangent[...].astype(F32)
    inverse = lax.rsqrt(jnp.mean(feed * feed, axis=-1, keepdims=True) + EPSILON)
    normal = feed * inverse
    layer_out[...] = (hidden[...] + normal * gain).astype(BF16)
    u = grad * gain
    grad_low[...] = (inverse * (u - normal * jnp.mean(u * normal, axis=-1, keepdims=True))).astype(BF16)
    gain_term[...] = jnp.sum(grad * normal, axis=0, keepdims=True)
    for copy in list(live.values()) + [relay]:
        copy.wait_send()
    moves.finish()


def ffn_down(inner, wd, hidden, gains, cotangent, n, pair, ident):
    rows, width = hidden.shape
    dma = pltpu.SemaphoreType.DMA
    return pl.pallas_call(
        functools.partial(down_kernel, pair),
        in_specs=any_specs(2) + vmem_specs(3),
        out_specs=vmem_specs(3) + any_specs(1),
        out_shape=[
            shape((rows, width), BF16),
            shape((rows, width), BF16),
            shape((1, width), F32),
            shape((wd.shape[1], width), BF16),
        ],
        scratch_shapes=[
            pltpu.VMEM(inner.shape, BF16),
            pltpu.VMEM((wd.shape[1], width), BF16),
            pltpu.VMEM((rows, width), F32),
            pltpu.VMEM((pair, n, rows, width), BF16),
        ]
        + scatter_scratch(pair, rows, width)
        + [dma((2,)), dma((2 + wd.shape[0],))],
        compiler_params=kernel_params(ident),
        cost_estimate=pl.CostEstimate(
            flops=2 * inner.shape[0] * inner.shape[1] * width, bytes_accessed=pair * n * rows * width * 40, transcendentals=0
        ),
        name=f"down_{ident}",
    )(inner, wd, hidden, gains, cotangent)


def grad_kernel(
    pair, g, wd, gate, up, inner_t, grad_gate, grad_up, gate_t, up_t, down_term,
    gs_v, w_v, g_v, u_v, gg_v, gu_v, gt_v, ut_v, it_v, acc, low_v, send, recv, sems
):
    place = Place(pair)
    moves = Moves(sems)
    deep = down_term.shape[2]
    loads = [moves.start(wd, w_v)]
    loads += [moves.start(gate, g_v), moves.start(up, u_v), moves.start(inner_t, it_v)]
    rows, width = g.shape
    block, share = 2 * rows, wd.shape[0]
    gs_v[place.q, place.s] = g[...]
    place.barrier()
    n = gs_v.shape[1]
    step = min(256, share)
    waited = []

    def ready(q, chip):
        new = not waited
        if new:
            moves.wait(loads)
            waited.append(True)
        slots = pl.ds(2 * chip, 2)
        here = pl.ds(pl.multiple_of(q * n * rows + chip * block, block), block)

        @pl.loop(0, share // step)
        def _(j):
            cols = pl.ds(pl.multiple_of(j * step, step), step)
            a = gs_v[q, slots].reshape(block, width)
            e = dot(a, w_v[cols, :], NT)
            v, u = g_v[here, cols], u_v[here, cols]
            s = 1.0 / (1.0 + jnp.exp(-v))
            dg = e * u * s * (1.0 + v * (1.0 - s))
            du = e * v * s
            gg_v[here, cols] = dg.astype(BF16)
            gu_v[here, cols] = du.astype(BF16)
            gt_v[cols, here] = dg.T.astype(BF16)
            ut_v[cols, here] = du.T.astype(BF16)

        wide = min(512, width)

        @pl.loop(0, width // wide)
        def _(j):
            cols = pl.ds(pl.multiple_of(j * wide, wide), wide)
            part = dot(it_v[:, here], gs_v[q, slots, :, cols].reshape(block, wide), NN)
            if new:
                acc[:, cols] = part
            else:
                acc[:, cols] += part

        moves.start(gg_v.at[here], grad_gate.at[here])
        moves.start(gu_v.at[here], grad_up.at[here])

    live = gather_pairs(place, Wires(send, recv), g, gs_v, ready)
    for j in range(down_term.shape[0]):
        low_v[j] = acc[:, pl.ds(j * deep, deep)].astype(BF16)
    moves.start(low_v, down_term)
    moves.start(gt_v, gate_t)
    moves.start(ut_v, up_t)
    for copy in live.values():
        copy.wait_send()
    moves.finish()


def ffn_grad(g, wd, gate, up, inner_t, n, m, pair, ident):
    rows, width = g.shape
    share, long = wd.shape[0], pair * n * rows
    dma = pltpu.SemaphoreType.DMA
    flat, tall = pltpu.VMEM((long, share), BF16), pltpu.VMEM((share, long), BF16)
    return pl.pallas_call(
        functools.partial(grad_kernel, pair),
        in_specs=vmem_specs(1) + any_specs(4),
        out_specs=any_specs(5),
        out_shape=[shape((long, share), BF16)] * 2
        + [shape((share, long), BF16)] * 2
        + [shape((m, share, width // m), BF16)],
        scratch_shapes=[
            pltpu.VMEM((pair, n, rows, width), BF16),
            pltpu.VMEM((share, width), BF16),
            pltpu.VMEM((long, share), F32),
            pltpu.VMEM((long, share), F32),
            flat,
            flat,
            tall,
            tall,
            tall,
            pltpu.VMEM((share, width), F32),
            pltpu.VMEM((m, share, width // m), BF16),
            dma((gather_wires(pair),)),
            dma((gather_wires(pair),)),
            dma((12 + 3 * pair * n // 2,)),
        ],
        compiler_params=kernel_params(ident, 63),
        cost_estimate=pl.CostEstimate(
            flops=2 * long * width * share, bytes_accessed=long * width * 40, transcendentals=0
        ),
        name=f"grad_{ident}",
    )(g, wd, gate, up, inner_t)


def back_kernel(
    pair, gg, gu, wg, wu, gate_t, hs, down_term, branch, gains, cotangent,
    grad_hidden, grad_low, gain_term, down_grad, gate_term,
    a_v, w_v, value, rc, rd, rx, ry, qbuf, zbuf, send, recv,
    gt_v, hs_v, gterm, down_own, down_near, down_total, down_from, dsem, sems
):
    place = Place(pair)
    place.peers.append((place.s, flip(place.f, 1)))
    moves = Moves(sems)
    loads = [moves.start(wg, w_v.at[0]), moves.start(wu, w_v.at[1])]
    loads += [moves.start(gg, a_v.at[0]), moves.start(gu, a_v.at[1])]
    late = [moves.start(gate_t, gt_v)] + [moves.start(hs.at[q], hs_v.at[q]) for q in range(pair)]
    down = Settle(place, dsem, down_term, down_own, down_near, down_total, down_from)
    pieces = term_work(gterm, gt_v, hs_v, lambda: moves.wait(late), gate_term, moves)
    work = Work(pieces[:2] + [down.middle] + pieces[2:])
    rows, width = branch.shape
    block = 2 * rows
    n = value.shape[1]
    step = min(256, width)
    place.barrier()
    down.start()
    moves.wait(loads)

    def make(q, chip, c):
        here = pl.ds(pl.multiple_of(q * n * rows + chip * block, block), block)

        @pl.loop(c * (width // 2) // step, (c + 1) * (width // 2) // step)
        def _(j):
            cols = pl.ds(pl.multiple_of(j * step, step), step)
            part = dot(a_v[0, here, :], w_v[0, cols, :], NT) + dot(a_v[1, here, :], w_v[1, cols, :], NT)
            value[q, pl.ds(2 * chip, 2), :, cols] = part.astype(BF16).reshape(2, rows, step)

    live = scatter_pairs(place, Wires(send, recv), value, rc, rd, rx, ry, qbuf, zbuf, make, grad_hidden, work)
    work.rest()
    grad = cotangent[...].astype(F32) + grad_hidden[...]
    grad_hidden[...] = grad
    back, term = rms_back(branch[...], gains[2:3, :], grad)
    grad_low[...] = back.astype(BF16)
    gain_term[...] = jnp.sum(term, axis=0, keepdims=True)
    share = down_grad.shape[0] // 2

    def store(u, value):
        down_grad[pl.ds(pl.multiple_of(u * share, share), share), :] = value

    down.finish(store)
    for copy in live.values():
        copy.wait_send()
    moves.finish()


def ffn_back(gg, gu, wg, wu, gate_t, hs, down_term, branch, gains, cotangent, n, m, pair, ident):
    rows, width = branch.shape
    share, deep = gate_t.shape[0], width // m
    term = down_term.shape
    dma = pltpu.SemaphoreType.DMA
    return pl.pallas_call(
        functools.partial(back_kernel, pair),
        in_specs=any_specs(7) + vmem_specs(3),
        out_specs=vmem_specs(4) + any_specs(1),
        out_shape=[
            shape((rows, width), F32),
            shape((rows, width), BF16),
            shape((1, width), F32),
            shape((2 * share, deep), F32),
            shape(term, BF16),
        ],
        scratch_shapes=[
            pltpu.VMEM((2,) + gg.shape, BF16),
            pltpu.VMEM((2,) + wg.shape, BF16),
            pltpu.VMEM((pair, n, rows, width), BF16),
        ]
        + scatter_scratch(pair, rows, width)
        + [pltpu.VMEM(v.shape, BF16) for v in (gate_t, hs)]
        + [pltpu.VMEM(term, BF16)]
        + settle_scratch(share, deep)
        + [dma((20,))],
        compiler_params=kernel_params(ident, 63),
        cost_estimate=pl.CostEstimate(
            flops=4 * gg.shape[0] * gg.shape[1] * width, bytes_accessed=pair * n * rows * width * 40, transcendentals=0
        ),
        name=f"back_{ident}",
    )(gg, gu, wg, wu, gate_t, hs, down_term, branch, gains, cotangent)


def opposite(f):
    return (f + 2) % 4


class Stream:
    def __init__(self, place, sems):
        self.place, self.sems = place, sems
        f = place.f
        self.half, self.far_f, self.near_f = f // 2, opposite(f), flip(f, 1)
        self.far, self.near = (place.s, self.far_f), (place.s, self.near_f)

    def remote(self, k, step, src, dst, device):
        return pltpu.make_async_remote_copy(
            src, dst, self.sems.at[k, step, 0], self.sems.at[k, step, 1], device_id=device, device_id_type=MESH
        )

    def far_copy(self, k, view, full):
        return self.remote(k, 0, view(1 - self.half), full.at[self.place.f], self.far)

    def near_copy(self, k, view, full):
        return self.remote(k, 1, view(self.half), full.at[self.place.f], self.near)

    def own_copy(self, k, view, full):
        return pltpu.make_async_copy(view(self.half), full.at[self.place.f], self.sems.at[k, 3, 0])

    def relay_copy(self, k, full):
        return self.remote(k, 2, full.at[self.far_f], full.at[self.far_f], self.near)

    def start_far(self, k, view, full):
        self.far_copy(k, view, full).start()

    def start_near(self, k, view, full):
        self.near_copy(k, view, full).start()
        self.own_copy(k, view, full).start()

    def relay(self, k, view, full):
        self.far_copy(k, view, full).wait_recv()
        self.relay_copy(k, full).start()

    def finish(self, k, view, full):
        self.near_copy(k, view, full).wait_recv()
        self.relay_copy(k, full).wait_recv()
        self.own_copy(k, view, full).wait()
        self.far_copy(k, view, full).wait_send()
        self.near_copy(k, view, full).wait_send()
        self.relay_copy(k, full).wait_send()


def half_columns(ref, share):
    return lambda u: ref.at[:, pl.ds(pl.multiple_of(u * share, share), share)]


def half_rows(ref, share):
    return lambda u: ref.at[pl.ds(pl.multiple_of(u * share, share), share), :]


def full_barrier(place, n, near):
    sem = pltpu.get_barrier_semaphore()
    s, f = place.s, place.f
    for d in range(1, n):
        pl.semaphore_signal(sem, inc=1, device_id=((s + d) % n, f), device_id_type=MESH)
    for other in near:
        pl.semaphore_signal(sem, inc=1, device_id=(s, other), device_id_type=MESH)
    pl.semaphore_wait(sem, n - 1 + len(near))


def swap_halves(v):
    return pltpu.roll(v, HD // 2, axis=1)


def to_rows(first, second):
    rows = first.shape[0]
    lane = lax.broadcasted_iota(jnp.int32, (rows, 128), 1)
    wide = jnp.where(lane == 0, first, jnp.where(lane == 1, second, 0.0))
    return wide.T[:8]


def to_columns(v):
    return jnp.concatenate([v, jnp.zeros((120, v.shape[1]), F32)], axis=0).T


def exchange(place, n, own, held, send, recv):
    copies = []
    for d in range(1, n):
        copy = pltpu.make_async_remote_copy(
            own,
            held.at[d - 1],
            send.at[d - 1],
            recv.at[d - 1],
            device_id=((place.s + d) % n, place.f),
            device_id_type=MESH,
        )
        copy.start()
        copies.append(copy)
    total = own[...]
    for d in range(1, n):
        copies[d - 1].wait_recv()
        total = total + held[d - 1]
    return total, copies


def attend(block, q_v, k_v, v_v, out_v, low_v, lt_v, log_v):
    length = q_v.shape[0]
    scale = HD ** (-0.5)

    @pl.loop(0, q_v.shape[1] // HD)
    def _(h):
        cols = pl.ds(pl.multiple_of(h * HD, HD), HD)
        for i in range(length // block):
            rows, wide = pl.ds(i * block, block), pl.ds(0, (i + 1) * block)
            s = dot(q_v[rows, cols], k_v[wide, cols], NT) * scale
            column = lax.broadcasted_iota(jnp.int32, s.shape, 1)
            row = lax.broadcasted_iota(jnp.int32, s.shape, 0) + i * block
            s = jnp.where(column <= row, s, -jnp.inf)
            top = jnp.max(s, axis=-1, keepdims=True)
            p = jnp.exp(s - top)
            total = jnp.sum(p, axis=-1, keepdims=True)
            out = dot((p * (1.0 / total)).astype(BF16), v_v[wide, cols], NN)
            out_v[rows, cols] = out
            low_v[rows, cols] = out.astype(BF16)
            lt_v[cols, rows] = out.T.astype(BF16)
            log_v[h, rows, :] = top + jnp.log(total)


def attention_kernel(
    x, gains, tables, xs, qkv, wo_own, gate_w, up_w, down_w,
    raw, heads, attended, low_t, xs_t, log_total, inverse, branch, hidden, hidden_low, wg, wu, wo,
    xs_v, xt_v, lt_v, w_v, wo_v, raw_v, heads_v, out_v, low_v, log_v, small, held, value,
    rc, rd, rx, ry, qbuf, zbuf, send, recv, ssend, srecv, zsem, osem, sems,
):
    place = Place(1)
    n, m = xs.shape[1], qkv.shape[1]
    rows, width = x.shape
    length, cols = raw.shape[1], raw.shape[2]
    share = wg.shape[2]
    moves = Moves(sems)
    loads = [moves.start(xs.at[0], xs_v)]
    for j in range(3):
        for f in range(m):
            loads.append(moves.start(qkv.at[j, f], w_v.at[j, :, f]))
    own_out = [moves.start(wo_own, wo_v.at[place.f])]
    full_barrier(place, n, [(place.f + d) % m for d in range(1, m)])
    out_copies = []
    for d, plane in enumerate((flip(place.f, 1), opposite(place.f), opposite(flip(place.f, 1)))):
        out_copies.append(
            pltpu.make_async_remote_copy(
                wo_own, wo_v.at[place.f], osem.at[0, d], osem.at[1, d], device_id=(place.s, plane), device_id_type=MESH
            )
        )
        out_copies[-1].start()
    stream = Stream(place, zsem)
    views = [half_columns(gate_w, share), half_columns(up_w, share)]
    fulls = [wg, wu]
    for k in range(2):
        stream.start_far(k, views[k], fulls[k])
    for k in range(2):
        stream.start_near(k, views[k], fulls[k])
    moves.wait(loads)
    block = min(256, length)
    per = block // rows

    @pl.loop(0, length // block)
    def _(i):
        here = pl.ds(pl.multiple_of(i * block, block), block)
        a = xs_v[pl.ds(i * per, per)].reshape(block, width)
        q = dot(a, w_v[0].reshape(width, cols), NN)
        k = dot(a, w_v[1].reshape(width, cols), NN)
        raw_v[0, here, :] = q
        raw_v[1, here, :] = k
        heads_v[2, here, :] = dot(a, w_v[2].reshape(width, cols), NN).astype(BF16)
        xt_v[:, here] = a.T
        small[0, :, here] = to_rows(
            jnp.sum(q * q, axis=1, keepdims=True), jnp.sum(k * k, axis=1, keepdims=True)
        )

    moves.start(raw_v, raw)
    moves.start(xt_v, xs_t)
    first_col = pl.multiple_of(place.s * cols, cols)
    total, stat_copies = exchange(place, n, small.at[0], held, ssend, srecv)
    small[1] = lax.rsqrt(total * (1.0 / width) + EPSILON)
    moves.start(small.at[1], inverse)

    @pl.loop(0, length // block)
    def _(i):
        here = pl.ds(pl.multiple_of(i * block, block), block)
        inv = to_columns(small[1, :, here])
        cosine, sine = tables[0, here, :], tables[1, here, :]
        for j in range(2):
            for h in range(cols // HD):
                part = pl.ds(h * HD, HD)
                v = raw_v[j, here, part] * inv[:, j : j + 1] * gains[j : j + 1, pl.ds(first_col + h * HD, HD)]
                heads_v[j, here, part] = (v * cosine + swap_halves(v) * sine).astype(BF16)

    moves.start(heads_v, heads)
    attend(block, heads_v.at[0], heads_v.at[1], heads_v.at[2], out_v, low_v, lt_v, log_v)
    moves.start(out_v, attended)
    moves.start(lt_v, low_t)
    moves.start(log_v, log_total)
    moves.wait(own_out)
    for copy in out_copies:
        copy.wait_recv()
    moves.start(wo_v, wo)
    step = min(512, width)

    def make(q, chip, c):
        here = pl.ds(pl.multiple_of(chip * 2 * rows, 2 * rows), 2 * rows)

        @pl.loop(c * (width // 2) // step, (c + 1) * (width // 2) // step)
        def _(j):
            at = pl.ds(pl.multiple_of(j * step, step), step)
            part = dot(low_v[here, :], wo_v[:, :, at].reshape(cols, step), NN).astype(BF16)
            value[q, pl.ds(2 * chip, 2), :, at] = part.reshape(2, rows, step)

    live = scatter_pairs(
        place, Wires(send, recv), value, rc, rd, rx, ry, qbuf, zbuf, make, branch,
        Work([lambda: None, lambda: stream.relay(0, views[0], fulls[0])]),
    )
    total = branch[...]
    inv = lax.rsqrt(jnp.mean(total * total, axis=-1, keepdims=True) + EPSILON)
    h = x[...].astype(F32) + total * inv * gains[2:3, :]
    hidden[...] = h
    hidden_low[...] = h.astype(BF16)
    stream.relay(1, views[1], fulls[1])
    for copy in list(live.values()) + stat_copies:
        copy.wait_send()
    moves.finish()
    for k in range(2):
        stream.finish(k, views[k], fulls[k])
    for copy in out_copies:
        copy.wait_send()


def attention_half(x, gains, tables, xs, qkv, wo, gate_w, up_w, down_w, ident):
    rows, width = x.shape
    n, m, part, cols = xs.shape[1], qkv.shape[1], qkv.shape[3], qkv.shape[4]
    length, share = n * rows, gate_w.shape[1] // 2
    dma = pltpu.SemaphoreType.DMA
    heads = cols // HD
    outs = [
        shape((2, length, cols), F32),
        shape((3, length, cols), BF16),
        shape((length, cols), F32),
        shape((cols, length), BF16),
        shape((width, length), BF16),
        shape((heads, length, 1), F32),
        shape((8, length), F32),
        shape((rows, width), F32),
        shape((rows, width), F32),
        shape((rows, width), BF16),
        shape((m,) + (gate_w.shape[0], share), BF16),
        shape((m,) + (gate_w.shape[0], share), BF16),
        shape((m,) + wo.shape, BF16),
    ]
    return pl.pallas_call(
        attention_kernel,
        in_specs=vmem_specs(3) + any_specs(6),
        out_specs=any_specs(7) + vmem_specs(3) + any_specs(3),
        out_shape=outs,
        scratch_shapes=[
            pltpu.VMEM((n, rows, width), BF16),
            pltpu.VMEM((width, length), BF16),
            pltpu.VMEM((cols, length), BF16),
            pltpu.VMEM((3, n, m, part, cols), BF16),
            pltpu.VMEM((m,) + wo.shape, BF16),
            pltpu.VMEM((2, length, cols), F32),
            pltpu.VMEM((3, length, cols), BF16),
            pltpu.VMEM((length, cols), F32),
            pltpu.VMEM((length, cols), BF16),
            pltpu.VMEM((heads, length, 1), F32),
            pltpu.VMEM((2, 8, length), F32),
            pltpu.VMEM((n - 1, 8, length), F32),
            pltpu.VMEM((1, n, rows, width), BF16),
        ]
        + scatter_scratch(1, rows, width)
        + [dma((n - 1,)), dma((n - 1,)), dma((2, 4, 2)), dma((2, m)), dma((20 + 3 * m,))],
        compiler_params=kernel_params(ident),
        cost_estimate=pl.CostEstimate(flops=10**10, bytes_accessed=200 * 2**20, transcendentals=0),
        name=f"attention_{ident}",
    )(x, gains, tables, xs, qkv, wo, gate_w, up_w, down_w)


class Settle:
    def __init__(self, place, sems, term, own, near, total, far):
        self.place, self.sems, self.term, self.own = place, sems, term, own
        self.near, self.total, self.far = near, total, far
        f = place.f
        self.f = f
        self.odd, self.half = f % 2, f // 2

    def remote(self, step, src, dst, plane):
        return pltpu.make_async_remote_copy(
            src, dst, self.sems.at[step, 0], self.sems.at[step, 1], device_id=(self.place.s, plane), device_id_type=MESH
        )

    def given(self, i):
        return 1 - self.odd + 2 * i

    def kept(self, i):
        return self.odd + 2 * i

    def near_copy(self, step):
        i = 1 - self.half if step == 0 else self.half
        return self.remote(step, self.term.at[self.given(i)], self.near.at[i], flip(self.f, 1))

    def far_copy(self):
        return self.remote(2, self.total.at[0], self.far, opposite(self.f))

    def load(self, i):
        return pltpu.make_async_copy(self.term.at[self.kept(i)], self.own.at[i], self.sems.at[3, i])

    def start(self):
        self.near_copy(0).start()
        for i in (0, 1):
            self.load(i).start()

    def mine(self, i):
        return self.term[self.kept(i)] if self.own is None else self.own[i]

    def middle(self):
        if self.own is not None:
            for i in (0, 1):
                self.load(i).wait()
        self.near_copy(0).wait_recv()
        other = 1 - self.half
        self.total[0] = add(self.mine(other), self.near[other])
        self.far_copy().start()
        self.near_copy(1).start()

    def finish(self, store):
        half = self.half
        self.near_copy(1).wait_recv()
        store(half, self.mine(half).astype(F32) + self.near[half].astype(F32))
        self.far_copy().wait_recv()
        store(1 - half, self.far[...].astype(F32))
        for step in (0, 1):
            self.near_copy(step).wait_send()
        self.far_copy().wait_send()


def settle_scratch(share, depth, own=True):
    block = lambda *lead: pltpu.VMEM(lead + (share, depth), BF16)
    return ([block(2)] if own else []) + [block(2), block(1), block(), pltpu.SemaphoreType.DMA((4, 2))]


def term_block(term, left, right, block):
    deep, long = term.shape[2], left.shape[1]
    step = min(256, deep)

    @pl.loop(0, deep // step)
    def _(j):
        at = pl.ds(pl.multiple_of(block * deep + j * step, step), step)
        to = pl.ds(pl.multiple_of(j * step, step), step)
        term[block, :, to] = dot(left[...], right[:, :, :, at].reshape(long, step), NN).astype(BF16)


class Work:
    def __init__(self, pieces):
        self.pieces = list(pieces)

    def __call__(self):
        if self.pieces:
            self.pieces.pop(0)()

    def rest(self):
        while self.pieces:
            self()


def term_work(term, left, right, prepare, out, moves):
    def piece(block):
        def run():
            if block == 0:
                prepare()
            term_block(term, left, right, block)
            moves.start(term.at[block], out.at[block])

        return run

    return [piece(block) for block in range(term.shape[0])]


def turn(v, cosine, sine):
    return v * cosine + swap_halves(v) * sine


def attend_back(block, q_v, k_v, v_v, out_v, log_v, g_v, dq, dk, dv):
    length = q_v.shape[0]
    scale = HD ** (-0.5)
    dk[...] = jnp.zeros_like(dk)
    dv[...] = jnp.zeros_like(dv)

    @pl.loop(0, q_v.shape[1] // HD)
    def _(h):
        cols = pl.ds(pl.multiple_of(h * HD, HD), HD)
        for i in range(length // block):
            rows, wide = pl.ds(i * block, block), pl.ds(0, (i + 1) * block)
            q, g = q_v[rows, cols], g_v[rows, cols]
            s = dot(q, k_v[wide, cols], NT) * scale
            column = lax.broadcasted_iota(jnp.int32, s.shape, 1)
            row = lax.broadcasted_iota(jnp.int32, s.shape, 0) + i * block
            s = jnp.where(column <= row, s, -jnp.inf)
            weights = jnp.exp(s - log_v[h, rows, :])
            correction = jnp.sum(g.astype(F32) * out_v[rows, cols], axis=-1, keepdims=True)
            gw = dot(g, v_v[wide, cols], NT)
            gs = (weights * (gw - correction)).astype(BF16)
            dq[rows, cols] = dot(gs, k_v[wide, cols], NN) * scale
            dk[wide, cols] += dot(gs, q, TN) * scale
            dv[wide, cols] += dot(weights.astype(BF16), g, TN)


def attention_back_kernel(
    g, gains, tables, inverse, wo, raw, heads, attended, low_t, log_total, xs_t, gate_term, up_t, hs,
    d3, term, gain_term, gate_grad, up_grad,
    bs, wo_v, raw_v, heads_v, out_v, low_v, log_v, ga_v, dq, dk, dv, d_v, xs_v, term_v, small, held,
    ut_v, hs_v, up_term, gown, gnear, gtotal, gfar, gsem, unear, utotal, ufar, usem,
    send, recv, ssend, srecv, sems,
):
    place = Place(1)
    n, m = bs.shape[1], wo.shape[0]
    rows, width = g.shape
    length, cols = raw.shape[1], raw.shape[2]
    share = gate_term.shape[1]
    first_col = pl.multiple_of(place.s * cols, cols)
    moves = Moves(sems)
    second = [moves.start(wo, wo_v)]
    fourth = [
        moves.start(heads, heads_v),
        moves.start(attended, out_v),
        moves.start(log_total, log_v),
        moves.start(low_t, low_v),
        moves.start(raw, raw_v),
        moves.start(xs_t, xs_v),
    ]
    bs[0, place.s] = g[...]
    full_barrier(place, n, [opposite(place.f), flip(place.f, 1)])
    gate = Settle(place, gsem, gate_term, gown, gnear, gtotal, gfar)
    up = Settle(place, usem, up_term, None, unear, utotal, ufar)
    gate.start()
    late = [moves.start(up_t, ut_v)] + [moves.start(hs.at[q], hs_v.at[q]) for q in range(hs.shape[0])]

    def up_block(i):
        b = (up.given(1 - up.half), up.given(up.half), up.kept(1 - up.half), up.kept(up.half))[i]
        if i == 0:
            moves.wait(late)
        term_block(up_term, ut_v, hs_v, b)
        if i == 0:
            up.near_copy(0).start()

    block = min(256, length)
    waited = []

    def ready(q, chip):
        if not waited:
            moves.wait(second)
            waited.append(True)
        here = pl.ds(pl.multiple_of(chip * 2 * rows, 2 * rows), 2 * rows)
        a = bs[0, pl.ds(2 * chip, 2)].reshape(2 * rows, width)
        ga_v[here, :] = dot(a, wo_v[...].reshape(cols, width), NT).astype(BF16)

    live = gather_pairs(place, Wires(send, recv), g, bs, ready, Work([lambda: up_block(0), lambda: up_block(2), gate.middle]))
    up_block(1)
    up.middle()
    moves.wait(fourth)
    up_block(3)
    attend_back(block, heads_v.at[0], heads_v.at[1], heads_v.at[2], out_v, log_v, ga_v, dq, dk, dv)
    @pl.loop(0, length // block)
    def _(i):
        here = pl.ds(pl.multiple_of(i * block, block), block)
        inv = to_columns(inverse[:, here])
        cosine, sine = tables[0, here, :], -tables[1, here, :]
        sums = []
        for j, d in enumerate((dq, dk)):
            total = jnp.zeros((block, 1), F32)
            for h in range(cols // HD):
                part = pl.ds(h * HD, HD)
                normal = raw_v[j, here, part] * inv[:, j : j + 1]
                v = turn(d[here, part].astype(BF16).astype(F32), cosine, sine)
                raw_v[j, here, part] = normal
                gained = v * gains[j : j + 1, pl.ds(first_col + h * HD, HD)]
                total = total + jnp.sum(gained * normal, axis=1, keepdims=True)
                term_sum = jnp.sum(v * normal, axis=0, keepdims=True)
                d[here, part] = gained

                @pl.when(i == 0)
                def _():
                    gain_term[j, :, part] = term_sum

                @pl.when(i > 0)
                def _():
                    gain_term[j, :, part] += term_sum

            sums.append(total)
        small[0, :, here] = to_rows(sums[0], sums[1])
        d_v[2, here, :] = dv[here, :].astype(BF16)

    total, stat_copies = exchange(place, n, small.at[0], held, ssend, srecv)
    small[1] = total * (1.0 / width)

    @pl.loop(0, length // block)
    def _(i):
        here = pl.ds(pl.multiple_of(i * block, block), block)
        inv = to_columns(inverse[:, here])
        mean = to_columns(small[1, :, here])
        for j, d in enumerate((dq, dk)):
            d_v[j, here, :] = (
                inv[:, j : j + 1] * (d[here, :] - raw_v[j, here, :] * mean[:, j : j + 1])
            ).astype(BF16)

    moves.start(d_v, d3)

    @pl.loop(0, n)
    def _(i):
        at = pl.ds(pl.multiple_of(i * cols, cols), cols)
        part = dot(low_v[...], bs[0, :, :, at].reshape(length, cols), NN)
        term_v[3, i] = part.astype(BF16).reshape(m, cols // m, cols)
        for j in range(3):
            part = dot(xs_v[at, :], d_v[j], NN)
            term_v[j, i] = part.astype(BF16).reshape(m, cols // m, cols)

    moves.start(term_v, term)

    def store(ref):
        def put(u, value):
            ref[:, pl.ds(pl.multiple_of(u * share, share), share)] = value.T

        return put

    gate.finish(store(gate_grad))
    up.finish(store(up_grad))
    for copy in list(live.values()) + stat_copies:
        copy.wait_send()
    moves.finish()


def attention_back(g, gains, tables, inverse, wo, raw, heads, attended, low_t, log_total, xs_t, gate_term, up_t, hs, n, ident):
    rows, width = g.shape
    m = wo.shape[0]
    length, cols = raw.shape[1], raw.shape[2]
    share, deep = gate_term.shape[1], width // m
    dma = pltpu.SemaphoreType.DMA
    vmem = pltpu.VMEM
    outs = [
        shape((3, length, cols), BF16),
        shape((4, n, m, cols // m, cols), BF16),
        shape((2, 1, cols), F32),
        shape((deep, 2 * share), F32),
        shape((deep, 2 * share), F32),
    ]
    return pl.pallas_call(
        attention_back_kernel,
        in_specs=vmem_specs(4) + any_specs(10),
        out_specs=any_specs(2) + vmem_specs(3),
        out_shape=outs,
        scratch_shapes=[
            vmem((1, n, rows, width), BF16),
            vmem(wo.shape, BF16),
            vmem(raw.shape, F32),
            vmem(heads.shape, BF16),
            vmem(attended.shape, F32),
            vmem(low_t.shape, BF16),
            vmem(log_total.shape, F32),
            vmem((length, cols), BF16),
            vmem((length, cols), F32),
            vmem((length, cols), F32),
            vmem((length, cols), F32),
            vmem((3, length, cols), BF16),
            vmem(xs_t.shape, BF16),
            vmem((4, n, m, cols // m, cols), BF16),
            vmem((2, 8, length), F32),
            vmem((n - 1, 8, length), F32),
        ]
        + [vmem(up_t.shape, BF16), vmem(hs.shape, BF16), vmem(gate_term.shape, BF16)]
        + settle_scratch(share, deep)
        + settle_scratch(share, deep, False)
        + [
            dma((gather_wires(1),)),
            dma((gather_wires(1),)),
            dma((n - 1,)),
            dma((n - 1,)),
            dma((20,)),
        ],
        compiler_params=kernel_params(ident, 63),
        cost_estimate=pl.CostEstimate(flops=10**10, bytes_accessed=200 * 2**20, transcendentals=0),
        name=f"attention_back_{ident}",
    )(g, gains, tables, inverse, wo, raw, heads, attended, low_t, log_total, xs_t, gate_term, up_t, hs)


def attention_forward_kernel(block, q_ref, k_ref, v_ref, out_ref, low_ref, log_ref):
    length = q_ref.shape[0]
    scale = HD ** (-0.5)
    for i in range(length // block):
        rows = pl.ds(i * block, block)
        width = (i + 1) * block
        s = dot(q_ref[rows, :], k_ref[pl.ds(0, width), :], NT) * scale
        column = lax.broadcasted_iota(jnp.int32, (block, width), 1)
        row = lax.broadcasted_iota(jnp.int32, (block, width), 0) + i * block
        s = jnp.where(column <= row, s, -jnp.inf)
        top = jnp.max(s, axis=-1, keepdims=True)
        p = jnp.exp(s - top)
        total = jnp.sum(p, axis=-1, keepdims=True)
        weights = (p * (1.0 / total)).astype(BF16)
        out = dot(weights, v_ref[pl.ds(0, width), :], NN)
        out_ref[rows, :] = out
        low_ref[rows, :] = out.astype(BF16)
        log_ref[0, rows, :] = top + jnp.log(total)


def attention_forward(q, k, v):
    length, width = q.shape
    heads = width // HD
    block = min(256, length)
    column = pl.BlockSpec((length, HD), lambda h: (0, h))
    return pl.pallas_call(
        functools.partial(attention_forward_kernel, block),
        grid=(heads,),
        in_specs=[column] * 3,
        out_specs=[column, column, pl.BlockSpec((1, length, 1), lambda h: (h, 0, 0))],
        out_shape=[
            jax.ShapeDtypeStruct((length, width), F32),
            jax.ShapeDtypeStruct((length, width), BF16),
            jax.ShapeDtypeStruct((heads, length, 1), F32),
        ],
        cost_estimate=pl.CostEstimate(
            flops=2 * heads * length * length * HD, bytes_accessed=10 * length * width, transcendentals=0
        ),
    )(q, k, v)


def attention_backward_kernel(block, q_ref, k_ref, v_ref, out_ref, log_ref, g_ref, dq_ref, dk_ref, dv_ref, dk, dv):
    length = q_ref.shape[0]
    scale = HD ** (-0.5)
    dk[...] = jnp.zeros_like(dk)
    dv[...] = jnp.zeros_like(dv)
    for i in range(length // block):
        rows = pl.ds(i * block, block)
        width = (i + 1) * block
        wide = pl.ds(0, width)
        q = q_ref[rows, :]
        g = g_ref[rows, :]
        s = dot(q, k_ref[wide, :], NT) * scale
        column = lax.broadcasted_iota(jnp.int32, (block, width), 1)
        row = lax.broadcasted_iota(jnp.int32, (block, width), 0) + i * block
        s = jnp.where(column <= row, s, -jnp.inf)
        weights = jnp.exp(s - log_ref[0, rows, :])
        correction = jnp.sum(g.astype(F32) * out_ref[rows, :], axis=-1, keepdims=True)
        gw = dot(g, v_ref[wide, :], NT)
        gs = (weights * (gw - correction)).astype(BF16)
        dq_ref[rows, :] = (dot(gs, k_ref[wide, :], NN) * scale).astype(BF16)
        dk[wide, :] += dot(gs, q, TN)
        dv[wide, :] += dot(weights.astype(BF16), g, TN)
    dk_ref[...] = (dk[...] * scale).astype(BF16)
    dv_ref[...] = dv[...].astype(BF16)


def attention_backward(q, k, v, out, log_total, g):
    length, width = q.shape
    heads = width // HD
    block = min(256, length)
    column = pl.BlockSpec((length, HD), lambda h: (0, h))
    return pl.pallas_call(
        functools.partial(attention_backward_kernel, block),
        grid=(heads,),
        in_specs=[column] * 4 + [pl.BlockSpec((1, length, 1), lambda h: (h, 0, 0)), column],
        out_specs=[column] * 3,
        out_shape=[jax.ShapeDtypeStruct((length, width), BF16)] * 3,
        scratch_shapes=[pltpu.VMEM((length, HD), F32)] * 2,
        cost_estimate=pl.CostEstimate(
            flops=5 * heads * length * length * HD, bytes_accessed=16 * length * width, transcendentals=0
        ),
    )(q, k, v, out, log_total, g)


def on_device(n, m, pair, *args):
    (
        tokens,
        query_weight,
        key_weight,
        value_weight,
        out_weight,
        query_gain,
        key_gain,
        attention_gain,
        gate_weight,
        up_weight,
        down_weight,
        feedforward_gain,
        cotangent,
    ) = args
    rows, width = tokens.shape[1], tokens.shape[2]
    length = rows * n
    part = query_weight.shape[0]
    cols = width // n
    depth, units = gate_weight.shape
    share = units // pair
    x = tokens.reshape(rows, width)
    groups = [[g * pair + u for u in range(pair)] for g in range(m // pair)]

    native = n == 8 and m == 4

    def gather_plane(v, ident):
        if native:
            return plane_gather(v, n, 1, ident)
        return lax.all_gather(v, "seq", axis=0, tiled=True)

    def scatter_plane(v, ident):
        if native:
            return plane_scatter(v, n, 1, ident)
        return lax.psum_scatter(v.astype(BF16), "seq", scatter_dimension=0, tiled=True).astype(F32)

    def gather_pair(v, ident):
        if native:
            return plane_gather(v, n, pair, ident)
        if pair > 1:
            v = lax.all_gather(v, "fsdp", axis=0, axis_index_groups=groups)
        v = lax.all_gather(v.reshape(pair, rows, width), "seq", axis=1, tiled=True)
        return v.reshape(pair * length, width)

    def scatter_pair(v, ident):
        if native:
            return plane_scatter(v, n, pair, ident)
        v = lax.psum_scatter(v.astype(BF16).reshape(pair, length, width), "seq", scatter_dimension=1, tiled=True)
        if pair > 1:
            v = lax.psum_scatter(v, "fsdp", scatter_dimension=0, axis_index_groups=groups)
        return v.reshape(rows, width).astype(F32)

    def total_plane(v, ident):
        return plane_sum(v, n, ident) if native else lax.psum(v, "seq")

    def spread(halves):
        return lax.all_to_all(jnp.tile(halves, (m // pair, 1, 1)), "fsdp", 0, 0, tiled=False)

    def settle(blocks):
        back = lax.all_to_all(blocks.astype(BF16), "fsdp", 0, 0, tiled=False)
        if native:
            return jnp.sum(back.reshape((pair, m // pair) + back.shape[1:]).astype(F32), axis=1)
        return jnp.sum(back.reshape((m // pair, pair) + back.shape[1:]).astype(F32), axis=0)

    gains = jnp.stack([query_gain, key_gain, attention_gain, feedforward_gain]).astype(F32)
    grad_out = cotangent.reshape(rows, width)
    if native:
        xs, qkv, gains, tables = entry(
            x, query_weight, key_weight, value_weight, jnp.pad(gains, ((0, 4), (0, 128 - part))), n, m, 1
        )
        raw, heads, attended, low_t, xs_t, log_total, inverse, branch, hidden, hidden_low, gate_cols, up_cols, out_rows = (
            attention_half(x, gains, tables, xs, qkv, out_weight, gate_weight, up_weight, down_weight, 3)
        )
        gate_cols, up_cols = gate_cols.reshape(width, share), up_cols.reshape(width, share)
        hs, gate, up, inner, inner_t, down_rows = ffn_up(hidden_low, gate_cols, up_cols, down_weight, n, pair, 5)
        layer_out, grad_low, feed_gain_term, down_rows = ffn_down(
            inner, down_rows, hidden, gains, grad_out, n, pair, 7
        )
        grad_gate, grad_up, gate_t, up_t, down_term = ffn_grad(
            grad_low, down_rows, gate, up, inner_t, n, m, pair, 6
        )
        grad_hidden, branch_low, branch_gain_term, down_grad, gate_term = ffn_back(
            grad_gate, grad_up, gate_cols, up_cols, gate_t, hs, down_term, branch, gains, grad_out, n, m, pair, 8
        )
        d3, term, gain_own, gate_grad, up_grad = attention_back(
            branch_low, gains, tables, inverse, out_rows, raw, heads, attended, low_t, log_total,
            xs_t, gate_term, up_t, hs, n, 2
        )
        tokens_grad, term, gain_grads = leave(
            d3, term, gain_own, branch_gain_term, feed_gain_term, grad_hidden, qkv, n, m, 4
        )
        layer_out, tokens_grad, *term, gate_grad, up_grad, down_grad = place_outputs(
            [layer_out, tokens_grad, term, gate_grad, up_grad, down_grad]
        )
        out_grad = term[3]
    else:
        cosine, sine = angles_of(length)
        seq = lax.axis_index("seq")
        stacked = jnp.stack([query_weight, key_weight, value_weight]).reshape(3, part, n, cols)
        mine = lax.all_to_all(stacked.transpose(2, 0, 1, 3), "seq", 0, 0)
        qkv = lax.all_gather(mine, "fsdp", axis=1).transpose(2, 0, 1, 3, 4).reshape(3, width, cols)
        full_gain = lax.all_gather(gains, ("seq", "fsdp"), axis=1).reshape(4, width)
        xs = gather_plane(x, 1)
        out_rows = lax.all_gather(out_weight, "fsdp", axis=0, tiled=True)
        own_gain = lax.dynamic_slice_in_dim(full_gain[:2], seq * cols, cols, 1)
        q_gain, k_gain, branch_gain, feed_gain = own_gain[0], own_gain[1], full_gain[2], full_gain[3]
        q_raw, k_raw, v = dot(xs, qkv[0], NN), dot(xs, qkv[1], NN), dot(xs, qkv[2], NN).astype(BF16)
        squares = jnp.stack([jnp.sum(q_raw * q_raw, axis=1), jnp.sum(k_raw * k_raw, axis=1)])
        inverse = lax.rsqrt(lax.psum(squares, "seq") / width + EPSILON)
        q_inv, k_inv = inverse[0][:, None], inverse[1][:, None]
        q = rotate(q_raw * q_inv * q_gain, cosine, sine, 1.0).astype(BF16)
        k = rotate(k_raw * k_inv * k_gain, cosine, sine, 1.0).astype(BF16)
        attended, attended_low, log_total = attention_forward(q, k, v)
        branch = scatter_plane(dot(attended_low, out_rows, NN), 3)
        branch_inv = lax.rsqrt(jnp.mean(branch * branch, axis=1, keepdims=True) + EPSILON)
        hidden = x.astype(F32) + branch * branch_inv * branch_gain
        hidden_low = hidden.astype(BF16)
        gate_cols = spread(gate_weight.reshape(depth, pair, share).transpose(1, 0, 2)).reshape(width, share)
        up_cols = spread(up_weight.reshape(depth, pair, share).transpose(1, 0, 2)).reshape(width, share)
        down_rows = spread(down_weight.reshape(pair, share, depth)).transpose(1, 0, 2).reshape(share, width)
        grad_out = grad_out.astype(F32)
        hs = gather_pair(hidden_low, 5)
        gate = dot(hs, gate_cols, NN)
        up = dot(hs, up_cols, NN)
        sig = jax.nn.sigmoid(gate)
        inner = (gate * sig * up).astype(BF16)
        feed = scatter_pair(dot(inner, down_rows, NN), 7)
        feed_inv = lax.rsqrt(jnp.mean(feed * feed, axis=1, keepdims=True) + EPSILON)
        layer_out = (hidden + feed * feed_inv * feed_gain).astype(BF16)
        grad_feed, term = rms_back(feed, feed_gain, grad_out)
        feed_gain_term = jnp.sum(term, axis=0)
        gs = gather_pair(grad_feed.astype(BF16), 6)
        grad_inner = dot(gs, down_rows, NT)
        grad_gate = (grad_inner * up * sig * (1.0 + gate * (1.0 - sig))).astype(BF16)
        grad_up = (grad_inner * gate * sig).astype(BF16)
        grad_hidden = grad_out + scatter_pair(dot(grad_gate, gate_cols, NT) + dot(grad_up, up_cols, NT), 8)
        grad_branch, term = rms_back(branch, branch_gain, grad_hidden)
        branch_low = grad_branch.astype(BF16)
        branch_gain_term = jnp.sum(term, axis=0)
        inner_t, gate_t, up_t = inner.T, grad_gate.T, grad_up.T

        def cut(v):
            return v.reshape(share, m, depth).transpose(1, 0, 2)

        down_grad = settle(cut(dot(inner_t, gs, NN))).reshape(units, depth)
        gate_grad = settle(cut(dot(gate_t, hs, NN))).transpose(2, 0, 1).reshape(depth, units)
        up_grad = settle(cut(dot(up_t, hs, NN))).transpose(2, 0, 1).reshape(depth, units)
        bs = gather_plane(branch_low, 2)
        out_grad = lax.psum_scatter(
            dot(attended_low, bs, TN).astype(BF16), "fsdp", scatter_dimension=0, tiled=True
        ).astype(F32)
        grad_attended = dot(bs, out_rows, NT).astype(BF16)
        dq, dk, dv = attention_backward(q, k, v, attended, log_total, grad_attended)
        dq = rotate(dq.astype(F32), cosine, sine, -1.0)
        dk = rotate(dk.astype(F32), cosine, sine, -1.0)
        q_normal, k_normal = q_raw * q_inv, k_raw * k_inv
        q_gain_term = jnp.sum(dq * q_normal, axis=0)
        k_gain_term = jnp.sum(dk * k_normal, axis=0)
        dq, dk = dq * q_gain, dk * k_gain
        means = total_plane(jnp.stack([jnp.sum(dq * q_normal, axis=1), jnp.sum(dk * k_normal, axis=1)]), 10) / width
        dq = (q_inv * (dq - q_normal * means[0][:, None])).astype(BF16)
        dk = (k_inv * (dk - k_normal * means[1][:, None])).astype(BF16)
        value = dot(dq, qkv[0], NT) + dot(dk, qkv[1], NT) + dot(dv, qkv[2], NT)
        term = jnp.stack([dot(xs, d, TN).astype(BF16) for d in (dq, dk, dv)]).reshape(3, n, m, part, cols)
        gain_own = jnp.stack([q_gain_term, k_gain_term])
        gain_own = lax.dynamic_update_slice(jnp.zeros((2, width), F32), gain_own, (0, seq * cols))
        gain_terms = jnp.concatenate([gain_own, jnp.stack([branch_gain_term, feed_gain_term])]).reshape(4, n, m, part)
        tokens_grad = grad_hidden + scatter_plane(value, 4)
        term = lax.psum_scatter(term, "fsdp", scatter_dimension=2)
        term = lax.all_to_all(term, "seq", 1, 1).astype(F32).transpose(0, 2, 1, 3)
        gain_grads = lax.psum_scatter(
            gain_terms.reshape(4, width), ("seq", "fsdp"), scatter_dimension=1, tiled=True
        )
        term = term.reshape(3, part, width)

    return (
        layer_out.reshape(tokens.shape),
        tokens_grad.reshape(tokens.shape),
        term[0],
        term[1],
        term[2],
        out_grad,
        gain_grads[0],
        gain_grads[1],
        gain_grads[2],
        gate_grad,
        up_grad,
        down_grad,
        gain_grads[3],
    )


def solution(mesh):
    n, m = mesh.shape["seq"], mesh.shape["fsdp"]
    tall, flat, act = P(("seq", "fsdp"), None), P(("seq", "fsdp")), P("fsdp", "seq", None)
    wide, deep = P("fsdp", "seq"), P("seq", "fsdp")
    return jax.shard_map(
        functools.partial(on_device, n, m, 2),
        mesh=mesh,
        in_specs=(act, tall, tall, tall, tall, flat, flat, flat, wide, wide, deep, flat, act),
        out_specs=(act, act, tall, tall, tall, tall, flat, flat, flat, wide, wide, deep, flat),
        check_vma=False,
    )
```

```python
import functools
import math

import jax
import jax.numpy as jnp
from jax import lax
from jax.experimental import pallas as pl
from jax.experimental.pallas import tpu as pltpu
from jax.sharding import PartitionSpec as P

EPSILON = 1e-06
THETA = 500000.0
HD = 128
F32 = jnp.float32
BF16 = jnp.bfloat16


def dot(a, b, dims):
    return lax.dot_general(a, b, (dims, ((), ())), preferred_element_type=F32)


NN = ((1,), (0,))
NT = ((1,), (1,))
TN = ((0,), (0,))


def angles_of(length):
    half = HD // 2
    frequency = jnp.exp(jnp.arange(half, dtype=F32) * (-2.0 * math.log(THETA) / HD))
    angle = jnp.arange(length, dtype=F32)[:, None] * frequency[None, :]
    return jnp.cos(angle), jnp.sin(angle)


def rotate(value, cosine, sine, sign):
    length, width = value.shape
    value = value.reshape(length, width // HD, 2, HD // 2)
    first, second = value[:, :, 0], value[:, :, 1]
    c, s = cosine[:, None, :], sign * sine[:, None, :]
    return jnp.stack([first * c - second * s, second * c + first * s], axis=2).reshape(length, width)


MESH = pl.DeviceIdType.MESH


def flip(index, bit):
    return index + bit - 2 * bit * ((index // bit) % 2)


class Place:
    def __init__(self, pair):
        self.s, self.f = lax.axis_index("seq"), lax.axis_index("fsdp")
        self.pair = pair
        s, f = self.s, self.f
        self.sx, self.sy = flip(s, 2), flip(s, 4)
        self.sd, self.sc = flip(self.sx, 4), flip(s, 1)
        self.q = f // 2 if pair > 1 else 0
        self.x, self.y, self.core = (self.sx, f), (self.sy, f), (self.sc, f)
        self.z = (s, opposite(f)) if pair > 1 else None
        self.peers = [self.x, self.y, self.core] + ([self.z] if pair > 1 else [])

    def barrier(self):
        sem = pltpu.get_barrier_semaphore()
        for peer in self.peers:
            pl.semaphore_signal(sem, inc=1, device_id=peer, device_id_type=MESH)
        pl.semaphore_wait(sem, len(self.peers))


class Wires:
    def __init__(self, send, recv):
        self.send, self.recv, self.count, self.open = send, recv, 0, {}

    def new(self, key):
        self.open[key] = self.count
        self.count += 1

    def go(self, key, src, dst, device):
        i = self.open[key]
        copy = pltpu.make_async_remote_copy(
            src, dst, self.send.at[i], self.recv.at[i], device_id=device, device_id_type=MESH
        )
        copy.start()
        return copy


def gather_steps(place, wires, own, out, ready):
    pair, rows = place.pair, own.shape[0]
    half = rows // 2
    top, low = pl.ds(0, half), pl.ds(half, half)
    p = place
    qs = [p.q] + ([1 - p.q] if pair > 1 else [])
    kinds = ["xa", "xb", "ya", "yb", "xd", "yd", "c0", "cxa", "cxb", "cya", "cyb", "cda", "cdb"]
    for t in range(pair):
        for kind in kinds:
            wires.new((t, kind))
    if pair > 1:
        wires.new("z")
    live = {}

    def go(key, src, dst, device):
        live[key] = wires.go(key, src, dst, device)

    def begin(t, src):
        q = qs[t]
        go((t, "xa"), src.at[top], out.at[q, p.s, top], p.x)
        go((t, "yb"), src.at[low], out.at[q, p.s, low], p.y)
        go((t, "xb"), src.at[low], out.at[q, p.s, low], p.x)
        go((t, "ya"), src.at[top], out.at[q, p.s, top], p.y)
        go((t, "c0"), src, out.at[q, p.s], p.core)

    def arrived(key):
        live[key].wait_recv()

    if pair > 1:
        go("z", own, out.at[qs[0], p.s], p.z)
    begin(0, own)
    ready(qs[0], p.s, None)

    def first(t):
        q = qs[t]
        arrived((t, "xa"))
        go((t, "xd"), out.at[q, p.sx, top], out.at[q, p.sx, top], p.y)
        go((t, "cxa"), out.at[q, p.sx, top], out.at[q, p.sx, top], p.core)
        arrived((t, "yb"))
        go((t, "yd"), out.at[q, p.sy, low], out.at[q, p.sy, low], p.x)
        go((t, "cyb"), out.at[q, p.sy, low], out.at[q, p.sy, low], p.core)
        arrived((t, "c0"))
        ready(q, p.sc, None)

    def second(t):
        q = qs[t]
        arrived((t, "xb"))
        go((t, "cxb"), out.at[q, p.sx, low], out.at[q, p.sx, low], p.core)
        ready(q, p.sx, None)
        arrived((t, "ya"))
        go((t, "cya"), out.at[q, p.sy, top], out.at[q, p.sy, top], p.core)
        ready(q, p.sy, None)
        arrived((t, "xd"))
        go((t, "cda"), out.at[q, p.sd, top], out.at[q, p.sd, top], p.core)
        arrived((t, "yd"))
        go((t, "cdb"), out.at[q, p.sd, low], out.at[q, p.sd, low], p.core)

    def third(t):
        q = qs[t]
        arrived((t, "cxa"))
        arrived((t, "cxb"))
        ready(q, flip(p.sx, 1), None)
        arrived((t, "cya"))
        arrived((t, "cyb"))
        ready(q, flip(p.sy, 1), None)
        ready(q, p.sd, None)
        arrived((t, "cda"))
        arrived((t, "cdb"))
        ready(q, flip(p.sd, 1), None)

    first(0)
    if pair > 1:
        arrived("z")
        begin(1, out.at[qs[1], p.s])
        ready(qs[1], p.s, None)
    second(0)
    if pair > 1:
        first(1)
    third(0)
    if pair > 1:
        second(1)
        third(1)
    for copy in live.values():
        copy.wait_send()


def gather_wires(pair):
    return 14 * pair + (2 if pair > 1 else 0)


def gather_kernel(pair, own, out, send, recv, local):
    place = Place(pair)
    keep = pltpu.make_async_copy(own, out.at[place.q, place.s], local)
    keep.start()
    place.barrier()
    gather_steps(place, Wires(send, recv), own, out, lambda q, slot, half: None)
    keep.wait()


def plane_gather(v, n, pair, ident):
    rows, width = v.shape
    return pl.pallas_call(
        functools.partial(gather_kernel, pair),
        in_specs=[pl.BlockSpec(memory_space=pltpu.VMEM)],
        out_specs=pl.BlockSpec(memory_space=pl.ANY),
        out_shape=jax.ShapeDtypeStruct((pair, n, rows, width), v.dtype),
        scratch_shapes=[pltpu.SemaphoreType.DMA((gather_wires(pair),))] * 2 + [pltpu.SemaphoreType.DMA],
        compiler_params=pltpu.CompilerParams(collective_id=ident, has_side_effects=True),
        cost_estimate=pl.CostEstimate(flops=0, bytes_accessed=pair * n * rows * width * 20, transcendentals=0),
        name=f"gather_{ident}",
    )(v).reshape(pair * n * rows, width)


def add(a, b):
    return (a.astype(F32) + b.astype(F32)).astype(BF16)


def scatter_steps(place, wires, part, rc, rd, rx, ry, qbuf, zbuf, make, finish):
    p, pair = place, place.pair
    rows = rx.shape[1]
    half = rows // 2
    top, low = pl.ds(0, half), pl.ds(half, half)
    slots = {"d": p.sd, "x": p.sx, "y": p.sy, "o": p.s}
    order = ["d", "x", "y", "o"]
    names = ["c" + k for k in order] + ["da", "db", "xa", "xb", "ya", "yb"]
    for t in range(pair):
        for name in names:
            wires.new((t, name))
    if pair > 1:
        wires.new("z")
    live = {}

    def go(key, src, dst, device):
        live[key] = wires.go(key, src, dst, device)

    def arrived(key):
        live[key].wait_recv()

    for t in range(pair):
        for i, k in enumerate(order):
            make(t, k, 1)
            go((t, "c" + k), part(t, flip(slots[k], 1)), rc.at[t, i], p.core)

    def start(t):
        make(t, "d", 0)
        arrived((t, "cd"))
        qbuf[t, 0] = add(part(t, p.sd)[...], rc[t, 0])
        go((t, "da"), qbuf.at[t, 0, top], rd.at[t, top], p.x)
        go((t, "db"), qbuf.at[t, 0, low], rd.at[t, low], p.y)
        make(t, "x", 0)
        arrived((t, "cx"))
        qbuf[t, 1, top] = add(part(t, p.sx)[top], rc[t, 1, top])
        go((t, "xa"), qbuf.at[t, 1, top], rx.at[t, top], p.x)
        make(t, "y", 0)
        arrived((t, "cy"))
        qbuf[t, 2, low] = add(part(t, p.sy)[low], rc[t, 2, low])
        go((t, "yb"), qbuf.at[t, 2, low], ry.at[t, low], p.y)

    def relay(t):
        held = part(t, p.sx)[low].astype(F32) + rc[t, 1, low].astype(F32)
        arrived((t, "db"))
        qbuf[t, 1, low] = (held + rd[t, low].astype(F32)).astype(BF16)
        go((t, "xb"), qbuf.at[t, 1, low], rx.at[t, low], p.x)
        held = part(t, p.sy)[top].astype(F32) + rc[t, 2, top].astype(F32)
        arrived((t, "da"))
        qbuf[t, 2, top] = (held + rd[t, top].astype(F32)).astype(BF16)
        go((t, "ya"), qbuf.at[t, 2, top], ry.at[t, top], p.y)

    def total(t):
        make(t, "o", 0)
        arrived((t, "co"))
        value = part(t, p.s)[...].astype(F32) + rc[t, 3].astype(F32)
        for key in ("xa", "yb", "xb", "ya"):
            arrived((t, key))
        return value + rx[t].astype(F32) + ry[t].astype(F32)

    if pair > 1:
        start(0)
        start(1)
        relay(0)
        relay(1)
        zbuf[0] = total(0).astype(BF16)
        go("z", zbuf.at[0], zbuf.at[1], p.z)
        value = total(1)
        arrived("z")
        value = value + zbuf[1].astype(F32)
    else:
        start(0)
        relay(0)
        value = total(0)
    finish(value)
    for copy in live.values():
        copy.wait_send()


def scatter_wires(pair):
    return 84 if pair > 1 else 20


def scatter_scratch(pair, rows, width):
    block = lambda *lead: pltpu.VMEM(lead + (rows, width), BF16)
    return [
        block(pair, 4),
        block(pair),
        block(pair),
        block(pair),
        block(pair, 3),
        block(2) if pair > 1 else pltpu.VMEM((2, 16, 128), BF16),
        pltpu.SemaphoreType.DMA((scatter_wires(pair),)),
        pltpu.SemaphoreType.DMA((scatter_wires(pair),)),
    ]


def scatter_kernel(pair, value, out, rc, rd, rx, ry, qbuf, zbuf, send, recv):
    place = Place(pair)
    place.barrier()
    planes = [1 - place.q, place.q] if pair > 1 else [0]

    def part(t, slot):
        return value.at[planes[t], slot]

    def finish(total):
        out[...] = total

    scatter_steps(
        place, Wires(send, recv), part, rc, rd, rx, ry, qbuf, zbuf, lambda *_: None, finish
    )


def plane_scatter(v, n, pair, ident):
    width = v.shape[1]
    rows = v.shape[0] // (pair * n)
    return pl.pallas_call(
        functools.partial(scatter_kernel, pair),
        in_specs=[pl.BlockSpec(memory_space=pltpu.VMEM)],
        out_specs=pl.BlockSpec(memory_space=pltpu.VMEM),
        out_shape=jax.ShapeDtypeStruct((rows, width), F32),
        scratch_shapes=scatter_scratch(pair, rows, width),
        compiler_params=pltpu.CompilerParams(
            collective_id=ident, has_side_effects=True, vmem_limit_bytes=40 * 2**20
        ),
        cost_estimate=pl.CostEstimate(flops=0, bytes_accessed=pair * n * rows * width * 20, transcendentals=0),
        name=f"scatter_{ident}",
    )(v.astype(BF16).reshape(pair, n, rows, width))


def sum_kernel(n, own, out, held, send, recv):
    s, f = lax.axis_index("seq"), lax.axis_index("fsdp")
    sem = pltpu.get_barrier_semaphore()
    for d in range(1, n):
        pl.semaphore_signal(sem, inc=1, device_id=((s + d) % n, f), device_id_type=MESH)
    pl.semaphore_wait(sem, n - 1)
    copies = []
    for d in range(1, n):
        copy = pltpu.make_async_remote_copy(
            own,
            held.at[d - 1],
            send.at[d - 1],
            recv.at[d - 1],
            device_id=((s + d) % n, f),
            device_id_type=MESH,
        )
        copy.start()
        copies.append(copy)
    total = own[...]
    for d in range(1, n):
        copies[d - 1].wait_recv()
        total = total + held[d - 1]
    out[...] = total
    for copy in copies:
        copy.wait_send()


def plane_sum(v, n, ident):
    return pl.pallas_call(
        functools.partial(sum_kernel, n),
        in_specs=[pl.BlockSpec(memory_space=pltpu.VMEM)],
        out_specs=pl.BlockSpec(memory_space=pltpu.VMEM),
        out_shape=jax.ShapeDtypeStruct(v.shape, v.dtype),
        scratch_shapes=[pltpu.VMEM((n - 1,) + v.shape, v.dtype)]
        + [pltpu.SemaphoreType.DMA((n - 1,))] * 2,
        compiler_params=pltpu.CompilerParams(collective_id=ident, has_side_effects=True),
        name=f"sum_{ident}",
    )(v)


def when(condition, body):
    pl.when(condition)(body)


def line_barrier(n, m):
    s, f = lax.axis_index("seq"), lax.axis_index("fsdp")
    sem = pltpu.get_barrier_semaphore()
    for d in range(1, n):
        pl.semaphore_signal(sem, inc=1, device_id=((s + d) % n, f), device_id_type=MESH)
    for d in range(1, m):
        pl.semaphore_signal(sem, inc=1, device_id=(s, (f + d) % m), device_id_type=MESH)
    pl.semaphore_wait(sem, n + m - 2)


def exit_kernel(
    n,
    m,
    d3,
    term,
    own_gain,
    branch_gain,
    feed_gain,
    grad_hidden,
    qkv,
    tokens_grad,
    weight_grad,
    gain_grad,
    w_v,
    value,
    rc,
    rd,
    rx,
    ry,
    qbuf,
    zbuf,
    send,
    recv,
    line,
    sums,
    done,
    got,
    gains,
    gplane,
    gsum,
    gline,
    zsend,
    zrecv,
    asend,
    arecv,
    gsend,
    grecv,
    lsend,
    lrecv,
    sems,
):
    place = Place(1)
    s, f = place.s, place.f
    moves = Moves(sems)
    moves.start(qkv, w_v)
    line_barrier(n, m)
    last = m - 1
    cols = term.shape[-1]

    def remote(src, dst, a, b, device):
        return pltpu.make_async_remote_copy(src, dst, a, b, device_id=device, device_id_type=MESH)

    def target(way, r):
        return last - r if way == 0 else r

    def hop(way, r, j, fresh):
        there = f + 1 if way == 0 else f - 1
        src = term.at[j, :, target(way, r)] if fresh else sums.at[way, r, j]
        return remote(src, line.at[way, r, j], zsend.at[way, r, j], zrecv.at[way, r, j], (s, there))

    ends = (f == 0, f == last)
    inner = (f > 0, f < last)

    def beyond(way, r):
        return target(way, r) > f if way == 0 else target(way, r) < f

    for group in ((0, 1, 2), (3,)):
        for r in range(last):
            for j in group:
                for way in (0, 1):
                    when(ends[way], lambda: hop(way, r, j, True).start())

    gain_copies = []
    for t in range(n):
        at = pl.ds(t * cols, cols)
        for j in range(2):
            gains[t, j : j + 1, :] = jnp.where(s == t, own_gain[j], 0.0)
        gains[t, 2:3, :] = branch_gain[:, at]
        gains[t, 3:4, :] = feed_gain[:, at]
        gains[t, 4:, :] = jnp.zeros((4, cols), F32)
    for d in range(1, n):
        t = (s + d) % n
        copy = remote(gains.at[t], gplane.at[d - 1], gsend.at[d], grecv.at[d], (t, f))
        copy.start()
        gain_copies.append(copy)

    moves.finish()
    rows, width = grad_hidden.shape
    block, step = 4 * rows, min(512, width)
    per = step // (m * qkv.shape[3])

    def make(q, chip, c, first):
        here = pl.ds(pl.multiple_of(chip * block, block), block)

        @pl.loop(0, width // 2 // step)
        def _(k):
            i = first // step + k
            at = pl.ds(pl.multiple_of(i * step, step), step)
            total = jnp.zeros((block, step), F32)
            for j in range(3):
                w = w_v[j, pl.ds(i * per, per)].reshape(step, cols)
                total = total + dot(d3[j, here, :], w, NT)
            value[q, pl.ds(4 * chip, 4), :, at] = total.astype(BF16).reshape(4, rows, step)

    side = f // (m // 2)
    middle = (f > 0) & (f < last)

    def relays(k, j, from_end):
        way = side if from_end else 1 - side
        o = way * k + (1 - way) * (last - k)

        def relay():
            there = f + 1 - 2 * way
            copy = remote(
                sums.at[way, k, j], line.at[way, k, j], zsend.at[way, k, j], zrecv.at[way, k, j], (s, there)
            )
            copy.wait_recv()
            sums[way, k, j] = add(term[j, :, o], line[way, k, j])
            copy.start()

        when(middle, relay)

    live = scatter_pairs(
        place, Wires(send, recv), value, rc, rd, rx, ry, qbuf, zbuf, make, tokens_grad,
        Work([lambda: None] + [lambda j=j: relays(0, j, True) for j in range(3)]),
    )
    tokens_grad[...] += grad_hidden[...]

    total = gains[s]
    for d in range(1, n):
        gain_copies[d - 1].wait_recv()
        total = total + gplane[d - 1]
    gsum[...] = total
    line_copies = []
    for d in range(1, m):
        t = (f + d) % m
        copy = remote(gsum, gline.at[d - 1], lsend.at[d], lrecv.at[d], (s, t))
        copy.start()
        line_copies.append(copy)

    copies = []
    plan = [(True, k, j) for k in range(1, m // 2) for j in range(3)]
    plan += [(False, k, j) for k in range(m // 2 - 1) for j in range(3)] + [(None, 0, j) for j in range(3)]
    plan += [(True, k, 3) for k in range(m // 2)] + [(False, k, 3) for k in range(m // 2 - 1)] + [(None, 0, 3)]
    for from_end, k, j in plan:
        if from_end is not None:
            relays(k, j, from_end)
            continue
        own = term[j, :, f].astype(F32)
        done[j] = own
        for way in (0, 1):
            r = last - f if way == 0 else f

            def take():
                pltpu.make_async_remote_copy(
                    sums.at[way, 0, j],
                    line.at[way, r, j],
                    zsend.at[way, r, j],
                    zrecv.at[way, r, j],
                    device_id=(s, f - 1 if way == 0 else f + 1),
                    device_id_type=MESH,
                ).wait_recv()
                done[j] += line[way, r, j].astype(F32)

            when(inner[way], take)
        if j == 3:
            for t in range(n):
                weight_grad[j, :, pl.ds(t * cols, cols)] = done[j, t]
            continue
        weight_grad[j, :, pl.ds(pl.multiple_of(s * cols, cols), cols)] = done[j, s]
        got[0, j] = done[j].astype(BF16)
        for d in range(1, n):
            t = (s + d) % n
            copy = remote(got.at[0, j, t], got.at[1, j, s], asend.at[j, d], arecv.at[j, d], (t, f))
            copy.start()
            copies.append(copy)
    total = gsum[...]
    for d in range(1, m):
        line_copies[d - 1].wait_recv()
        total = total + gline[d - 1]
    small = cols // m
    gain = jnp.zeros((8, small), F32)
    for plane in range(m):
        gain = gain + jnp.where(f == plane, total[:, plane * small : (plane + 1) * small], 0.0)
    gain_grad[...] = gain
    for copy in copies:
        copy.wait_recv()
    for j in range(3):
        for d in range(1, n):
            t = (s + d) % n
            weight_grad[j, :, pl.ds(pl.multiple_of(t * cols, cols), cols)] = got[1, j, t].astype(F32)
    for copy in copies + gain_copies + line_copies + list(live.values()):
        copy.wait_send()
    for r in range(last):
        for j in range(4):
            for way in (0, 1):
                when(ends[way] | (inner[way] & beyond(way, r)), lambda: hop(way, r, j, False).wait_send())


def leave(d3, term, own_gain, branch_gain, feed_gain, grad_hidden, qkv, n, m, ident):
    rows, width = grad_hidden.shape
    part, cols = term.shape[-2:]
    vmem = pl.BlockSpec(memory_space=pltpu.VMEM)
    dma = pltpu.SemaphoreType.DMA
    block = pltpu.VMEM((2, m - 1, 4, n, part, cols), BF16)
    return pl.pallas_call(
        functools.partial(exit_kernel, n, m),
        in_specs=[vmem] * 6 + [pl.BlockSpec(memory_space=pl.ANY)],
        out_specs=[vmem] * 3,
        out_shape=[
            jax.ShapeDtypeStruct((rows, width), F32),
            jax.ShapeDtypeStruct((4, part, width), F32),
            jax.ShapeDtypeStruct((8, cols // m), F32),
        ],
        scratch_shapes=[pltpu.VMEM((3, n, m, part, cols), BF16), pltpu.VMEM((1, n, rows, width), BF16)]
        + scatter_scratch(1, rows, width)
        + [
            block,
            block,
            pltpu.VMEM((4, n, part, cols), F32),
            pltpu.VMEM((2, 3, n, part, cols), BF16),
            pltpu.VMEM((n, 8, cols), F32),
            pltpu.VMEM((n - 1, 8, cols), F32),
            pltpu.VMEM((8, cols), F32),
            pltpu.VMEM((m - 1, 8, cols), F32),
        ]
        + [dma((2, m, 4))] * 2
        + [dma((3, n))] * 2
        + [dma((n,))] * 2
        + [dma((m,))] * 2
        + [dma((3 * m,))],
        compiler_params=pltpu.CompilerParams(
            collective_id=ident, has_side_effects=True, vmem_limit_bytes=60 * 2**20
        ),
        cost_estimate=pl.CostEstimate(flops=0, bytes_accessed=200 * 2**20, transcendentals=0),
        name=f"leave_{ident}",
    )(d3, term, own_gain, branch_gain, feed_gain, grad_hidden, qkv)


class Moves:
    def __init__(self, sems):
        self.sems, self.count, self.open = sems, 0, []

    def start(self, src, dst):
        copy = pltpu.make_async_copy(src, dst, self.sems.at[self.count])
        self.count += 1
        copy.start()
        self.open.append(copy)
        return copy

    def finish(self):
        for copy in self.open:
            copy.wait()
        self.open = []

    def wait(self, copies):
        for copy in copies:
            copy.wait()
        self.open = [copy for copy in self.open if all(copy is not other for other in copies)]


def place_kernel(parts, count, *refs):
    ins, outs = refs[:count], refs[count : count + len(parts)]
    held, sems = refs[count + len(parts) : -1], refs[-1]
    copies = []
    for i, (source, row) in enumerate(parts):
        src = ins[source] if row is None else ins[source].at[row]
        copies.append(pltpu.make_async_copy(src, held[i], sems.at[0, i]))
        copies[-1].start()
    back = []
    for i in range(len(parts)):
        copies[i].wait()
        back.append(pltpu.make_async_copy(held[i], outs[i], sems.at[1, i]))
        back[-1].start()
    for copy in back:
        copy.wait()


def place_outputs(arrays):
    parts, shapes = [], []
    for source, a in enumerate(arrays):
        for row in range(a.shape[0]) if a.ndim == 3 else [None]:
            parts.append((source, row))
            shapes.append(shape(a.shape[-2:], a.dtype))
    return pl.pallas_call(
        functools.partial(place_kernel, tuple(parts), len(arrays)),
        in_specs=[pl.BlockSpec(memory_space=pltpu.MemorySpace.HBM)] * len(arrays),
        out_specs=[pl.BlockSpec(memory_space=pltpu.MemorySpace.HBM)] * len(parts),
        out_shape=shapes,
        scratch_shapes=[pltpu.VMEM(a.shape, a.dtype) for a in shapes] + [pltpu.SemaphoreType.DMA((2, len(parts)))],
        compiler_params=pltpu.CompilerParams(vmem_limit_bytes=63 * 2**20),
        name="place",
    )(*arrays)


def gather_pairs(place, wires, own, out, ready, hook=lambda: None):
    p, pair = place, place.pair
    half = own.shape[0] // 2
    top, low = pl.ds(0, half), pl.ds(half, half)
    qs = [p.q] + ([1 - p.q] if pair > 1 else [])
    for t in range(pair):
        for kind in ["xa", "xb", "ya", "yb", "xd", "yd", "ca", "cb", "cxa", "cxb", "cya", "cyb", "cda", "cdb"]:
            wires.new((t, kind))
    if pair > 1:
        wires.new("za")
        wires.new("zb")
    live = {}

    def go(key, src, dst, device):
        live[key] = wires.go(key, src, dst, device)

    def arrived(*keys):
        for key in keys:
            live[key].wait_recv()

    def begin(t, src, tops):
        q = qs[t]
        rows = top if tops else low
        go((t, "xa" if tops else "xb"), src.at[rows], out.at[q, p.s, rows], p.x)
        go((t, "ya" if tops else "yb"), src.at[rows], out.at[q, p.s, rows], p.y)
        go((t, "ca" if tops else "cb"), src.at[rows], out.at[q, p.s, rows], p.core)

    def pass_on(t, name, slot, rows, device):
        ref = out.at[qs[t], slot, rows]
        go((t, name), ref, ref, device)

    def first(t):
        arrived((t, "xa"))
        pass_on(t, "xd", p.sx, top, p.y)
        pass_on(t, "cxa", p.sx, top, p.core)
        arrived((t, "ya"))
        pass_on(t, "cya", p.sy, top, p.core)

    def second(t):
        arrived((t, "yb"))
        pass_on(t, "yd", p.sy, low, p.x)
        pass_on(t, "cyb", p.sy, low, p.core)
        arrived((t, "xb"))
        pass_on(t, "cxb", p.sx, low, p.core)

    def third(t):
        arrived((t, "xd"))
        pass_on(t, "cda", p.sd, top, p.core)
        arrived((t, "yd"))
        pass_on(t, "cdb", p.sd, low, p.core)

    def use(t, slot, *keys):
        arrived(*[(t, key) for key in keys])
        ready(qs[t], slot // 2)

    if pair > 1:
        go("za", own.at[top], out.at[qs[0], p.s, top], p.z)
        go("zb", own.at[low], out.at[qs[0], p.s, low], p.z)
    begin(0, own, True)
    begin(0, own, False)
    use(0, p.s, "ca", "cb")
    hook()
    first(0)
    if pair > 1:
        second(0)
        use(0, p.sx, "cxa", "cxb")
        arrived("za")
        begin(1, out.at[qs[1], p.s], True)
        use(0, p.sy, "cya", "cyb")
        third(0)
        hook()
        arrived("zb")
        begin(1, out.at[qs[1], p.s], False)
        use(0, p.sd, "cda", "cdb")
        first(1)
        use(1, p.s, "ca", "cb")
        hook()
        second(1)
        hook()
        use(1, p.sx, "cxa", "cxb")
        use(1, p.sy, "cya", "cyb")
        third(1)
        use(1, p.sd, "cda", "cdb")
    else:
        hook()
        second(0)
        use(0, p.sx, "cxa", "cxb")
        use(0, p.sy, "cya", "cyb")
        hook()
        third(0)
        use(0, p.sd, "cda", "cdb")
    return live


def by_rows(first, count, body):
    @pl.loop(0, count // 32)
    def _(i):
        body(pl.ds(pl.multiple_of(first + i * 32, 32), 32))


def scatter_pairs(
    place, wires, value, rc, rd, rx, ry, qbuf, zbuf, make, result, hook=lambda: None, jobs=None, mine=None, theirs=None
):
    p, pair = place, place.pair
    rows, width = rx.shape[1], rx.shape[2]
    count = 4 if pair > 1 else 2
    half, wide = rows // 2, width // count
    top, low = pl.ds(0, half), pl.ds(half, half)
    slots = {"d": p.sd, "x": p.sx, "y": p.sy, "o": p.s}
    order = ["d", "x", "y", "o"]
    planes = [1 - p.q, p.q] if pair > 1 else [p.q]
    jobs = jobs or [(t, c) for t in range(pair) for c in range(count)]
    mine = mine or list(range(count))
    theirs = theirs or mine
    for job in jobs:
        for name in ["c" + k for k in order] + ["da", "db", "xa", "xb", "ya", "yb"]:
            wires.new((job, name))
    if pair > 1:
        for c in range(count):
            wires.new(f"z{c}")
    live = {}

    def go(key, src, dst, device):
        live[key] = wires.go(key, src, dst, device)

    def arrived(*keys):
        for key in keys:
            live[key].wait_recv()

    def span(block):
        return pl.ds(block * wide if isinstance(block, int) else pl.multiple_of(block * wide, wide), wide)

    def at(c):
        return span(mine[c])

    def part(job, slot, rows_):
        return value.at[planes[job[0]], slot, rows_, at(job[1])]

    every = pl.ds(0, rows)

    def begin(job):
        t, c = job

        @pl.loop(0, 2)
        def _(k):
            make(planes[t], k, c, mine[c] * wide)

        for i, k in enumerate(order):
            go((job, "c" + k), part(job, flip(slots[k], 1), every), rc.at[t, i, :, at(c)], p.core)

    def rest(job):
        t, c = job

        def sum_of(i, slot):
            def body(r):
                qbuf[t, i, r, at(c)] = add(value[planes[t], slot, r, at(c)], rc[t, i, r, at(c)])

            return body

        arrived((job, "cd"))
        by_rows(0, rows, sum_of(0, p.sd))
        go((job, "da"), qbuf.at[t, 0, top, at(c)], rd.at[t, top, at(c)], p.x)
        go((job, "db"), qbuf.at[t, 0, low, at(c)], rd.at[t, low, at(c)], p.y)
        arrived((job, "cx"))
        by_rows(0, half, sum_of(1, p.sx))
        go((job, "xa"), qbuf.at[t, 1, top, at(c)], rx.at[t, top, at(c)], p.x)
        arrived((job, "cy"))
        by_rows(half, half, sum_of(2, p.sy))
        go((job, "yb"), qbuf.at[t, 2, low, at(c)], ry.at[t, low, at(c)], p.y)

    def relay(job):
        t, c = job

        def sum_of(i, slot):
            def body(r):
                held = value[planes[t], slot, r, at(c)].astype(F32) + rc[t, i, r, at(c)].astype(F32)
                qbuf[t, i, r, at(c)] = (held + rd[t, r, at(c)].astype(F32)).astype(BF16)

            return body

        arrived((job, "db"))
        by_rows(half, half, sum_of(1, p.sx))
        go((job, "xb"), qbuf.at[t, 1, low, at(c)], rx.at[t, low, at(c)], p.x)
        arrived((job, "da"))
        by_rows(0, half, sum_of(2, p.sy))
        go((job, "ya"), qbuf.at[t, 2, top, at(c)], ry.at[t, top, at(c)], p.y)

    def total(job):
        t, c = job
        arrived((job, "co"), (job, "xa"), (job, "yb"), (job, "xb"), (job, "ya"))

        def body(r):
            held = value[planes[t], p.s, r, at(c)].astype(F32) + rc[t, 3, r, at(c)].astype(F32)
            held = held + rx[t, r, at(c)].astype(F32) + ry[t, r, at(c)].astype(F32)
            if pair > 1 and t == 0:
                zbuf[0, r, at(c)] = held.astype(BF16)
            else:
                result[r, at(c)] = held

        by_rows(0, rows, body)
        if pair > 1 and t == 0:
            go(f"z{c}", zbuf.at[0, :, at(c)], zbuf.at[1, :, at(c)], p.z)

    begin(jobs[0])
    rest(jobs[0])
    if len(jobs) > 1:
        begin(jobs[1])
    for i, job in enumerate(jobs):
        if i + 1 < len(jobs):
            rest(jobs[i + 1])
        hook()
        if i + 2 < len(jobs):
            begin(jobs[i + 2])
        relay(job)
        hook()
        if i > 0:
            total(jobs[i - 1])
    total(jobs[-1])
    if pair > 1:
        for c in range(count):
            here = span(theirs[c])
            arrived(f"z{c}")

            def body(r):
                result[r, here] += zbuf[1, r, here].astype(F32)

            by_rows(0, rows, body)
    return live


def rms_back(value, gain, grad):
    inverse = lax.rsqrt(jnp.mean(value * value, axis=-1, keepdims=True) + EPSILON)
    normal = value * inverse
    u = grad * gain
    return inverse * (u - normal * jnp.mean(u * normal, axis=-1, keepdims=True)), grad * normal


def up_kernel(
    pair, h, wg, wu, down_w, hs, gate, up, inner, inner_t, wd, wu_all, hs_v, w_v, g_v, u_v, i_v, t_v, send, recv, zsem, rsem, sems
):
    place = Place(pair)
    place.peers.append((place.s, flip(place.f, 1)))
    moves = Moves(sems)
    deep = wu.shape[1]
    loads = [moves.start(wg, w_v.at[0])]
    far_f, near_f = opposite(place.f), flip(place.f, 1)

    def up_rows(plane):
        return w_v.at[1, pl.ds(pl.multiple_of(plane * deep, deep), deep)]

    loads += [moves.start(wu.at[plane], up_rows(plane)) for plane in (place.f, near_f, far_f)]
    rows, width = h.shape
    block, share = 2 * rows, wg.shape[1]
    up_pass = pltpu.make_async_remote_copy(
        wu.at[far_f], up_rows(far_f), rsem.at[0], rsem.at[1], device_id=(place.s, near_f), device_id_type=MESH
    )
    hs_v[place.q, place.s] = h[...]
    place.barrier()
    stream, view = Stream(place, zsem), half_rows(down_w, share)
    down_copies = [stream.near_copy(0, view, wd), stream.own_copy(0, view, wd), stream.far_copy(0, view, wd)]

    def pass_up():
        up_pass.start()
        down_copies[0].start()
        down_copies[1].start()

    def pass_down():
        down_copies[2].start()

    n = hs.shape[1]
    step = min(256, share)
    waited = []

    def ready(q, chip):
        if not waited:
            moves.wait(loads)
            waited.append(True)
        slots = pl.ds(2 * chip, 2)
        moves.start(hs_v.at[q, slots], hs.at[q, slots])
        at = pl.multiple_of(q * n * rows + chip * block, block)
        here = pl.ds(at, block)

        @pl.loop(0, share // step)
        def _(j):
            cols = pl.ds(pl.multiple_of(j * step, step), step)
            g_v[here, cols] = dot(hs_v[q, slots].reshape(block, width), w_v[0, :, cols], NN)

        moves.start(g_v.at[here], gate.at[here])
        if whole:
            second(q, slots, here)
        else:
            held.append((q, slots, here))

    whole, held = [], []

    def second(q, slots, here):
        @pl.loop(0, share // step)
        def _(j):
            cols = pl.ds(pl.multiple_of(j * step, step), step)
            u = dot(hs_v[q, slots].reshape(block, width), w_v[1, :, cols], NN)
            g = g_v[here, cols]
            u_v[here, cols] = u
            value = g * (1.0 / (1.0 + jnp.exp(-g))) * u
            i_v[here, cols] = value.astype(BF16)
            t_v[cols, here] = value.T.astype(BF16)

        moves.start(u_v.at[here], up.at[here])
        moves.start(i_v.at[here], inner.at[here])

    def complete():
        up_pass.wait_recv()
        whole.append(True)
        for args in held:
            second(*args)

    live = gather_pairs(place, Wires(send, recv), h, hs_v, ready, Work([pass_up, lambda: None, pass_down, complete]))
    moves.start(w_v.at[1], wu_all)
    moves.start(t_v, inner_t)
    for copy in down_copies:
        copy.wait()
    up_pass.wait_send()
    for copy in live.values():
        copy.wait_send()
    moves.finish()


def any_specs(count):
    return [pl.BlockSpec(memory_space=pl.ANY)] * count


def vmem_specs(count):
    return [pl.BlockSpec(memory_space=pltpu.VMEM)] * count


def kernel_params(ident, mib=60):
    return pltpu.CompilerParams(collective_id=ident, has_side_effects=True, vmem_limit_bytes=mib * 2**20)


def shape(dims, kind):
    return jax.ShapeDtypeStruct(dims, kind)


def ffn_up(h, wg, wu, down_w, n, pair, ident):
    rows, width = h.shape
    share, long = wg.shape[1], pair * n * rows
    dma = pltpu.SemaphoreType.DMA
    outs = [
        shape((pair, n, rows, width), BF16),
        shape((long, share), F32),
        shape((long, share), F32),
        shape((long, share), BF16),
        shape((share, long), BF16),
        shape((width // down_w.shape[1], share, down_w.shape[1]), BF16),
        shape((width, share), BF16),
    ]
    return pl.pallas_call(
        functools.partial(up_kernel, pair),
        in_specs=vmem_specs(1) + any_specs(3),
        out_specs=any_specs(7),
        out_shape=outs,
        scratch_shapes=[
            pltpu.VMEM((pair, n, rows, width), BF16),
            pltpu.VMEM((2, width, share), BF16),
            pltpu.VMEM((long, share), F32),
            pltpu.VMEM((long, share), F32),
            pltpu.VMEM((long, share), BF16),
            pltpu.VMEM((share, long), BF16),
            dma((gather_wires(pair),)),
            dma((gather_wires(pair),)),
            dma((1, 4, 2)),
            dma((2,)),
            dma((8 + 4 * pair * n // 2,)),
        ],
        compiler_params=kernel_params(ident),
        cost_estimate=pl.CostEstimate(
            flops=4 * long * width * share, bytes_accessed=long * width * 40, transcendentals=0
        ),
        name=f"up_{ident}",
    )(h, wg, wu, down_w)


def down_kernel(
    pair, inner, wd, hidden, gains, cotangent, layer_out, grad_low, gain_term, wd_all,
    i_v, w_v, sum_v, value, rc, rd, rx, ry, qbuf, zbuf, send, recv, wsem, sems
):
    place = Place(pair)
    place.peers.append((place.s, flip(place.f, 1)))
    moves = Moves(sems)
    gain = gains[3:4, :]
    f, far_f, near_f = place.f, opposite(place.f), flip(place.f, 1)
    deep = wd.shape[2]

    def columns(plane):
        return w_v.at[:, pl.ds(pl.multiple_of(plane * deep, deep), deep)]

    for plane in (f, near_f, far_f):
        moves.start(wd.at[plane], columns(plane))
    moves.start(inner, i_v)
    rows, width = hidden.shape
    block = 2 * rows
    n = value.shape[1]
    step = min(512, width)
    place.barrier()
    relay = pltpu.make_async_remote_copy(
        wd.at[far_f], columns(far_f), wsem.at[0], wsem.at[1], device_id=(place.s, near_f), device_id_type=MESH
    )
    relay.start()
    moves.finish()

    def make(q, chip, c, at):
        here = pl.ds(pl.multiple_of(q * n * rows + chip * 2 * block, 2 * block), 2 * block)
        cols = pl.ds(pl.multiple_of(at, deep), deep)
        part = dot(i_v[here, :], w_v[:, cols], NN).astype(BF16)
        value[q, pl.ds(4 * chip, 4), :, cols] = part.reshape(4, rows, deep)

    mine = [f, near_f, far_f, opposite(near_f)]
    theirs = [far_f, opposite(near_f), f, near_f]
    jobs = [(0, 0), (0, 1), (0, 2), (1, 0), (1, 1), (0, 3), (1, 2), (1, 3)]
    live = scatter_pairs(
        place, Wires(send, recv), value, rc, rd, rx, ry, qbuf, zbuf, make, sum_v,
        Work([lambda: None] * 6 + [relay.wait_recv]), jobs, mine, theirs,
    )
    moves.start(w_v, wd_all)
    feed = sum_v[...]
    grad = cotangent[...].astype(F32)
    inverse = lax.rsqrt(jnp.mean(feed * feed, axis=-1, keepdims=True) + EPSILON)
    normal = feed * inverse
    layer_out[...] = (hidden[...] + normal * gain).astype(BF16)
    u = grad * gain
    grad_low[...] = (inverse * (u - normal * jnp.mean(u * normal, axis=-1, keepdims=True))).astype(BF16)
    gain_term[...] = jnp.sum(grad * normal, axis=0, keepdims=True)
    for copy in list(live.values()) + [relay]:
        copy.wait_send()
    moves.finish()


def ffn_down(inner, wd, hidden, gains, cotangent, n, pair, ident):
    rows, width = hidden.shape
    dma = pltpu.SemaphoreType.DMA
    return pl.pallas_call(
        functools.partial(down_kernel, pair),
        in_specs=any_specs(2) + vmem_specs(3),
        out_specs=vmem_specs(3) + any_specs(1),
        out_shape=[
            shape((rows, width), BF16),
            shape((rows, width), BF16),
            shape((1, width), F32),
            shape((wd.shape[1], width), BF16),
        ],
        scratch_shapes=[
            pltpu.VMEM(inner.shape, BF16),
            pltpu.VMEM((wd.shape[1], width), BF16),
            pltpu.VMEM((rows, width), F32),
            pltpu.VMEM((pair, n, rows, width), BF16),
        ]
        + scatter_scratch(pair, rows, width)
        + [dma((2,)), dma((2 + wd.shape[0],))],
        compiler_params=kernel_params(ident),
        cost_estimate=pl.CostEstimate(
            flops=2 * inner.shape[0] * inner.shape[1] * width, bytes_accessed=pair * n * rows * width * 40, transcendentals=0
        ),
        name=f"down_{ident}",
    )(inner, wd, hidden, gains, cotangent)


def grad_kernel(
    pair, g, wd, gate, up, inner_t, grad_gate, grad_up, gate_t, up_t, down_term,
    gs_v, w_v, g_v, u_v, gg_v, gu_v, gt_v, ut_v, it_v, acc, low_v, send, recv, sems
):
    place = Place(pair)
    moves = Moves(sems)
    deep = down_term.shape[2]
    loads = [moves.start(wd, w_v)]
    loads += [moves.start(gate, g_v), moves.start(up, u_v), moves.start(inner_t, it_v)]
    rows, width = g.shape
    block, share = 2 * rows, wd.shape[0]
    gs_v[place.q, place.s] = g[...]
    place.barrier()
    n = gs_v.shape[1]
    step = min(256, share)
    waited = []

    def ready(q, chip):
        if not waited:
            moves.wait(loads)
            waited.append(True)
        slots = pl.ds(2 * chip, 2)
        here = pl.ds(pl.multiple_of(q * n * rows + chip * block, block), block)

        @pl.loop(0, share // step)
        def _(j):
            cols = pl.ds(pl.multiple_of(j * step, step), step)
            a = gs_v[q, slots].reshape(block, width)
            e = dot(a, w_v[cols, :], NT)
            v, u = g_v[here, cols], u_v[here, cols]
            s = 1.0 / (1.0 + jnp.exp(-v))
            dg = e * u * s * (1.0 + v * (1.0 - s))
            du = e * v * s
            gg_v[here, cols] = dg.astype(BF16)
            gu_v[here, cols] = du.astype(BF16)
            gt_v[cols, here] = dg.T.astype(BF16)
            ut_v[cols, here] = du.T.astype(BF16)

        moves.start(gg_v.at[here], grad_gate.at[here])
        moves.start(gu_v.at[here], grad_up.at[here])

    def add_term(t):
        q = place.q if t == 0 else 1 - place.q
        tokens = pl.ds(pl.multiple_of(q * n * rows, n * rows), n * rows)

        @pl.loop(0, width // step)
        def _(j):
            cols = pl.ds(pl.multiple_of(j * step, step), step)
            part = dot(it_v[:, tokens], gs_v[q, :, :, cols].reshape(n * rows, step), NN)
            if t == 0:
                acc[:, cols] = part
            else:
                acc[:, cols] += part

    nothing = lambda: None
    live = gather_pairs(
        place, Wires(send, recv), g, gs_v, ready, Work([nothing, nothing, nothing, lambda: add_term(0)])
    )
    add_term(1)
    for j in range(down_term.shape[0]):
        low_v[j] = acc[:, pl.ds(j * deep, deep)].astype(BF16)
    moves.start(low_v, down_term)
    moves.start(gt_v, gate_t)
    moves.start(ut_v, up_t)
    for copy in live.values():
        copy.wait_send()
    moves.finish()


def ffn_grad(g, wd, gate, up, inner_t, n, m, pair, ident):
    rows, width = g.shape
    share, long = wd.shape[0], pair * n * rows
    dma = pltpu.SemaphoreType.DMA
    flat, tall = pltpu.VMEM((long, share), BF16), pltpu.VMEM((share, long), BF16)
    return pl.pallas_call(
        functools.partial(grad_kernel, pair),
        in_specs=vmem_specs(1) + any_specs(4),
        out_specs=any_specs(5),
        out_shape=[shape((long, share), BF16)] * 2
        + [shape((share, long), BF16)] * 2
        + [shape((m, share, width // m), BF16)],
        scratch_shapes=[
            pltpu.VMEM((pair, n, rows, width), BF16),
            pltpu.VMEM((share, width), BF16),
            pltpu.VMEM((long, share), F32),
            pltpu.VMEM((long, share), F32),
            flat,
            flat,
            tall,
            tall,
            tall,
            pltpu.VMEM((share, width), F32),
            pltpu.VMEM((m, share, width // m), BF16),
            dma((gather_wires(pair),)),
            dma((gather_wires(pair),)),
            dma((12 + 3 * pair * n // 2,)),
        ],
        compiler_params=kernel_params(ident, 63),
        cost_estimate=pl.CostEstimate(
            flops=2 * long * width * share, bytes_accessed=long * width * 40, transcendentals=0
        ),
        name=f"grad_{ident}",
    )(g, wd, gate, up, inner_t)


def back_kernel(
    pair, gg, gu, wg, wu, gate_t, hs, down_term, branch, gains, cotangent,
    grad_hidden, grad_low, gain_term, down_grad, gate_term,
    a_v, w_v, value, rc, rd, rx, ry, qbuf, zbuf, send, recv,
    gt_v, hs_v, gterm, down_own, down_near, down_total, down_from, dsem, sems
):
    place = Place(pair)
    place.peers.append((place.s, flip(place.f, 1)))
    moves = Moves(sems)
    loads = [moves.start(wg, w_v.at[0]), moves.start(wu, w_v.at[1])]
    loads += [moves.start(gg, a_v.at[0]), moves.start(gu, a_v.at[1])]
    late = []
    down = Settle(place, dsem, down_term, down_own, down_near, down_total, down_from)
    pieces = term_work(gterm, gt_v, hs_v, lambda: moves.wait(late), gate_term, moves)
    idle = [lambda: None]
    work = Work(idle + pieces[:1] + idle + pieces[1:2] + idle + pieces[2:3] + idle + pieces[3:] + idle * 2 + [down.middle])
    rows, width = branch.shape
    block = 2 * rows
    n = value.shape[1]
    step = min(256, width)
    place.barrier()
    down.start(True)
    moves.wait(loads)
    late.append(moves.start(gate_t, gt_v))
    for q in range(pair):
        late.append(moves.start(hs.at[q], hs_v.at[q]))

    def make(q, chip, c, at):
        here = pl.ds(pl.multiple_of(q * n * rows + chip * 2 * block, 2 * block), 2 * block)

        @pl.loop(0, width // 4 // step)
        def _(j):
            cols = pl.ds(pl.multiple_of(at + j * step, step), step)
            part = dot(a_v[0, here, :], w_v[0, cols, :], NT) + dot(a_v[1, here, :], w_v[1, cols, :], NT)
            value[q, pl.ds(4 * chip, 4), :, cols] = part.astype(BF16).reshape(4, rows, step)

    live = scatter_pairs(place, Wires(send, recv), value, rc, rd, rx, ry, qbuf, zbuf, make, grad_hidden, work)
    work.rest()
    grad = cotangent[...].astype(F32) + grad_hidden[...]
    grad_hidden[...] = grad
    back, term = rms_back(branch[...], gains[2:3, :], grad)
    grad_low[...] = back.astype(BF16)
    gain_term[...] = jnp.sum(term, axis=0, keepdims=True)
    share = down_grad.shape[0] // 2

    def store(u, value):
        down_grad[pl.ds(pl.multiple_of(u * share, share), share), :] = value

    down.finish(store)
    for copy in live.values():
        copy.wait_send()
    moves.finish()


def ffn_back(gg, gu, wg, wu, gate_t, hs, down_term, branch, gains, cotangent, n, m, pair, ident):
    rows, width = branch.shape
    share, deep = gate_t.shape[0], width // m
    term = down_term.shape
    dma = pltpu.SemaphoreType.DMA
    return pl.pallas_call(
        functools.partial(back_kernel, pair),
        in_specs=any_specs(7) + vmem_specs(3),
        out_specs=vmem_specs(4) + any_specs(1),
        out_shape=[
            shape((rows, width), F32),
            shape((rows, width), BF16),
            shape((1, width), F32),
            shape((2 * share, deep), F32),
            shape(term, BF16),
        ],
        scratch_shapes=[
            pltpu.VMEM((2,) + gg.shape, BF16),
            pltpu.VMEM((2,) + wg.shape, BF16),
            pltpu.VMEM((pair, n, rows, width), BF16),
        ]
        + scatter_scratch(pair, rows, width)
        + [pltpu.VMEM(v.shape, BF16) for v in (gate_t, hs)]
        + [pltpu.VMEM(term, BF16)]
        + settle_scratch(share, deep)
        + [dma((20,))],
        compiler_params=kernel_params(ident, 63),
        cost_estimate=pl.CostEstimate(
            flops=4 * gg.shape[0] * gg.shape[1] * width, bytes_accessed=pair * n * rows * width * 40, transcendentals=0
        ),
        name=f"back_{ident}",
    )(gg, gu, wg, wu, gate_t, hs, down_term, branch, gains, cotangent)


def opposite(f):
    return (f + 2) % 4


class Stream:
    def __init__(self, place, sems):
        self.place, self.sems = place, sems
        f = place.f
        self.half, self.far_f, self.near_f = f // 2, opposite(f), flip(f, 1)
        self.far, self.near = (place.s, self.far_f), (place.s, self.near_f)

    def remote(self, k, step, src, dst, device):
        return pltpu.make_async_remote_copy(
            src, dst, self.sems.at[k, step, 0], self.sems.at[k, step, 1], device_id=device, device_id_type=MESH
        )

    def far_copy(self, k, view, full):
        return self.remote(k, 0, view(1 - self.half), full.at[self.place.f], self.far)

    def near_copy(self, k, view, full):
        return self.remote(k, 1, view(self.half), full.at[self.place.f], self.near)

    def own_copy(self, k, view, full):
        return pltpu.make_async_copy(view(self.half), full.at[self.place.f], self.sems.at[k, 3, 0])

    def relay_copy(self, k, full):
        return self.remote(k, 2, full.at[self.far_f], full.at[self.far_f], self.near)

    def start_far(self, k, view, full):
        self.far_copy(k, view, full).start()

    def start_near(self, k, view, full):
        self.near_copy(k, view, full).start()
        self.own_copy(k, view, full).start()

    def relay(self, k, view, full):
        self.far_copy(k, view, full).wait_recv()
        self.relay_copy(k, full).start()

    def finish(self, k, view, full):
        self.near_copy(k, view, full).wait_recv()
        self.relay_copy(k, full).wait_recv()
        self.own_copy(k, view, full).wait()
        self.far_copy(k, view, full).wait_send()
        self.near_copy(k, view, full).wait_send()
        self.relay_copy(k, full).wait_send()


def half_columns(ref, share):
    return lambda u: ref.at[:, pl.ds(pl.multiple_of(u * share, share), share)]


def half_rows(ref, share):
    return lambda u: ref.at[pl.ds(pl.multiple_of(u * share, share), share), :]


def full_barrier(place, n, near):
    sem = pltpu.get_barrier_semaphore()
    s, f = place.s, place.f
    for d in range(1, n):
        pl.semaphore_signal(sem, inc=1, device_id=((s + d) % n, f), device_id_type=MESH)
    for other in near:
        pl.semaphore_signal(sem, inc=1, device_id=(s, other), device_id_type=MESH)
    pl.semaphore_wait(sem, n - 1 + len(near))


def swap_halves(v):
    return pltpu.roll(v, HD // 2, axis=1)


def to_rows(first, second):
    rows = first.shape[0]
    lane = lax.broadcasted_iota(jnp.int32, (rows, 128), 1)
    wide = jnp.where(lane == 0, first, jnp.where(lane == 1, second, 0.0))
    return wide.T[:8]


def to_columns(v):
    return jnp.concatenate([v, jnp.zeros((120, v.shape[1]), F32)], axis=0).T


def exchange(place, n, own, held, send, recv):
    copies = []
    for d in range(1, n):
        copy = pltpu.make_async_remote_copy(
            own,
            held.at[d - 1],
            send.at[d - 1],
            recv.at[d - 1],
            device_id=((place.s + d) % n, place.f),
            device_id_type=MESH,
        )
        copy.start()
        copies.append(copy)
    total = own[...]
    for d in range(1, n):
        copies[d - 1].wait_recv()
        total = total + held[d - 1]
    return total, copies


def attend(block, q_v, k_v, v_v, out_v, low_v, lt_v, log_v):
    length = q_v.shape[0]
    scale = HD ** (-0.5)

    @pl.loop(0, q_v.shape[1] // HD)
    def _(h):
        cols = pl.ds(pl.multiple_of(h * HD, HD), HD)
        for i in range(length // block):
            rows, wide = pl.ds(i * block, block), pl.ds(0, (i + 1) * block)
            s = dot(q_v[rows, cols], k_v[wide, cols], NT) * scale
            column = lax.broadcasted_iota(jnp.int32, s.shape, 1)
            row = lax.broadcasted_iota(jnp.int32, s.shape, 0) + i * block
            s = jnp.where(column <= row, s, -jnp.inf)
            top = jnp.max(s, axis=-1, keepdims=True)
            p = jnp.exp(s - top)
            total = jnp.sum(p, axis=-1, keepdims=True)
            out = dot((p * (1.0 / total)).astype(BF16), v_v[wide, cols], NN)
            out_v[rows, cols] = out
            low_v[rows, cols] = out.astype(BF16)
            lt_v[cols, rows] = out.T.astype(BF16)
            log_v[h, rows, :] = top + jnp.log(total)


def opening_kernel(
    n, m, x, wq, wk, wv, own_gains, wo_own, gate_w, up_w, down_w,
    qkv, all_gains, tables, raw, heads, attended, low_t, xs_t, log_total, inverse, branch, hidden, hidden_low, wg, wu, wo,
    full, xs_v, xt_v, lt_v, w_v, wo_v, raw_v, heads_v, out_v, low_v, log_v, small, held, value,
    rc, rd, rx, ry, qbuf, zbuf, send, recv, ssend, srecv, zsem, osem,
    tsend, trecv, asend, arecv, zsend, zrecv, gsend, grecv, sems,
):
    place = Place(1)
    s, f = place.s, place.f
    rows, width = x.shape
    part = wq.shape[0]
    length, cols = raw.shape[1], raw.shape[2]
    share = wg.shape[2]
    block = min(256, length)
    per = block // rows
    weights = (wq, wk, wv)
    moves = Moves(sems)
    kept = []
    for j, w in enumerate(weights):
        own = w.at[:, pl.ds(pl.multiple_of(s * cols, cols), cols)]
        kept.append(moves.start(own, w_v.at[j, s, f]))
    own_out = [moves.start(wo_own, wo_v.at[f])]
    full[f, s] = own_gains[...]
    xs_v[0, s] = x[...]
    line_barrier(n, m)
    sent = []

    def remote(src, dst, a, b, device):
        copy = pltpu.make_async_remote_copy(src, dst, a, b, device_id=device, device_id_type=MESH)
        copy.start()
        sent.append(copy)
        return copy

    second = []
    for j, w in enumerate(weights):
        row = []
        for d in range(1, n):
            t = (s + d) % n
            src = w.at[:, pl.ds(pl.multiple_of(t * cols, cols), cols)]
            row.append(remote(src, w_v.at[j, s, f], asend.at[j, d], arecv.at[j, d], (t, f)))
        second.append(row)
    first = []
    for d in range(1, n):
        first.append(remote(own_gains, full.at[f, s], gsend.at[d], grecv.at[d], ((s + d) % n, f)))

    def piece(j, o):
        return full.at[o] if j == 3 else w_v.at[j, :, o]

    def hop(way, h, j):
        o = f - h if way == 0 else f + h
        there = f + 1 if way == 0 else f - 1
        place_ = piece(j, o)
        return pltpu.make_async_remote_copy(
            place_, place_, zsend.at[way, h, j], zrecv.at[way, h, j], device_id=(s, there), device_id_type=MESH
        )

    def sends(way, h):
        return ((f - h >= 0) & (f < m - 1)) if way == 0 else ((f + h <= m - 1) & (f > 0))

    def receives(way, h):
        return (f - h - 1 >= 0) if way == 0 else (f + h + 1 <= m - 1)

    def start(h, j):
        for way in (0, 1):
            when(sends(way, h), lambda: hop(way, h, j).start())

    def landed(h, j):
        for way in (0, 1):
            o = f - h - 1 if way == 0 else f + h + 1

            def wait():
                there = f - 1 if way == 0 else f + 1
                place_ = piece(j, o)
                pltpu.make_async_remote_copy(
                    place_, place_, zsend.at[way, h, j], zrecv.at[way, h, j], device_id=(s, there), device_id_type=MESH
                ).wait_recv()

            when(receives(way, h), wait)

    def step(h, j):
        landed(h, j)
        if h + 1 < m - 1:
            start(h + 1, j)

    moves.wait(kept)
    for j in range(3):
        for copy in second[j]:
            copy.wait_recv()
        start(0, j)
    for copy in first:
        copy.wait_recv()
    start(0, 3)
    gathered = gather_pairs(
        place, Wires(tsend, trecv), x, xs_v, lambda *_: None, Work([lambda: None, lambda: step(0, 0), lambda: step(0, 1)])
    )
    step(0, 2)
    step(0, 3)
    half = HD // 2
    lane = lax.broadcasted_iota(jnp.int32, (block, HD), 1)
    row = lax.broadcasted_iota(jnp.int32, (block, HD), 0)
    frequency = jnp.exp((lane % half).astype(F32) * (-2.0 * math.log(THETA) / HD))

    @pl.loop(0, length // block)
    def _(i):
        angle = (row + i * block).astype(F32) * frequency
        here = pl.ds(pl.multiple_of(i * block, block), block)
        tables[0, here, :] = jnp.cos(angle)
        sine = jnp.sin(angle)
        tables[1, here, :] = jnp.where(lane < half, -sine, sine)

    for h in range(1, m - 2):
        for j in range(4):
            step(h, j)

    out_copies = []
    for d, plane in enumerate((flip(f, 1), opposite(f), opposite(flip(f, 1)))):
        out_copies.append(
            pltpu.make_async_remote_copy(
                wo_own, wo_v.at[f], osem.at[0, d], osem.at[1, d], device_id=(s, plane), device_id_type=MESH
            )
        )
        out_copies[-1].start()
    stream = Stream(place, zsem)
    views = [half_columns(gate_w, share), half_columns(up_w, share)]
    fulls = [wg, wu]
    for k in range(2):
        stream.start_far(k, views[k], fulls[k])
    for k in range(2):
        stream.start_near(k, views[k], fulls[k])

    @pl.loop(0, length // block)
    def _(i):
        here = pl.ds(pl.multiple_of(i * block, block), block)
        xt_v[:, here] = xs_v[0, pl.ds(i * per, per)].reshape(block, width).T

    def project(j):
        @pl.loop(0, length // block)
        def _(i):
            here = pl.ds(pl.multiple_of(i * block, block), block)
            a = xs_v[0, pl.ds(i * per, per)].reshape(block, width)
            product = dot(a, w_v[j].reshape(width, cols), NN)
            if j == 2:
                heads_v[2, here, :] = product.astype(BF16)
            else:
                raw_v[j, here, :] = product

    moves.start(xt_v, xs_t)
    for j in range(3):
        landed(m - 2, j)
        project(j)
    landed(m - 2, 3)
    for t in range(n):
        for plane in range(m):
            at = (t * m + plane) * part
            all_gains[:, at : at + part] = full[plane, t, :, :part]
    moves.start(w_v, qkv)

    @pl.loop(0, length // block)
    def _(i):
        here = pl.ds(pl.multiple_of(i * block, block), block)
        q, k = raw_v[0, here, :], raw_v[1, here, :]
        small[0, :, here] = to_rows(
            jnp.sum(q * q, axis=1, keepdims=True), jnp.sum(k * k, axis=1, keepdims=True)
        )

    moves.start(raw_v, raw)
    first_col = pl.multiple_of(s * cols, cols)
    total, stat_copies = exchange(place, n, small.at[0], held, ssend, srecv)
    small[1] = lax.rsqrt(total * (1.0 / width) + EPSILON)
    moves.start(small.at[1], inverse)

    @pl.loop(0, length // block)
    def _(i):
        here = pl.ds(pl.multiple_of(i * block, block), block)
        inv = to_columns(small[1, :, here])
        cosine, sine = tables[0, here, :], tables[1, here, :]
        for j in range(2):
            for h in range(cols // HD):
                part = pl.ds(h * HD, HD)
                v = raw_v[j, here, part] * inv[:, j : j + 1] * all_gains[j : j + 1, pl.ds(first_col + h * HD, HD)]
                heads_v[j, here, part] = (v * cosine + swap_halves(v) * sine).astype(BF16)

    moves.start(heads_v, heads)
    attend(block, heads_v.at[0], heads_v.at[1], heads_v.at[2], out_v, low_v, lt_v, log_v)
    moves.start(out_v, attended)
    moves.start(lt_v, low_t)
    moves.start(log_v, log_total)
    moves.wait(own_out)
    for copy in out_copies:
        copy.wait_recv()
    moves.start(wo_v, wo)
    step = min(512, width)

    def make(q, chip, c, first):
        here = pl.ds(pl.multiple_of(chip * 4 * rows, 4 * rows), 4 * rows)

        @pl.loop(0, width // 2 // step)
        def _(j):
            at = pl.ds(pl.multiple_of(first + j * step, step), step)
            part = dot(low_v[here, :], wo_v[:, :, at].reshape(cols, step), NN).astype(BF16)
            value[q, pl.ds(4 * chip, 4), :, at] = part.reshape(4, rows, step)

    live = scatter_pairs(
        place, Wires(send, recv), value, rc, rd, rx, ry, qbuf, zbuf, make, branch,
        Work([lambda: None, lambda: stream.relay(0, views[0], fulls[0])]),
    )
    total = branch[...]
    inv = lax.rsqrt(jnp.mean(total * total, axis=-1, keepdims=True) + EPSILON)
    h = x[...].astype(F32) + total * inv * all_gains[2:3, :]
    hidden[...] = h
    hidden_low[...] = h.astype(BF16)
    for copy in list(live.values()) + list(gathered.values()) + stat_copies + sent:
        copy.wait_send()
    for h in range(m - 1):
        for j in range(4):
            for way in (0, 1):
                when(sends(way, h), lambda: hop(way, h, j).wait_send())
    moves.finish()
    stream.finish(0, views[0], fulls[0])
    for copy in (
        stream.near_copy(1, views[1], fulls[1]),
        stream.far_copy(1, views[1], fulls[1]),
        stream.own_copy(1, views[1], fulls[1]),
    ):
        copy.wait()
    for copy in out_copies:
        copy.wait_send()


def opening(x, wq, wk, wv, gains, wo, gate_w, up_w, down_w, n, m, ident):
    rows, width = x.shape
    part, cols = wq.shape[0], width // n
    length, share = n * rows, gate_w.shape[1] // 2
    dma = pltpu.SemaphoreType.DMA
    heads = cols // HD
    outs = [
        shape((3, n, m, part, cols), BF16),
        shape((gains.shape[0], width), F32),
        shape((2, length, HD), F32),
        shape((2, length, cols), F32),
        shape((3, length, cols), BF16),
        shape((length, cols), F32),
        shape((cols, length), BF16),
        shape((width, length), BF16),
        shape((heads, length, 1), F32),
        shape((8, length), F32),
        shape((rows, width), F32),
        shape((rows, width), F32),
        shape((rows, width), BF16),
        shape((m, gate_w.shape[0], share), BF16),
        shape((m, gate_w.shape[0], share), BF16),
        shape((m,) + wo.shape, BF16),
    ]
    return pl.pallas_call(
        functools.partial(opening_kernel, n, m),
        in_specs=vmem_specs(5) + any_specs(4),
        out_specs=any_specs(1) + vmem_specs(2) + any_specs(7) + vmem_specs(3) + any_specs(3),
        out_shape=outs,
        scratch_shapes=[
            pltpu.VMEM((m, n) + gains.shape, F32),
            pltpu.VMEM((1, n, rows, width), BF16),
            pltpu.VMEM((width, length), BF16),
            pltpu.VMEM((cols, length), BF16),
            pltpu.VMEM((3, n, m, part, cols), BF16),
            pltpu.VMEM((m,) + wo.shape, BF16),
            pltpu.VMEM((2, length, cols), F32),
            pltpu.VMEM((3, length, cols), BF16),
            pltpu.VMEM((length, cols), F32),
            pltpu.VMEM((length, cols), BF16),
            pltpu.VMEM((heads, length, 1), F32),
            pltpu.VMEM((2, 8, length), F32),
            pltpu.VMEM((n - 1, 8, length), F32),
            pltpu.VMEM((1, n, rows, width), BF16),
        ]
        + scatter_scratch(1, rows, width)
        + [dma((n - 1,)), dma((n - 1,)), dma((2, 4, 2)), dma((2, m))]
        + [dma((gather_wires(1),))] * 2
        + [dma((3, n))] * 2
        + [dma((2, m, 4))] * 2
        + [dma((n,))] * 2
        + [dma((16,))],
        compiler_params=kernel_params(ident),
        cost_estimate=pl.CostEstimate(flops=10**10, bytes_accessed=200 * 2**20, transcendentals=0),
        name=f"opening_{ident}",
    )(x, wq, wk, wv, gains, wo, gate_w, up_w, down_w)


class Settle:
    def __init__(self, place, sems, term, own, near, total, far):
        self.place, self.sems, self.term, self.own = place, sems, term, own
        self.near, self.total, self.far = near, total, far
        f = place.f
        self.f = f
        self.odd, self.half = f % 2, f // 2

    def remote(self, step, src, dst, plane):
        return pltpu.make_async_remote_copy(
            src, dst, self.sems.at[step, 0], self.sems.at[step, 1], device_id=(self.place.s, plane), device_id_type=MESH
        )

    def given(self, i):
        return 1 - self.odd + 2 * i

    def kept(self, i):
        return self.odd + 2 * i

    def near_copy(self, step):
        i = 1 - self.half if step == 0 else self.half
        return self.remote(step, self.term.at[self.given(i)], self.near.at[i], flip(self.f, 1))

    def far_copy(self):
        return self.remote(2, self.total.at[0], self.far, opposite(self.f))

    def load(self, i):
        return pltpu.make_async_copy(self.term.at[self.kept(i)], self.own.at[i], self.sems.at[3, i])

    def start(self, both=False):
        self.near_copy(0).start()
        self.both = both
        if both:
            self.near_copy(1).start()
        for i in (0, 1):
            self.load(i).start()

    def mine(self, i):
        return self.term[self.kept(i)] if self.own is None else self.own[i]

    def middle(self):
        if self.own is not None:
            for i in (0, 1):
                self.load(i).wait()
        self.near_copy(0).wait_recv()
        other = 1 - self.half
        self.total[0] = add(self.mine(other), self.near[other])
        self.far_copy().start()
        if not self.both:
            self.near_copy(1).start()

    def finish(self, store):
        half = self.half
        self.near_copy(1).wait_recv()
        store(half, self.mine(half).astype(F32) + self.near[half].astype(F32))
        self.far_copy().wait_recv()
        store(1 - half, self.far[...].astype(F32))
        for step in (0, 1):
            self.near_copy(step).wait_send()
        self.far_copy().wait_send()


def settle_scratch(share, depth, own=True):
    block = lambda *lead: pltpu.VMEM(lead + (share, depth), BF16)
    return ([block(2)] if own else []) + [block(2), block(1), block(), pltpu.SemaphoreType.DMA((4, 2))]


def term_block(term, left, right, block):
    deep, long = term.shape[2], left.shape[1]
    step = min(256, deep)

    @pl.loop(0, deep // step)
    def _(j):
        at = pl.ds(pl.multiple_of(block * deep + j * step, step), step)
        to = pl.ds(pl.multiple_of(j * step, step), step)
        term[block, :, to] = dot(left[...], right[:, :, :, at].reshape(long, step), NN).astype(BF16)


class Work:
    def __init__(self, pieces):
        self.pieces = list(pieces)

    def __call__(self):
        if self.pieces:
            self.pieces.pop(0)()

    def rest(self):
        while self.pieces:
            self()


def term_work(term, left, right, prepare, out, moves):
    def piece(block):
        def run():
            if block == 0:
                prepare()
            term_block(term, left, right, block)
            moves.start(term.at[block], out.at[block])

        return run

    return [piece(block) for block in range(term.shape[0])]


def turn(v, cosine, sine):
    return v * cosine + swap_halves(v) * sine


def attend_back(block, q_v, k_v, v_v, out_v, log_v, g_v, dq, dk, dv):
    length = q_v.shape[0]
    scale = HD ** (-0.5)
    dk[...] = jnp.zeros_like(dk)
    dv[...] = jnp.zeros_like(dv)

    @pl.loop(0, q_v.shape[1] // HD)
    def _(h):
        cols = pl.ds(pl.multiple_of(h * HD, HD), HD)
        for i in range(length // block):
            rows, wide = pl.ds(i * block, block), pl.ds(0, (i + 1) * block)
            q, g = q_v[rows, cols], g_v[rows, cols]
            s = dot(q, k_v[wide, cols], NT) * scale
            column = lax.broadcasted_iota(jnp.int32, s.shape, 1)
            row = lax.broadcasted_iota(jnp.int32, s.shape, 0) + i * block
            s = jnp.where(column <= row, s, -jnp.inf)
            weights = jnp.exp(s - log_v[h, rows, :])
            correction = jnp.sum(g.astype(F32) * out_v[rows, cols], axis=-1, keepdims=True)
            gw = dot(g, v_v[wide, cols], NT)
            gs = (weights * (gw - correction)).astype(BF16)
            dq[rows, cols] = dot(gs, k_v[wide, cols], NN) * scale
            dk[wide, cols] += dot(gs, q, TN) * scale
            dv[wide, cols] += dot(weights.astype(BF16), g, TN)


def attention_back_kernel(
    g, gains, tables, inverse, wo, raw, heads, attended, low_t, log_total, xs_t, gate_term, up_t, hs,
    d3, term, gain_term, gate_grad, up_grad,
    bs, wo_v, raw_v, heads_v, out_v, low_v, log_v, ga_v, dq, dk, dv, d_v, xs_v, term_v, small, held,
    ut_v, hs_v, up_term, gown, gnear, gtotal, gfar, gsem, unear, utotal, ufar, usem,
    send, recv, ssend, srecv, sems,
):
    place = Place(1)
    n, m = bs.shape[1], wo.shape[0]
    rows, width = g.shape
    length, cols = raw.shape[1], raw.shape[2]
    share = gate_term.shape[1]
    first_col = pl.multiple_of(place.s * cols, cols)
    moves = Moves(sems)
    second = [moves.start(wo, wo_v)]
    fourth = [
        moves.start(heads, heads_v),
        moves.start(attended, out_v),
        moves.start(log_total, log_v),
        moves.start(low_t, low_v),
        moves.start(raw, raw_v),
        moves.start(xs_t, xs_v),
    ]
    bs[0, place.s] = g[...]
    full_barrier(place, n, [opposite(place.f), flip(place.f, 1)])
    gate = Settle(place, gsem, gate_term, gown, gnear, gtotal, gfar)
    up = Settle(place, usem, up_term, None, unear, utotal, ufar)
    gate.start()
    late = [moves.start(up_t, ut_v)] + [moves.start(hs.at[q], hs_v.at[q]) for q in range(hs.shape[0])]

    up.both = False

    def up_block(i):
        b = (up.given(1 - up.half), up.given(up.half), up.kept(1 - up.half), up.kept(up.half))[i]
        if i == 0:
            moves.wait(late)
        term_block(up_term, ut_v, hs_v, b)
        if i == 0:
            up.near_copy(0).start()

    block = min(256, length)
    waited = []

    def ready(q, chip):
        if not waited:
            moves.wait(second)
            waited.append(True)
        here = pl.ds(pl.multiple_of(chip * 2 * rows, 2 * rows), 2 * rows)
        a = bs[0, pl.ds(2 * chip, 2)].reshape(2 * rows, width)
        ga_v[here, :] = dot(a, wo_v[...].reshape(cols, width), NT).astype(BF16)

    live = gather_pairs(place, Wires(send, recv), g, bs, ready, Work([lambda: up_block(0), lambda: up_block(2), gate.middle]))
    up_block(1)
    up.middle()
    moves.wait(fourth)
    up_block(3)
    attend_back(block, heads_v.at[0], heads_v.at[1], heads_v.at[2], out_v, log_v, ga_v, dq, dk, dv)
    @pl.loop(0, length // block)
    def _(i):
        here = pl.ds(pl.multiple_of(i * block, block), block)
        inv = to_columns(inverse[:, here])
        cosine, sine = tables[0, here, :], -tables[1, here, :]
        sums = []
        for j, d in enumerate((dq, dk)):
            total = jnp.zeros((block, 1), F32)
            for h in range(cols // HD):
                part = pl.ds(h * HD, HD)
                normal = raw_v[j, here, part] * inv[:, j : j + 1]
                v = turn(d[here, part].astype(BF16).astype(F32), cosine, sine)
                raw_v[j, here, part] = normal
                gained = v * gains[j : j + 1, pl.ds(first_col + h * HD, HD)]
                total = total + jnp.sum(gained * normal, axis=1, keepdims=True)
                term_sum = jnp.sum(v * normal, axis=0, keepdims=True)
                d[here, part] = gained

                @pl.when(i == 0)
                def _():
                    gain_term[j, :, part] = term_sum

                @pl.when(i > 0)
                def _():
                    gain_term[j, :, part] += term_sum

            sums.append(total)
        small[0, :, here] = to_rows(sums[0], sums[1])
        d_v[2, here, :] = dv[here, :].astype(BF16)

    total, stat_copies = exchange(place, n, small.at[0], held, ssend, srecv)
    small[1] = total * (1.0 / width)

    @pl.loop(0, length // block)
    def _(i):
        here = pl.ds(pl.multiple_of(i * block, block), block)
        inv = to_columns(inverse[:, here])
        mean = to_columns(small[1, :, here])
        for j, d in enumerate((dq, dk)):
            d_v[j, here, :] = (
                inv[:, j : j + 1] * (d[here, :] - raw_v[j, here, :] * mean[:, j : j + 1])
            ).astype(BF16)

    moves.start(d_v, d3)

    @pl.loop(0, n)
    def _(i):
        at = pl.ds(pl.multiple_of(i * cols, cols), cols)
        part = dot(low_v[...], bs[0, :, :, at].reshape(length, cols), NN)
        term_v[3, i] = part.astype(BF16).reshape(m, cols // m, cols)
        for j in range(3):
            part = dot(xs_v[at, :], d_v[j], NN)
            term_v[j, i] = part.astype(BF16).reshape(m, cols // m, cols)

    moves.start(term_v, term)

    def store(ref):
        def put(u, value):
            ref[:, pl.ds(pl.multiple_of(u * share, share), share)] = value.T

        return put

    gate.finish(store(gate_grad))
    up.finish(store(up_grad))
    for copy in list(live.values()) + stat_copies:
        copy.wait_send()
    moves.finish()


def attention_back(g, gains, tables, inverse, wo, raw, heads, attended, low_t, log_total, xs_t, gate_term, up_t, hs, n, ident):
    rows, width = g.shape
    m = wo.shape[0]
    length, cols = raw.shape[1], raw.shape[2]
    share, deep = gate_term.shape[1], width // m
    dma = pltpu.SemaphoreType.DMA
    vmem = pltpu.VMEM
    outs = [
        shape((3, length, cols), BF16),
        shape((4, n, m, cols // m, cols), BF16),
        shape((2, 1, cols), F32),
        shape((deep, 2 * share), F32),
        shape((deep, 2 * share), F32),
    ]
    return pl.pallas_call(
        attention_back_kernel,
        in_specs=vmem_specs(4) + any_specs(10),
        out_specs=any_specs(2) + vmem_specs(3),
        out_shape=outs,
        scratch_shapes=[
            vmem((1, n, rows, width), BF16),
            vmem(wo.shape, BF16),
            vmem(raw.shape, F32),
            vmem(heads.shape, BF16),
            vmem(attended.shape, F32),
            vmem(low_t.shape, BF16),
            vmem(log_total.shape, F32),
            vmem((length, cols), BF16),
            vmem((length, cols), F32),
            vmem((length, cols), F32),
            vmem((length, cols), F32),
            vmem((3, length, cols), BF16),
            vmem(xs_t.shape, BF16),
            vmem((4, n, m, cols // m, cols), BF16),
            vmem((2, 8, length), F32),
            vmem((n - 1, 8, length), F32),
        ]
        + [vmem(up_t.shape, BF16), vmem(hs.shape, BF16), vmem(gate_term.shape, BF16)]
        + settle_scratch(share, deep)
        + settle_scratch(share, deep, False)
        + [
            dma((gather_wires(1),)),
            dma((gather_wires(1),)),
            dma((n - 1,)),
            dma((n - 1,)),
            dma((20,)),
        ],
        compiler_params=kernel_params(ident, 63),
        cost_estimate=pl.CostEstimate(flops=10**10, bytes_accessed=200 * 2**20, transcendentals=0),
        name=f"attention_back_{ident}",
    )(g, gains, tables, inverse, wo, raw, heads, attended, low_t, log_total, xs_t, gate_term, up_t, hs)


def attention_forward_kernel(block, q_ref, k_ref, v_ref, out_ref, low_ref, log_ref):
    length = q_ref.shape[0]
    scale = HD ** (-0.5)
    for i in range(length // block):
        rows = pl.ds(i * block, block)
        width = (i + 1) * block
        s = dot(q_ref[rows, :], k_ref[pl.ds(0, width), :], NT) * scale
        column = lax.broadcasted_iota(jnp.int32, (block, width), 1)
        row = lax.broadcasted_iota(jnp.int32, (block, width), 0) + i * block
        s = jnp.where(column <= row, s, -jnp.inf)
        top = jnp.max(s, axis=-1, keepdims=True)
        p = jnp.exp(s - top)
        total = jnp.sum(p, axis=-1, keepdims=True)
        weights = (p * (1.0 / total)).astype(BF16)
        out = dot(weights, v_ref[pl.ds(0, width), :], NN)
        out_ref[rows, :] = out
        low_ref[rows, :] = out.astype(BF16)
        log_ref[0, rows, :] = top + jnp.log(total)


def attention_forward(q, k, v):
    length, width = q.shape
    heads = width // HD
    block = min(256, length)
    column = pl.BlockSpec((length, HD), lambda h: (0, h))
    return pl.pallas_call(
        functools.partial(attention_forward_kernel, block),
        grid=(heads,),
        in_specs=[column] * 3,
        out_specs=[column, column, pl.BlockSpec((1, length, 1), lambda h: (h, 0, 0))],
        out_shape=[
            jax.ShapeDtypeStruct((length, width), F32),
            jax.ShapeDtypeStruct((length, width), BF16),
            jax.ShapeDtypeStruct((heads, length, 1), F32),
        ],
        cost_estimate=pl.CostEstimate(
            flops=2 * heads * length * length * HD, bytes_accessed=10 * length * width, transcendentals=0
        ),
    )(q, k, v)


def attention_backward_kernel(block, q_ref, k_ref, v_ref, out_ref, log_ref, g_ref, dq_ref, dk_ref, dv_ref, dk, dv):
    length = q_ref.shape[0]
    scale = HD ** (-0.5)
    dk[...] = jnp.zeros_like(dk)
    dv[...] = jnp.zeros_like(dv)
    for i in range(length // block):
        rows = pl.ds(i * block, block)
        width = (i + 1) * block
        wide = pl.ds(0, width)
        q = q_ref[rows, :]
        g = g_ref[rows, :]
        s = dot(q, k_ref[wide, :], NT) * scale
        column = lax.broadcasted_iota(jnp.int32, (block, width), 1)
        row = lax.broadcasted_iota(jnp.int32, (block, width), 0) + i * block
        s = jnp.where(column <= row, s, -jnp.inf)
        weights = jnp.exp(s - log_ref[0, rows, :])
        correction = jnp.sum(g.astype(F32) * out_ref[rows, :], axis=-1, keepdims=True)
        gw = dot(g, v_ref[wide, :], NT)
        gs = (weights * (gw - correction)).astype(BF16)
        dq_ref[rows, :] = (dot(gs, k_ref[wide, :], NN) * scale).astype(BF16)
        dk[wide, :] += dot(gs, q, TN)
        dv[wide, :] += dot(weights.astype(BF16), g, TN)
    dk_ref[...] = (dk[...] * scale).astype(BF16)
    dv_ref[...] = dv[...].astype(BF16)


def attention_backward(q, k, v, out, log_total, g):
    length, width = q.shape
    heads = width // HD
    block = min(256, length)
    column = pl.BlockSpec((length, HD), lambda h: (0, h))
    return pl.pallas_call(
        functools.partial(attention_backward_kernel, block),
        grid=(heads,),
        in_specs=[column] * 4 + [pl.BlockSpec((1, length, 1), lambda h: (h, 0, 0)), column],
        out_specs=[column] * 3,
        out_shape=[jax.ShapeDtypeStruct((length, width), BF16)] * 3,
        scratch_shapes=[pltpu.VMEM((length, HD), F32)] * 2,
        cost_estimate=pl.CostEstimate(
            flops=5 * heads * length * length * HD, bytes_accessed=16 * length * width, transcendentals=0
        ),
    )(q, k, v, out, log_total, g)


def on_device(n, m, pair, *args):
    (
        tokens,
        query_weight,
        key_weight,
        value_weight,
        out_weight,
        query_gain,
        key_gain,
        attention_gain,
        gate_weight,
        up_weight,
        down_weight,
        feedforward_gain,
        cotangent,
    ) = args
    rows, width = tokens.shape[1], tokens.shape[2]
    length = rows * n
    part = query_weight.shape[0]
    cols = width // n
    depth, units = gate_weight.shape
    share = units // pair
    x = tokens.reshape(rows, width)
    groups = [[g * pair + u for u in range(pair)] for g in range(m // pair)]

    native = n == 8 and m == 4

    def gather_plane(v, ident):
        if native:
            return plane_gather(v, n, 1, ident)
        return lax.all_gather(v, "seq", axis=0, tiled=True)

    def scatter_plane(v, ident):
        if native:
            return plane_scatter(v, n, 1, ident)
        return lax.psum_scatter(v.astype(BF16), "seq", scatter_dimension=0, tiled=True).astype(F32)

    def gather_pair(v, ident):
        if native:
            return plane_gather(v, n, pair, ident)
        if pair > 1:
            v = lax.all_gather(v, "fsdp", axis=0, axis_index_groups=groups)
        v = lax.all_gather(v.reshape(pair, rows, width), "seq", axis=1, tiled=True)
        return v.reshape(pair * length, width)

    def scatter_pair(v, ident):
        if native:
            return plane_scatter(v, n, pair, ident)
        v = lax.psum_scatter(v.astype(BF16).reshape(pair, length, width), "seq", scatter_dimension=1, tiled=True)
        if pair > 1:
            v = lax.psum_scatter(v, "fsdp", scatter_dimension=0, axis_index_groups=groups)
        return v.reshape(rows, width).astype(F32)

    def total_plane(v, ident):
        return plane_sum(v, n, ident) if native else lax.psum(v, "seq")

    def spread(halves):
        return lax.all_to_all(jnp.tile(halves, (m // pair, 1, 1)), "fsdp", 0, 0, tiled=False)

    def settle(blocks):
        back = lax.all_to_all(blocks.astype(BF16), "fsdp", 0, 0, tiled=False)
        if native:
            return jnp.sum(back.reshape((pair, m // pair) + back.shape[1:]).astype(F32), axis=1)
        return jnp.sum(back.reshape((m // pair, pair) + back.shape[1:]).astype(F32), axis=0)

    gains = jnp.stack([query_gain, key_gain, attention_gain, feedforward_gain]).astype(F32)
    grad_out = cotangent.reshape(rows, width)
    if native:
        (
            qkv, gains, tables, raw, heads, attended, low_t, xs_t, log_total, inverse, branch, hidden, hidden_low,
            gate_cols, up_cols, out_rows,
        ) = opening(
            x, query_weight, key_weight, value_weight, jnp.pad(gains, ((0, 4), (0, 128 - part))),
            out_weight, gate_weight, up_weight, down_weight, n, m, 1
        )
        gate_cols = gate_cols.reshape(width, share)
        hs, gate, up, inner, inner_t, down_rows, up_cols = ffn_up(hidden_low, gate_cols, up_cols, down_weight, n, pair, 5)
        layer_out, grad_low, feed_gain_term, down_rows = ffn_down(
            inner, down_rows, hidden, gains, grad_out, n, pair, 7
        )
        grad_gate, grad_up, gate_t, up_t, down_term = ffn_grad(
            grad_low, down_rows, gate, up, inner_t, n, m, pair, 6
        )
        grad_hidden, branch_low, branch_gain_term, down_grad, gate_term = ffn_back(
            grad_gate, grad_up, gate_cols, up_cols, gate_t, hs, down_term, branch, gains, grad_out, n, m, pair, 8
        )
        d3, term, gain_own, gate_grad, up_grad = attention_back(
            branch_low, gains, tables, inverse, out_rows, raw, heads, attended, low_t, log_total,
            xs_t, gate_term, up_t, hs, n, 2
        )
        tokens_grad, term, gain_grads = leave(
            d3, term, gain_own, branch_gain_term, feed_gain_term, grad_hidden, qkv, n, m, 4
        )
        layer_out, tokens_grad, *term, gate_grad, up_grad, down_grad = place_outputs(
            [layer_out, tokens_grad, term, gate_grad, up_grad, down_grad]
        )
        out_grad = term[3]
    else:
        cosine, sine = angles_of(length)
        seq = lax.axis_index("seq")
        stacked = jnp.stack([query_weight, key_weight, value_weight]).reshape(3, part, n, cols)
        mine = lax.all_to_all(stacked.transpose(2, 0, 1, 3), "seq", 0, 0)
        qkv = lax.all_gather(mine, "fsdp", axis=1).transpose(2, 0, 1, 3, 4).reshape(3, width, cols)
        full_gain = lax.all_gather(gains, ("seq", "fsdp"), axis=1).reshape(4, width)
        xs = gather_plane(x, 1)
        out_rows = lax.all_gather(out_weight, "fsdp", axis=0, tiled=True)
        own_gain = lax.dynamic_slice_in_dim(full_gain[:2], seq * cols, cols, 1)
        q_gain, k_gain, branch_gain, feed_gain = own_gain[0], own_gain[1], full_gain[2], full_gain[3]
        q_raw, k_raw, v = dot(xs, qkv[0], NN), dot(xs, qkv[1], NN), dot(xs, qkv[2], NN).astype(BF16)
        squares = jnp.stack([jnp.sum(q_raw * q_raw, axis=1), jnp.sum(k_raw * k_raw, axis=1)])
        inverse = lax.rsqrt(lax.psum(squares, "seq") / width + EPSILON)
        q_inv, k_inv = inverse[0][:, None], inverse[1][:, None]
        q = rotate(q_raw * q_inv * q_gain, cosine, sine, 1.0).astype(BF16)
        k = rotate(k_raw * k_inv * k_gain, cosine, sine, 1.0).astype(BF16)
        attended, attended_low, log_total = attention_forward(q, k, v)
        branch = scatter_plane(dot(attended_low, out_rows, NN), 3)
        branch_inv = lax.rsqrt(jnp.mean(branch * branch, axis=1, keepdims=True) + EPSILON)
        hidden = x.astype(F32) + branch * branch_inv * branch_gain
        hidden_low = hidden.astype(BF16)
        gate_cols = spread(gate_weight.reshape(depth, pair, share).transpose(1, 0, 2)).reshape(width, share)
        up_cols = spread(up_weight.reshape(depth, pair, share).transpose(1, 0, 2)).reshape(width, share)
        down_rows = spread(down_weight.reshape(pair, share, depth)).transpose(1, 0, 2).reshape(share, width)
        grad_out = grad_out.astype(F32)
        hs = gather_pair(hidden_low, 5)
        gate = dot(hs, gate_cols, NN)
        up = dot(hs, up_cols, NN)
        sig = jax.nn.sigmoid(gate)
        inner = (gate * sig * up).astype(BF16)
        feed = scatter_pair(dot(inner, down_rows, NN), 7)
        feed_inv = lax.rsqrt(jnp.mean(feed * feed, axis=1, keepdims=True) + EPSILON)
        layer_out = (hidden + feed * feed_inv * feed_gain).astype(BF16)
        grad_feed, term = rms_back(feed, feed_gain, grad_out)
        feed_gain_term = jnp.sum(term, axis=0)
        gs = gather_pair(grad_feed.astype(BF16), 6)
        grad_inner = dot(gs, down_rows, NT)
        grad_gate = (grad_inner * up * sig * (1.0 + gate * (1.0 - sig))).astype(BF16)
        grad_up = (grad_inner * gate * sig).astype(BF16)
        grad_hidden = grad_out + scatter_pair(dot(grad_gate, gate_cols, NT) + dot(grad_up, up_cols, NT), 8)
        grad_branch, term = rms_back(branch, branch_gain, grad_hidden)
        branch_low = grad_branch.astype(BF16)
        branch_gain_term = jnp.sum(term, axis=0)
        inner_t, gate_t, up_t = inner.T, grad_gate.T, grad_up.T

        def cut(v):
            return v.reshape(share, m, depth).transpose(1, 0, 2)

        down_grad = settle(cut(dot(inner_t, gs, NN))).reshape(units, depth)
        gate_grad = settle(cut(dot(gate_t, hs, NN))).transpose(2, 0, 1).reshape(depth, units)
        up_grad = settle(cut(dot(up_t, hs, NN))).transpose(2, 0, 1).reshape(depth, units)
        bs = gather_plane(branch_low, 2)
        out_grad = lax.psum_scatter(
            dot(attended_low, bs, TN).astype(BF16), "fsdp", scatter_dimension=0, tiled=True
        ).astype(F32)
        grad_attended = dot(bs, out_rows, NT).astype(BF16)
        dq, dk, dv = attention_backward(q, k, v, attended, log_total, grad_attended)
        dq = rotate(dq.astype(F32), cosine, sine, -1.0)
        dk = rotate(dk.astype(F32), cosine, sine, -1.0)
        q_normal, k_normal = q_raw * q_inv, k_raw * k_inv
        q_gain_term = jnp.sum(dq * q_normal, axis=0)
        k_gain_term = jnp.sum(dk * k_normal, axis=0)
        dq, dk = dq * q_gain, dk * k_gain
        means = total_plane(jnp.stack([jnp.sum(dq * q_normal, axis=1), jnp.sum(dk * k_normal, axis=1)]), 10) / width
        dq = (q_inv * (dq - q_normal * means[0][:, None])).astype(BF16)
        dk = (k_inv * (dk - k_normal * means[1][:, None])).astype(BF16)
        value = dot(dq, qkv[0], NT) + dot(dk, qkv[1], NT) + dot(dv, qkv[2], NT)
        term = jnp.stack([dot(xs, d, TN).astype(BF16) for d in (dq, dk, dv)]).reshape(3, n, m, part, cols)
        gain_own = jnp.stack([q_gain_term, k_gain_term])
        gain_own = lax.dynamic_update_slice(jnp.zeros((2, width), F32), gain_own, (0, seq * cols))
        gain_terms = jnp.concatenate([gain_own, jnp.stack([branch_gain_term, feed_gain_term])]).reshape(4, n, m, part)
        tokens_grad = grad_hidden + scatter_plane(value, 4)
        term = lax.psum_scatter(term, "fsdp", scatter_dimension=2)
        term = lax.all_to_all(term, "seq", 1, 1).astype(F32).transpose(0, 2, 1, 3)
        gain_grads = lax.psum_scatter(
            gain_terms.reshape(4, width), ("seq", "fsdp"), scatter_dimension=1, tiled=True
        )
        term = term.reshape(3, part, width)

    return (
        layer_out.reshape(tokens.shape),
        tokens_grad.reshape(tokens.shape),
        term[0],
        term[1],
        term[2],
        out_grad,
        gain_grads[0],
        gain_grads[1],
        gain_grads[2],
        gate_grad,
        up_grad,
        down_grad,
        gain_grads[3],
    )


def solution(mesh):
    n, m = mesh.shape["seq"], mesh.shape["fsdp"]
    tall, flat, act = P(("seq", "fsdp"), None), P(("seq", "fsdp")), P("fsdp", "seq", None)
    wide, deep = P("fsdp", "seq"), P("seq", "fsdp")
    return jax.shard_map(
        functools.partial(on_device, n, m, 2),
        mesh=mesh,
        in_specs=(act, tall, tall, tall, tall, flat, flat, flat, wide, wide, deep, flat, act),
        out_specs=(act, act, tall, tall, tall, tall, flat, flat, flat, wide, wide, deep, flat),
        check_vma=False,
    )
```

```python
import functools
import math

import jax
import jax.numpy as jnp
from jax import lax
from jax.experimental import pallas as pl
from jax.experimental.pallas import tpu as pltpu
from jax.sharding import PartitionSpec as P

EPSILON = 1e-06
THETA = 500000.0
HD = 128
F32 = jnp.float32
BF16 = jnp.bfloat16


def dot(a, b, dims):
    return lax.dot_general(a, b, (dims, ((), ())), preferred_element_type=F32)


NN = ((1,), (0,))
NT = ((1,), (1,))
TN = ((0,), (0,))


def angles_of(length):
    half = HD // 2
    frequency = jnp.exp(jnp.arange(half, dtype=F32) * (-2.0 * math.log(THETA) / HD))
    angle = jnp.arange(length, dtype=F32)[:, None] * frequency[None, :]
    return jnp.cos(angle), jnp.sin(angle)


def rotate(value, cosine, sine, sign):
    length, width = value.shape
    value = value.reshape(length, width // HD, 2, HD // 2)
    first, second = value[:, :, 0], value[:, :, 1]
    c, s = cosine[:, None, :], sign * sine[:, None, :]
    return jnp.stack([first * c - second * s, second * c + first * s], axis=2).reshape(length, width)


MESH = pl.DeviceIdType.MESH


def flip(index, bit):
    return index + bit - 2 * bit * ((index // bit) % 2)


class Place:
    def __init__(self, pair):
        self.s, self.f = lax.axis_index("seq"), lax.axis_index("fsdp")
        self.pair = pair
        s, f = self.s, self.f
        self.sx, self.sy = flip(s, 2), flip(s, 4)
        self.sd, self.sc = flip(self.sx, 4), flip(s, 1)
        self.q = f // 2 if pair > 1 else 0
        self.x, self.y, self.core = (self.sx, f), (self.sy, f), (self.sc, f)
        self.z = (s, opposite(f)) if pair > 1 else None
        self.peers = [self.x, self.y, self.core] + ([self.z] if pair > 1 else [])

    def barrier(self):
        sem = pltpu.get_barrier_semaphore()
        for peer in self.peers:
            pl.semaphore_signal(sem, inc=1, device_id=peer, device_id_type=MESH)
        pl.semaphore_wait(sem, len(self.peers))


class Wires:
    def __init__(self, send, recv):
        self.send, self.recv, self.count, self.open = send, recv, 0, {}

    def new(self, key):
        self.open[key] = self.count
        self.count += 1

    def go(self, key, src, dst, device):
        i = self.open[key]
        copy = pltpu.make_async_remote_copy(
            src, dst, self.send.at[i], self.recv.at[i], device_id=device, device_id_type=MESH
        )
        copy.start()
        return copy


def gather_steps(place, wires, own, out, ready):
    pair, rows = place.pair, own.shape[0]
    half = rows // 2
    top, low = pl.ds(0, half), pl.ds(half, half)
    p = place
    qs = [p.q] + ([1 - p.q] if pair > 1 else [])
    kinds = ["xa", "xb", "ya", "yb", "xd", "yd", "c0", "cxa", "cxb", "cya", "cyb", "cda", "cdb"]
    for t in range(pair):
        for kind in kinds:
            wires.new((t, kind))
    if pair > 1:
        wires.new("z")
    live = {}

    def go(key, src, dst, device):
        live[key] = wires.go(key, src, dst, device)

    def begin(t, src):
        q = qs[t]
        go((t, "xa"), src.at[top], out.at[q, p.s, top], p.x)
        go((t, "yb"), src.at[low], out.at[q, p.s, low], p.y)
        go((t, "xb"), src.at[low], out.at[q, p.s, low], p.x)
        go((t, "ya"), src.at[top], out.at[q, p.s, top], p.y)
        go((t, "c0"), src, out.at[q, p.s], p.core)

    def arrived(key):
        live[key].wait_recv()

    if pair > 1:
        go("z", own, out.at[qs[0], p.s], p.z)
    begin(0, own)
    ready(qs[0], p.s, None)

    def first(t):
        q = qs[t]
        arrived((t, "xa"))
        go((t, "xd"), out.at[q, p.sx, top], out.at[q, p.sx, top], p.y)
        go((t, "cxa"), out.at[q, p.sx, top], out.at[q, p.sx, top], p.core)
        arrived((t, "yb"))
        go((t, "yd"), out.at[q, p.sy, low], out.at[q, p.sy, low], p.x)
        go((t, "cyb"), out.at[q, p.sy, low], out.at[q, p.sy, low], p.core)
        arrived((t, "c0"))
        ready(q, p.sc, None)

    def second(t):
        q = qs[t]
        arrived((t, "xb"))
        go((t, "cxb"), out.at[q, p.sx, low], out.at[q, p.sx, low], p.core)
        ready(q, p.sx, None)
        arrived((t, "ya"))
        go((t, "cya"), out.at[q, p.sy, top], out.at[q, p.sy, top], p.core)
        ready(q, p.sy, None)
        arrived((t, "xd"))
        go((t, "cda"), out.at[q, p.sd, top], out.at[q, p.sd, top], p.core)
        arrived((t, "yd"))
        go((t, "cdb"), out.at[q, p.sd, low], out.at[q, p.sd, low], p.core)

    def third(t):
        q = qs[t]
        arrived((t, "cxa"))
        arrived((t, "cxb"))
        ready(q, flip(p.sx, 1), None)
        arrived((t, "cya"))
        arrived((t, "cyb"))
        ready(q, flip(p.sy, 1), None)
        ready(q, p.sd, None)
        arrived((t, "cda"))
        arrived((t, "cdb"))
        ready(q, flip(p.sd, 1), None)

    first(0)
    if pair > 1:
        arrived("z")
        begin(1, out.at[qs[1], p.s])
        ready(qs[1], p.s, None)
    second(0)
    if pair > 1:
        first(1)
    third(0)
    if pair > 1:
        second(1)
        third(1)
    for copy in live.values():
        copy.wait_send()


def gather_wires(pair):
    return 14 * pair + (2 if pair > 1 else 0)


def gather_kernel(pair, own, out, send, recv, local):
    place = Place(pair)
    keep = pltpu.make_async_copy(own, out.at[place.q, place.s], local)
    keep.start()
    place.barrier()
    gather_steps(place, Wires(send, recv), own, out, lambda q, slot, half: None)
    keep.wait()


def plane_gather(v, n, pair, ident):
    rows, width = v.shape
    return pl.pallas_call(
        functools.partial(gather_kernel, pair),
        in_specs=[pl.BlockSpec(memory_space=pltpu.VMEM)],
        out_specs=pl.BlockSpec(memory_space=pl.ANY),
        out_shape=jax.ShapeDtypeStruct((pair, n, rows, width), v.dtype),
        scratch_shapes=[pltpu.SemaphoreType.DMA((gather_wires(pair),))] * 2 + [pltpu.SemaphoreType.DMA],
        compiler_params=pltpu.CompilerParams(collective_id=ident, has_side_effects=True),
        cost_estimate=pl.CostEstimate(flops=0, bytes_accessed=pair * n * rows * width * 20, transcendentals=0),
        name=f"gather_{ident}",
    )(v).reshape(pair * n * rows, width)


def add(a, b):
    return (a.astype(F32) + b.astype(F32)).astype(BF16)


def scatter_steps(place, wires, part, rc, rd, rx, ry, qbuf, zbuf, make, finish):
    p, pair = place, place.pair
    rows = rx.shape[1]
    half = rows // 2
    top, low = pl.ds(0, half), pl.ds(half, half)
    slots = {"d": p.sd, "x": p.sx, "y": p.sy, "o": p.s}
    order = ["d", "x", "y", "o"]
    names = ["c" + k for k in order] + ["da", "db", "xa", "xb", "ya", "yb"]
    for t in range(pair):
        for name in names:
            wires.new((t, name))
    if pair > 1:
        wires.new("z")
    live = {}

    def go(key, src, dst, device):
        live[key] = wires.go(key, src, dst, device)

    def arrived(key):
        live[key].wait_recv()

    for t in range(pair):
        for i, k in enumerate(order):
            make(t, k, 1)
            go((t, "c" + k), part(t, flip(slots[k], 1)), rc.at[t, i], p.core)

    def start(t):
        make(t, "d", 0)
        arrived((t, "cd"))
        qbuf[t, 0] = add(part(t, p.sd)[...], rc[t, 0])
        go((t, "da"), qbuf.at[t, 0, top], rd.at[t, top], p.x)
        go((t, "db"), qbuf.at[t, 0, low], rd.at[t, low], p.y)
        make(t, "x", 0)
        arrived((t, "cx"))
        qbuf[t, 1, top] = add(part(t, p.sx)[top], rc[t, 1, top])
        go((t, "xa"), qbuf.at[t, 1, top], rx.at[t, top], p.x)
        make(t, "y", 0)
        arrived((t, "cy"))
        qbuf[t, 2, low] = add(part(t, p.sy)[low], rc[t, 2, low])
        go((t, "yb"), qbuf.at[t, 2, low], ry.at[t, low], p.y)

    def relay(t):
        held = part(t, p.sx)[low].astype(F32) + rc[t, 1, low].astype(F32)
        arrived((t, "db"))
        qbuf[t, 1, low] = (held + rd[t, low].astype(F32)).astype(BF16)
        go((t, "xb"), qbuf.at[t, 1, low], rx.at[t, low], p.x)
        held = part(t, p.sy)[top].astype(F32) + rc[t, 2, top].astype(F32)
        arrived((t, "da"))
        qbuf[t, 2, top] = (held + rd[t, top].astype(F32)).astype(BF16)
        go((t, "ya"), qbuf.at[t, 2, top], ry.at[t, top], p.y)

    def total(t):
        make(t, "o", 0)
        arrived((t, "co"))
        value = part(t, p.s)[...].astype(F32) + rc[t, 3].astype(F32)
        for key in ("xa", "yb", "xb", "ya"):
            arrived((t, key))
        return value + rx[t].astype(F32) + ry[t].astype(F32)

    if pair > 1:
        start(0)
        start(1)
        relay(0)
        relay(1)
        zbuf[0] = total(0).astype(BF16)
        go("z", zbuf.at[0], zbuf.at[1], p.z)
        value = total(1)
        arrived("z")
        value = value + zbuf[1].astype(F32)
    else:
        start(0)
        relay(0)
        value = total(0)
    finish(value)
    for copy in live.values():
        copy.wait_send()


def scatter_wires(pair):
    return 84 if pair > 1 else 20


def scatter_scratch(pair, rows, width):
    block = lambda *lead: pltpu.VMEM(lead + (rows, width), BF16)
    return [
        block(pair, 4),
        block(pair),
        block(pair),
        block(pair),
        block(pair, 3),
        block(2) if pair > 1 else pltpu.VMEM((2, 16, 128), BF16),
        pltpu.SemaphoreType.DMA((scatter_wires(pair),)),
        pltpu.SemaphoreType.DMA((scatter_wires(pair),)),
    ]


def scatter_kernel(pair, value, out, rc, rd, rx, ry, qbuf, zbuf, send, recv):
    place = Place(pair)
    place.barrier()
    planes = [1 - place.q, place.q] if pair > 1 else [0]

    def part(t, slot):
        return value.at[planes[t], slot]

    def finish(total):
        out[...] = total

    scatter_steps(
        place, Wires(send, recv), part, rc, rd, rx, ry, qbuf, zbuf, lambda *_: None, finish
    )


def plane_scatter(v, n, pair, ident):
    width = v.shape[1]
    rows = v.shape[0] // (pair * n)
    return pl.pallas_call(
        functools.partial(scatter_kernel, pair),
        in_specs=[pl.BlockSpec(memory_space=pltpu.VMEM)],
        out_specs=pl.BlockSpec(memory_space=pltpu.VMEM),
        out_shape=jax.ShapeDtypeStruct((rows, width), F32),
        scratch_shapes=scatter_scratch(pair, rows, width),
        compiler_params=pltpu.CompilerParams(
            collective_id=ident, has_side_effects=True, vmem_limit_bytes=40 * 2**20
        ),
        cost_estimate=pl.CostEstimate(flops=0, bytes_accessed=pair * n * rows * width * 20, transcendentals=0),
        name=f"scatter_{ident}",
    )(v.astype(BF16).reshape(pair, n, rows, width))


def sum_kernel(n, own, out, held, send, recv):
    s, f = lax.axis_index("seq"), lax.axis_index("fsdp")
    sem = pltpu.get_barrier_semaphore()
    for d in range(1, n):
        pl.semaphore_signal(sem, inc=1, device_id=((s + d) % n, f), device_id_type=MESH)
    pl.semaphore_wait(sem, n - 1)
    copies = []
    for d in range(1, n):
        copy = pltpu.make_async_remote_copy(
            own,
            held.at[d - 1],
            send.at[d - 1],
            recv.at[d - 1],
            device_id=((s + d) % n, f),
            device_id_type=MESH,
        )
        copy.start()
        copies.append(copy)
    total = own[...]
    for d in range(1, n):
        copies[d - 1].wait_recv()
        total = total + held[d - 1]
    out[...] = total
    for copy in copies:
        copy.wait_send()


def plane_sum(v, n, ident):
    return pl.pallas_call(
        functools.partial(sum_kernel, n),
        in_specs=[pl.BlockSpec(memory_space=pltpu.VMEM)],
        out_specs=pl.BlockSpec(memory_space=pltpu.VMEM),
        out_shape=jax.ShapeDtypeStruct(v.shape, v.dtype),
        scratch_shapes=[pltpu.VMEM((n - 1,) + v.shape, v.dtype)]
        + [pltpu.SemaphoreType.DMA((n - 1,))] * 2,
        compiler_params=pltpu.CompilerParams(collective_id=ident, has_side_effects=True),
        name=f"sum_{ident}",
    )(v)


def when(condition, body):
    pl.when(condition)(body)


def line_barrier(n, m):
    s, f = lax.axis_index("seq"), lax.axis_index("fsdp")
    sem = pltpu.get_barrier_semaphore()
    for d in range(1, n):
        pl.semaphore_signal(sem, inc=1, device_id=((s + d) % n, f), device_id_type=MESH)
    for d in range(1, m):
        pl.semaphore_signal(sem, inc=1, device_id=(s, (f + d) % m), device_id_type=MESH)
    pl.semaphore_wait(sem, n + m - 2)


def exit_kernel(
    n,
    m,
    d3,
    term,
    own_gain,
    branch_gain,
    feed_gain,
    grad_hidden,
    qkv,
    tokens_grad,
    weight_grad,
    gain_grad,
    w_v,
    value,
    rc,
    rd,
    rx,
    ry,
    qbuf,
    zbuf,
    send,
    recv,
    line,
    sums,
    done,
    got,
    gains,
    gplane,
    gsum,
    gline,
    zsend,
    zrecv,
    asend,
    arecv,
    gsend,
    grecv,
    lsend,
    lrecv,
    sems,
):
    place = Place(1)
    s, f = place.s, place.f
    moves = Moves(sems)
    moves.start(qkv, w_v)
    line_barrier(n, m)
    last = m - 1
    cols = term.shape[-1]

    def remote(src, dst, a, b, device):
        return pltpu.make_async_remote_copy(src, dst, a, b, device_id=device, device_id_type=MESH)

    def target(way, r):
        return last - r if way == 0 else r

    def hop(way, r, j, fresh):
        there = f + 1 if way == 0 else f - 1
        src = term.at[j, :, target(way, r)] if fresh else sums.at[way, r, j]
        return remote(src, line.at[way, r, j], zsend.at[way, r, j], zrecv.at[way, r, j], (s, there))

    ends = (f == 0, f == last)
    inner = (f > 0, f < last)

    def beyond(way, r):
        return target(way, r) > f if way == 0 else target(way, r) < f

    for group in ((0, 1, 2), (3,)):
        for r in range(last):
            for j in group:
                for way in (0, 1):
                    when(ends[way], lambda: hop(way, r, j, True).start())

    gain_copies = []
    for t in range(n):
        at = pl.ds(t * cols, cols)
        for j in range(2):
            gains[t, j : j + 1, :] = jnp.where(s == t, own_gain[j], 0.0)
        gains[t, 2:3, :] = branch_gain[:, at]
        gains[t, 3:4, :] = feed_gain[:, at]
        gains[t, 4:, :] = jnp.zeros((4, cols), F32)
    for d in range(1, n):
        t = (s + d) % n
        copy = remote(gains.at[t], gplane.at[d - 1], gsend.at[d], grecv.at[d], (t, f))
        copy.start()
        gain_copies.append(copy)

    moves.finish()
    rows, width = grad_hidden.shape
    block, step = 4 * rows, min(512, width)
    per = step // (m * qkv.shape[3])

    def make(q, chip, c, first):
        here = pl.ds(pl.multiple_of(chip * block, block), block)

        @pl.loop(0, width // 2 // step)
        def _(k):
            i = first // step + k
            at = pl.ds(pl.multiple_of(i * step, step), step)
            total = jnp.zeros((block, step), F32)
            for j in range(3):
                w = w_v[j, pl.ds(i * per, per)].reshape(step, cols)
                total = total + dot(d3[j, here, :], w, NT)
            value[q, pl.ds(4 * chip, 4), :, at] = total.astype(BF16).reshape(4, rows, step)

    side = f // (m // 2)
    middle = (f > 0) & (f < last)

    def relays(k, j, from_end):
        way = side if from_end else 1 - side
        o = way * k + (1 - way) * (last - k)

        def relay():
            there = f + 1 - 2 * way
            copy = remote(
                sums.at[way, k, j], line.at[way, k, j], zsend.at[way, k, j], zrecv.at[way, k, j], (s, there)
            )
            copy.wait_recv()
            sums[way, k, j] = add(term[j, :, o], line[way, k, j])
            copy.start()

        when(middle, relay)

    live = scatter_pairs(
        place, Wires(send, recv), value, rc, rd, rx, ry, qbuf, zbuf, make, tokens_grad,
        Work([lambda: None] + [lambda j=j: relays(0, j, True) for j in range(3)]),
    )

    def join(r):
        tokens_grad[r] += grad_hidden[r]

    by_rows(0, rows, join)

    total = gains[s]
    for d in range(1, n):
        gain_copies[d - 1].wait_recv()
        total = total + gplane[d - 1]
    gsum[...] = total
    line_copies = []
    for d in range(1, m):
        t = (f + d) % m
        copy = remote(gsum, gline.at[d - 1], lsend.at[d], lrecv.at[d], (s, t))
        copy.start()
        line_copies.append(copy)

    copies = []
    plan = [(True, k, j) for k in range(1, m // 2) for j in range(3)]
    plan += [(False, k, j) for k in range(m // 2 - 1) for j in range(3)] + [(None, 0, j) for j in range(3)]
    plan += [(True, k, 3) for k in range(m // 2)] + [(False, k, 3) for k in range(m // 2 - 1)] + [(None, 0, 3)]
    for from_end, k, j in plan:
        if from_end is not None:
            relays(k, j, from_end)
            continue
        own = term[j, :, f].astype(F32)
        done[j] = own
        for way in (0, 1):
            r = last - f if way == 0 else f

            def take():
                pltpu.make_async_remote_copy(
                    sums.at[way, 0, j],
                    line.at[way, r, j],
                    zsend.at[way, r, j],
                    zrecv.at[way, r, j],
                    device_id=(s, f - 1 if way == 0 else f + 1),
                    device_id_type=MESH,
                ).wait_recv()
                done[j] += line[way, r, j].astype(F32)

            when(inner[way], take)
        if j == 3:
            for t in range(n):
                weight_grad[j, :, pl.ds(t * cols, cols)] = done[j, t]
            continue
        weight_grad[j, :, pl.ds(pl.multiple_of(s * cols, cols), cols)] = done[j, s]
        got[0, j] = done[j].astype(BF16)
        for d in range(1, n):
            t = (s + d) % n
            copy = remote(got.at[0, j, t], got.at[1, j, s], asend.at[j, d], arecv.at[j, d], (t, f))
            copy.start()
            copies.append(copy)
    total = gsum[...]
    for d in range(1, m):
        line_copies[d - 1].wait_recv()
        total = total + gline[d - 1]
    small = cols // m
    gain = jnp.zeros((8, small), F32)
    for plane in range(m):
        gain = gain + jnp.where(f == plane, total[:, plane * small : (plane + 1) * small], 0.0)
    gain_grad[...] = gain
    for copy in copies:
        copy.wait_recv()
    for j in range(3):
        for d in range(1, n):
            t = (s + d) % n
            weight_grad[j, :, pl.ds(pl.multiple_of(t * cols, cols), cols)] = got[1, j, t].astype(F32)
    for copy in copies + gain_copies + line_copies + list(live.values()):
        copy.wait_send()
    for r in range(last):
        for j in range(4):
            for way in (0, 1):
                when(ends[way] | (inner[way] & beyond(way, r)), lambda: hop(way, r, j, False).wait_send())


def leave(d3, term, own_gain, branch_gain, feed_gain, grad_hidden, qkv, n, m, ident):
    rows, width = grad_hidden.shape
    part, cols = term.shape[-2:]
    vmem = pl.BlockSpec(memory_space=pltpu.VMEM)
    dma = pltpu.SemaphoreType.DMA
    block = pltpu.VMEM((2, m - 1, 4, n, part, cols), BF16)
    return pl.pallas_call(
        functools.partial(exit_kernel, n, m),
        in_specs=[vmem] * 6 + [pl.BlockSpec(memory_space=pl.ANY)],
        out_specs=[vmem] * 3,
        out_shape=[
            jax.ShapeDtypeStruct((rows, width), F32),
            jax.ShapeDtypeStruct((4, part, width), F32),
            jax.ShapeDtypeStruct((8, cols // m), F32),
        ],
        scratch_shapes=[pltpu.VMEM((3, n, m, part, cols), BF16), pltpu.VMEM((1, n, rows, width), BF16)]
        + scatter_scratch(1, rows, width)
        + [
            block,
            block,
            pltpu.VMEM((4, n, part, cols), F32),
            pltpu.VMEM((2, 3, n, part, cols), BF16),
            pltpu.VMEM((n, 8, cols), F32),
            pltpu.VMEM((n - 1, 8, cols), F32),
            pltpu.VMEM((8, cols), F32),
            pltpu.VMEM((m - 1, 8, cols), F32),
        ]
        + [dma((2, m, 4))] * 2
        + [dma((3, n))] * 2
        + [dma((n,))] * 2
        + [dma((m,))] * 2
        + [dma((3 * m,))],
        compiler_params=pltpu.CompilerParams(
            collective_id=ident, has_side_effects=True, vmem_limit_bytes=60 * 2**20
        ),
        cost_estimate=pl.CostEstimate(flops=0, bytes_accessed=200 * 2**20, transcendentals=0),
        name=f"leave_{ident}",
    )(d3, term, own_gain, branch_gain, feed_gain, grad_hidden, qkv)


class Moves:
    def __init__(self, sems):
        self.sems, self.count, self.open = sems, 0, []

    def start(self, src, dst):
        copy = pltpu.make_async_copy(src, dst, self.sems.at[self.count])
        self.count += 1
        copy.start()
        self.open.append(copy)
        return copy

    def finish(self):
        for copy in self.open:
            copy.wait()
        self.open = []

    def wait(self, copies):
        for copy in copies:
            copy.wait()
        self.open = [copy for copy in self.open if all(copy is not other for other in copies)]


def place_kernel(parts, count, *refs):
    ins, outs = refs[:count], refs[count : count + len(parts)]
    held, sems = refs[count + len(parts) : -1], refs[-1]
    copies = []
    for i, (source, row) in enumerate(parts):
        src = ins[source] if row is None else ins[source].at[row]
        copies.append(pltpu.make_async_copy(src, held[i], sems.at[0, i]))
        copies[-1].start()
    back = []
    for i in range(len(parts)):
        copies[i].wait()
        back.append(pltpu.make_async_copy(held[i], outs[i], sems.at[1, i]))
        back[-1].start()
    for copy in back:
        copy.wait()


def place_outputs(arrays):
    parts, shapes = [], []
    for source, a in enumerate(arrays):
        for row in range(a.shape[0]) if a.ndim == 3 else [None]:
            parts.append((source, row))
            shapes.append(shape(a.shape[-2:], a.dtype))
    return pl.pallas_call(
        functools.partial(place_kernel, tuple(parts), len(arrays)),
        in_specs=[pl.BlockSpec(memory_space=pltpu.MemorySpace.HBM)] * len(arrays),
        out_specs=[pl.BlockSpec(memory_space=pltpu.MemorySpace.HBM)] * len(parts),
        out_shape=shapes,
        scratch_shapes=[pltpu.VMEM(a.shape, a.dtype) for a in shapes] + [pltpu.SemaphoreType.DMA((2, len(parts)))],
        compiler_params=pltpu.CompilerParams(vmem_limit_bytes=63 * 2**20),
        name="place",
    )(*arrays)


def gather_pairs(place, wires, own, out, work, hook=lambda: None, done=lambda q, chip: None):
    p, pair = place, place.pair
    half = own.shape[0] // 2
    top, low = pl.ds(0, half), pl.ds(half, half)
    qs = [p.q] + ([1 - p.q] if pair > 1 else [])
    for t in range(pair):
        for kind in ["xa", "xb", "ya", "yb", "xd", "yd", "ca", "cb", "cxa", "cxb", "cya", "cyb", "cda", "cdb"]:
            wires.new((t, kind))
    if pair > 1:
        wires.new("za")
        wires.new("zb")
    live = {}

    def go(key, src, dst, device):
        live[key] = wires.go(key, src, dst, device)

    def arrived(*keys):
        for key in keys:
            live[key].wait_recv()

    def begin(t, src, tops):
        q = qs[t]
        rows = top if tops else low
        go((t, "xa" if tops else "xb"), src.at[rows], out.at[q, p.s, rows], p.x)
        go((t, "ya" if tops else "yb"), src.at[rows], out.at[q, p.s, rows], p.y)
        go((t, "ca" if tops else "cb"), src.at[rows], out.at[q, p.s, rows], p.core)

    def pass_on(t, name, slot, rows, device):
        ref = out.at[qs[t], slot, rows]
        go((t, name), ref, ref, device)

    def first(t):
        arrived((t, "xa"))
        pass_on(t, "xd", p.sx, top, p.y)
        pass_on(t, "cxa", p.sx, top, p.core)
        arrived((t, "ya"))
        pass_on(t, "cya", p.sy, top, p.core)

    def second(t):
        arrived((t, "yb"))
        pass_on(t, "yd", p.sy, low, p.x)
        pass_on(t, "cyb", p.sy, low, p.core)
        arrived((t, "xb"))
        pass_on(t, "cxb", p.sx, low, p.core)

    def third(t):
        arrived((t, "xd"))
        pass_on(t, "cda", p.sd, top, p.core)
        arrived((t, "yd"))
        pass_on(t, "cdb", p.sd, low, p.core)

    def chip_at(k):
        chip = p.s // 2
        return (chip % 2 + k % 2) % 2 + 2 * ((chip // 2 + k // 2) % 2)

    def use(t, first, count, *keys):
        arrived(*[(t, key) for key in keys])
        if count == 1:
            work(qs[t], chip_at(first))
        else:

            @pl.loop(first, first + count)
            def _(k):
                work(qs[t], chip_at(k))

        for k in range(first, first + count):
            done(qs[t], chip_at(k))

    if pair > 1:
        go("za", own.at[top], out.at[qs[0], p.s, top], p.z)
        go("zb", own.at[low], out.at[qs[0], p.s, low], p.z)
    begin(0, own, True)
    begin(0, own, False)
    if pair > 1:
        arrived((0, "ca"), (0, "cb"))
        hook()
        first(0)
        second(0)
        use(0, 0, 2, "cxa", "cxb")
        arrived("za")
        begin(1, out.at[qs[1], p.s], True)
        third(0)
        hook()
        use(0, 2, 2, "cya", "cyb", "cda", "cdb")
        arrived("zb")
        begin(1, out.at[qs[1], p.s], False)
        first(1)
        use(1, 0, 1, "ca", "cb")
        hook()
        second(1)
        hook()
        use(1, 1, 2, "cxa", "cxb", "cya", "cyb")
        third(1)
        use(1, 3, 1, "cda", "cdb")
    else:
        use(0, 0, 1, "ca", "cb")
        hook()
        first(0)
        hook()
        second(0)
        use(0, 1, 2, "cxa", "cxb", "cya", "cyb")
        hook()
        third(0)
        use(0, 3, 1, "cda", "cdb")
    return live


def by_rows(first, count, body):
    @pl.loop(0, count // 32)
    def _(i):
        body(pl.ds(pl.multiple_of(first + i * 32, 32), 32))


def scatter_pairs(
    place, wires, value, rc, rd, rx, ry, qbuf, zbuf, make, result, hook=lambda: None, jobs=None, mine=None, theirs=None
):
    p, pair = place, place.pair
    rows, width = rx.shape[1], rx.shape[2]
    count = 4 if pair > 1 else 2
    half, wide = rows // 2, width // count
    top, low = pl.ds(0, half), pl.ds(half, half)
    slots = {"d": p.sd, "x": p.sx, "y": p.sy, "o": p.s}
    order = ["d", "x", "y", "o"]
    planes = [1 - p.q, p.q] if pair > 1 else [p.q]
    jobs = jobs or [(t, c) for t in range(pair) for c in range(count)]
    mine = mine or list(range(count))
    theirs = theirs or mine
    for job in jobs:
        for name in ["c" + k for k in order] + ["da", "db", "xa", "xb", "ya", "yb"]:
            wires.new((job, name))
    if pair > 1:
        for c in range(count):
            wires.new(f"z{c}")
    live = {}

    def go(key, src, dst, device):
        live[key] = wires.go(key, src, dst, device)

    def arrived(*keys):
        for key in keys:
            live[key].wait_recv()

    def span(block):
        return pl.ds(block * wide if isinstance(block, int) else pl.multiple_of(block * wide, wide), wide)

    def at(c):
        return span(mine[c])

    def part(job, slot, rows_):
        return value.at[planes[job[0]], slot, rows_, at(job[1])]

    every = pl.ds(0, rows)

    def begin(job):
        t, c = job

        @pl.loop(0, 2)
        def _(k):
            make(planes[t], k, c, mine[c] * wide)

        for i, k in enumerate(order):
            go((job, "c" + k), part(job, flip(slots[k], 1), every), rc.at[t, i, :, at(c)], p.core)

    def rest(job):
        t, c = job

        def sum_of(i, slot):
            def body(r):
                qbuf[t, i, r, at(c)] = add(value[planes[t], slot, r, at(c)], rc[t, i, r, at(c)])

            return body

        arrived((job, "cd"))
        by_rows(0, rows, sum_of(0, p.sd))
        go((job, "da"), qbuf.at[t, 0, top, at(c)], rd.at[t, top, at(c)], p.x)
        go((job, "db"), qbuf.at[t, 0, low, at(c)], rd.at[t, low, at(c)], p.y)
        arrived((job, "cx"))
        by_rows(0, half, sum_of(1, p.sx))
        go((job, "xa"), qbuf.at[t, 1, top, at(c)], rx.at[t, top, at(c)], p.x)
        arrived((job, "cy"))
        by_rows(half, half, sum_of(2, p.sy))
        go((job, "yb"), qbuf.at[t, 2, low, at(c)], ry.at[t, low, at(c)], p.y)

    def relay(job):
        t, c = job

        def sum_of(i, slot):
            def body(r):
                held = value[planes[t], slot, r, at(c)].astype(F32) + rc[t, i, r, at(c)].astype(F32)
                qbuf[t, i, r, at(c)] = (held + rd[t, r, at(c)].astype(F32)).astype(BF16)

            return body

        arrived((job, "db"))
        by_rows(half, half, sum_of(1, p.sx))
        go((job, "xb"), qbuf.at[t, 1, low, at(c)], rx.at[t, low, at(c)], p.x)
        arrived((job, "da"))
        by_rows(0, half, sum_of(2, p.sy))
        go((job, "ya"), qbuf.at[t, 2, top, at(c)], ry.at[t, top, at(c)], p.y)

    def total(job):
        t, c = job
        arrived((job, "co"), (job, "xa"), (job, "yb"), (job, "xb"), (job, "ya"))

        def body(r):
            held = value[planes[t], p.s, r, at(c)].astype(F32) + rc[t, 3, r, at(c)].astype(F32)
            held = held + rx[t, r, at(c)].astype(F32) + ry[t, r, at(c)].astype(F32)
            if pair > 1 and t == 0:
                zbuf[0, r, at(c)] = held.astype(BF16)
            else:
                result[r, at(c)] = held

        by_rows(0, rows, body)
        if pair > 1 and t == 0:
            go(f"z{c}", zbuf.at[0, :, at(c)], zbuf.at[1, :, at(c)], p.z)

    begin(jobs[0])
    rest(jobs[0])
    if len(jobs) > 1:
        begin(jobs[1])
    for i, job in enumerate(jobs):
        if i + 1 < len(jobs):
            rest(jobs[i + 1])
        hook()
        if i + 2 < len(jobs):
            begin(jobs[i + 2])
        relay(job)
        hook()
        if i > 0:
            total(jobs[i - 1])
    total(jobs[-1])
    if pair > 1:
        for c in range(count):
            here = span(theirs[c])
            arrived(f"z{c}")

            def body(r):
                result[r, here] += zbuf[1, r, here].astype(F32)

            by_rows(0, rows, body)
    return live


def rms_back(value, gain, grad):
    inverse = lax.rsqrt(jnp.mean(value * value, axis=-1, keepdims=True) + EPSILON)
    normal = value * inverse
    u = grad * gain
    return inverse * (u - normal * jnp.mean(u * normal, axis=-1, keepdims=True)), grad * normal


def up_kernel(
    pair, h, wg, wu, down_w, hs, gate, up, inner, inner_t, wd, wu_all, hs_v, w_v, g_v, u_v, i_v, t_v, send, recv, zsem, rsem, sems
):
    place = Place(pair)
    place.peers.append((place.s, flip(place.f, 1)))
    moves = Moves(sems)
    deep = wu.shape[1]
    loads = [moves.start(wg, w_v.at[0])]
    far_f, near_f = opposite(place.f), flip(place.f, 1)

    def up_rows(plane):
        return w_v.at[1, pl.ds(pl.multiple_of(plane * deep, deep), deep)]

    loads += [moves.start(wu.at[plane], up_rows(plane)) for plane in (place.f, near_f, far_f)]
    rows, width = h.shape
    block, share = 2 * rows, wg.shape[1]
    up_pass = pltpu.make_async_remote_copy(
        wu.at[far_f], up_rows(far_f), rsem.at[0], rsem.at[1], device_id=(place.s, near_f), device_id_type=MESH
    )
    hs_v[place.q, place.s] = h[...]
    place.barrier()
    stream, view = Stream(place, zsem), half_rows(down_w, share)
    down_copies = [stream.near_copy(0, view, wd), stream.own_copy(0, view, wd), stream.far_copy(0, view, wd)]

    def pass_up():
        moves.wait(loads)
        up_pass.start()
        down_copies[0].start()
        down_copies[1].start()

    def pass_down():
        down_copies[2].start()

    n = hs.shape[1]
    step = min(256, share)

    def ready(q, chip):
        slots, here = where(q, chip)

        @pl.loop(0, share // step)
        def _(j):
            cols = pl.ds(pl.multiple_of(j * step, step), step)
            g_v[here, cols] = dot(hs_v[q, slots].reshape(block, width), w_v[0, :, cols], NN)

        if whole:
            second(q, slots, here)

    def done(q, chip):
        slots, here = where(q, chip)
        moves.start(hs_v.at[q, slots], hs.at[q, slots])
        moves.start(g_v.at[here], gate.at[here])
        if whole:
            put(here)
        else:
            held.append((q, chip))

    whole, held = [], []

    def where(q, chip):
        return pl.ds(2 * chip, 2), pl.ds(pl.multiple_of(q * n * rows + chip * block, block), block)

    def second(q, slots, here):
        @pl.loop(0, share // step)
        def _(j):
            cols = pl.ds(pl.multiple_of(j * step, step), step)
            u = dot(hs_v[q, slots].reshape(block, width), w_v[1, :, cols], NN)
            g = g_v[here, cols]
            u_v[here, cols] = u
            value = g * (1.0 / (1.0 + jnp.exp(-g))) * u
            i_v[here, cols] = value.astype(BF16)
            t_v[cols, here] = value.T.astype(BF16)

    def put(here):
        moves.start(u_v.at[here], up.at[here])
        moves.start(i_v.at[here], inner.at[here])

    def complete():
        up_pass.wait_recv()
        whole.append(True)

        @pl.loop(0, n // 2)
        def _(chip):
            second(place.q, *where(place.q, chip))

        for q, chip in held[n // 2 :]:
            second(q, *where(q, chip))
        for q, chip in held:
            put(where(q, chip)[1])

    live = gather_pairs(place, Wires(send, recv), h, hs_v, ready, Work([pass_up, lambda: None, pass_down, complete]), done)
    moves.start(w_v.at[1], wu_all)
    moves.start(t_v, inner_t)
    for copy in down_copies:
        copy.wait()
    up_pass.wait_send()
    for copy in live.values():
        copy.wait_send()
    moves.finish()


def any_specs(count):
    return [pl.BlockSpec(memory_space=pl.ANY)] * count


def vmem_specs(count):
    return [pl.BlockSpec(memory_space=pltpu.VMEM)] * count


def kernel_params(ident, mib=60):
    return pltpu.CompilerParams(collective_id=ident, has_side_effects=True, vmem_limit_bytes=mib * 2**20)


def shape(dims, kind):
    return jax.ShapeDtypeStruct(dims, kind)


def ffn_up(h, wg, wu, down_w, n, pair, ident):
    rows, width = h.shape
    share, long = wg.shape[1], pair * n * rows
    dma = pltpu.SemaphoreType.DMA
    outs = [
        shape((pair, n, rows, width), BF16),
        shape((long, share), F32),
        shape((long, share), F32),
        shape((long, share), BF16),
        shape((share, long), BF16),
        shape((width // down_w.shape[1], share, down_w.shape[1]), BF16),
        shape((width, share), BF16),
    ]
    return pl.pallas_call(
        functools.partial(up_kernel, pair),
        in_specs=vmem_specs(1) + any_specs(3),
        out_specs=any_specs(7),
        out_shape=outs,
        scratch_shapes=[
            pltpu.VMEM((pair, n, rows, width), BF16),
            pltpu.VMEM((2, width, share), BF16),
            pltpu.VMEM((long, share), F32),
            pltpu.VMEM((long, share), F32),
            pltpu.VMEM((long, share), BF16),
            pltpu.VMEM((share, long), BF16),
            dma((gather_wires(pair),)),
            dma((gather_wires(pair),)),
            dma((1, 4, 2)),
            dma((2,)),
            dma((8 + 4 * pair * n // 2,)),
        ],
        compiler_params=kernel_params(ident),
        cost_estimate=pl.CostEstimate(
            flops=4 * long * width * share, bytes_accessed=long * width * 40, transcendentals=0
        ),
        name=f"up_{ident}",
    )(h, wg, wu, down_w)


def down_kernel(
    pair, inner, wd, hidden, gains, cotangent, layer_out, grad_low, gain_term, wd_all,
    i_v, w_v, sum_v, value, rc, rd, rx, ry, qbuf, zbuf, send, recv, wsem, sems
):
    place = Place(pair)
    place.peers.append((place.s, flip(place.f, 1)))
    moves = Moves(sems)
    gain = gains[3:4, :]
    f, far_f, near_f = place.f, opposite(place.f), flip(place.f, 1)
    deep = wd.shape[2]

    def columns(plane):
        return w_v.at[:, pl.ds(pl.multiple_of(plane * deep, deep), deep)]

    for plane in (f, near_f, far_f):
        moves.start(wd.at[plane], columns(plane))
    moves.start(inner, i_v)
    rows, width = hidden.shape
    block = 2 * rows
    n = value.shape[1]
    step = min(512, width)
    place.barrier()
    relay = pltpu.make_async_remote_copy(
        wd.at[far_f], columns(far_f), wsem.at[0], wsem.at[1], device_id=(place.s, near_f), device_id_type=MESH
    )
    relay.start()
    moves.finish()

    def make(q, chip, c, at):
        here = pl.ds(pl.multiple_of(q * n * rows + chip * 2 * block, 2 * block), 2 * block)
        cols = pl.ds(pl.multiple_of(at, deep), deep)
        part = dot(i_v[here, :], w_v[:, cols], NN).astype(BF16)
        value[q, pl.ds(4 * chip, 4), :, cols] = part.reshape(4, rows, deep)

    mine = [f, near_f, far_f, opposite(near_f)]
    theirs = [far_f, opposite(near_f), f, near_f]
    jobs = [(0, 0), (0, 1), (0, 2), (1, 0), (1, 1), (0, 3), (1, 2), (1, 3)]
    live = scatter_pairs(
        place, Wires(send, recv), value, rc, rd, rx, ry, qbuf, zbuf, make, sum_v,
        Work([lambda: None] * 6 + [relay.wait_recv]), jobs, mine, theirs,
    )
    moves.start(w_v, wd_all)
    gain_term[...] = jnp.zeros_like(gain_term)

    def last(r):
        feed, grad = sum_v[r], cotangent[r].astype(F32)
        back, term = rms_back(feed, gain, grad)
        inverse = lax.rsqrt(jnp.mean(feed * feed, axis=-1, keepdims=True) + EPSILON)
        layer_out[r] = (hidden[r] + feed * inverse * gain).astype(BF16)
        grad_low[r] = back.astype(BF16)
        gain_term[...] += jnp.sum(term, axis=0, keepdims=True)

    by_rows(0, rows, last)
    for copy in list(live.values()) + [relay]:
        copy.wait_send()
    moves.finish()


def ffn_down(inner, wd, hidden, gains, cotangent, n, pair, ident):
    rows, width = hidden.shape
    dma = pltpu.SemaphoreType.DMA
    return pl.pallas_call(
        functools.partial(down_kernel, pair),
        in_specs=any_specs(2) + vmem_specs(3),
        out_specs=vmem_specs(3) + any_specs(1),
        out_shape=[
            shape((rows, width), BF16),
            shape((rows, width), BF16),
            shape((1, width), F32),
            shape((wd.shape[1], width), BF16),
        ],
        scratch_shapes=[
            pltpu.VMEM(inner.shape, BF16),
            pltpu.VMEM((wd.shape[1], width), BF16),
            pltpu.VMEM((rows, width), F32),
            pltpu.VMEM((pair, n, rows, width), BF16),
        ]
        + scatter_scratch(pair, rows, width)
        + [dma((2,)), dma((2 + wd.shape[0],))],
        compiler_params=kernel_params(ident),
        cost_estimate=pl.CostEstimate(
            flops=2 * inner.shape[0] * inner.shape[1] * width, bytes_accessed=pair * n * rows * width * 40, transcendentals=0
        ),
        name=f"down_{ident}",
    )(inner, wd, hidden, gains, cotangent)


def grad_kernel(
    pair, g, wd, gate, up, inner_t, grad_gate, grad_up, gate_t, up_t, down_term,
    gs_v, w_v, g_v, u_v, gg_v, gu_v, gt_v, ut_v, it_v, acc, low_v, send, recv, sems
):
    place = Place(pair)
    moves = Moves(sems)
    deep = down_term.shape[2]
    loads = [moves.start(wd, w_v)]
    loads += [moves.start(gate, g_v), moves.start(up, u_v), moves.start(inner_t, it_v)]
    rows, width = g.shape
    block, share = 2 * rows, wd.shape[0]
    gs_v[place.q, place.s] = g[...]
    place.barrier()
    n = gs_v.shape[1]
    step = min(256, share)

    def ready(q, chip):
        slots = pl.ds(2 * chip, 2)
        here = pl.ds(pl.multiple_of(q * n * rows + chip * block, block), block)

        @pl.loop(0, share // step)
        def _(j):
            cols = pl.ds(pl.multiple_of(j * step, step), step)
            a = gs_v[q, slots].reshape(block, width)
            e = dot(a, w_v[cols, :], NT)
            v, u = g_v[here, cols], u_v[here, cols]
            s = 1.0 / (1.0 + jnp.exp(-v))
            dg = e * u * s * (1.0 + v * (1.0 - s))
            du = e * v * s
            gg_v[here, cols] = dg.astype(BF16)
            gu_v[here, cols] = du.astype(BF16)
            gt_v[cols, here] = dg.T.astype(BF16)
            ut_v[cols, here] = du.T.astype(BF16)

    def done(q, chip):
        here = pl.ds(pl.multiple_of(q * n * rows + chip * block, block), block)
        moves.start(gg_v.at[here], grad_gate.at[here])
        moves.start(gu_v.at[here], grad_up.at[here])

    def add_term(t):
        q = place.q if t == 0 else 1 - place.q
        tokens = pl.ds(pl.multiple_of(q * n * rows, n * rows), n * rows)

        @pl.loop(0, width // step)
        def _(j):
            cols = pl.ds(pl.multiple_of(j * step, step), step)
            part = dot(it_v[:, tokens], gs_v[q, :, :, cols].reshape(n * rows, step), NN)
            if t == 0:
                acc[:, cols] = part
            else:
                acc[:, cols] += part

    nothing = lambda: None
    live = gather_pairs(
        place, Wires(send, recv), g, gs_v, ready, Work([lambda: moves.wait(loads), nothing, nothing, lambda: add_term(0)]), done
    )
    add_term(1)
    for j in range(down_term.shape[0]):
        low_v[j] = acc[:, pl.ds(j * deep, deep)].astype(BF16)
    moves.start(low_v, down_term)
    moves.start(gt_v, gate_t)
    moves.start(ut_v, up_t)
    for copy in live.values():
        copy.wait_send()
    moves.finish()


def ffn_grad(g, wd, gate, up, inner_t, n, m, pair, ident):
    rows, width = g.shape
    share, long = wd.shape[0], pair * n * rows
    dma = pltpu.SemaphoreType.DMA
    flat, tall = pltpu.VMEM((long, share), BF16), pltpu.VMEM((share, long), BF16)
    return pl.pallas_call(
        functools.partial(grad_kernel, pair),
        in_specs=vmem_specs(1) + any_specs(4),
        out_specs=any_specs(5),
        out_shape=[shape((long, share), BF16)] * 2
        + [shape((share, long), BF16)] * 2
        + [shape((m, share, width // m), BF16)],
        scratch_shapes=[
            pltpu.VMEM((pair, n, rows, width), BF16),
            pltpu.VMEM((share, width), BF16),
            pltpu.VMEM((long, share), F32),
            pltpu.VMEM((long, share), F32),
            flat,
            flat,
            tall,
            tall,
            tall,
            pltpu.VMEM((share, width), F32),
            pltpu.VMEM((m, share, width // m), BF16),
            dma((gather_wires(pair),)),
            dma((gather_wires(pair),)),
            dma((12 + 3 * pair * n // 2,)),
        ],
        compiler_params=kernel_params(ident, 63),
        cost_estimate=pl.CostEstimate(
            flops=2 * long * width * share, bytes_accessed=long * width * 40, transcendentals=0
        ),
        name=f"grad_{ident}",
    )(g, wd, gate, up, inner_t)


def back_kernel(
    pair, gg, gu, wg, wu, gate_t, hs, down_term, branch, gains, cotangent,
    grad_hidden, grad_low, gain_term, down_grad, gate_term,
    a_v, w_v, value, rc, rd, rx, ry, qbuf, zbuf, send, recv,
    gt_v, hs_v, gterm, down_own, down_near, down_total, down_from, dsem, sems
):
    place = Place(pair)
    place.peers.append((place.s, flip(place.f, 1)))
    moves = Moves(sems)
    loads = [moves.start(wg, w_v.at[0]), moves.start(wu, w_v.at[1])]
    loads += [moves.start(gg, a_v.at[0]), moves.start(gu, a_v.at[1])]
    late = []
    down = Settle(place, dsem, down_term, down_own, down_near, down_total, down_from)
    pieces = term_work(gterm, gt_v, hs_v, lambda: moves.wait(late), gate_term, moves)
    idle = [lambda: None]
    work = Work(idle + pieces[:1] + idle + [down.middle] + pieces[1:2] + idle + pieces[2:3] + idle + pieces[3:])
    rows, width = branch.shape
    block = 2 * rows
    n = value.shape[1]
    step = min(256, width)
    place.barrier()
    down.start(True)
    moves.wait(loads)
    late.append(moves.start(gate_t, gt_v))
    for q in range(pair):
        late.append(moves.start(hs.at[q], hs_v.at[q]))

    def make(q, chip, c, at):
        here = pl.ds(pl.multiple_of(q * n * rows + chip * 2 * block, 2 * block), 2 * block)

        @pl.loop(0, width // 4 // step)
        def _(j):
            cols = pl.ds(pl.multiple_of(at + j * step, step), step)
            part = dot(a_v[0, here, :], w_v[0, cols, :], NT) + dot(a_v[1, here, :], w_v[1, cols, :], NT)
            value[q, pl.ds(4 * chip, 4), :, cols] = part.astype(BF16).reshape(4, rows, step)

    live = scatter_pairs(place, Wires(send, recv), value, rc, rd, rx, ry, qbuf, zbuf, make, grad_hidden, work)
    work.rest()
    gain_term[...] = jnp.zeros_like(gain_term)

    def last(r):
        grad = cotangent[r].astype(F32) + grad_hidden[r]
        grad_hidden[r] = grad
        back, term = rms_back(branch[r], gains[2:3, :], grad)
        grad_low[r] = back.astype(BF16)
        gain_term[...] += jnp.sum(term, axis=0, keepdims=True)

    by_rows(0, rows, last)
    share = down_grad.shape[0] // 2

    def store(u, i, value):
        size = value.shape[0]
        down_grad[pl.ds(pl.multiple_of(u * share + i * size, size), size), :] = value

    down.finish(store)
    for copy in live.values():
        copy.wait_send()
    moves.finish()


def ffn_back(gg, gu, wg, wu, gate_t, hs, down_term, branch, gains, cotangent, n, m, pair, ident):
    rows, width = branch.shape
    share, deep = gate_t.shape[0], width // m
    term = down_term.shape
    dma = pltpu.SemaphoreType.DMA
    return pl.pallas_call(
        functools.partial(back_kernel, pair),
        in_specs=any_specs(7) + vmem_specs(3),
        out_specs=vmem_specs(4) + any_specs(1),
        out_shape=[
            shape((rows, width), F32),
            shape((rows, width), BF16),
            shape((1, width), F32),
            shape((2 * share, deep), F32),
            shape(term, BF16),
        ],
        scratch_shapes=[
            pltpu.VMEM((2,) + gg.shape, BF16),
            pltpu.VMEM((2,) + wg.shape, BF16),
            pltpu.VMEM((pair, n, rows, width), BF16),
        ]
        + scatter_scratch(pair, rows, width)
        + [pltpu.VMEM(v.shape, BF16) for v in (gate_t, hs)]
        + [pltpu.VMEM(term, BF16)]
        + settle_scratch(share, deep)
        + [dma((20,))],
        compiler_params=kernel_params(ident, 63),
        cost_estimate=pl.CostEstimate(
            flops=4 * gg.shape[0] * gg.shape[1] * width, bytes_accessed=pair * n * rows * width * 40, transcendentals=0
        ),
        name=f"back_{ident}",
    )(gg, gu, wg, wu, gate_t, hs, down_term, branch, gains, cotangent)


def opposite(f):
    return (f + 2) % 4


class Stream:
    def __init__(self, place, sems):
        self.place, self.sems = place, sems
        f = place.f
        self.half, self.far_f, self.near_f = f // 2, opposite(f), flip(f, 1)
        self.far, self.near = (place.s, self.far_f), (place.s, self.near_f)

    def remote(self, k, step, src, dst, device):
        return pltpu.make_async_remote_copy(
            src, dst, self.sems.at[k, step, 0], self.sems.at[k, step, 1], device_id=device, device_id_type=MESH
        )

    def far_copy(self, k, view, full):
        return self.remote(k, 0, view(1 - self.half), full.at[self.place.f], self.far)

    def near_copy(self, k, view, full):
        return self.remote(k, 1, view(self.half), full.at[self.place.f], self.near)

    def own_copy(self, k, view, full):
        return pltpu.make_async_copy(view(self.half), full.at[self.place.f], self.sems.at[k, 3, 0])

    def relay_copy(self, k, full):
        return self.remote(k, 2, full.at[self.far_f], full.at[self.far_f], self.near)

    def start_far(self, k, view, full):
        self.far_copy(k, view, full).start()

    def start_near(self, k, view, full):
        self.near_copy(k, view, full).start()
        self.own_copy(k, view, full).start()

    def relay(self, k, view, full):
        self.far_copy(k, view, full).wait_recv()
        self.relay_copy(k, full).start()

    def finish(self, k, view, full):
        self.near_copy(k, view, full).wait_recv()
        self.relay_copy(k, full).wait_recv()
        self.own_copy(k, view, full).wait()
        self.far_copy(k, view, full).wait_send()
        self.near_copy(k, view, full).wait_send()
        self.relay_copy(k, full).wait_send()


def half_columns(ref, share):
    return lambda u: ref.at[:, pl.ds(pl.multiple_of(u * share, share), share)]


def half_rows(ref, share):
    return lambda u: ref.at[pl.ds(pl.multiple_of(u * share, share), share), :]


def full_barrier(place, n, near):
    sem = pltpu.get_barrier_semaphore()
    s, f = place.s, place.f
    for d in range(1, n):
        pl.semaphore_signal(sem, inc=1, device_id=((s + d) % n, f), device_id_type=MESH)
    for other in near:
        pl.semaphore_signal(sem, inc=1, device_id=(s, other), device_id_type=MESH)
    pl.semaphore_wait(sem, n - 1 + len(near))


def swap_halves(v):
    return pltpu.roll(v, HD // 2, axis=1)


def to_rows(first, second):
    rows = first.shape[0]
    lane = lax.broadcasted_iota(jnp.int32, (rows, 128), 1)
    wide = jnp.where(lane == 0, first, jnp.where(lane == 1, second, 0.0))
    return wide.T[:8]


def to_columns(v):
    return jnp.concatenate([v, jnp.zeros((120, v.shape[1]), F32)], axis=0).T


def exchange(place, n, own, held, send, recv):
    copies = []
    for d in range(1, n):
        copy = pltpu.make_async_remote_copy(
            own,
            held.at[d - 1],
            send.at[d - 1],
            recv.at[d - 1],
            device_id=((place.s + d) % n, place.f),
            device_id_type=MESH,
        )
        copy.start()
        copies.append(copy)
    total = own[...]
    for d in range(1, n):
        copies[d - 1].wait_recv()
        total = total + held[d - 1]
    return total, copies


def attend(block, q_v, k_v, v_v, out_v, low_v, lt_v, log_v):
    length = q_v.shape[0]
    scale = HD ** (-0.5)

    @pl.loop(0, q_v.shape[1] // HD)
    def _(h):
        cols = pl.ds(pl.multiple_of(h * HD, HD), HD)
        for half in range(2):
            wide = pl.ds(0, (half + 1) * length // 2)

            @pl.loop(half * length // 2 // block, (half + 1) * length // 2 // block)
            def _(i):
                rows = pl.ds(pl.multiple_of(i * block, block), block)
                s = dot(q_v[rows, cols], k_v[wide, cols], NT) * scale
                column = lax.broadcasted_iota(jnp.int32, s.shape, 1)
                row = lax.broadcasted_iota(jnp.int32, s.shape, 0) + i * block
                s = jnp.where(column <= row, s, -jnp.inf)
                top = jnp.max(s, axis=-1, keepdims=True)
                p = jnp.exp(s - top)
                total = jnp.sum(p, axis=-1, keepdims=True)
                out = dot((p * (1.0 / total)).astype(BF16), v_v[wide, cols], NN)
                out_v[rows, cols] = out
                low_v[rows, cols] = out.astype(BF16)
                lt_v[cols, rows] = out.T.astype(BF16)
                log_v[h, rows, :] = top + jnp.log(total)


def opening_kernel(
    n, m, x, wq, wk, wv, own_gains, wo_own, gate_w, up_w, down_w,
    qkv, all_gains, tables, raw, heads, attended, low_t, xs_t, log_total, inverse, branch, hidden, hidden_low, wg, wu, wo,
    full, xs_v, xt_v, lt_v, w_v, wo_v, raw_v, heads_v, out_v, low_v, log_v, small, held, value,
    rc, rd, rx, ry, qbuf, zbuf, send, recv, ssend, srecv, zsem, osem,
    tsend, trecv, asend, arecv, zsend, zrecv, gsend, grecv, sems,
):
    place = Place(1)
    s, f = place.s, place.f
    rows, width = x.shape
    part = wq.shape[0]
    length, cols = raw.shape[1], raw.shape[2]
    share = wg.shape[2]
    block = min(256, length)
    per = block // rows
    weights = (wq, wk, wv)
    moves = Moves(sems)
    kept = []
    for j, w in enumerate(weights):
        own = w.at[:, pl.ds(pl.multiple_of(s * cols, cols), cols)]
        kept.append(moves.start(own, w_v.at[j, s, f]))
    own_out = [moves.start(wo_own, wo_v.at[f])]
    full[f, s] = own_gains[...]
    xs_v[0, s] = x[...]
    line_barrier(n, m)
    sent = []

    def remote(src, dst, a, b, device):
        copy = pltpu.make_async_remote_copy(src, dst, a, b, device_id=device, device_id_type=MESH)
        copy.start()
        sent.append(copy)
        return copy

    second = []
    for j, w in enumerate(weights):
        row = []
        for d in range(1, n):
            t = (s + d) % n
            src = w.at[:, pl.ds(pl.multiple_of(t * cols, cols), cols)]
            row.append(remote(src, w_v.at[j, s, f], asend.at[j, d], arecv.at[j, d], (t, f)))
        second.append(row)
    first = []
    for d in range(1, n):
        first.append(remote(own_gains, full.at[f, s], gsend.at[d], grecv.at[d], ((s + d) % n, f)))

    def piece(j, o):
        return full.at[o] if j == 3 else w_v.at[j, :, o]

    def hop(way, h, j):
        o = f - h if way == 0 else f + h
        there = f + 1 if way == 0 else f - 1
        place_ = piece(j, o)
        return pltpu.make_async_remote_copy(
            place_, place_, zsend.at[way, h, j], zrecv.at[way, h, j], device_id=(s, there), device_id_type=MESH
        )

    def sends(way, h):
        return ((f - h >= 0) & (f < m - 1)) if way == 0 else ((f + h <= m - 1) & (f > 0))

    def receives(way, h):
        return (f - h - 1 >= 0) if way == 0 else (f + h + 1 <= m - 1)

    def start(h, j):
        for way in (0, 1):
            when(sends(way, h), lambda: hop(way, h, j).start())

    def landed(h, j):
        for way in (0, 1):
            o = f - h - 1 if way == 0 else f + h + 1

            def wait():
                there = f - 1 if way == 0 else f + 1
                place_ = piece(j, o)
                pltpu.make_async_remote_copy(
                    place_, place_, zsend.at[way, h, j], zrecv.at[way, h, j], device_id=(s, there), device_id_type=MESH
                ).wait_recv()

            when(receives(way, h), wait)

    def step(h, j):
        landed(h, j)
        if h + 1 < m - 1:
            start(h + 1, j)

    moves.wait(kept)
    for j in range(3):
        for copy in second[j]:
            copy.wait_recv()
        start(0, j)
    for copy in first:
        copy.wait_recv()
    start(0, 3)
    gathered = gather_pairs(
        place, Wires(tsend, trecv), x, xs_v, lambda *_: None, Work([lambda: None, lambda: step(0, 0), lambda: step(0, 1)])
    )
    step(0, 2)
    step(0, 3)
    half = HD // 2
    lane = lax.broadcasted_iota(jnp.int32, (block, HD), 1)
    row = lax.broadcasted_iota(jnp.int32, (block, HD), 0)
    frequency = jnp.exp((lane % half).astype(F32) * (-2.0 * math.log(THETA) / HD))

    @pl.loop(0, length // block)
    def _(i):
        angle = (row + i * block).astype(F32) * frequency
        here = pl.ds(pl.multiple_of(i * block, block), block)
        tables[0, here, :] = jnp.cos(angle)
        sine = jnp.sin(angle)
        tables[1, here, :] = jnp.where(lane < half, -sine, sine)

    for h in range(1, m - 2):
        for j in range(4):
            step(h, j)

    out_copies = []
    for d, plane in enumerate((flip(f, 1), opposite(f), opposite(flip(f, 1)))):
        out_copies.append(
            pltpu.make_async_remote_copy(
                wo_own, wo_v.at[f], osem.at[0, d], osem.at[1, d], device_id=(s, plane), device_id_type=MESH
            )
        )
        out_copies[-1].start()
    stream = Stream(place, zsem)
    views = [half_columns(gate_w, share), half_columns(up_w, share)]
    fulls = [wg, wu]
    for k in range(2):
        stream.start_far(k, views[k], fulls[k])
    for k in range(2):
        stream.start_near(k, views[k], fulls[k])

    @pl.loop(0, length // block)
    def _(i):
        here = pl.ds(pl.multiple_of(i * block, block), block)
        xt_v[:, here] = xs_v[0, pl.ds(i * per, per)].reshape(block, width).T

    def project(j):
        @pl.loop(0, length // block)
        def _(i):
            here = pl.ds(pl.multiple_of(i * block, block), block)
            a = xs_v[0, pl.ds(i * per, per)].reshape(block, width)
            product = dot(a, w_v[j].reshape(width, cols), NN)
            if j == 2:
                heads_v[2, here, :] = product.astype(BF16)
            else:
                raw_v[j, here, :] = product

    moves.start(xt_v, xs_t)
    for j in range(3):
        landed(m - 2, j)
        project(j)
    landed(m - 2, 3)
    for t in range(n):
        for plane in range(m):
            at = (t * m + plane) * part
            all_gains[:, at : at + part] = full[plane, t, :, :part]
    moves.start(w_v, qkv)

    @pl.loop(0, length // block)
    def _(i):
        here = pl.ds(pl.multiple_of(i * block, block), block)
        q, k = raw_v[0, here, :], raw_v[1, here, :]
        small[0, :, here] = to_rows(
            jnp.sum(q * q, axis=1, keepdims=True), jnp.sum(k * k, axis=1, keepdims=True)
        )

    moves.start(raw_v, raw)
    first_col = pl.multiple_of(s * cols, cols)
    total, stat_copies = exchange(place, n, small.at[0], held, ssend, srecv)
    small[1] = lax.rsqrt(total * (1.0 / width) + EPSILON)
    moves.start(small.at[1], inverse)

    @pl.loop(0, length // block)
    def _(i):
        here = pl.ds(pl.multiple_of(i * block, block), block)
        inv = to_columns(small[1, :, here])
        cosine, sine = tables[0, here, :], tables[1, here, :]
        for j in range(2):
            for h in range(cols // HD):
                part = pl.ds(h * HD, HD)
                v = raw_v[j, here, part] * inv[:, j : j + 1] * all_gains[j : j + 1, pl.ds(first_col + h * HD, HD)]
                heads_v[j, here, part] = (v * cosine + swap_halves(v) * sine).astype(BF16)

    moves.start(heads_v, heads)
    attend(block, heads_v.at[0], heads_v.at[1], heads_v.at[2], out_v, low_v, lt_v, log_v)
    moves.start(out_v, attended)
    moves.start(lt_v, low_t)
    moves.start(log_v, log_total)
    moves.wait(own_out)
    for copy in out_copies:
        copy.wait_recv()
    moves.start(wo_v, wo)
    step = min(512, width)

    def make(q, chip, c, first):
        here = pl.ds(pl.multiple_of(chip * 4 * rows, 4 * rows), 4 * rows)

        @pl.loop(0, width // 2 // step)
        def _(j):
            at = pl.ds(pl.multiple_of(first + j * step, step), step)
            part = dot(low_v[here, :], wo_v[:, :, at].reshape(cols, step), NN).astype(BF16)
            value[q, pl.ds(4 * chip, 4), :, at] = part.reshape(4, rows, step)

    live = scatter_pairs(
        place, Wires(send, recv), value, rc, rd, rx, ry, qbuf, zbuf, make, branch,
        Work([lambda: None, lambda: stream.relay(0, views[0], fulls[0])]),
    )

    def last(r):
        total = branch[r]
        inv = lax.rsqrt(jnp.mean(total * total, axis=-1, keepdims=True) + EPSILON)
        h = x[r].astype(F32) + total * inv * all_gains[2:3, :]
        hidden[r] = h
        hidden_low[r] = h.astype(BF16)

    by_rows(0, rows, last)
    for copy in list(live.values()) + list(gathered.values()) + stat_copies + sent:
        copy.wait_send()
    for h in range(m - 1):
        for j in range(4):
            for way in (0, 1):
                when(sends(way, h), lambda: hop(way, h, j).wait_send())
    moves.finish()
    stream.finish(0, views[0], fulls[0])
    for copy in (
        stream.near_copy(1, views[1], fulls[1]),
        stream.far_copy(1, views[1], fulls[1]),
        stream.own_copy(1, views[1], fulls[1]),
    ):
        copy.wait()
    for copy in out_copies:
        copy.wait_send()


def opening(x, wq, wk, wv, gains, wo, gate_w, up_w, down_w, n, m, ident):
    rows, width = x.shape
    part, cols = wq.shape[0], width // n
    length, share = n * rows, gate_w.shape[1] // 2
    dma = pltpu.SemaphoreType.DMA
    heads = cols // HD
    outs = [
        shape((3, n, m, part, cols), BF16),
        shape((gains.shape[0], width), F32),
        shape((2, length, HD), F32),
        shape((2, length, cols), F32),
        shape((3, length, cols), BF16),
        shape((length, cols), F32),
        shape((cols, length), BF16),
        shape((width, length), BF16),
        shape((heads, length, 1), F32),
        shape((8, length), F32),
        shape((rows, width), F32),
        shape((rows, width), F32),
        shape((rows, width), BF16),
        shape((m, gate_w.shape[0], share), BF16),
        shape((m, gate_w.shape[0], share), BF16),
        shape((m,) + wo.shape, BF16),
    ]
    return pl.pallas_call(
        functools.partial(opening_kernel, n, m),
        in_specs=vmem_specs(5) + any_specs(4),
        out_specs=any_specs(1) + vmem_specs(2) + any_specs(7) + vmem_specs(3) + any_specs(3),
        out_shape=outs,
        scratch_shapes=[
            pltpu.VMEM((m, n) + gains.shape, F32),
            pltpu.VMEM((1, n, rows, width), BF16),
            pltpu.VMEM((width, length), BF16),
            pltpu.VMEM((cols, length), BF16),
            pltpu.VMEM((3, n, m, part, cols), BF16),
            pltpu.VMEM((m,) + wo.shape, BF16),
            pltpu.VMEM((2, length, cols), F32),
            pltpu.VMEM((3, length, cols), BF16),
            pltpu.VMEM((length, cols), F32),
            pltpu.VMEM((length, cols), BF16),
            pltpu.VMEM((heads, length, 1), F32),
            pltpu.VMEM((2, 8, length), F32),
            pltpu.VMEM((n - 1, 8, length), F32),
            pltpu.VMEM((1, n, rows, width), BF16),
        ]
        + scatter_scratch(1, rows, width)
        + [dma((n - 1,)), dma((n - 1,)), dma((2, 4, 2)), dma((2, m))]
        + [dma((gather_wires(1),))] * 2
        + [dma((3, n))] * 2
        + [dma((2, m, 4))] * 2
        + [dma((n,))] * 2
        + [dma((16,))],
        compiler_params=kernel_params(ident),
        cost_estimate=pl.CostEstimate(flops=10**10, bytes_accessed=200 * 2**20, transcendentals=0),
        name=f"opening_{ident}",
    )(x, wq, wk, wv, gains, wo, gate_w, up_w, down_w)


class Settle:
    def __init__(self, place, sems, term, own, near, total, far):
        self.place, self.sems, self.term, self.own = place, sems, term, own
        self.near, self.total, self.far = near, total, far
        f = place.f
        self.f = f
        self.odd, self.half = f % 2, f // 2

    def remote(self, step, src, dst, plane):
        return pltpu.make_async_remote_copy(
            src, dst, self.sems.at[step, 0], self.sems.at[step, 1], device_id=(self.place.s, plane), device_id_type=MESH
        )

    def given(self, i):
        return 1 - self.odd + 2 * i

    def kept(self, i):
        return self.odd + 2 * i

    def near_copy(self, step):
        i = 1 - self.half if step == 0 else self.half
        return self.remote(step, self.term.at[self.given(i)], self.near.at[i], flip(self.f, 1))

    def far_copy(self):
        return self.remote(2, self.total.at[0], self.far, opposite(self.f))

    def load(self, i):
        return pltpu.make_async_copy(self.term.at[self.kept(i)], self.own.at[i], self.sems.at[3, i])

    def start(self, both=False):
        self.near_copy(0).start()
        self.both = both
        if both:
            self.near_copy(1).start()
        for i in (0, 1):
            self.load(i).start()

    def mine(self, i):
        return self.term.at[self.kept(i)] if self.own is None else self.own.at[i]

    def chunks(self, body):
        size = 128

        @pl.loop(0, self.far.shape[0] // size)
        def _(i):
            body(i, pl.ds(pl.multiple_of(i * size, size), size))

    def middle(self):
        if self.own is not None:
            for i in (0, 1):
                self.load(i).wait()
        self.near_copy(0).wait_recv()
        other = 1 - self.half
        mine = self.mine(other)

        def body(i, r):
            self.total[0, r] = add(mine[r], self.near[other, r])

        self.chunks(body)
        self.far_copy().start()
        if not self.both:
            self.near_copy(1).start()

    def finish(self, store):
        half = self.half
        self.near_copy(1).wait_recv()
        mine = self.mine(half)
        self.chunks(lambda i, r: store(half, i, mine[r].astype(F32) + self.near[half, r].astype(F32)))
        self.far_copy().wait_recv()
        self.chunks(lambda i, r: store(1 - half, i, self.far[r].astype(F32)))
        for step in (0, 1):
            self.near_copy(step).wait_send()
        self.far_copy().wait_send()


def settle_scratch(share, depth, own=True):
    block = lambda *lead: pltpu.VMEM(lead + (share, depth), BF16)
    return ([block(2)] if own else []) + [block(2), block(1), block(), pltpu.SemaphoreType.DMA((4, 2))]


def term_block(term, left, right, block):
    deep, long = term.shape[2], left.shape[1]
    step = min(256, deep)

    @pl.loop(0, deep // step)
    def _(j):
        at = pl.ds(pl.multiple_of(block * deep + j * step, step), step)
        to = pl.ds(pl.multiple_of(j * step, step), step)
        term[block, :, to] = dot(left[...], right[:, :, :, at].reshape(long, step), NN).astype(BF16)


class Work:
    def __init__(self, pieces):
        self.pieces = list(pieces)

    def __call__(self):
        if self.pieces:
            self.pieces.pop(0)()

    def rest(self):
        while self.pieces:
            self()


def term_work(term, left, right, prepare, out, moves):
    def piece(block):
        def run():
            if block == 0:
                prepare()
            term_block(term, left, right, block)
            moves.start(term.at[block], out.at[block])

        return run

    return [piece(block) for block in range(term.shape[0])]


def turn(v, cosine, sine):
    return v * cosine + swap_halves(v) * sine


def attend_back(block, q_v, k_v, v_v, out_v, log_v, g_v, dq, dk, dv):
    length = q_v.shape[0]
    scale = HD ** (-0.5)
    dk[...] = jnp.zeros_like(dk)
    dv[...] = jnp.zeros_like(dv)

    @pl.loop(0, q_v.shape[1] // HD)
    def _(h):
        cols = pl.ds(pl.multiple_of(h * HD, HD), HD)
        for half in range(2):
            wide = pl.ds(0, (half + 1) * length // 2)

            @pl.loop(half * length // 2 // block, (half + 1) * length // 2 // block)
            def _(i):
                rows = pl.ds(pl.multiple_of(i * block, block), block)
                q, g = q_v[rows, cols], g_v[rows, cols]
                s = dot(q, k_v[wide, cols], NT) * scale
                column = lax.broadcasted_iota(jnp.int32, s.shape, 1)
                row = lax.broadcasted_iota(jnp.int32, s.shape, 0) + i * block
                s = jnp.where(column <= row, s, -jnp.inf)
                weights = jnp.exp(s - log_v[h, rows, :])
                correction = jnp.sum(g.astype(F32) * out_v[rows, cols], axis=-1, keepdims=True)
                gw = dot(g, v_v[wide, cols], NT)
                gs = (weights * (gw - correction)).astype(BF16)
                dq[rows, cols] = dot(gs, k_v[wide, cols], NN) * scale
                dk[wide, cols] += dot(gs, q, TN) * scale
                dv[wide, cols] += dot(weights.astype(BF16), g, TN)


def attention_back_kernel(
    g, gains, tables, inverse, wo, raw, heads, attended, low_t, log_total, xs_t, gate_term, up_t, hs,
    d3, term, gain_term, gate_grad, up_grad,
    bs, wo_v, raw_v, heads_v, out_v, low_v, log_v, ga_v, dq, dk, dv, d_v, xs_v, term_v, small, held,
    ut_v, hs_v, up_term, gown, gnear, gtotal, gfar, gsem, unear, utotal, ufar, usem,
    send, recv, ssend, srecv, sems,
):
    place = Place(1)
    n, m = bs.shape[1], wo.shape[0]
    rows, width = g.shape
    length, cols = raw.shape[1], raw.shape[2]
    share = gate_term.shape[1]
    first_col = pl.multiple_of(place.s * cols, cols)
    moves = Moves(sems)
    second = [moves.start(wo, wo_v)]
    fourth = [
        moves.start(heads, heads_v),
        moves.start(attended, out_v),
        moves.start(log_total, log_v),
        moves.start(low_t, low_v),
        moves.start(raw, raw_v),
        moves.start(xs_t, xs_v),
    ]
    bs[0, place.s] = g[...]
    full_barrier(place, n, [opposite(place.f), flip(place.f, 1)])
    gate = Settle(place, gsem, gate_term, gown, gnear, gtotal, gfar)
    up = Settle(place, usem, up_term, None, unear, utotal, ufar)
    gate.start()
    late = [moves.start(up_t, ut_v)] + [moves.start(hs.at[q], hs_v.at[q]) for q in range(hs.shape[0])]

    up.both = False

    def up_block(i):
        b = (up.given(1 - up.half), up.given(up.half), up.kept(1 - up.half), up.kept(up.half))[i]
        if i == 0:
            moves.wait(late)
        term_block(up_term, ut_v, hs_v, b)
        if i == 0:
            up.near_copy(0).start()

    block = min(256, length)

    def ready(q, chip):
        here = pl.ds(pl.multiple_of(chip * 2 * rows, 2 * rows), 2 * rows)
        a = bs[0, pl.ds(2 * chip, 2)].reshape(2 * rows, width)
        ga_v[here, :] = dot(a, wo_v[...].reshape(cols, width), NT).astype(BF16)

    moves.wait(second)
    live = gather_pairs(place, Wires(send, recv), g, bs, ready, Work([lambda: up_block(0), lambda: up_block(2), gate.middle]))
    up_block(1)
    up.middle()
    moves.wait(fourth)
    up_block(3)
    attend_back(block, heads_v.at[0], heads_v.at[1], heads_v.at[2], out_v, log_v, ga_v, dq, dk, dv)
    @pl.loop(0, length // block)
    def _(i):
        here = pl.ds(pl.multiple_of(i * block, block), block)
        inv = to_columns(inverse[:, here])
        cosine, sine = tables[0, here, :], -tables[1, here, :]
        sums = []
        for j, d in enumerate((dq, dk)):
            total = jnp.zeros((block, 1), F32)
            for h in range(cols // HD):
                part = pl.ds(h * HD, HD)
                normal = raw_v[j, here, part] * inv[:, j : j + 1]
                v = turn(d[here, part].astype(BF16).astype(F32), cosine, sine)
                raw_v[j, here, part] = normal
                gained = v * gains[j : j + 1, pl.ds(first_col + h * HD, HD)]
                total = total + jnp.sum(gained * normal, axis=1, keepdims=True)
                term_sum = jnp.sum(v * normal, axis=0, keepdims=True)
                d[here, part] = gained

                @pl.when(i == 0)
                def _():
                    gain_term[j, :, part] = term_sum

                @pl.when(i > 0)
                def _():
                    gain_term[j, :, part] += term_sum

            sums.append(total)
        small[0, :, here] = to_rows(sums[0], sums[1])
        d_v[2, here, :] = dv[here, :].astype(BF16)

    total, stat_copies = exchange(place, n, small.at[0], held, ssend, srecv)
    small[1] = total * (1.0 / width)

    @pl.loop(0, length // block)
    def _(i):
        here = pl.ds(pl.multiple_of(i * block, block), block)
        inv = to_columns(inverse[:, here])
        mean = to_columns(small[1, :, here])
        for j, d in enumerate((dq, dk)):
            d_v[j, here, :] = (
                inv[:, j : j + 1] * (d[here, :] - raw_v[j, here, :] * mean[:, j : j + 1])
            ).astype(BF16)

    moves.start(d_v, d3)

    @pl.loop(0, n)
    def _(i):
        at = pl.ds(pl.multiple_of(i * cols, cols), cols)
        part = dot(low_v[...], bs[0, :, :, at].reshape(length, cols), NN)
        term_v[3, i] = part.astype(BF16).reshape(m, cols // m, cols)
        for j in range(3):
            part = dot(xs_v[at, :], d_v[j], NN)
            term_v[j, i] = part.astype(BF16).reshape(m, cols // m, cols)

    moves.start(term_v, term)

    def store(ref):
        def put(u, i, value):
            size = value.shape[0]
            ref[:, pl.ds(pl.multiple_of(u * share + i * size, size), size)] = value.T

        return put

    gate.finish(store(gate_grad))
    up.finish(store(up_grad))
    for copy in list(live.values()) + stat_copies:
        copy.wait_send()
    moves.finish()


def attention_back(g, gains, tables, inverse, wo, raw, heads, attended, low_t, log_total, xs_t, gate_term, up_t, hs, n, ident):
    rows, width = g.shape
    m = wo.shape[0]
    length, cols = raw.shape[1], raw.shape[2]
    share, deep = gate_term.shape[1], width // m
    dma = pltpu.SemaphoreType.DMA
    vmem = pltpu.VMEM
    outs = [
        shape((3, length, cols), BF16),
        shape((4, n, m, cols // m, cols), BF16),
        shape((2, 1, cols), F32),
        shape((deep, 2 * share), F32),
        shape((deep, 2 * share), F32),
    ]
    return pl.pallas_call(
        attention_back_kernel,
        in_specs=vmem_specs(4) + any_specs(10),
        out_specs=any_specs(2) + vmem_specs(3),
        out_shape=outs,
        scratch_shapes=[
            vmem((1, n, rows, width), BF16),
            vmem(wo.shape, BF16),
            vmem(raw.shape, F32),
            vmem(heads.shape, BF16),
            vmem(attended.shape, F32),
            vmem(low_t.shape, BF16),
            vmem(log_total.shape, F32),
            vmem((length, cols), BF16),
            vmem((length, cols), F32),
            vmem((length, cols), F32),
            vmem((length, cols), F32),
            vmem((3, length, cols), BF16),
            vmem(xs_t.shape, BF16),
            vmem((4, n, m, cols // m, cols), BF16),
            vmem((2, 8, length), F32),
            vmem((n - 1, 8, length), F32),
        ]
        + [vmem(up_t.shape, BF16), vmem(hs.shape, BF16), vmem(gate_term.shape, BF16)]
        + settle_scratch(share, deep)
        + settle_scratch(share, deep, False)
        + [
            dma((gather_wires(1),)),
            dma((gather_wires(1),)),
            dma((n - 1,)),
            dma((n - 1,)),
            dma((20,)),
        ],
        compiler_params=kernel_params(ident, 63),
        cost_estimate=pl.CostEstimate(flops=10**10, bytes_accessed=200 * 2**20, transcendentals=0),
        name=f"attention_back_{ident}",
    )(g, gains, tables, inverse, wo, raw, heads, attended, low_t, log_total, xs_t, gate_term, up_t, hs)


def attention_forward_kernel(block, q_ref, k_ref, v_ref, out_ref, low_ref, log_ref):
    length = q_ref.shape[0]
    scale = HD ** (-0.5)
    for i in range(length // block):
        rows = pl.ds(i * block, block)
        width = (i + 1) * block
        s = dot(q_ref[rows, :], k_ref[pl.ds(0, width), :], NT) * scale
        column = lax.broadcasted_iota(jnp.int32, (block, width), 1)
        row = lax.broadcasted_iota(jnp.int32, (block, width), 0) + i * block
        s = jnp.where(column <= row, s, -jnp.inf)
        top = jnp.max(s, axis=-1, keepdims=True)
        p = jnp.exp(s - top)
        total = jnp.sum(p, axis=-1, keepdims=True)
        weights = (p * (1.0 / total)).astype(BF16)
        out = dot(weights, v_ref[pl.ds(0, width), :], NN)
        out_ref[rows, :] = out
        low_ref[rows, :] = out.astype(BF16)
        log_ref[0, rows, :] = top + jnp.log(total)


def attention_forward(q, k, v):
    length, width = q.shape
    heads = width // HD
    block = min(256, length)
    column = pl.BlockSpec((length, HD), lambda h: (0, h))
    return pl.pallas_call(
        functools.partial(attention_forward_kernel, block),
        grid=(heads,),
        in_specs=[column] * 3,
        out_specs=[column, column, pl.BlockSpec((1, length, 1), lambda h: (h, 0, 0))],
        out_shape=[
            jax.ShapeDtypeStruct((length, width), F32),
            jax.ShapeDtypeStruct((length, width), BF16),
            jax.ShapeDtypeStruct((heads, length, 1), F32),
        ],
        cost_estimate=pl.CostEstimate(
            flops=2 * heads * length * length * HD, bytes_accessed=10 * length * width, transcendentals=0
        ),
    )(q, k, v)


def attention_backward_kernel(block, q_ref, k_ref, v_ref, out_ref, log_ref, g_ref, dq_ref, dk_ref, dv_ref, dk, dv):
    length = q_ref.shape[0]
    scale = HD ** (-0.5)
    dk[...] = jnp.zeros_like(dk)
    dv[...] = jnp.zeros_like(dv)
    for i in range(length // block):
        rows = pl.ds(i * block, block)
        width = (i + 1) * block
        wide = pl.ds(0, width)
        q = q_ref[rows, :]
        g = g_ref[rows, :]
        s = dot(q, k_ref[wide, :], NT) * scale
        column = lax.broadcasted_iota(jnp.int32, (block, width), 1)
        row = lax.broadcasted_iota(jnp.int32, (block, width), 0) + i * block
        s = jnp.where(column <= row, s, -jnp.inf)
        weights = jnp.exp(s - log_ref[0, rows, :])
        correction = jnp.sum(g.astype(F32) * out_ref[rows, :], axis=-1, keepdims=True)
        gw = dot(g, v_ref[wide, :], NT)
        gs = (weights * (gw - correction)).astype(BF16)
        dq_ref[rows, :] = (dot(gs, k_ref[wide, :], NN) * scale).astype(BF16)
        dk[wide, :] += dot(gs, q, TN)
        dv[wide, :] += dot(weights.astype(BF16), g, TN)
    dk_ref[...] = (dk[...] * scale).astype(BF16)
    dv_ref[...] = dv[...].astype(BF16)


def attention_backward(q, k, v, out, log_total, g):
    length, width = q.shape
    heads = width // HD
    block = min(256, length)
    column = pl.BlockSpec((length, HD), lambda h: (0, h))
    return pl.pallas_call(
        functools.partial(attention_backward_kernel, block),
        grid=(heads,),
        in_specs=[column] * 4 + [pl.BlockSpec((1, length, 1), lambda h: (h, 0, 0)), column],
        out_specs=[column] * 3,
        out_shape=[jax.ShapeDtypeStruct((length, width), BF16)] * 3,
        scratch_shapes=[pltpu.VMEM((length, HD), F32)] * 2,
        cost_estimate=pl.CostEstimate(
            flops=5 * heads * length * length * HD, bytes_accessed=16 * length * width, transcendentals=0
        ),
    )(q, k, v, out, log_total, g)


def on_device(n, m, pair, *args):
    (
        tokens,
        query_weight,
        key_weight,
        value_weight,
        out_weight,
        query_gain,
        key_gain,
        attention_gain,
        gate_weight,
        up_weight,
        down_weight,
        feedforward_gain,
        cotangent,
    ) = args
    rows, width = tokens.shape[1], tokens.shape[2]
    length = rows * n
    part = query_weight.shape[0]
    cols = width // n
    depth, units = gate_weight.shape
    share = units // pair
    x = tokens.reshape(rows, width)
    groups = [[g * pair + u for u in range(pair)] for g in range(m // pair)]

    native = n == 8 and m == 4

    def gather_plane(v, ident):
        if native:
            return plane_gather(v, n, 1, ident)
        return lax.all_gather(v, "seq", axis=0, tiled=True)

    def scatter_plane(v, ident):
        if native:
            return plane_scatter(v, n, 1, ident)
        return lax.psum_scatter(v.astype(BF16), "seq", scatter_dimension=0, tiled=True).astype(F32)

    def gather_pair(v, ident):
        if native:
            return plane_gather(v, n, pair, ident)
        if pair > 1:
            v = lax.all_gather(v, "fsdp", axis=0, axis_index_groups=groups)
        v = lax.all_gather(v.reshape(pair, rows, width), "seq", axis=1, tiled=True)
        return v.reshape(pair * length, width)

    def scatter_pair(v, ident):
        if native:
            return plane_scatter(v, n, pair, ident)
        v = lax.psum_scatter(v.astype(BF16).reshape(pair, length, width), "seq", scatter_dimension=1, tiled=True)
        if pair > 1:
            v = lax.psum_scatter(v, "fsdp", scatter_dimension=0, axis_index_groups=groups)
        return v.reshape(rows, width).astype(F32)

    def total_plane(v, ident):
        return plane_sum(v, n, ident) if native else lax.psum(v, "seq")

    def spread(halves):
        return lax.all_to_all(jnp.tile(halves, (m // pair, 1, 1)), "fsdp", 0, 0, tiled=False)

    def settle(blocks):
        back = lax.all_to_all(blocks.astype(BF16), "fsdp", 0, 0, tiled=False)
        if native:
            return jnp.sum(back.reshape((pair, m // pair) + back.shape[1:]).astype(F32), axis=1)
        return jnp.sum(back.reshape((m // pair, pair) + back.shape[1:]).astype(F32), axis=0)

    gains = jnp.stack([query_gain, key_gain, attention_gain, feedforward_gain]).astype(F32)
    grad_out = cotangent.reshape(rows, width)
    if native:
        (
            qkv, gains, tables, raw, heads, attended, low_t, xs_t, log_total, inverse, branch, hidden, hidden_low,
            gate_cols, up_cols, out_rows,
        ) = opening(
            x, query_weight, key_weight, value_weight, jnp.pad(gains, ((0, 4), (0, 128 - part))),
            out_weight, gate_weight, up_weight, down_weight, n, m, 1
        )
        gate_cols = gate_cols.reshape(width, share)
        hs, gate, up, inner, inner_t, down_rows, up_cols = ffn_up(hidden_low, gate_cols, up_cols, down_weight, n, pair, 5)
        layer_out, grad_low, feed_gain_term, down_rows = ffn_down(
            inner, down_rows, hidden, gains, grad_out, n, pair, 7
        )
        grad_gate, grad_up, gate_t, up_t, down_term = ffn_grad(
            grad_low, down_rows, gate, up, inner_t, n, m, pair, 6
        )
        grad_hidden, branch_low, branch_gain_term, down_grad, gate_term = ffn_back(
            grad_gate, grad_up, gate_cols, up_cols, gate_t, hs, down_term, branch, gains, grad_out, n, m, pair, 8
        )
        d3, term, gain_own, gate_grad, up_grad = attention_back(
            branch_low, gains, tables, inverse, out_rows, raw, heads, attended, low_t, log_total,
            xs_t, gate_term, up_t, hs, n, 2
        )
        tokens_grad, term, gain_grads = leave(
            d3, term, gain_own, branch_gain_term, feed_gain_term, grad_hidden, qkv, n, m, 4
        )
        layer_out, tokens_grad, *term, gate_grad, up_grad, down_grad = place_outputs(
            [layer_out, tokens_grad, term, gate_grad, up_grad, down_grad]
        )
        out_grad = term[3]
    else:
        cosine, sine = angles_of(length)
        seq = lax.axis_index("seq")
        stacked = jnp.stack([query_weight, key_weight, value_weight]).reshape(3, part, n, cols)
        mine = lax.all_to_all(stacked.transpose(2, 0, 1, 3), "seq", 0, 0)
        qkv = lax.all_gather(mine, "fsdp", axis=1).transpose(2, 0, 1, 3, 4).reshape(3, width, cols)
        full_gain = lax.all_gather(gains, ("seq", "fsdp"), axis=1).reshape(4, width)
        xs = gather_plane(x, 1)
        out_rows = lax.all_gather(out_weight, "fsdp", axis=0, tiled=True)
        own_gain = lax.dynamic_slice_in_dim(full_gain[:2], seq * cols, cols, 1)
        q_gain, k_gain, branch_gain, feed_gain = own_gain[0], own_gain[1], full_gain[2], full_gain[3]
        q_raw, k_raw, v = dot(xs, qkv[0], NN), dot(xs, qkv[1], NN), dot(xs, qkv[2], NN).astype(BF16)
        squares = jnp.stack([jnp.sum(q_raw * q_raw, axis=1), jnp.sum(k_raw * k_raw, axis=1)])
        inverse = lax.rsqrt(lax.psum(squares, "seq") / width + EPSILON)
        q_inv, k_inv = inverse[0][:, None], inverse[1][:, None]
        q = rotate(q_raw * q_inv * q_gain, cosine, sine, 1.0).astype(BF16)
        k = rotate(k_raw * k_inv * k_gain, cosine, sine, 1.0).astype(BF16)
        attended, attended_low, log_total = attention_forward(q, k, v)
        branch = scatter_plane(dot(attended_low, out_rows, NN), 3)
        branch_inv = lax.rsqrt(jnp.mean(branch * branch, axis=1, keepdims=True) + EPSILON)
        hidden = x.astype(F32) + branch * branch_inv * branch_gain
        hidden_low = hidden.astype(BF16)
        gate_cols = spread(gate_weight.reshape(depth, pair, share).transpose(1, 0, 2)).reshape(width, share)
        up_cols = spread(up_weight.reshape(depth, pair, share).transpose(1, 0, 2)).reshape(width, share)
        down_rows = spread(down_weight.reshape(pair, share, depth)).transpose(1, 0, 2).reshape(share, width)
        grad_out = grad_out.astype(F32)
        hs = gather_pair(hidden_low, 5)
        gate = dot(hs, gate_cols, NN)
        up = dot(hs, up_cols, NN)
        sig = jax.nn.sigmoid(gate)
        inner = (gate * sig * up).astype(BF16)
        feed = scatter_pair(dot(inner, down_rows, NN), 7)
        feed_inv = lax.rsqrt(jnp.mean(feed * feed, axis=1, keepdims=True) + EPSILON)
        layer_out = (hidden + feed * feed_inv * feed_gain).astype(BF16)
        grad_feed, term = rms_back(feed, feed_gain, grad_out)
        feed_gain_term = jnp.sum(term, axis=0)
        gs = gather_pair(grad_feed.astype(BF16), 6)
        grad_inner = dot(gs, down_rows, NT)
        grad_gate = (grad_inner * up * sig * (1.0 + gate * (1.0 - sig))).astype(BF16)
        grad_up = (grad_inner * gate * sig).astype(BF16)
        grad_hidden = grad_out + scatter_pair(dot(grad_gate, gate_cols, NT) + dot(grad_up, up_cols, NT), 8)
        grad_branch, term = rms_back(branch, branch_gain, grad_hidden)
        branch_low = grad_branch.astype(BF16)
        branch_gain_term = jnp.sum(term, axis=0)
        inner_t, gate_t, up_t = inner.T, grad_gate.T, grad_up.T

        def cut(v):
            return v.reshape(share, m, depth).transpose(1, 0, 2)

        down_grad = settle(cut(dot(inner_t, gs, NN))).reshape(units, depth)
        gate_grad = settle(cut(dot(gate_t, hs, NN))).transpose(2, 0, 1).reshape(depth, units)
        up_grad = settle(cut(dot(up_t, hs, NN))).transpose(2, 0, 1).reshape(depth, units)
        bs = gather_plane(branch_low, 2)
        out_grad = lax.psum_scatter(
            dot(attended_low, bs, TN).astype(BF16), "fsdp", scatter_dimension=0, tiled=True
        ).astype(F32)
        grad_attended = dot(bs, out_rows, NT).astype(BF16)
        dq, dk, dv = attention_backward(q, k, v, attended, log_total, grad_attended)
        dq = rotate(dq.astype(F32), cosine, sine, -1.0)
        dk = rotate(dk.astype(F32), cosine, sine, -1.0)
        q_normal, k_normal = q_raw * q_inv, k_raw * k_inv
        q_gain_term = jnp.sum(dq * q_normal, axis=0)
        k_gain_term = jnp.sum(dk * k_normal, axis=0)
        dq, dk = dq * q_gain, dk * k_gain
        means = total_plane(jnp.stack([jnp.sum(dq * q_normal, axis=1), jnp.sum(dk * k_normal, axis=1)]), 10) / width
        dq = (q_inv * (dq - q_normal * means[0][:, None])).astype(BF16)
        dk = (k_inv * (dk - k_normal * means[1][:, None])).astype(BF16)
        value = dot(dq, qkv[0], NT) + dot(dk, qkv[1], NT) + dot(dv, qkv[2], NT)
        term = jnp.stack([dot(xs, d, TN).astype(BF16) for d in (dq, dk, dv)]).reshape(3, n, m, part, cols)
        gain_own = jnp.stack([q_gain_term, k_gain_term])
        gain_own = lax.dynamic_update_slice(jnp.zeros((2, width), F32), gain_own, (0, seq * cols))
        gain_terms = jnp.concatenate([gain_own, jnp.stack([branch_gain_term, feed_gain_term])]).reshape(4, n, m, part)
        tokens_grad = grad_hidden + scatter_plane(value, 4)
        term = lax.psum_scatter(term, "fsdp", scatter_dimension=2)
        term = lax.all_to_all(term, "seq", 1, 1).astype(F32).transpose(0, 2, 1, 3)
        gain_grads = lax.psum_scatter(
            gain_terms.reshape(4, width), ("seq", "fsdp"), scatter_dimension=1, tiled=True
        )
        term = term.reshape(3, part, width)

    return (
        layer_out.reshape(tokens.shape),
        tokens_grad.reshape(tokens.shape),
        term[0],
        term[1],
        term[2],
        out_grad,
        gain_grads[0],
        gain_grads[1],
        gain_grads[2],
        gate_grad,
        up_grad,
        down_grad,
        gain_grads[3],
    )


def solution(mesh):
    n, m = mesh.shape["seq"], mesh.shape["fsdp"]
    tall, flat, act = P(("seq", "fsdp"), None), P(("seq", "fsdp")), P("fsdp", "seq", None)
    wide, deep = P("fsdp", "seq"), P("seq", "fsdp")
    return jax.shard_map(
        functools.partial(on_device, n, m, 2),
        mesh=mesh,
        in_specs=(act, tall, tall, tall, tall, flat, flat, flat, wide, wide, deep, flat, act),
        out_specs=(act, act, tall, tall, tall, tall, flat, flat, flat, wide, wide, deep, flat),
        check_vma=False,
    )
```

```python
import functools
import math

import jax
import jax.numpy as jnp
from jax import lax
from jax.experimental import pallas as pl
from jax.experimental.pallas import tpu as pltpu
from jax.sharding import PartitionSpec as P

EPSILON = 1e-06
THETA = 500000.0
HD = 128
F32 = jnp.float32
BF16 = jnp.bfloat16


def dot(a, b, dims):
    return lax.dot_general(a, b, (dims, ((), ())), preferred_element_type=F32)


NN = ((1,), (0,))
NT = ((1,), (1,))
TN = ((0,), (0,))


def angles_of(length):
    half = HD // 2
    frequency = jnp.exp(jnp.arange(half, dtype=F32) * (-2.0 * math.log(THETA) / HD))
    angle = jnp.arange(length, dtype=F32)[:, None] * frequency[None, :]
    return jnp.cos(angle), jnp.sin(angle)


def rotate(value, cosine, sine, sign):
    length, width = value.shape
    value = value.reshape(length, width // HD, 2, HD // 2)
    first, second = value[:, :, 0], value[:, :, 1]
    c, s = cosine[:, None, :], sign * sine[:, None, :]
    return jnp.stack([first * c - second * s, second * c + first * s], axis=2).reshape(length, width)


MESH = pl.DeviceIdType.MESH


def flip(index, bit):
    return index + bit - 2 * bit * ((index // bit) % 2)


class Place:
    def __init__(self, pair):
        self.s, self.f = lax.axis_index("seq"), lax.axis_index("fsdp")
        self.pair = pair
        s, f = self.s, self.f
        self.sx, self.sy = flip(s, 2), flip(s, 4)
        self.sd, self.sc = flip(self.sx, 4), flip(s, 1)
        self.q = f // 2 if pair > 1 else 0
        self.x, self.y, self.core = (self.sx, f), (self.sy, f), (self.sc, f)
        self.z = (s, opposite(f)) if pair > 1 else None
        self.peers = [self.x, self.y, self.core] + ([self.z] if pair > 1 else [])

    def barrier(self):
        sem = pltpu.get_barrier_semaphore()
        for peer in self.peers:
            pl.semaphore_signal(sem, inc=1, device_id=peer, device_id_type=MESH)
        pl.semaphore_wait(sem, len(self.peers))


class Wires:
    def __init__(self, send, recv):
        self.send, self.recv, self.count, self.open = send, recv, 0, {}

    def new(self, key):
        self.open[key] = self.count
        self.count += 1

    def go(self, key, src, dst, device):
        i = self.open[key]
        copy = pltpu.make_async_remote_copy(
            src, dst, self.send.at[i], self.recv.at[i], device_id=device, device_id_type=MESH
        )
        copy.start()
        return copy


def gather_steps(place, wires, own, out, ready):
    pair, rows = place.pair, own.shape[0]
    half = rows // 2
    top, low = pl.ds(0, half), pl.ds(half, half)
    p = place
    qs = [p.q] + ([1 - p.q] if pair > 1 else [])
    kinds = ["xa", "xb", "ya", "yb", "xd", "yd", "c0", "cxa", "cxb", "cya", "cyb", "cda", "cdb"]
    for t in range(pair):
        for kind in kinds:
            wires.new((t, kind))
    if pair > 1:
        wires.new("z")
    live = {}

    def go(key, src, dst, device):
        live[key] = wires.go(key, src, dst, device)

    def begin(t, src):
        q = qs[t]
        go((t, "xa"), src.at[top], out.at[q, p.s, top], p.x)
        go((t, "yb"), src.at[low], out.at[q, p.s, low], p.y)
        go((t, "xb"), src.at[low], out.at[q, p.s, low], p.x)
        go((t, "ya"), src.at[top], out.at[q, p.s, top], p.y)
        go((t, "c0"), src, out.at[q, p.s], p.core)

    def arrived(key):
        live[key].wait_recv()

    if pair > 1:
        go("z", own, out.at[qs[0], p.s], p.z)
    begin(0, own)
    ready(qs[0], p.s, None)

    def first(t):
        q = qs[t]
        arrived((t, "xa"))
        go((t, "xd"), out.at[q, p.sx, top], out.at[q, p.sx, top], p.y)
        go((t, "cxa"), out.at[q, p.sx, top], out.at[q, p.sx, top], p.core)
        arrived((t, "yb"))
        go((t, "yd"), out.at[q, p.sy, low], out.at[q, p.sy, low], p.x)
        go((t, "cyb"), out.at[q, p.sy, low], out.at[q, p.sy, low], p.core)
        arrived((t, "c0"))
        ready(q, p.sc, None)

    def second(t):
        q = qs[t]
        arrived((t, "xb"))
        go((t, "cxb"), out.at[q, p.sx, low], out.at[q, p.sx, low], p.core)
        ready(q, p.sx, None)
        arrived((t, "ya"))
        go((t, "cya"), out.at[q, p.sy, top], out.at[q, p.sy, top], p.core)
        ready(q, p.sy, None)
        arrived((t, "xd"))
        go((t, "cda"), out.at[q, p.sd, top], out.at[q, p.sd, top], p.core)
        arrived((t, "yd"))
        go((t, "cdb"), out.at[q, p.sd, low], out.at[q, p.sd, low], p.core)

    def third(t):
        q = qs[t]
        arrived((t, "cxa"))
        arrived((t, "cxb"))
        ready(q, flip(p.sx, 1), None)
        arrived((t, "cya"))
        arrived((t, "cyb"))
        ready(q, flip(p.sy, 1), None)
        ready(q, p.sd, None)
        arrived((t, "cda"))
        arrived((t, "cdb"))
        ready(q, flip(p.sd, 1), None)

    first(0)
    if pair > 1:
        arrived("z")
        begin(1, out.at[qs[1], p.s])
        ready(qs[1], p.s, None)
    second(0)
    if pair > 1:
        first(1)
    third(0)
    if pair > 1:
        second(1)
        third(1)
    for copy in live.values():
        copy.wait_send()


def gather_wires(pair):
    return 14 * pair + (2 if pair > 1 else 0)


def gather_kernel(pair, own, out, send, recv, local):
    place = Place(pair)
    keep = pltpu.make_async_copy(own, out.at[place.q, place.s], local)
    keep.start()
    place.barrier()
    gather_steps(place, Wires(send, recv), own, out, lambda q, slot, half: None)
    keep.wait()


def plane_gather(v, n, pair, ident):
    rows, width = v.shape
    return pl.pallas_call(
        functools.partial(gather_kernel, pair),
        in_specs=[pl.BlockSpec(memory_space=pltpu.VMEM)],
        out_specs=pl.BlockSpec(memory_space=pl.ANY),
        out_shape=jax.ShapeDtypeStruct((pair, n, rows, width), v.dtype),
        scratch_shapes=[pltpu.SemaphoreType.DMA((gather_wires(pair),))] * 2 + [pltpu.SemaphoreType.DMA],
        compiler_params=pltpu.CompilerParams(collective_id=ident, has_side_effects=True),
        cost_estimate=pl.CostEstimate(flops=0, bytes_accessed=pair * n * rows * width * 20, transcendentals=0),
        name=f"gather_{ident}",
    )(v).reshape(pair * n * rows, width)


def add(a, b):
    return (a.astype(F32) + b.astype(F32)).astype(BF16)


def scatter_steps(place, wires, part, rc, rd, rx, ry, qbuf, zbuf, make, finish):
    p, pair = place, place.pair
    rows = rx.shape[1]
    half = rows // 2
    top, low = pl.ds(0, half), pl.ds(half, half)
    slots = {"d": p.sd, "x": p.sx, "y": p.sy, "o": p.s}
    order = ["d", "x", "y", "o"]
    names = ["c" + k for k in order] + ["da", "db", "xa", "xb", "ya", "yb"]
    for t in range(pair):
        for name in names:
            wires.new((t, name))
    if pair > 1:
        wires.new("z")
    live = {}

    def go(key, src, dst, device):
        live[key] = wires.go(key, src, dst, device)

    def arrived(key):
        live[key].wait_recv()

    for t in range(pair):
        for i, k in enumerate(order):
            make(t, k, 1)
            go((t, "c" + k), part(t, flip(slots[k], 1)), rc.at[t, i], p.core)

    def start(t):
        make(t, "d", 0)
        arrived((t, "cd"))
        qbuf[t, 0] = add(part(t, p.sd)[...], rc[t, 0])
        go((t, "da"), qbuf.at[t, 0, top], rd.at[t, top], p.x)
        go((t, "db"), qbuf.at[t, 0, low], rd.at[t, low], p.y)
        make(t, "x", 0)
        arrived((t, "cx"))
        qbuf[t, 1, top] = add(part(t, p.sx)[top], rc[t, 1, top])
        go((t, "xa"), qbuf.at[t, 1, top], rx.at[t, top], p.x)
        make(t, "y", 0)
        arrived((t, "cy"))
        qbuf[t, 2, low] = add(part(t, p.sy)[low], rc[t, 2, low])
        go((t, "yb"), qbuf.at[t, 2, low], ry.at[t, low], p.y)

    def relay(t):
        held = part(t, p.sx)[low].astype(F32) + rc[t, 1, low].astype(F32)
        arrived((t, "db"))
        qbuf[t, 1, low] = (held + rd[t, low].astype(F32)).astype(BF16)
        go((t, "xb"), qbuf.at[t, 1, low], rx.at[t, low], p.x)
        held = part(t, p.sy)[top].astype(F32) + rc[t, 2, top].astype(F32)
        arrived((t, "da"))
        qbuf[t, 2, top] = (held + rd[t, top].astype(F32)).astype(BF16)
        go((t, "ya"), qbuf.at[t, 2, top], ry.at[t, top], p.y)

    def total(t):
        make(t, "o", 0)
        arrived((t, "co"))
        value = part(t, p.s)[...].astype(F32) + rc[t, 3].astype(F32)
        for key in ("xa", "yb", "xb", "ya"):
            arrived((t, key))
        return value + rx[t].astype(F32) + ry[t].astype(F32)

    if pair > 1:
        start(0)
        start(1)
        relay(0)
        relay(1)
        zbuf[0] = total(0).astype(BF16)
        go("z", zbuf.at[0], zbuf.at[1], p.z)
        value = total(1)
        arrived("z")
        value = value + zbuf[1].astype(F32)
    else:
        start(0)
        relay(0)
        value = total(0)
    finish(value)
    for copy in live.values():
        copy.wait_send()


def scatter_wires(pair):
    return 84 if pair > 1 else 20


def scatter_scratch(pair, rows, width):
    block = lambda *lead: pltpu.VMEM(lead + (rows, width), BF16)
    return [
        block(pair, 4),
        block(pair),
        block(pair),
        block(pair),
        block(pair, 3),
        block(2) if pair > 1 else pltpu.VMEM((2, 16, 128), BF16),
        pltpu.SemaphoreType.DMA((scatter_wires(pair),)),
        pltpu.SemaphoreType.DMA((scatter_wires(pair),)),
    ]


def scatter_kernel(pair, value, out, rc, rd, rx, ry, qbuf, zbuf, send, recv):
    place = Place(pair)
    place.barrier()
    planes = [1 - place.q, place.q] if pair > 1 else [0]

    def part(t, slot):
        return value.at[planes[t], slot]

    def finish(total):
        out[...] = total

    scatter_steps(
        place, Wires(send, recv), part, rc, rd, rx, ry, qbuf, zbuf, lambda *_: None, finish
    )


def plane_scatter(v, n, pair, ident):
    width = v.shape[1]
    rows = v.shape[0] // (pair * n)
    return pl.pallas_call(
        functools.partial(scatter_kernel, pair),
        in_specs=[pl.BlockSpec(memory_space=pltpu.VMEM)],
        out_specs=pl.BlockSpec(memory_space=pltpu.VMEM),
        out_shape=jax.ShapeDtypeStruct((rows, width), F32),
        scratch_shapes=scatter_scratch(pair, rows, width),
        compiler_params=pltpu.CompilerParams(
            collective_id=ident, has_side_effects=True, vmem_limit_bytes=40 * 2**20
        ),
        cost_estimate=pl.CostEstimate(flops=0, bytes_accessed=pair * n * rows * width * 20, transcendentals=0),
        name=f"scatter_{ident}",
    )(v.astype(BF16).reshape(pair, n, rows, width))


def sum_kernel(n, own, out, held, send, recv):
    s, f = lax.axis_index("seq"), lax.axis_index("fsdp")
    sem = pltpu.get_barrier_semaphore()
    for d in range(1, n):
        pl.semaphore_signal(sem, inc=1, device_id=((s + d) % n, f), device_id_type=MESH)
    pl.semaphore_wait(sem, n - 1)
    copies = []
    for d in range(1, n):
        copy = pltpu.make_async_remote_copy(
            own,
            held.at[d - 1],
            send.at[d - 1],
            recv.at[d - 1],
            device_id=((s + d) % n, f),
            device_id_type=MESH,
        )
        copy.start()
        copies.append(copy)
    total = own[...]
    for d in range(1, n):
        copies[d - 1].wait_recv()
        total = total + held[d - 1]
    out[...] = total
    for copy in copies:
        copy.wait_send()


def plane_sum(v, n, ident):
    return pl.pallas_call(
        functools.partial(sum_kernel, n),
        in_specs=[pl.BlockSpec(memory_space=pltpu.VMEM)],
        out_specs=pl.BlockSpec(memory_space=pltpu.VMEM),
        out_shape=jax.ShapeDtypeStruct(v.shape, v.dtype),
        scratch_shapes=[pltpu.VMEM((n - 1,) + v.shape, v.dtype)]
        + [pltpu.SemaphoreType.DMA((n - 1,))] * 2,
        compiler_params=pltpu.CompilerParams(collective_id=ident, has_side_effects=True),
        name=f"sum_{ident}",
    )(v)


def when(condition, body):
    pl.when(condition)(body)


def line_barrier(n, m):
    s, f = lax.axis_index("seq"), lax.axis_index("fsdp")
    sem = pltpu.get_barrier_semaphore()
    for d in range(1, n):
        pl.semaphore_signal(sem, inc=1, device_id=((s + d) % n, f), device_id_type=MESH)
    for d in range(1, m):
        pl.semaphore_signal(sem, inc=1, device_id=(s, (f + d) % m), device_id_type=MESH)
    pl.semaphore_wait(sem, n + m - 2)


def exit_kernel(
    n,
    m,
    d3_,
    term_,
    own_gain,
    branch_gain,
    feed_gain,
    grad_hidden_,
    qkv,
    tokens_grad,
    weight_grad,
    gain_grad,
    d3,
    term,
    grad_hidden,
    w_v,
    value,
    rc,
    rd,
    rx,
    ry,
    qbuf,
    zbuf,
    send,
    recv,
    line,
    sums,
    done,
    got,
    gains,
    gplane,
    gsum,
    gline,
    zsend,
    zrecv,
    asend,
    arecv,
    gsend,
    grecv,
    lsend,
    lrecv,
    sems,
):
    place = Place(1)
    s, f = place.s, place.f
    moves = Moves(sems)
    moves.start(term_, term)
    moves.start(d3_, d3)
    moves.start(qkv, w_v)
    moves.start(grad_hidden_, grad_hidden)
    line_barrier(n, m)
    last = m - 1
    cols = term.shape[-1]

    def remote(src, dst, a, b, device):
        return pltpu.make_async_remote_copy(src, dst, a, b, device_id=device, device_id_type=MESH)

    def target(way, r):
        return last - r if way == 0 else r

    def hop(way, r, j, fresh):
        there = f + 1 if way == 0 else f - 1
        src = term_.at[j, :, target(way, r)] if fresh else sums.at[way, r, j]
        return remote(src, line.at[way, r, j], zsend.at[way, r, j], zrecv.at[way, r, j], (s, there))

    ends = (f == 0, f == last)
    inner = (f > 0, f < last)

    def beyond(way, r):
        return target(way, r) > f if way == 0 else target(way, r) < f

    for group in ((0, 1, 2), (3,)):
        for r in range(last):
            for j in group:
                for way in (0, 1):
                    when(ends[way], lambda: hop(way, r, j, True).start())

    gain_copies = []
    for t in range(n):
        at = pl.ds(t * cols, cols)
        for j in range(2):
            gains[t, j : j + 1, :] = jnp.where(s == t, own_gain[j], 0.0)
        gains[t, 2:3, :] = branch_gain[:, at]
        gains[t, 3:4, :] = feed_gain[:, at]
        gains[t, 4:, :] = jnp.zeros((4, cols), F32)
    for d in range(1, n):
        t = (s + d) % n
        copy = remote(gains.at[t], gplane.at[d - 1], gsend.at[d], grecv.at[d], (t, f))
        copy.start()
        gain_copies.append(copy)

    moves.finish()
    rows, width = grad_hidden.shape
    block, step = 4 * rows, min(512, width)
    per = step // (m * qkv.shape[3])

    def make(q, chip, c, first):
        here = pl.ds(pl.multiple_of(chip * block, block), block)

        @pl.loop(0, width // 2 // step)
        def _(k):
            i = first // step + k
            at = pl.ds(pl.multiple_of(i * step, step), step)
            total = jnp.zeros((block, step), F32)
            for j in range(3):
                w = w_v[j, pl.ds(i * per, per)].reshape(step, cols)
                total = total + dot(d3[j, here, :], w, NT)
            value[q, pl.ds(4 * chip, 4), :, at] = total.astype(BF16).reshape(4, rows, step)

    side = f // (m // 2)
    middle = (f > 0) & (f < last)

    def relays(k, j, from_end):
        way = side if from_end else 1 - side
        o = way * k + (1 - way) * (last - k)

        def relay():
            there = f + 1 - 2 * way
            copy = remote(
                sums.at[way, k, j], line.at[way, k, j], zsend.at[way, k, j], zrecv.at[way, k, j], (s, there)
            )
            copy.wait_recv()
            sums[way, k, j] = add(term[j, :, o], line[way, k, j])
            copy.start()

        when(middle, relay)

    live = scatter_pairs(
        place, Wires(send, recv), value, rc, rd, rx, ry, qbuf, zbuf, make, tokens_grad,
        Work([lambda: None] + [lambda j=j: relays(0, j, True) for j in range(3)]),
    )

    def join(r):
        tokens_grad[r] += grad_hidden[r]

    by_rows(0, rows, join)

    total = gains[s]
    for d in range(1, n):
        gain_copies[d - 1].wait_recv()
        total = total + gplane[d - 1]
    gsum[...] = total
    line_copies = []
    for d in range(1, m):
        t = (f + d) % m
        copy = remote(gsum, gline.at[d - 1], lsend.at[d], lrecv.at[d], (s, t))
        copy.start()
        line_copies.append(copy)

    copies = []
    plan = [(True, k, j) for k in range(1, m // 2) for j in range(3)]
    plan += [(False, k, j) for k in range(m // 2 - 1) for j in range(3)] + [(None, 0, j) for j in range(3)]
    plan += [(True, k, 3) for k in range(m // 2)] + [(False, k, 3) for k in range(m // 2 - 1)] + [(None, 0, 3)]
    for from_end, k, j in plan:
        if from_end is not None:
            relays(k, j, from_end)
            continue
        own = term[j, :, f].astype(F32)
        done[j] = own
        for way in (0, 1):
            r = last - f if way == 0 else f

            def take():
                pltpu.make_async_remote_copy(
                    sums.at[way, 0, j],
                    line.at[way, r, j],
                    zsend.at[way, r, j],
                    zrecv.at[way, r, j],
                    device_id=(s, f - 1 if way == 0 else f + 1),
                    device_id_type=MESH,
                ).wait_recv()
                done[j] += line[way, r, j].astype(F32)

            when(inner[way], take)
        if j == 3:
            for t in range(n):
                weight_grad[j, :, pl.ds(t * cols, cols)] = done[j, t]
            continue
        weight_grad[j, :, pl.ds(pl.multiple_of(s * cols, cols), cols)] = done[j, s]
        got[0, j] = done[j].astype(BF16)
        for d in range(1, n):
            t = (s + d) % n
            copy = remote(got.at[0, j, t], got.at[1, j, s], asend.at[j, d], arecv.at[j, d], (t, f))
            copy.start()
            copies.append(copy)
    total = gsum[...]
    for d in range(1, m):
        line_copies[d - 1].wait_recv()
        total = total + gline[d - 1]
    small = cols // m
    gain = jnp.zeros((8, small), F32)
    for plane in range(m):
        gain = gain + jnp.where(f == plane, total[:, plane * small : (plane + 1) * small], 0.0)
    gain_grad[...] = gain
    for copy in copies:
        copy.wait_recv()
    for j in range(3):
        for d in range(1, n):
            t = (s + d) % n
            weight_grad[j, :, pl.ds(pl.multiple_of(t * cols, cols), cols)] = got[1, j, t].astype(F32)
    for copy in copies + gain_copies + line_copies + list(live.values()):
        copy.wait_send()
    for r in range(last):
        for j in range(4):
            for way in (0, 1):
                when(ends[way] | (inner[way] & beyond(way, r)), lambda: hop(way, r, j, False).wait_send())


def leave(d3, term, own_gain, branch_gain, feed_gain, grad_hidden, qkv, n, m, ident):
    rows, width = grad_hidden.shape
    part, cols = term.shape[-2:]
    vmem = pl.BlockSpec(memory_space=pltpu.VMEM)
    dma = pltpu.SemaphoreType.DMA
    block = pltpu.VMEM((2, m - 1, 4, n, part, cols), BF16)
    return pl.pallas_call(
        functools.partial(exit_kernel, n, m),
        in_specs=any_specs(2) + [vmem] * 3 + any_specs(2),
        out_specs=[vmem] * 3,
        out_shape=[
            jax.ShapeDtypeStruct((rows, width), F32),
            jax.ShapeDtypeStruct((4, part, width), F32),
            jax.ShapeDtypeStruct((8, cols // m), F32),
        ],
        scratch_shapes=[pltpu.VMEM(d3.shape, BF16), pltpu.VMEM(term.shape, BF16), pltpu.VMEM((rows, width), F32)]
        + [pltpu.VMEM((3, n, m, part, cols), BF16), pltpu.VMEM((1, n, rows, width), BF16)]
        + scatter_scratch(1, rows, width)
        + [
            block,
            block,
            pltpu.VMEM((4, n, part, cols), F32),
            pltpu.VMEM((2, 3, n, part, cols), BF16),
            pltpu.VMEM((n, 8, cols), F32),
            pltpu.VMEM((n - 1, 8, cols), F32),
            pltpu.VMEM((8, cols), F32),
            pltpu.VMEM((m - 1, 8, cols), F32),
        ]
        + [dma((2, m, 4))] * 2
        + [dma((3, n))] * 2
        + [dma((n,))] * 2
        + [dma((m,))] * 2
        + [dma((3 * m,))],
        compiler_params=pltpu.CompilerParams(
            collective_id=ident, has_side_effects=True, vmem_limit_bytes=60 * 2**20
        ),
        cost_estimate=pl.CostEstimate(flops=0, bytes_accessed=200 * 2**20, transcendentals=0),
        name=f"leave_{ident}",
    )(d3, term, own_gain, branch_gain, feed_gain, grad_hidden, qkv)


class Moves:
    def __init__(self, sems):
        self.sems, self.count, self.open = sems, 0, []

    def start(self, src, dst):
        copy = pltpu.make_async_copy(src, dst, self.sems.at[self.count])
        self.count += 1
        copy.start()
        self.open.append(copy)
        return copy

    def finish(self):
        for copy in self.open:
            copy.wait()
        self.open = []

    def wait(self, copies):
        for copy in copies:
            copy.wait()
        self.open = [copy for copy in self.open if all(copy is not other for other in copies)]


def place_kernel(parts, count, *refs):
    ins, outs = refs[:count], refs[count : count + len(parts)]
    held, sems = refs[count + len(parts) : -1], refs[-1]
    copies = []
    for i, (source, row) in enumerate(parts):
        src = ins[source] if row is None else ins[source].at[row]
        copies.append(pltpu.make_async_copy(src, held[i], sems.at[0, i]))
        copies[-1].start()
    back = []
    for i in range(len(parts)):
        copies[i].wait()
        back.append(pltpu.make_async_copy(held[i], outs[i], sems.at[1, i]))
        back[-1].start()
    for copy in back:
        copy.wait()


def place_outputs(arrays):
    parts, shapes = [], []
    for source, a in enumerate(arrays):
        for row in range(a.shape[0]) if a.ndim == 3 else [None]:
            parts.append((source, row))
            shapes.append(shape(a.shape[-2:], a.dtype))
    return pl.pallas_call(
        functools.partial(place_kernel, tuple(parts), len(arrays)),
        in_specs=[pl.BlockSpec(memory_space=pltpu.MemorySpace.HBM)] * len(arrays),
        out_specs=[pl.BlockSpec(memory_space=pltpu.MemorySpace.HBM)] * len(parts),
        out_shape=shapes,
        scratch_shapes=[pltpu.VMEM(a.shape, a.dtype) for a in shapes] + [pltpu.SemaphoreType.DMA((2, len(parts)))],
        compiler_params=pltpu.CompilerParams(vmem_limit_bytes=63 * 2**20),
        name="place",
    )(*arrays)


def gather_pairs(place, wires, own, out, work, hook=lambda: None, done=lambda q, chip: None):
    p, pair = place, place.pair
    half = own.shape[0] // 2
    top, low = pl.ds(0, half), pl.ds(half, half)
    qs = [p.q] + ([1 - p.q] if pair > 1 else [])
    for t in range(pair):
        for kind in ["xa", "xb", "ya", "yb", "xd", "yd", "ca", "cb", "cxa", "cxb", "cya", "cyb", "cda", "cdb"]:
            wires.new((t, kind))
    if pair > 1:
        wires.new("za")
        wires.new("zb")
    live = {}

    def go(key, src, dst, device):
        live[key] = wires.go(key, src, dst, device)

    def arrived(*keys):
        for key in keys:
            live[key].wait_recv()

    def begin(t, src, tops):
        q = qs[t]
        rows = top if tops else low
        go((t, "xa" if tops else "xb"), src.at[rows], out.at[q, p.s, rows], p.x)
        go((t, "ya" if tops else "yb"), src.at[rows], out.at[q, p.s, rows], p.y)
        go((t, "ca" if tops else "cb"), src.at[rows], out.at[q, p.s, rows], p.core)

    def pass_on(t, name, slot, rows, device):
        ref = out.at[qs[t], slot, rows]
        go((t, name), ref, ref, device)

    def first(t):
        arrived((t, "xa"))
        pass_on(t, "xd", p.sx, top, p.y)
        pass_on(t, "cxa", p.sx, top, p.core)
        arrived((t, "ya"))
        pass_on(t, "cya", p.sy, top, p.core)

    def second(t):
        arrived((t, "yb"))
        pass_on(t, "yd", p.sy, low, p.x)
        pass_on(t, "cyb", p.sy, low, p.core)
        arrived((t, "xb"))
        pass_on(t, "cxb", p.sx, low, p.core)

    def third(t):
        arrived((t, "xd"))
        pass_on(t, "cda", p.sd, top, p.core)
        arrived((t, "yd"))
        pass_on(t, "cdb", p.sd, low, p.core)

    def chip_at(k):
        chip = p.s // 2
        return (chip % 2 + k % 2) % 2 + 2 * ((chip // 2 + k // 2) % 2)

    def use(t, first, count, *keys):
        arrived(*[(t, key) for key in keys])
        if count == 1:
            work(qs[t], chip_at(first))
        else:

            @pl.loop(first, first + count)
            def _(k):
                work(qs[t], chip_at(k))

        for k in range(first, first + count):
            done(qs[t], chip_at(k))

    if pair > 1:
        go("za", own.at[top], out.at[qs[0], p.s, top], p.z)
        go("zb", own.at[low], out.at[qs[0], p.s, low], p.z)
    begin(0, own, True)
    begin(0, own, False)
    if pair > 1:
        arrived((0, "ca"), (0, "cb"))
        hook()
        first(0)
        second(0)
        use(0, 0, 2, "cxa", "cxb")
        arrived("za")
        begin(1, out.at[qs[1], p.s], True)
        third(0)
        hook()
        use(0, 2, 2, "cya", "cyb", "cda", "cdb")
        arrived("zb")
        begin(1, out.at[qs[1], p.s], False)
        first(1)
        use(1, 0, 1, "ca", "cb")
        hook()
        second(1)
        hook()
        use(1, 1, 2, "cxa", "cxb", "cya", "cyb")
        third(1)
        use(1, 3, 1, "cda", "cdb")
    else:
        use(0, 0, 1, "ca", "cb")
        hook()
        first(0)
        hook()
        second(0)
        use(0, 1, 2, "cxa", "cxb", "cya", "cyb")
        hook()
        third(0)
        use(0, 3, 1, "cda", "cdb")
    return live


def by_rows(first, count, body):
    @pl.loop(0, count // 32)
    def _(i):
        body(pl.ds(pl.multiple_of(first + i * 32, 32), 32))


def scatter_pairs(
    place, wires, value, rc, rd, rx, ry, qbuf, zbuf, make, result, hook=lambda: None, jobs=None, mine=None, theirs=None
):
    p, pair = place, place.pair
    rows, width = rx.shape[1], rx.shape[2]
    count = 4 if pair > 1 else 2
    half, wide = rows // 2, width // count
    top, low = pl.ds(0, half), pl.ds(half, half)
    slots = {"d": p.sd, "x": p.sx, "y": p.sy, "o": p.s}
    order = ["d", "x", "y", "o"]
    planes = [1 - p.q, p.q] if pair > 1 else [p.q]
    jobs = jobs or [(t, c) for t in range(pair) for c in range(count)]
    mine = mine or list(range(count))
    theirs = theirs or mine
    for job in jobs:
        for name in ["c" + k for k in order] + ["da", "db", "xa", "xb", "ya", "yb"]:
            wires.new((job, name))
    if pair > 1:
        for c in range(count):
            wires.new(f"z{c}")
    live = {}

    def go(key, src, dst, device):
        live[key] = wires.go(key, src, dst, device)

    def arrived(*keys):
        for key in keys:
            live[key].wait_recv()

    def span(block):
        return pl.ds(block * wide if isinstance(block, int) else pl.multiple_of(block * wide, wide), wide)

    def at(c):
        return span(mine[c])

    def part(job, slot, rows_):
        return value.at[planes[job[0]], slot, rows_, at(job[1])]

    every = pl.ds(0, rows)

    def begin(job):
        t, c = job

        @pl.loop(0, 2)
        def _(k):
            make(planes[t], k, c, mine[c] * wide)

        for i, k in enumerate(order):
            go((job, "c" + k), part(job, flip(slots[k], 1), every), rc.at[t, i, :, at(c)], p.core)

    def rest(job):
        t, c = job

        def sum_of(i, slot):
            def body(r):
                qbuf[t, i, r, at(c)] = add(value[planes[t], slot, r, at(c)], rc[t, i, r, at(c)])

            return body

        arrived((job, "cd"))
        by_rows(0, rows, sum_of(0, p.sd))
        go((job, "da"), qbuf.at[t, 0, top, at(c)], rd.at[t, top, at(c)], p.x)
        go((job, "db"), qbuf.at[t, 0, low, at(c)], rd.at[t, low, at(c)], p.y)
        arrived((job, "cx"))
        by_rows(0, half, sum_of(1, p.sx))
        go((job, "xa"), qbuf.at[t, 1, top, at(c)], rx.at[t, top, at(c)], p.x)
        arrived((job, "cy"))
        by_rows(half, half, sum_of(2, p.sy))
        go((job, "yb"), qbuf.at[t, 2, low, at(c)], ry.at[t, low, at(c)], p.y)

    def relay(job):
        t, c = job

        def sum_of(i, slot):
            def body(r):
                held = value[planes[t], slot, r, at(c)].astype(F32) + rc[t, i, r, at(c)].astype(F32)
                qbuf[t, i, r, at(c)] = (held + rd[t, r, at(c)].astype(F32)).astype(BF16)

            return body

        arrived((job, "db"))
        by_rows(half, half, sum_of(1, p.sx))
        go((job, "xb"), qbuf.at[t, 1, low, at(c)], rx.at[t, low, at(c)], p.x)
        arrived((job, "da"))
        by_rows(0, half, sum_of(2, p.sy))
        go((job, "ya"), qbuf.at[t, 2, top, at(c)], ry.at[t, top, at(c)], p.y)

    def total(job):
        t, c = job
        arrived((job, "co"), (job, "xa"), (job, "yb"), (job, "xb"), (job, "ya"))

        def body(r):
            held = value[planes[t], p.s, r, at(c)].astype(F32) + rc[t, 3, r, at(c)].astype(F32)
            held = held + rx[t, r, at(c)].astype(F32) + ry[t, r, at(c)].astype(F32)
            if pair > 1 and t == 0:
                zbuf[0, r, at(c)] = held.astype(BF16)
            else:
                result[r, at(c)] = held

        by_rows(0, rows, body)
        if pair > 1 and t == 0:
            go(f"z{c}", zbuf.at[0, :, at(c)], zbuf.at[1, :, at(c)], p.z)

    begin(jobs[0])
    rest(jobs[0])
    if len(jobs) > 1:
        begin(jobs[1])
    for i, job in enumerate(jobs):
        if i + 1 < len(jobs):
            rest(jobs[i + 1])
        hook()
        if i + 2 < len(jobs):
            begin(jobs[i + 2])
        relay(job)
        hook()
        if i > 0:
            total(jobs[i - 1])
    total(jobs[-1])
    if pair > 1:
        for c in range(count):
            here = span(theirs[c])
            arrived(f"z{c}")

            def body(r):
                result[r, here] += zbuf[1, r, here].astype(F32)

            by_rows(0, rows, body)
    return live


def rms_back(value, gain, grad):
    inverse = lax.rsqrt(jnp.mean(value * value, axis=-1, keepdims=True) + EPSILON)
    normal = value * inverse
    u = grad * gain
    return inverse * (u - normal * jnp.mean(u * normal, axis=-1, keepdims=True)), grad * normal


def any_specs(count):
    return [pl.BlockSpec(memory_space=pl.ANY)] * count


def vmem_specs(count):
    return [pl.BlockSpec(memory_space=pltpu.VMEM)] * count


def kernel_params(ident, mib=60):
    return pltpu.CompilerParams(collective_id=ident, has_side_effects=True, vmem_limit_bytes=mib * 2**20)


def shape(dims, kind):
    return jax.ShapeDtypeStruct(dims, kind)


def feed_kernel(
    pair, h, hidden, gains, cotangent, wg, wu, down_w,
    layer_out, gain_term, hs, wu_all, grad_gate, grad_up, gate_t, up_t, down_term,
    hs_v, w_v, d_v, g_v, u_v, i_v, t_v, gt_v, ut_v, acc, grad_low, sum_v, value,
    rc, rd, rx, ry, qbuf, zbuf, ssend, srecv, send, recv, gsend, grecv, zsem, rsem, sems
):
    place = Place(pair)
    place.peers.append((place.s, flip(place.f, 1)))
    moves = Moves(sems)
    deep = wu.shape[1]
    loads = [moves.start(wg, w_v.at[0])]
    far_f, near_f = opposite(place.f), flip(place.f, 1)

    def up_rows(plane):
        return w_v.at[1, pl.ds(pl.multiple_of(plane * deep, deep), deep)]

    loads += [moves.start(wu.at[plane], up_rows(plane)) for plane in (place.f, near_f, far_f)]
    rows, width = h.shape
    block, share = 2 * rows, wg.shape[1]
    up_pass = pltpu.make_async_remote_copy(
        wu.at[far_f], up_rows(far_f), rsem.at[0], rsem.at[1], device_id=(place.s, near_f), device_id_type=MESH
    )
    hs_v[place.q, place.s] = h[...]
    place.barrier()
    stream, view = Stream(place, zsem), half_rows(down_w, share)
    deep_d = down_w.shape[1]

    def columns(plane):
        return d_v.at[:, pl.ds(pl.multiple_of(plane * deep_d, deep_d), deep_d)]

    own_copy = pltpu.make_async_copy(view(stream.half), columns(place.f), zsem.at[0, 3, 0])
    near_copy = stream.remote(0, 1, view(stream.half), columns(place.f), stream.near)
    far_copy = stream.remote(0, 0, view(1 - stream.half), columns(place.f), stream.far)
    relay = stream.remote(0, 2, columns(far_f), columns(far_f), stream.near)

    def pass_up():
        moves.wait(loads)
        up_pass.start()
        near_copy.start()
        own_copy.start()

    def pass_down():
        far_copy.start()

    n = hs.shape[1]
    step = min(256, share)

    def ready(q, chip):
        slots, here = where(q, chip)

        @pl.loop(0, share // step)
        def _(j):
            cols = pl.ds(pl.multiple_of(j * step, step), step)
            g_v[here, cols] = dot(hs_v[q, slots].reshape(block, width), w_v[0, :, cols], NN)

        if whole:
            second(q, slots, here)

    def done(q, chip):
        slots, here = where(q, chip)
        moves.start(hs_v.at[q, slots], hs.at[q, slots])
        if not whole:
            held.append((q, chip))

    whole, held = [], []

    def where(q, chip):
        return pl.ds(2 * chip, 2), pl.ds(pl.multiple_of(q * n * rows + chip * block, block), block)

    def second(q, slots, here):
        @pl.loop(0, share // step)
        def _(j):
            cols = pl.ds(pl.multiple_of(j * step, step), step)
            u = dot(hs_v[q, slots].reshape(block, width), w_v[1, :, cols], NN)
            g = g_v[here, cols]
            u_v[here, cols] = u
            value = g * (1.0 / (1.0 + jnp.exp(-g))) * u
            i_v[here, cols] = value.astype(BF16)
            t_v[cols, here] = value.T.astype(BF16)

    def complete():
        up_pass.wait_recv()
        whole.append(True)

        @pl.loop(0, n // 2)
        def _(chip):
            second(place.q, *where(place.q, chip))

        for q, chip in held[n // 2 :]:
            second(q, *where(q, chip))

    gathered = gather_pairs(place, Wires(send, recv), h, hs_v, ready, Work([pass_up, lambda: None, pass_down, complete]), done)
    moves.start(w_v.at[1], wu_all)
    for copy in gathered.values():
        copy.wait_send()
    moves.finish()
    gain = gains[3:4, :]
    own_copy.wait()
    near_copy.wait_recv()

    def pass_on():
        far_copy.wait_recv()
        relay.start()

    def make(q, chip, c, at):
        here = pl.ds(pl.multiple_of(q * n * rows + chip * 2 * block, 2 * block), 2 * block)
        cols = pl.ds(pl.multiple_of(at, deep_d), deep_d)
        part = dot(i_v[here, :], d_v[:, cols], NN).astype(BF16)
        value[q, pl.ds(4 * chip, 4), :, cols] = part.reshape(4, rows, deep_d)

    f = place.f
    mine = [f, near_f, far_f, opposite(near_f)]
    theirs = [far_f, opposite(near_f), f, near_f]
    jobs = [(0, 0), (0, 1), (1, 0), (0, 2), (1, 1), (0, 3), (1, 2), (1, 3)]
    live = scatter_pairs(
        place, Wires(ssend, srecv), value, rc, rd, rx, ry, qbuf, zbuf, make, sum_v,
        Work([lambda: None] * 2 + [pass_on] + [lambda: None] * 3 + [relay.wait_recv]), jobs, mine, theirs,
    )
    gain_term[...] = jnp.zeros_like(gain_term)

    def last(r):
        feed, grad = sum_v[r], cotangent[r].astype(F32)
        back, term = rms_back(feed, gain, grad)
        inverse = lax.rsqrt(jnp.mean(feed * feed, axis=-1, keepdims=True) + EPSILON)
        layer_out[r] = (hidden[r] + feed * inverse * gain).astype(BF16)
        grad_low[r] = back.astype(BF16)
        gain_term[...] += jnp.sum(term, axis=0, keepdims=True)

    by_rows(0, rows, last)
    def turn_back(q, chip):
        slots = pl.ds(2 * chip, 2)
        here = pl.ds(pl.multiple_of(q * n * rows + chip * block, block), block)

        @pl.loop(0, share // step)
        def _(j):
            cols = pl.ds(pl.multiple_of(j * step, step), step)
            a = hs_v[q, slots].reshape(block, width)
            e = dot(a, d_v[cols, :], NT)
            v, u = g_v[here, cols], u_v[here, cols]
            s = 1.0 / (1.0 + jnp.exp(-v))
            dg = e * u * s * (1.0 + v * (1.0 - s))
            du = e * v * s
            i_v[here, cols] = dg.astype(BF16)
            w_v[1, here, cols] = du.astype(BF16)
            gt_v[cols, here] = dg.T.astype(BF16)
            ut_v[cols, here] = du.T.astype(BF16)

    def keep(q, chip):
        here = pl.ds(pl.multiple_of(q * n * rows + chip * block, block), block)
        moves.start(i_v.at[here], grad_gate.at[here])
        moves.start(w_v.at[1, here], grad_up.at[here])

    def add_term(t):
        q = place.q if t == 0 else 1 - place.q
        tokens = pl.ds(pl.multiple_of(q * n * rows, n * rows), n * rows)

        @pl.loop(0, width // step)
        def _(j):
            cols = pl.ds(pl.multiple_of(j * step, step), step)
            part = dot(t_v[:, tokens], hs_v[q, :, :, cols].reshape(n * rows, step), NN)
            if t == 0:
                acc[:, cols] = part
            else:
                acc[:, cols] += part

    nothing = lambda: None
    hs_v[place.q, place.s] = grad_low[...]
    returned = gather_pairs(
        place, Wires(gsend, grecv), grad_low, hs_v, turn_back,
        Work([nothing, nothing, nothing, lambda: add_term(0)]), keep
    )
    add_term(1)
    for j in range(down_term.shape[0]):
        to = w_v.at[0, pl.ds(j * share, share)]
        to[...] = acc[:, pl.ds(j * deep_d, deep_d)].astype(BF16)
        moves.start(to, down_term.at[j])
    moves.start(gt_v, gate_t)
    moves.start(ut_v, up_t)
    for copy in list(live.values()) + list(returned.values()) + [relay, near_copy, far_copy, up_pass]:
        copy.wait_send()
    moves.finish()


def ffn_feed(h, hidden, gains, cotangent, wg, wu, down_w, n, m, pair, ident):
    rows, width = h.shape
    share, long = wg.shape[1], pair * n * rows
    dma = pltpu.SemaphoreType.DMA
    vmem = pltpu.VMEM
    outs = [
        shape((rows, width), BF16),
        shape((1, width), F32),
        shape((pair, n, rows, width), BF16),
        shape((width, share), BF16),
        shape((long, share), BF16),
        shape((long, share), BF16),
        shape((share, long), BF16),
        shape((share, long), BF16),
        shape((m, share, width // m), BF16),
    ]
    return pl.pallas_call(
        functools.partial(feed_kernel, pair),
        in_specs=vmem_specs(4) + any_specs(3),
        out_specs=vmem_specs(2) + any_specs(7),
        out_shape=outs,
        scratch_shapes=[
            vmem((pair, n, rows, width), BF16),
            vmem((2, width, share), BF16),
            vmem((share, width), BF16),
            vmem((long, share), F32),
            vmem((long, share), F32),
            vmem((long, share), BF16),
            vmem((share, long), BF16),
            vmem((share, long), BF16),
            vmem((share, long), BF16),
            vmem((share, width), F32),
            vmem((rows, width), BF16),
            vmem((rows, width), F32),
            vmem((pair, n, rows, width), BF16),
        ]
        + scatter_scratch(pair, rows, width)
        + [dma((gather_wires(pair),))] * 4
        + [dma((1, 4, 2)), dma((2,)), dma((16 + 4 * pair * n // 2,))],
        compiler_params=kernel_params(ident, 63),
        cost_estimate=pl.CostEstimate(
            flops=10 * long * width * share, bytes_accessed=long * width * 90, transcendentals=0
        ),
        name=f"feed_{ident}",
    )(h, hidden, gains, cotangent, wg, wu, down_w)


def back_kernel(
    pair, gg, gu, wg, wu, gate_t, hs, down_term, branch, gains, cotangent,
    grad_hidden, grad_low, gain_term, down_grad, gate_term,
    a_v, w_v, value, rc, rd, rx, ry, qbuf, zbuf, send, recv,
    gt_v, hs_v, gterm, down_own, down_near, down_total, down_from, dsem, sems
):
    place = Place(pair)
    place.peers.append((place.s, flip(place.f, 1)))
    moves = Moves(sems)
    loads = [moves.start(wg, w_v.at[0]), moves.start(wu, w_v.at[1])]
    loads += [moves.start(gg, a_v.at[0]), moves.start(gu, a_v.at[1])]
    late = []
    down = Settle(place, dsem, down_term, down_own, down_near, down_total, down_from)
    pieces = term_work(gterm, gt_v, hs_v, lambda: moves.wait(late), gate_term, moves)
    idle = [lambda: None]
    work = Work(idle + pieces[:1] + idle + [down.middle] + pieces[1:2] + idle + pieces[2:3] + idle + pieces[3:])
    rows, width = branch.shape
    block = 2 * rows
    n = value.shape[1]
    step = min(256, width)
    place.barrier()
    down.start(True)
    moves.wait(loads)
    late.append(moves.start(gate_t, gt_v))
    for q in range(pair):
        late.append(moves.start(hs.at[q], hs_v.at[q]))

    def make(q, chip, c, at):
        here = pl.ds(pl.multiple_of(q * n * rows + chip * 2 * block, 2 * block), 2 * block)

        @pl.loop(0, width // 4 // step)
        def _(j):
            cols = pl.ds(pl.multiple_of(at + j * step, step), step)
            part = dot(a_v[0, here, :], w_v[0, cols, :], NT) + dot(a_v[1, here, :], w_v[1, cols, :], NT)
            value[q, pl.ds(4 * chip, 4), :, cols] = part.astype(BF16).reshape(4, rows, step)

    live = scatter_pairs(place, Wires(send, recv), value, rc, rd, rx, ry, qbuf, zbuf, make, grad_hidden, work)
    work.rest()
    gain_term[...] = jnp.zeros_like(gain_term)

    def last(r):
        grad = cotangent[r].astype(F32) + grad_hidden[r]
        grad_hidden[r] = grad
        back, term = rms_back(branch[r], gains[2:3, :], grad)
        grad_low[r] = back.astype(BF16)
        gain_term[...] += jnp.sum(term, axis=0, keepdims=True)

    by_rows(0, rows, last)
    share = down_grad.shape[0] // 2

    def store(u, i, value):
        size = value.shape[0]
        down_grad[pl.ds(pl.multiple_of(u * share + i * size, size), size), :] = value

    down.finish(store)
    for copy in live.values():
        copy.wait_send()
    moves.finish()


def ffn_back(gg, gu, wg, wu, gate_t, hs, down_term, branch, gains, cotangent, n, m, pair, ident):
    rows, width = branch.shape
    share, deep = gate_t.shape[0], width // m
    term = down_term.shape
    dma = pltpu.SemaphoreType.DMA
    return pl.pallas_call(
        functools.partial(back_kernel, pair),
        in_specs=any_specs(7) + vmem_specs(3),
        out_specs=vmem_specs(4) + any_specs(1),
        out_shape=[
            shape((rows, width), F32),
            shape((rows, width), BF16),
            shape((1, width), F32),
            shape((2 * share, deep), F32),
            shape(term, BF16),
        ],
        scratch_shapes=[
            pltpu.VMEM((2,) + gg.shape, BF16),
            pltpu.VMEM((2,) + wg.shape, BF16),
            pltpu.VMEM((pair, n, rows, width), BF16),
        ]
        + scatter_scratch(pair, rows, width)
        + [pltpu.VMEM(v.shape, BF16) for v in (gate_t, hs)]
        + [pltpu.VMEM(term, BF16)]
        + settle_scratch(share, deep)
        + [dma((20,))],
        compiler_params=kernel_params(ident, 63),
        cost_estimate=pl.CostEstimate(
            flops=4 * gg.shape[0] * gg.shape[1] * width, bytes_accessed=pair * n * rows * width * 40, transcendentals=0
        ),
        name=f"back_{ident}",
    )(gg, gu, wg, wu, gate_t, hs, down_term, branch, gains, cotangent)


def opposite(f):
    return (f + 2) % 4


class Stream:
    def __init__(self, place, sems):
        self.place, self.sems = place, sems
        f = place.f
        self.half, self.far_f, self.near_f = f // 2, opposite(f), flip(f, 1)
        self.far, self.near = (place.s, self.far_f), (place.s, self.near_f)

    def remote(self, k, step, src, dst, device):
        return pltpu.make_async_remote_copy(
            src, dst, self.sems.at[k, step, 0], self.sems.at[k, step, 1], device_id=device, device_id_type=MESH
        )

    def far_copy(self, k, view, full):
        return self.remote(k, 0, view(1 - self.half), full.at[self.place.f], self.far)

    def near_copy(self, k, view, full):
        return self.remote(k, 1, view(self.half), full.at[self.place.f], self.near)

    def own_copy(self, k, view, full):
        return pltpu.make_async_copy(view(self.half), full.at[self.place.f], self.sems.at[k, 3, 0])

    def relay_copy(self, k, full):
        return self.remote(k, 2, full.at[self.far_f], full.at[self.far_f], self.near)

    def start_far(self, k, view, full):
        self.far_copy(k, view, full).start()

    def start_near(self, k, view, full):
        self.near_copy(k, view, full).start()
        self.own_copy(k, view, full).start()

    def relay(self, k, view, full):
        self.far_copy(k, view, full).wait_recv()
        self.relay_copy(k, full).start()

    def finish(self, k, view, full):
        self.near_copy(k, view, full).wait_recv()
        self.relay_copy(k, full).wait_recv()
        self.own_copy(k, view, full).wait()
        self.far_copy(k, view, full).wait_send()
        self.near_copy(k, view, full).wait_send()
        self.relay_copy(k, full).wait_send()


def half_columns(ref, share):
    return lambda u: ref.at[:, pl.ds(pl.multiple_of(u * share, share), share)]


def half_rows(ref, share):
    return lambda u: ref.at[pl.ds(pl.multiple_of(u * share, share), share), :]


def full_barrier(place, n, near):
    sem = pltpu.get_barrier_semaphore()
    s, f = place.s, place.f
    for d in range(1, n):
        pl.semaphore_signal(sem, inc=1, device_id=((s + d) % n, f), device_id_type=MESH)
    for other in near:
        pl.semaphore_signal(sem, inc=1, device_id=(s, other), device_id_type=MESH)
    pl.semaphore_wait(sem, n - 1 + len(near))


def swap_halves(v):
    return pltpu.roll(v, HD // 2, axis=1)


def to_rows(first, second):
    rows = first.shape[0]
    lane = lax.broadcasted_iota(jnp.int32, (rows, 128), 1)
    wide = jnp.where(lane == 0, first, jnp.where(lane == 1, second, 0.0))
    return wide.T[:8]


def to_columns(v):
    return jnp.concatenate([v, jnp.zeros((120, v.shape[1]), F32)], axis=0).T


def exchange(place, n, own, held, send, recv):
    copies = []
    for d in range(1, n):
        copy = pltpu.make_async_remote_copy(
            own,
            held.at[d - 1],
            send.at[d - 1],
            recv.at[d - 1],
            device_id=((place.s + d) % n, place.f),
            device_id_type=MESH,
        )
        copy.start()
        copies.append(copy)
    total = own[...]
    for d in range(1, n):
        copies[d - 1].wait_recv()
        total = total + held[d - 1]
    return total, copies


def attend(block, q_v, k_v, v_v, out_v, low_v, lt_v, log_v):
    length = q_v.shape[0]
    scale = HD ** (-0.5)

    @pl.loop(0, q_v.shape[1] // HD)
    def _(h):
        cols = pl.ds(pl.multiple_of(h * HD, HD), HD)
        for half in range(2):
            wide = pl.ds(0, (half + 1) * length // 2)

            @pl.loop(half * length // 2 // block, (half + 1) * length // 2 // block)
            def _(i):
                rows = pl.ds(pl.multiple_of(i * block, block), block)
                s = dot(q_v[rows, cols], k_v[wide, cols], NT) * scale
                column = lax.broadcasted_iota(jnp.int32, s.shape, 1)
                row = lax.broadcasted_iota(jnp.int32, s.shape, 0) + i * block
                s = jnp.where(column <= row, s, -jnp.inf)
                top = jnp.max(s, axis=-1, keepdims=True)
                p = jnp.exp(s - top)
                total = jnp.sum(p, axis=-1, keepdims=True)
                out = dot((p * (1.0 / total)).astype(BF16), v_v[wide, cols], NN)
                out_v[rows, cols] = out
                low_v[rows, cols] = out.astype(BF16)
                lt_v[cols, rows] = out.T.astype(BF16)
                log_v[h, rows, :] = top + jnp.log(total)


def opening_kernel(
    n, m, x, wq, wk, wv, own_gains, wo_own, gate_w, up_w, down_w,
    qkv, all_gains, tables, raw, heads, attended, low_t, xs_t, log_total, inverse, branch, hidden, hidden_low, wg, wu, wo,
    full, xs_v, xt_v, lt_v, w_v, wo_v, raw_v, heads_v, out_v, low_v, log_v, small, held, value,
    rc, rd, rx, ry, qbuf, zbuf, send, recv, ssend, srecv, zsem, osem,
    tsend, trecv, asend, arecv, zsend, zrecv, gsend, grecv, sems,
):
    place = Place(1)
    s, f = place.s, place.f
    rows, width = x.shape
    part = wq.shape[0]
    length, cols = raw.shape[1], raw.shape[2]
    share = wg.shape[2]
    block = min(256, length)
    per = block // rows
    weights = (wq, wk, wv)
    moves = Moves(sems)
    kept = []
    for j, w in enumerate(weights):
        own = w.at[:, pl.ds(pl.multiple_of(s * cols, cols), cols)]
        kept.append(moves.start(own, w_v.at[j, s, f]))
    own_out = [moves.start(wo_own, wo_v.at[f])]
    full[f, s] = own_gains[...]
    xs_v[0, s] = x[...]
    line_barrier(n, m)
    sent = []

    def remote(src, dst, a, b, device):
        copy = pltpu.make_async_remote_copy(src, dst, a, b, device_id=device, device_id_type=MESH)
        copy.start()
        sent.append(copy)
        return copy

    second = []
    for j, w in enumerate(weights):
        row = []
        for d in range(1, n):
            t = (s + d) % n
            src = w.at[:, pl.ds(pl.multiple_of(t * cols, cols), cols)]
            row.append(remote(src, w_v.at[j, s, f], asend.at[j, d], arecv.at[j, d], (t, f)))
        second.append(row)
    first = []
    for d in range(1, n):
        first.append(remote(own_gains, full.at[f, s], gsend.at[d], grecv.at[d], ((s + d) % n, f)))

    def piece(j, o):
        return full.at[o] if j == 3 else w_v.at[j, :, o]

    def hop(way, h, j):
        o = f - h if way == 0 else f + h
        there = f + 1 if way == 0 else f - 1
        place_ = piece(j, o)
        return pltpu.make_async_remote_copy(
            place_, place_, zsend.at[way, h, j], zrecv.at[way, h, j], device_id=(s, there), device_id_type=MESH
        )

    def sends(way, h):
        return ((f - h >= 0) & (f < m - 1)) if way == 0 else ((f + h <= m - 1) & (f > 0))

    def receives(way, h):
        return (f - h - 1 >= 0) if way == 0 else (f + h + 1 <= m - 1)

    def start(h, j):
        for way in (0, 1):
            when(sends(way, h), lambda: hop(way, h, j).start())

    def landed(h, j):
        for way in (0, 1):
            o = f - h - 1 if way == 0 else f + h + 1

            def wait():
                there = f - 1 if way == 0 else f + 1
                place_ = piece(j, o)
                pltpu.make_async_remote_copy(
                    place_, place_, zsend.at[way, h, j], zrecv.at[way, h, j], device_id=(s, there), device_id_type=MESH
                ).wait_recv()

            when(receives(way, h), wait)

    def step(h, j):
        landed(h, j)
        if h + 1 < m - 1:
            start(h + 1, j)

    moves.wait(kept)
    for j in range(3):
        for copy in second[j]:
            copy.wait_recv()
        start(0, j)
    for copy in first:
        copy.wait_recv()
    start(0, 3)
    gathered = gather_pairs(
        place, Wires(tsend, trecv), x, xs_v, lambda *_: None, Work([lambda: None, lambda: step(0, 0), lambda: step(0, 1)])
    )
    step(0, 2)
    step(0, 3)
    half = HD // 2
    lane = lax.broadcasted_iota(jnp.int32, (block, HD), 1)
    row = lax.broadcasted_iota(jnp.int32, (block, HD), 0)
    frequency = jnp.exp((lane % half).astype(F32) * (-2.0 * math.log(THETA) / HD))

    @pl.loop(0, length // block)
    def _(i):
        angle = (row + i * block).astype(F32) * frequency
        here = pl.ds(pl.multiple_of(i * block, block), block)
        tables[0, here, :] = jnp.cos(angle)
        sine = jnp.sin(angle)
        tables[1, here, :] = jnp.where(lane < half, -sine, sine)

    for h in range(1, m - 2):
        for j in range(4):
            step(h, j)

    out_copies = []
    for d, plane in enumerate((flip(f, 1), opposite(f), opposite(flip(f, 1)))):
        out_copies.append(
            pltpu.make_async_remote_copy(
                wo_own, wo_v.at[f], osem.at[0, d], osem.at[1, d], device_id=(s, plane), device_id_type=MESH
            )
        )
        out_copies[-1].start()
    stream = Stream(place, zsem)
    views = [half_columns(gate_w, share), half_columns(up_w, share)]
    fulls = [wg, wu]
    for k in range(2):
        stream.start_far(k, views[k], fulls[k])
    for k in range(2):
        stream.start_near(k, views[k], fulls[k])

    @pl.loop(0, length // block)
    def _(i):
        here = pl.ds(pl.multiple_of(i * block, block), block)
        xt_v[:, here] = xs_v[0, pl.ds(i * per, per)].reshape(block, width).T

    def project(j):
        @pl.loop(0, length // block)
        def _(i):
            here = pl.ds(pl.multiple_of(i * block, block), block)
            a = xs_v[0, pl.ds(i * per, per)].reshape(block, width)
            product = dot(a, w_v[j].reshape(width, cols), NN)
            if j == 2:
                heads_v[2, here, :] = product.astype(BF16)
            else:
                raw_v[j, here, :] = product

    moves.start(xt_v, xs_t)
    for j in range(3):
        landed(m - 2, j)
        project(j)
    landed(m - 2, 3)
    for t in range(n):
        for plane in range(m):
            at = (t * m + plane) * part
            all_gains[:, at : at + part] = full[plane, t, :, :part]
    moves.start(w_v, qkv)

    @pl.loop(0, length // block)
    def _(i):
        here = pl.ds(pl.multiple_of(i * block, block), block)
        q, k = raw_v[0, here, :], raw_v[1, here, :]
        small[0, :, here] = to_rows(
            jnp.sum(q * q, axis=1, keepdims=True), jnp.sum(k * k, axis=1, keepdims=True)
        )

    moves.start(raw_v, raw)
    first_col = pl.multiple_of(s * cols, cols)
    total, stat_copies = exchange(place, n, small.at[0], held, ssend, srecv)
    small[1] = lax.rsqrt(total * (1.0 / width) + EPSILON)
    moves.start(small.at[1], inverse)

    @pl.loop(0, length // block)
    def _(i):
        here = pl.ds(pl.multiple_of(i * block, block), block)
        inv = to_columns(small[1, :, here])
        cosine, sine = tables[0, here, :], tables[1, here, :]
        for j in range(2):
            for h in range(cols // HD):
                part = pl.ds(h * HD, HD)
                v = raw_v[j, here, part] * inv[:, j : j + 1] * all_gains[j : j + 1, pl.ds(first_col + h * HD, HD)]
                heads_v[j, here, part] = (v * cosine + swap_halves(v) * sine).astype(BF16)

    moves.start(heads_v, heads)
    attend(block, heads_v.at[0], heads_v.at[1], heads_v.at[2], out_v, low_v, lt_v, log_v)
    moves.start(out_v, attended)
    moves.start(lt_v, low_t)
    moves.start(log_v, log_total)
    moves.wait(own_out)
    for copy in out_copies:
        copy.wait_recv()
    moves.start(wo_v, wo)
    step = min(512, width)

    def make(q, chip, c, first):
        here = pl.ds(pl.multiple_of(chip * 4 * rows, 4 * rows), 4 * rows)

        @pl.loop(0, width // 2 // step)
        def _(j):
            at = pl.ds(pl.multiple_of(first + j * step, step), step)
            part = dot(low_v[here, :], wo_v[:, :, at].reshape(cols, step), NN).astype(BF16)
            value[q, pl.ds(4 * chip, 4), :, at] = part.reshape(4, rows, step)

    live = scatter_pairs(
        place, Wires(send, recv), value, rc, rd, rx, ry, qbuf, zbuf, make, branch,
        Work([lambda: None, lambda: stream.relay(0, views[0], fulls[0])]),
    )

    def last(r):
        total = branch[r]
        inv = lax.rsqrt(jnp.mean(total * total, axis=-1, keepdims=True) + EPSILON)
        h = x[r].astype(F32) + total * inv * all_gains[2:3, :]
        hidden[r] = h
        hidden_low[r] = h.astype(BF16)

    by_rows(0, rows, last)
    for copy in list(live.values()) + list(gathered.values()) + stat_copies + sent:
        copy.wait_send()
    for h in range(m - 1):
        for j in range(4):
            for way in (0, 1):
                when(sends(way, h), lambda: hop(way, h, j).wait_send())
    moves.finish()
    stream.finish(0, views[0], fulls[0])
    for copy in (
        stream.near_copy(1, views[1], fulls[1]),
        stream.far_copy(1, views[1], fulls[1]),
        stream.own_copy(1, views[1], fulls[1]),
    ):
        copy.wait()
    for copy in out_copies:
        copy.wait_send()


def opening(x, wq, wk, wv, gains, wo, gate_w, up_w, down_w, n, m, ident):
    rows, width = x.shape
    part, cols = wq.shape[0], width // n
    length, share = n * rows, gate_w.shape[1] // 2
    dma = pltpu.SemaphoreType.DMA
    heads = cols // HD
    outs = [
        shape((3, n, m, part, cols), BF16),
        shape((gains.shape[0], width), F32),
        shape((2, length, HD), F32),
        shape((2, length, cols), F32),
        shape((3, length, cols), BF16),
        shape((length, cols), F32),
        shape((cols, length), BF16),
        shape((width, length), BF16),
        shape((heads, length, 1), F32),
        shape((8, length), F32),
        shape((rows, width), F32),
        shape((rows, width), F32),
        shape((rows, width), BF16),
        shape((m, gate_w.shape[0], share), BF16),
        shape((m, gate_w.shape[0], share), BF16),
        shape((m,) + wo.shape, BF16),
    ]
    return pl.pallas_call(
        functools.partial(opening_kernel, n, m),
        in_specs=vmem_specs(5) + any_specs(4),
        out_specs=any_specs(1) + vmem_specs(2) + any_specs(7) + vmem_specs(3) + any_specs(3),
        out_shape=outs,
        scratch_shapes=[
            pltpu.VMEM((m, n) + gains.shape, F32),
            pltpu.VMEM((1, n, rows, width), BF16),
            pltpu.VMEM((width, length), BF16),
            pltpu.VMEM((cols, length), BF16),
            pltpu.VMEM((3, n, m, part, cols), BF16),
            pltpu.VMEM((m,) + wo.shape, BF16),
            pltpu.VMEM((2, length, cols), F32),
            pltpu.VMEM((3, length, cols), BF16),
            pltpu.VMEM((length, cols), F32),
            pltpu.VMEM((length, cols), BF16),
            pltpu.VMEM((heads, length, 1), F32),
            pltpu.VMEM((2, 8, length), F32),
            pltpu.VMEM((n - 1, 8, length), F32),
            pltpu.VMEM((1, n, rows, width), BF16),
        ]
        + scatter_scratch(1, rows, width)
        + [dma((n - 1,)), dma((n - 1,)), dma((2, 4, 2)), dma((2, m))]
        + [dma((gather_wires(1),))] * 2
        + [dma((3, n))] * 2
        + [dma((2, m, 4))] * 2
        + [dma((n,))] * 2
        + [dma((16,))],
        compiler_params=kernel_params(ident),
        cost_estimate=pl.CostEstimate(flops=10**10, bytes_accessed=200 * 2**20, transcendentals=0),
        name=f"opening_{ident}",
    )(x, wq, wk, wv, gains, wo, gate_w, up_w, down_w)


class Settle:
    def __init__(self, place, sems, term, own, near, total, far):
        self.place, self.sems, self.term, self.own = place, sems, term, own
        self.near, self.total, self.far = near, total, far
        f = place.f
        self.f = f
        self.odd, self.half = f % 2, f // 2

    def remote(self, step, src, dst, plane):
        return pltpu.make_async_remote_copy(
            src, dst, self.sems.at[step, 0], self.sems.at[step, 1], device_id=(self.place.s, plane), device_id_type=MESH
        )

    def given(self, i):
        return 1 - self.odd + 2 * i

    def kept(self, i):
        return self.odd + 2 * i

    def near_copy(self, step):
        i = 1 - self.half if step == 0 else self.half
        return self.remote(step, self.term.at[self.given(i)], self.near.at[i], flip(self.f, 1))

    def far_copy(self):
        return self.remote(2, self.total.at[0], self.far, opposite(self.f))

    def load(self, i):
        return pltpu.make_async_copy(self.term.at[self.kept(i)], self.own.at[i], self.sems.at[3, i])

    def start(self, both=False):
        self.near_copy(0).start()
        self.both = both
        if both:
            self.near_copy(1).start()
        for i in (0, 1):
            self.load(i).start()

    def mine(self, i):
        return self.term.at[self.kept(i)] if self.own is None else self.own.at[i]

    def chunks(self, body):
        size = 128

        @pl.loop(0, self.far.shape[0] // size)
        def _(i):
            body(i, pl.ds(pl.multiple_of(i * size, size), size))

    def middle(self):
        if self.own is not None:
            for i in (0, 1):
                self.load(i).wait()
        self.near_copy(0).wait_recv()
        other = 1 - self.half
        mine = self.mine(other)

        def body(i, r):
            self.total[0, r] = add(mine[r], self.near[other, r])

        self.chunks(body)
        self.far_copy().start()
        if not self.both:
            self.near_copy(1).start()

    def finish(self, store):
        half = self.half
        self.near_copy(1).wait_recv()
        mine = self.mine(half)
        self.chunks(lambda i, r: store(half, i, mine[r].astype(F32) + self.near[half, r].astype(F32)))
        self.far_copy().wait_recv()
        self.chunks(lambda i, r: store(1 - half, i, self.far[r].astype(F32)))
        for step in (0, 1):
            self.near_copy(step).wait_send()
        self.far_copy().wait_send()


def settle_scratch(share, depth, own=True):
    block = lambda *lead: pltpu.VMEM(lead + (share, depth), BF16)
    return ([block(2)] if own else []) + [block(2), block(1), block(), pltpu.SemaphoreType.DMA((4, 2))]


def term_block(term, left, right, block):
    deep, long = term.shape[2], left.shape[1]
    step = min(256, deep)

    @pl.loop(0, deep // step)
    def _(j):
        at = pl.ds(pl.multiple_of(block * deep + j * step, step), step)
        to = pl.ds(pl.multiple_of(j * step, step), step)
        term[block, :, to] = dot(left[...], right[:, :, :, at].reshape(long, step), NN).astype(BF16)


class Work:
    def __init__(self, pieces):
        self.pieces = list(pieces)

    def __call__(self):
        if self.pieces:
            self.pieces.pop(0)()

    def rest(self):
        while self.pieces:
            self()


def term_work(term, left, right, prepare, out, moves):
    def piece(block):
        def run():
            if block == 0:
                prepare()
            term_block(term, left, right, block)
            moves.start(term.at[block], out.at[block])

        return run

    return [piece(block) for block in range(term.shape[0])]


def turn(v, cosine, sine):
    return v * cosine + swap_halves(v) * sine


def attend_back(block, q_v, k_v, v_v, out_v, log_v, g_v, dq, dk, dv):
    length = q_v.shape[0]
    scale = HD ** (-0.5)
    dk[...] = jnp.zeros_like(dk)
    dv[...] = jnp.zeros_like(dv)

    @pl.loop(0, q_v.shape[1] // HD)
    def _(h):
        cols = pl.ds(pl.multiple_of(h * HD, HD), HD)
        for half in range(2):
            wide = pl.ds(0, (half + 1) * length // 2)

            @pl.loop(half * length // 2 // block, (half + 1) * length // 2 // block)
            def _(i):
                rows = pl.ds(pl.multiple_of(i * block, block), block)
                q, g = q_v[rows, cols], g_v[rows, cols]
                s = dot(q, k_v[wide, cols], NT) * scale
                column = lax.broadcasted_iota(jnp.int32, s.shape, 1)
                row = lax.broadcasted_iota(jnp.int32, s.shape, 0) + i * block
                s = jnp.where(column <= row, s, -jnp.inf)
                weights = jnp.exp(s - log_v[h, rows, :])
                correction = jnp.sum(g.astype(F32) * out_v[rows, cols], axis=-1, keepdims=True)
                gw = dot(g, v_v[wide, cols], NT)
                gs = (weights * (gw - correction)).astype(BF16)
                dq[rows, cols] = dot(gs, k_v[wide, cols], NN) * scale
                dk[wide, cols] += dot(gs, q, TN) * scale
                dv[wide, cols] += dot(weights.astype(BF16), g, TN)


def attention_back_kernel(
    g, gains, tables, inverse, wo, raw, heads, attended, low_t, log_total, xs_t, gate_term, up_t, hs,
    d3, term, gain_term, gate_grad, up_grad,
    bs, wo_v, raw_v, heads_v, out_v, low_v, log_v, ga_v, dq, dk, dv, d_v, xs_v, term_v, small, held,
    ut_v, hs_v, up_term, gown, gnear, gtotal, gfar, gsem, unear, utotal, ufar, usem,
    send, recv, ssend, srecv, sems,
):
    place = Place(1)
    n, m = bs.shape[1], wo.shape[0]
    rows, width = g.shape
    length, cols = raw.shape[1], raw.shape[2]
    share = gate_term.shape[1]
    first_col = pl.multiple_of(place.s * cols, cols)
    moves = Moves(sems)
    second = [moves.start(wo, wo_v)]
    fourth = [
        moves.start(heads, heads_v),
        moves.start(attended, out_v),
        moves.start(log_total, log_v),
        moves.start(low_t, low_v),
        moves.start(raw, raw_v),
        moves.start(xs_t, xs_v),
    ]
    bs[0, place.s] = g[...]
    full_barrier(place, n, [opposite(place.f), flip(place.f, 1)])
    gate = Settle(place, gsem, gate_term, gown, gnear, gtotal, gfar)
    up = Settle(place, usem, up_term, None, unear, utotal, ufar)
    gate.start()
    late = [moves.start(up_t, ut_v)] + [moves.start(hs.at[q], hs_v.at[q]) for q in range(hs.shape[0])]

    up.both = False

    def up_block(i):
        b = (up.given(1 - up.half), up.given(up.half), up.kept(1 - up.half), up.kept(up.half))[i]
        if i == 0:
            moves.wait(late)
        term_block(up_term, ut_v, hs_v, b)
        if i == 0:
            up.near_copy(0).start()

    block = min(256, length)

    def ready(q, chip):
        here = pl.ds(pl.multiple_of(chip * 2 * rows, 2 * rows), 2 * rows)
        a = bs[0, pl.ds(2 * chip, 2)].reshape(2 * rows, width)
        ga_v[here, :] = dot(a, wo_v[...].reshape(cols, width), NT).astype(BF16)

    moves.wait(second)
    live = gather_pairs(place, Wires(send, recv), g, bs, ready, Work([lambda: up_block(0), lambda: up_block(2), gate.middle]))
    up_block(1)
    up.middle()
    moves.wait(fourth)
    up_block(3)
    attend_back(block, heads_v.at[0], heads_v.at[1], heads_v.at[2], out_v, log_v, ga_v, dq, dk, dv)
    @pl.loop(0, length // block)
    def _(i):
        here = pl.ds(pl.multiple_of(i * block, block), block)
        inv = to_columns(inverse[:, here])
        cosine, sine = tables[0, here, :], -tables[1, here, :]
        sums = []
        for j, d in enumerate((dq, dk)):
            total = jnp.zeros((block, 1), F32)
            for h in range(cols // HD):
                part = pl.ds(h * HD, HD)
                normal = raw_v[j, here, part] * inv[:, j : j + 1]
                v = turn(d[here, part].astype(BF16).astype(F32), cosine, sine)
                raw_v[j, here, part] = normal
                gained = v * gains[j : j + 1, pl.ds(first_col + h * HD, HD)]
                total = total + jnp.sum(gained * normal, axis=1, keepdims=True)
                term_sum = jnp.sum(v * normal, axis=0, keepdims=True)
                d[here, part] = gained

                @pl.when(i == 0)
                def _():
                    gain_term[j, :, part] = term_sum

                @pl.when(i > 0)
                def _():
                    gain_term[j, :, part] += term_sum

            sums.append(total)
        small[0, :, here] = to_rows(sums[0], sums[1])
        d_v[2, here, :] = dv[here, :].astype(BF16)

    total, stat_copies = exchange(place, n, small.at[0], held, ssend, srecv)
    small[1] = total * (1.0 / width)

    @pl.loop(0, length // block)
    def _(i):
        here = pl.ds(pl.multiple_of(i * block, block), block)
        inv = to_columns(inverse[:, here])
        mean = to_columns(small[1, :, here])
        for j, d in enumerate((dq, dk)):
            d_v[j, here, :] = (
                inv[:, j : j + 1] * (d[here, :] - raw_v[j, here, :] * mean[:, j : j + 1])
            ).astype(BF16)

    moves.start(d_v, d3)

    @pl.loop(0, n)
    def _(i):
        at = pl.ds(pl.multiple_of(i * cols, cols), cols)
        part = dot(low_v[...], bs[0, :, :, at].reshape(length, cols), NN)
        term_v[3, i] = part.astype(BF16).reshape(m, cols // m, cols)
        for j in range(3):
            part = dot(xs_v[at, :], d_v[j], NN)
            term_v[j, i] = part.astype(BF16).reshape(m, cols // m, cols)

    moves.start(term_v, term)

    def store(ref):
        def put(u, i, value):
            size = value.shape[0]
            ref[:, pl.ds(pl.multiple_of(u * share + i * size, size), size)] = value.T

        return put

    gate.finish(store(gate_grad))
    up.finish(store(up_grad))
    for copy in list(live.values()) + stat_copies:
        copy.wait_send()
    moves.finish()


def attention_back(g, gains, tables, inverse, wo, raw, heads, attended, low_t, log_total, xs_t, gate_term, up_t, hs, n, ident):
    rows, width = g.shape
    m = wo.shape[0]
    length, cols = raw.shape[1], raw.shape[2]
    share, deep = gate_term.shape[1], width // m
    dma = pltpu.SemaphoreType.DMA
    vmem = pltpu.VMEM
    outs = [
        shape((3, length, cols), BF16),
        shape((4, n, m, cols // m, cols), BF16),
        shape((2, 1, cols), F32),
        shape((deep, 2 * share), F32),
        shape((deep, 2 * share), F32),
    ]
    return pl.pallas_call(
        attention_back_kernel,
        in_specs=vmem_specs(4) + any_specs(10),
        out_specs=any_specs(2) + vmem_specs(3),
        out_shape=outs,
        scratch_shapes=[
            vmem((1, n, rows, width), BF16),
            vmem(wo.shape, BF16),
            vmem(raw.shape, F32),
            vmem(heads.shape, BF16),
            vmem(attended.shape, F32),
            vmem(low_t.shape, BF16),
            vmem(log_total.shape, F32),
            vmem((length, cols), BF16),
            vmem((length, cols), F32),
            vmem((length, cols), F32),
            vmem((length, cols), F32),
            vmem((3, length, cols), BF16),
            vmem(xs_t.shape, BF16),
            vmem((4, n, m, cols // m, cols), BF16),
            vmem((2, 8, length), F32),
            vmem((n - 1, 8, length), F32),
        ]
        + [vmem(up_t.shape, BF16), vmem(hs.shape, BF16), vmem(gate_term.shape, BF16)]
        + settle_scratch(share, deep)
        + settle_scratch(share, deep, False)
        + [
            dma((gather_wires(1),)),
            dma((gather_wires(1),)),
            dma((n - 1,)),
            dma((n - 1,)),
            dma((20,)),
        ],
        compiler_params=kernel_params(ident, 63),
        cost_estimate=pl.CostEstimate(flops=10**10, bytes_accessed=200 * 2**20, transcendentals=0),
        name=f"attention_back_{ident}",
    )(g, gains, tables, inverse, wo, raw, heads, attended, low_t, log_total, xs_t, gate_term, up_t, hs)


def attention_forward_kernel(block, q_ref, k_ref, v_ref, out_ref, low_ref, log_ref):
    length = q_ref.shape[0]
    scale = HD ** (-0.5)
    for i in range(length // block):
        rows = pl.ds(i * block, block)
        width = (i + 1) * block
        s = dot(q_ref[rows, :], k_ref[pl.ds(0, width), :], NT) * scale
        column = lax.broadcasted_iota(jnp.int32, (block, width), 1)
        row = lax.broadcasted_iota(jnp.int32, (block, width), 0) + i * block
        s = jnp.where(column <= row, s, -jnp.inf)
        top = jnp.max(s, axis=-1, keepdims=True)
        p = jnp.exp(s - top)
        total = jnp.sum(p, axis=-1, keepdims=True)
        weights = (p * (1.0 / total)).astype(BF16)
        out = dot(weights, v_ref[pl.ds(0, width), :], NN)
        out_ref[rows, :] = out
        low_ref[rows, :] = out.astype(BF16)
        log_ref[0, rows, :] = top + jnp.log(total)


def attention_forward(q, k, v):
    length, width = q.shape
    heads = width // HD
    block = min(256, length)
    column = pl.BlockSpec((length, HD), lambda h: (0, h))
    return pl.pallas_call(
        functools.partial(attention_forward_kernel, block),
        grid=(heads,),
        in_specs=[column] * 3,
        out_specs=[column, column, pl.BlockSpec((1, length, 1), lambda h: (h, 0, 0))],
        out_shape=[
            jax.ShapeDtypeStruct((length, width), F32),
            jax.ShapeDtypeStruct((length, width), BF16),
            jax.ShapeDtypeStruct((heads, length, 1), F32),
        ],
        cost_estimate=pl.CostEstimate(
            flops=2 * heads * length * length * HD, bytes_accessed=10 * length * width, transcendentals=0
        ),
    )(q, k, v)


def attention_backward_kernel(block, q_ref, k_ref, v_ref, out_ref, log_ref, g_ref, dq_ref, dk_ref, dv_ref, dk, dv):
    length = q_ref.shape[0]
    scale = HD ** (-0.5)
    dk[...] = jnp.zeros_like(dk)
    dv[...] = jnp.zeros_like(dv)
    for i in range(length // block):
        rows = pl.ds(i * block, block)
        width = (i + 1) * block
        wide = pl.ds(0, width)
        q = q_ref[rows, :]
        g = g_ref[rows, :]
        s = dot(q, k_ref[wide, :], NT) * scale
        column = lax.broadcasted_iota(jnp.int32, (block, width), 1)
        row = lax.broadcasted_iota(jnp.int32, (block, width), 0) + i * block
        s = jnp.where(column <= row, s, -jnp.inf)
        weights = jnp.exp(s - log_ref[0, rows, :])
        correction = jnp.sum(g.astype(F32) * out_ref[rows, :], axis=-1, keepdims=True)
        gw = dot(g, v_ref[wide, :], NT)
        gs = (weights * (gw - correction)).astype(BF16)
        dq_ref[rows, :] = (dot(gs, k_ref[wide, :], NN) * scale).astype(BF16)
        dk[wide, :] += dot(gs, q, TN)
        dv[wide, :] += dot(weights.astype(BF16), g, TN)
    dk_ref[...] = (dk[...] * scale).astype(BF16)
    dv_ref[...] = dv[...].astype(BF16)


def attention_backward(q, k, v, out, log_total, g):
    length, width = q.shape
    heads = width // HD
    block = min(256, length)
    column = pl.BlockSpec((length, HD), lambda h: (0, h))
    return pl.pallas_call(
        functools.partial(attention_backward_kernel, block),
        grid=(heads,),
        in_specs=[column] * 4 + [pl.BlockSpec((1, length, 1), lambda h: (h, 0, 0)), column],
        out_specs=[column] * 3,
        out_shape=[jax.ShapeDtypeStruct((length, width), BF16)] * 3,
        scratch_shapes=[pltpu.VMEM((length, HD), F32)] * 2,
        cost_estimate=pl.CostEstimate(
            flops=5 * heads * length * length * HD, bytes_accessed=16 * length * width, transcendentals=0
        ),
    )(q, k, v, out, log_total, g)


def on_device(n, m, pair, *args):
    (
        tokens,
        query_weight,
        key_weight,
        value_weight,
        out_weight,
        query_gain,
        key_gain,
        attention_gain,
        gate_weight,
        up_weight,
        down_weight,
        feedforward_gain,
        cotangent,
    ) = args
    rows, width = tokens.shape[1], tokens.shape[2]
    length = rows * n
    part = query_weight.shape[0]
    cols = width // n
    depth, units = gate_weight.shape
    share = units // pair
    x = tokens.reshape(rows, width)
    groups = [[g * pair + u for u in range(pair)] for g in range(m // pair)]

    native = n == 8 and m == 4

    def gather_plane(v, ident):
        if native:
            return plane_gather(v, n, 1, ident)
        return lax.all_gather(v, "seq", axis=0, tiled=True)

    def scatter_plane(v, ident):
        if native:
            return plane_scatter(v, n, 1, ident)
        return lax.psum_scatter(v.astype(BF16), "seq", scatter_dimension=0, tiled=True).astype(F32)

    def gather_pair(v, ident):
        if native:
            return plane_gather(v, n, pair, ident)
        if pair > 1:
            v = lax.all_gather(v, "fsdp", axis=0, axis_index_groups=groups)
        v = lax.all_gather(v.reshape(pair, rows, width), "seq", axis=1, tiled=True)
        return v.reshape(pair * length, width)

    def scatter_pair(v, ident):
        if native:
            return plane_scatter(v, n, pair, ident)
        v = lax.psum_scatter(v.astype(BF16).reshape(pair, length, width), "seq", scatter_dimension=1, tiled=True)
        if pair > 1:
            v = lax.psum_scatter(v, "fsdp", scatter_dimension=0, axis_index_groups=groups)
        return v.reshape(rows, width).astype(F32)

    def total_plane(v, ident):
        return plane_sum(v, n, ident) if native else lax.psum(v, "seq")

    def spread(halves):
        return lax.all_to_all(jnp.tile(halves, (m // pair, 1, 1)), "fsdp", 0, 0, tiled=False)

    def settle(blocks):
        back = lax.all_to_all(blocks.astype(BF16), "fsdp", 0, 0, tiled=False)
        if native:
            return jnp.sum(back.reshape((pair, m // pair) + back.shape[1:]).astype(F32), axis=1)
        return jnp.sum(back.reshape((m // pair, pair) + back.shape[1:]).astype(F32), axis=0)

    gains = jnp.stack([query_gain, key_gain, attention_gain, feedforward_gain]).astype(F32)
    grad_out = cotangent.reshape(rows, width)
    if native:
        (
            qkv, gains, tables, raw, heads, attended, low_t, xs_t, log_total, inverse, branch, hidden, hidden_low,
            gate_cols, up_cols, out_rows,
        ) = opening(
            x, query_weight, key_weight, value_weight, jnp.pad(gains, ((0, 4), (0, 128 - part))),
            out_weight, gate_weight, up_weight, down_weight, n, m, 1
        )
        gate_cols = gate_cols.reshape(width, share)
        layer_out, feed_gain_term, hs, up_cols, grad_gate, grad_up, gate_t, up_t, down_term = ffn_feed(
            hidden_low, hidden, gains, grad_out, gate_cols, up_cols, down_weight, n, m, pair, 5
        )
        grad_hidden, branch_low, branch_gain_term, down_grad, gate_term = ffn_back(
            grad_gate, grad_up, gate_cols, up_cols, gate_t, hs, down_term, branch, gains, grad_out, n, m, pair, 8
        )
        d3, term, gain_own, gate_grad, up_grad = attention_back(
            branch_low, gains, tables, inverse, out_rows, raw, heads, attended, low_t, log_total,
            xs_t, gate_term, up_t, hs, n, 2
        )
        tokens_grad, term, gain_grads = leave(
            d3, term, gain_own, branch_gain_term, feed_gain_term, grad_hidden, qkv, n, m, 4
        )
        layer_out, tokens_grad, *term, gate_grad, up_grad, down_grad = place_outputs(
            [layer_out, tokens_grad, term, gate_grad, up_grad, down_grad]
        )
        out_grad = term[3]
    else:
        cosine, sine = angles_of(length)
        seq = lax.axis_index("seq")
        stacked = jnp.stack([query_weight, key_weight, value_weight]).reshape(3, part, n, cols)
        mine = lax.all_to_all(stacked.transpose(2, 0, 1, 3), "seq", 0, 0)
        qkv = lax.all_gather(mine, "fsdp", axis=1).transpose(2, 0, 1, 3, 4).reshape(3, width, cols)
        full_gain = lax.all_gather(gains, ("seq", "fsdp"), axis=1).reshape(4, width)
        xs = gather_plane(x, 1)
        out_rows = lax.all_gather(out_weight, "fsdp", axis=0, tiled=True)
        own_gain = lax.dynamic_slice_in_dim(full_gain[:2], seq * cols, cols, 1)
        q_gain, k_gain, branch_gain, feed_gain = own_gain[0], own_gain[1], full_gain[2], full_gain[3]
        q_raw, k_raw, v = dot(xs, qkv[0], NN), dot(xs, qkv[1], NN), dot(xs, qkv[2], NN).astype(BF16)
        squares = jnp.stack([jnp.sum(q_raw * q_raw, axis=1), jnp.sum(k_raw * k_raw, axis=1)])
        inverse = lax.rsqrt(lax.psum(squares, "seq") / width + EPSILON)
        q_inv, k_inv = inverse[0][:, None], inverse[1][:, None]
        q = rotate(q_raw * q_inv * q_gain, cosine, sine, 1.0).astype(BF16)
        k = rotate(k_raw * k_inv * k_gain, cosine, sine, 1.0).astype(BF16)
        attended, attended_low, log_total = attention_forward(q, k, v)
        branch = scatter_plane(dot(attended_low, out_rows, NN), 3)
        branch_inv = lax.rsqrt(jnp.mean(branch * branch, axis=1, keepdims=True) + EPSILON)
        hidden = x.astype(F32) + branch * branch_inv * branch_gain
        hidden_low = hidden.astype(BF16)
        gate_cols = spread(gate_weight.reshape(depth, pair, share).transpose(1, 0, 2)).reshape(width, share)
        up_cols = spread(up_weight.reshape(depth, pair, share).transpose(1, 0, 2)).reshape(width, share)
        down_rows = spread(down_weight.reshape(pair, share, depth)).transpose(1, 0, 2).reshape(share, width)
        grad_out = grad_out.astype(F32)
        hs = gather_pair(hidden_low, 5)
        gate = dot(hs, gate_cols, NN)
        up = dot(hs, up_cols, NN)
        sig = jax.nn.sigmoid(gate)
        inner = (gate * sig * up).astype(BF16)
        feed = scatter_pair(dot(inner, down_rows, NN), 7)
        feed_inv = lax.rsqrt(jnp.mean(feed * feed, axis=1, keepdims=True) + EPSILON)
        layer_out = (hidden + feed * feed_inv * feed_gain).astype(BF16)
        grad_feed, term = rms_back(feed, feed_gain, grad_out)
        feed_gain_term = jnp.sum(term, axis=0)
        gs = gather_pair(grad_feed.astype(BF16), 6)
        grad_inner = dot(gs, down_rows, NT)
        grad_gate = (grad_inner * up * sig * (1.0 + gate * (1.0 - sig))).astype(BF16)
        grad_up = (grad_inner * gate * sig).astype(BF16)
        grad_hidden = grad_out + scatter_pair(dot(grad_gate, gate_cols, NT) + dot(grad_up, up_cols, NT), 8)
        grad_branch, term = rms_back(branch, branch_gain, grad_hidden)
        branch_low = grad_branch.astype(BF16)
        branch_gain_term = jnp.sum(term, axis=0)
        inner_t, gate_t, up_t = inner.T, grad_gate.T, grad_up.T

        def cut(v):
            return v.reshape(share, m, depth).transpose(1, 0, 2)

        down_grad = settle(cut(dot(inner_t, gs, NN))).reshape(units, depth)
        gate_grad = settle(cut(dot(gate_t, hs, NN))).transpose(2, 0, 1).reshape(depth, units)
        up_grad = settle(cut(dot(up_t, hs, NN))).transpose(2, 0, 1).reshape(depth, units)
        bs = gather_plane(branch_low, 2)
        out_grad = lax.psum_scatter(
            dot(attended_low, bs, TN).astype(BF16), "fsdp", scatter_dimension=0, tiled=True
        ).astype(F32)
        grad_attended = dot(bs, out_rows, NT).astype(BF16)
        dq, dk, dv = attention_backward(q, k, v, attended, log_total, grad_attended)
        dq = rotate(dq.astype(F32), cosine, sine, -1.0)
        dk = rotate(dk.astype(F32), cosine, sine, -1.0)
        q_normal, k_normal = q_raw * q_inv, k_raw * k_inv
        q_gain_term = jnp.sum(dq * q_normal, axis=0)
        k_gain_term = jnp.sum(dk * k_normal, axis=0)
        dq, dk = dq * q_gain, dk * k_gain
        means = total_plane(jnp.stack([jnp.sum(dq * q_normal, axis=1), jnp.sum(dk * k_normal, axis=1)]), 10) / width
        dq = (q_inv * (dq - q_normal * means[0][:, None])).astype(BF16)
        dk = (k_inv * (dk - k_normal * means[1][:, None])).astype(BF16)
        value = dot(dq, qkv[0], NT) + dot(dk, qkv[1], NT) + dot(dv, qkv[2], NT)
        term = jnp.stack([dot(xs, d, TN).astype(BF16) for d in (dq, dk, dv)]).reshape(3, n, m, part, cols)
        gain_own = jnp.stack([q_gain_term, k_gain_term])
        gain_own = lax.dynamic_update_slice(jnp.zeros((2, width), F32), gain_own, (0, seq * cols))
        gain_terms = jnp.concatenate([gain_own, jnp.stack([branch_gain_term, feed_gain_term])]).reshape(4, n, m, part)
        tokens_grad = grad_hidden + scatter_plane(value, 4)
        term = lax.psum_scatter(term, "fsdp", scatter_dimension=2)
        term = lax.all_to_all(term, "seq", 1, 1).astype(F32).transpose(0, 2, 1, 3)
        gain_grads = lax.psum_scatter(
            gain_terms.reshape(4, width), ("seq", "fsdp"), scatter_dimension=1, tiled=True
        )
        term = term.reshape(3, part, width)

    return (
        layer_out.reshape(tokens.shape),
        tokens_grad.reshape(tokens.shape),
        term[0],
        term[1],
        term[2],
        out_grad,
        gain_grads[0],
        gain_grads[1],
        gain_grads[2],
        gate_grad,
        up_grad,
        down_grad,
        gain_grads[3],
    )


def solution(mesh):
    n, m = mesh.shape["seq"], mesh.shape["fsdp"]
    tall, flat, act = P(("seq", "fsdp"), None), P(("seq", "fsdp")), P("fsdp", "seq", None)
    wide, deep = P("fsdp", "seq"), P("seq", "fsdp")
    return jax.shard_map(
        functools.partial(on_device, n, m, 2),
        mesh=mesh,
        in_specs=(act, tall, tall, tall, tall, flat, flat, flat, wide, wide, deep, flat, act),
        out_specs=(act, act, tall, tall, tall, tall, flat, flat, flat, wide, wide, deep, flat),
        check_vma=False,
    )
```

```python
import functools
import math

import jax
import jax.numpy as jnp
from jax import lax
from jax.experimental import pallas as pl
from jax.experimental.pallas import tpu as pltpu
from jax.sharding import PartitionSpec as P

EPSILON = 1e-06
THETA = 500000.0
HD = 128
F32 = jnp.float32
BF16 = jnp.bfloat16


def dot(a, b, dims):
    return lax.dot_general(a, b, (dims, ((), ())), preferred_element_type=F32)


NN = ((1,), (0,))
NT = ((1,), (1,))
TN = ((0,), (0,))


def angles_of(length):
    half = HD // 2
    frequency = jnp.exp(jnp.arange(half, dtype=F32) * (-2.0 * math.log(THETA) / HD))
    angle = jnp.arange(length, dtype=F32)[:, None] * frequency[None, :]
    return jnp.cos(angle), jnp.sin(angle)


def rotate(value, cosine, sine, sign):
    length, width = value.shape
    value = value.reshape(length, width // HD, 2, HD // 2)
    first, second = value[:, :, 0], value[:, :, 1]
    c, s = cosine[:, None, :], sign * sine[:, None, :]
    return jnp.stack([first * c - second * s, second * c + first * s], axis=2).reshape(length, width)


MESH = pl.DeviceIdType.MESH


def flip(index, bit):
    return index + bit - 2 * bit * ((index // bit) % 2)


class Place:
    def __init__(self, pair):
        self.s, self.f = lax.axis_index("seq"), lax.axis_index("fsdp")
        self.pair = pair
        s, f = self.s, self.f
        self.sx, self.sy = flip(s, 2), flip(s, 4)
        self.sd, self.sc = flip(self.sx, 4), flip(s, 1)
        self.q = f // 2 if pair > 1 else 0
        self.x, self.y, self.core = (self.sx, f), (self.sy, f), (self.sc, f)
        self.z = (s, opposite(f)) if pair > 1 else None
        self.peers = [self.x, self.y, self.core] + ([self.z] if pair > 1 else [])

    def barrier(self):
        sem = pltpu.get_barrier_semaphore()
        for peer in self.peers:
            pl.semaphore_signal(sem, inc=1, device_id=peer, device_id_type=MESH)
        pl.semaphore_wait(sem, len(self.peers))


class Wires:
    def __init__(self, send, recv):
        self.send, self.recv, self.count, self.open = send, recv, 0, {}

    def new(self, key):
        self.open[key] = self.count
        self.count += 1

    def go(self, key, src, dst, device):
        i = self.open[key]
        copy = pltpu.make_async_remote_copy(
            src, dst, self.send.at[i], self.recv.at[i], device_id=device, device_id_type=MESH
        )
        copy.start()
        return copy


def gather_steps(place, wires, own, out, ready):
    pair, rows = place.pair, own.shape[0]
    half = rows // 2
    top, low = pl.ds(0, half), pl.ds(half, half)
    p = place
    qs = [p.q] + ([1 - p.q] if pair > 1 else [])
    kinds = ["xa", "xb", "ya", "yb", "xd", "yd", "c0", "cxa", "cxb", "cya", "cyb", "cda", "cdb"]
    for t in range(pair):
        for kind in kinds:
            wires.new((t, kind))
    if pair > 1:
        wires.new("z")
    live = {}

    def go(key, src, dst, device):
        live[key] = wires.go(key, src, dst, device)

    def begin(t, src):
        q = qs[t]
        go((t, "xa"), src.at[top], out.at[q, p.s, top], p.x)
        go((t, "yb"), src.at[low], out.at[q, p.s, low], p.y)
        go((t, "xb"), src.at[low], out.at[q, p.s, low], p.x)
        go((t, "ya"), src.at[top], out.at[q, p.s, top], p.y)
        go((t, "c0"), src, out.at[q, p.s], p.core)

    def arrived(key):
        live[key].wait_recv()

    if pair > 1:
        go("z", own, out.at[qs[0], p.s], p.z)
    begin(0, own)
    ready(qs[0], p.s, None)

    def first(t):
        q = qs[t]
        arrived((t, "xa"))
        go((t, "xd"), out.at[q, p.sx, top], out.at[q, p.sx, top], p.y)
        go((t, "cxa"), out.at[q, p.sx, top], out.at[q, p.sx, top], p.core)
        arrived((t, "yb"))
        go((t, "yd"), out.at[q, p.sy, low], out.at[q, p.sy, low], p.x)
        go((t, "cyb"), out.at[q, p.sy, low], out.at[q, p.sy, low], p.core)
        arrived((t, "c0"))
        ready(q, p.sc, None)

    def second(t):
        q = qs[t]
        arrived((t, "xb"))
        go((t, "cxb"), out.at[q, p.sx, low], out.at[q, p.sx, low], p.core)
        ready(q, p.sx, None)
        arrived((t, "ya"))
        go((t, "cya"), out.at[q, p.sy, top], out.at[q, p.sy, top], p.core)
        ready(q, p.sy, None)
        arrived((t, "xd"))
        go((t, "cda"), out.at[q, p.sd, top], out.at[q, p.sd, top], p.core)
        arrived((t, "yd"))
        go((t, "cdb"), out.at[q, p.sd, low], out.at[q, p.sd, low], p.core)

    def third(t):
        q = qs[t]
        arrived((t, "cxa"))
        arrived((t, "cxb"))
        ready(q, flip(p.sx, 1), None)
        arrived((t, "cya"))
        arrived((t, "cyb"))
        ready(q, flip(p.sy, 1), None)
        ready(q, p.sd, None)
        arrived((t, "cda"))
        arrived((t, "cdb"))
        ready(q, flip(p.sd, 1), None)

    first(0)
    if pair > 1:
        arrived("z")
        begin(1, out.at[qs[1], p.s])
        ready(qs[1], p.s, None)
    second(0)
    if pair > 1:
        first(1)
    third(0)
    if pair > 1:
        second(1)
        third(1)
    for copy in live.values():
        copy.wait_send()


def gather_wires(pair):
    return 14 * pair + (2 if pair > 1 else 0)


def gather_kernel(pair, own, out, send, recv, local):
    place = Place(pair)
    keep = pltpu.make_async_copy(own, out.at[place.q, place.s], local)
    keep.start()
    place.barrier()
    gather_steps(place, Wires(send, recv), own, out, lambda q, slot, half: None)
    keep.wait()


def plane_gather(v, n, pair, ident):
    rows, width = v.shape
    return pl.pallas_call(
        functools.partial(gather_kernel, pair),
        in_specs=[pl.BlockSpec(memory_space=pltpu.VMEM)],
        out_specs=pl.BlockSpec(memory_space=pl.ANY),
        out_shape=jax.ShapeDtypeStruct((pair, n, rows, width), v.dtype),
        scratch_shapes=[pltpu.SemaphoreType.DMA((gather_wires(pair),))] * 2 + [pltpu.SemaphoreType.DMA],
        compiler_params=pltpu.CompilerParams(collective_id=ident, has_side_effects=True),
        cost_estimate=pl.CostEstimate(flops=0, bytes_accessed=pair * n * rows * width * 20, transcendentals=0),
        name=f"gather_{ident}",
    )(v).reshape(pair * n * rows, width)


def add(a, b):
    return (a.astype(F32) + b.astype(F32)).astype(BF16)


def scatter_steps(place, wires, part, rc, rd, rx, ry, qbuf, zbuf, make, finish):
    p, pair = place, place.pair
    rows = rx.shape[1]
    half = rows // 2
    top, low = pl.ds(0, half), pl.ds(half, half)
    slots = {"d": p.sd, "x": p.sx, "y": p.sy, "o": p.s}
    order = ["d", "x", "y", "o"]
    names = ["c" + k for k in order] + ["da", "db", "xa", "xb", "ya", "yb"]
    for t in range(pair):
        for name in names:
            wires.new((t, name))
    if pair > 1:
        wires.new("z")
    live = {}

    def go(key, src, dst, device):
        live[key] = wires.go(key, src, dst, device)

    def arrived(key):
        live[key].wait_recv()

    for t in range(pair):
        for i, k in enumerate(order):
            make(t, k, 1)
            go((t, "c" + k), part(t, flip(slots[k], 1)), rc.at[t, i], p.core)

    def start(t):
        make(t, "d", 0)
        arrived((t, "cd"))
        qbuf[t, 0] = add(part(t, p.sd)[...], rc[t, 0])
        go((t, "da"), qbuf.at[t, 0, top], rd.at[t, top], p.x)
        go((t, "db"), qbuf.at[t, 0, low], rd.at[t, low], p.y)
        make(t, "x", 0)
        arrived((t, "cx"))
        qbuf[t, 1, top] = add(part(t, p.sx)[top], rc[t, 1, top])
        go((t, "xa"), qbuf.at[t, 1, top], rx.at[t, top], p.x)
        make(t, "y", 0)
        arrived((t, "cy"))
        qbuf[t, 2, low] = add(part(t, p.sy)[low], rc[t, 2, low])
        go((t, "yb"), qbuf.at[t, 2, low], ry.at[t, low], p.y)

    def relay(t):
        held = part(t, p.sx)[low].astype(F32) + rc[t, 1, low].astype(F32)
        arrived((t, "db"))
        qbuf[t, 1, low] = (held + rd[t, low].astype(F32)).astype(BF16)
        go((t, "xb"), qbuf.at[t, 1, low], rx.at[t, low], p.x)
        held = part(t, p.sy)[top].astype(F32) + rc[t, 2, top].astype(F32)
        arrived((t, "da"))
        qbuf[t, 2, top] = (held + rd[t, top].astype(F32)).astype(BF16)
        go((t, "ya"), qbuf.at[t, 2, top], ry.at[t, top], p.y)

    def total(t):
        make(t, "o", 0)
        arrived((t, "co"))
        value = part(t, p.s)[...].astype(F32) + rc[t, 3].astype(F32)
        for key in ("xa", "yb", "xb", "ya"):
            arrived((t, key))
        return value + rx[t].astype(F32) + ry[t].astype(F32)

    if pair > 1:
        start(0)
        start(1)
        relay(0)
        relay(1)
        zbuf[0] = total(0).astype(BF16)
        go("z", zbuf.at[0], zbuf.at[1], p.z)
        value = total(1)
        arrived("z")
        value = value + zbuf[1].astype(F32)
    else:
        start(0)
        relay(0)
        value = total(0)
    finish(value)
    for copy in live.values():
        copy.wait_send()


def scatter_wires(pair):
    return 84 if pair > 1 else 20


def scatter_scratch(pair, rows, width):
    block = lambda *lead: pltpu.VMEM(lead + (rows, width), BF16)
    return [
        block(pair, 4),
        block(pair),
        block(pair),
        block(pair),
        block(pair, 3),
        block(2) if pair > 1 else pltpu.VMEM((2, 16, 128), BF16),
        pltpu.SemaphoreType.DMA((scatter_wires(pair),)),
        pltpu.SemaphoreType.DMA((scatter_wires(pair),)),
    ]


def scatter_kernel(pair, value, out, rc, rd, rx, ry, qbuf, zbuf, send, recv):
    place = Place(pair)
    place.barrier()
    planes = [1 - place.q, place.q] if pair > 1 else [0]

    def part(t, slot):
        return value.at[planes[t], slot]

    def finish(total):
        out[...] = total

    scatter_steps(
        place, Wires(send, recv), part, rc, rd, rx, ry, qbuf, zbuf, lambda *_: None, finish
    )


def plane_scatter(v, n, pair, ident):
    width = v.shape[1]
    rows = v.shape[0] // (pair * n)
    return pl.pallas_call(
        functools.partial(scatter_kernel, pair),
        in_specs=[pl.BlockSpec(memory_space=pltpu.VMEM)],
        out_specs=pl.BlockSpec(memory_space=pltpu.VMEM),
        out_shape=jax.ShapeDtypeStruct((rows, width), F32),
        scratch_shapes=scatter_scratch(pair, rows, width),
        compiler_params=pltpu.CompilerParams(
            collective_id=ident, has_side_effects=True, vmem_limit_bytes=40 * 2**20
        ),
        cost_estimate=pl.CostEstimate(flops=0, bytes_accessed=pair * n * rows * width * 20, transcendentals=0),
        name=f"scatter_{ident}",
    )(v.astype(BF16).reshape(pair, n, rows, width))


def sum_kernel(n, own, out, held, send, recv):
    s, f = lax.axis_index("seq"), lax.axis_index("fsdp")
    sem = pltpu.get_barrier_semaphore()
    for d in range(1, n):
        pl.semaphore_signal(sem, inc=1, device_id=((s + d) % n, f), device_id_type=MESH)
    pl.semaphore_wait(sem, n - 1)
    copies = []
    for d in range(1, n):
        copy = pltpu.make_async_remote_copy(
            own,
            held.at[d - 1],
            send.at[d - 1],
            recv.at[d - 1],
            device_id=((s + d) % n, f),
            device_id_type=MESH,
        )
        copy.start()
        copies.append(copy)
    total = own[...]
    for d in range(1, n):
        copies[d - 1].wait_recv()
        total = total + held[d - 1]
    out[...] = total
    for copy in copies:
        copy.wait_send()


def plane_sum(v, n, ident):
    return pl.pallas_call(
        functools.partial(sum_kernel, n),
        in_specs=[pl.BlockSpec(memory_space=pltpu.VMEM)],
        out_specs=pl.BlockSpec(memory_space=pltpu.VMEM),
        out_shape=jax.ShapeDtypeStruct(v.shape, v.dtype),
        scratch_shapes=[pltpu.VMEM((n - 1,) + v.shape, v.dtype)]
        + [pltpu.SemaphoreType.DMA((n - 1,))] * 2,
        compiler_params=pltpu.CompilerParams(collective_id=ident, has_side_effects=True),
        name=f"sum_{ident}",
    )(v)


def when(condition, body):
    pl.when(condition)(body)


def line_barrier(n, m):
    s, f = lax.axis_index("seq"), lax.axis_index("fsdp")
    sem = pltpu.get_barrier_semaphore()
    for d in range(1, n):
        pl.semaphore_signal(sem, inc=1, device_id=((s + d) % n, f), device_id_type=MESH)
    for d in range(1, m):
        pl.semaphore_signal(sem, inc=1, device_id=(s, (f + d) % m), device_id_type=MESH)
    pl.semaphore_wait(sem, n + m - 2)


class Moves:
    def __init__(self, sems):
        self.sems, self.count, self.open = sems, 0, []

    def start(self, src, dst):
        copy = pltpu.make_async_copy(src, dst, self.sems.at[self.count])
        self.count += 1
        copy.start()
        self.open.append(copy)
        return copy

    def finish(self):
        for copy in self.open:
            copy.wait()
        self.open = []

    def wait(self, copies):
        for copy in copies:
            copy.wait()
        self.open = [copy for copy in self.open if all(copy is not other for other in copies)]


def place_kernel(parts, count, *refs):
    ins, outs = refs[:count], refs[count : count + len(parts)]
    held, sems = refs[count + len(parts) : -1], refs[-1]
    copies = []
    for i, (source, row) in enumerate(parts):
        src = ins[source] if row is None else ins[source].at[row]
        copies.append(pltpu.make_async_copy(src, held[i], sems.at[0, i]))
        copies[-1].start()
    back = []
    for i in range(len(parts)):
        copies[i].wait()
        back.append(pltpu.make_async_copy(held[i], outs[i], sems.at[1, i]))
        back[-1].start()
    for copy in back:
        copy.wait()


def place_outputs(arrays):
    parts, shapes = [], []
    for source, a in enumerate(arrays):
        for row in range(a.shape[0]) if a.ndim == 3 else [None]:
            parts.append((source, row))
            shapes.append(shape(a.shape[-2:], a.dtype))
    return pl.pallas_call(
        functools.partial(place_kernel, tuple(parts), len(arrays)),
        in_specs=[pl.BlockSpec(memory_space=pltpu.MemorySpace.HBM)] * len(arrays),
        out_specs=[pl.BlockSpec(memory_space=pltpu.MemorySpace.HBM)] * len(parts),
        out_shape=shapes,
        scratch_shapes=[pltpu.VMEM(a.shape, a.dtype) for a in shapes] + [pltpu.SemaphoreType.DMA((2, len(parts)))],
        compiler_params=pltpu.CompilerParams(vmem_limit_bytes=63 * 2**20),
        name="place",
    )(*arrays)


def gather_pairs(place, wires, own, out, work, hook=lambda: None, done=lambda q, chip: None):
    p, pair = place, place.pair
    half = own.shape[0] // 2
    top, low = pl.ds(0, half), pl.ds(half, half)
    qs = [p.q] + ([1 - p.q] if pair > 1 else [])
    for t in range(pair):
        for kind in ["xa", "xb", "ya", "yb", "xd", "yd", "ca", "cb", "cxa", "cxb", "cya", "cyb", "cda", "cdb"]:
            wires.new((t, kind))
    if pair > 1:
        wires.new("za")
        wires.new("zb")
    live = {}

    def go(key, src, dst, device):
        live[key] = wires.go(key, src, dst, device)

    def arrived(*keys):
        for key in keys:
            live[key].wait_recv()

    def begin(t, src, tops):
        q = qs[t]
        rows = top if tops else low
        go((t, "xa" if tops else "xb"), src.at[rows], out.at[q, p.s, rows], p.x)
        go((t, "ya" if tops else "yb"), src.at[rows], out.at[q, p.s, rows], p.y)
        go((t, "ca" if tops else "cb"), src.at[rows], out.at[q, p.s, rows], p.core)

    def pass_on(t, name, slot, rows, device):
        ref = out.at[qs[t], slot, rows]
        go((t, name), ref, ref, device)

    def first(t):
        arrived((t, "xa"))
        pass_on(t, "xd", p.sx, top, p.y)
        pass_on(t, "cxa", p.sx, top, p.core)
        arrived((t, "ya"))
        pass_on(t, "cya", p.sy, top, p.core)

    def second(t):
        arrived((t, "yb"))
        pass_on(t, "yd", p.sy, low, p.x)
        pass_on(t, "cyb", p.sy, low, p.core)
        arrived((t, "xb"))
        pass_on(t, "cxb", p.sx, low, p.core)

    def third(t):
        arrived((t, "xd"))
        pass_on(t, "cda", p.sd, top, p.core)
        arrived((t, "yd"))
        pass_on(t, "cdb", p.sd, low, p.core)

    def chip_at(k):
        chip = p.s // 2
        return (chip % 2 + k % 2) % 2 + 2 * ((chip // 2 + k // 2) % 2)

    def use(t, first, count, *keys):
        arrived(*[(t, key) for key in keys])
        if count == 1:
            work(qs[t], chip_at(first))
        else:

            @pl.loop(first, first + count)
            def _(k):
                work(qs[t], chip_at(k))

        for k in range(first, first + count):
            done(qs[t], chip_at(k))

    if pair > 1:
        go("za", own.at[top], out.at[qs[0], p.s, top], p.z)
        go("zb", own.at[low], out.at[qs[0], p.s, low], p.z)
    begin(0, own, True)
    begin(0, own, False)
    if pair > 1:
        arrived((0, "ca"), (0, "cb"))
        hook()
        first(0)
        second(0)
        use(0, 0, 2, "cxa", "cxb")
        arrived("za")
        begin(1, out.at[qs[1], p.s], True)
        third(0)
        hook()
        use(0, 2, 2, "cya", "cyb", "cda", "cdb")
        arrived("zb")
        begin(1, out.at[qs[1], p.s], False)
        first(1)
        use(1, 0, 1, "ca", "cb")
        hook()
        second(1)
        hook()
        use(1, 1, 2, "cxa", "cxb", "cya", "cyb")
        third(1)
        use(1, 3, 1, "cda", "cdb")
    else:
        use(0, 0, 1, "ca", "cb")
        hook()
        first(0)
        hook()
        second(0)
        use(0, 1, 2, "cxa", "cxb", "cya", "cyb")
        hook()
        third(0)
        use(0, 3, 1, "cda", "cdb")
    return live


def by_rows(first, count, body):
    @pl.loop(0, count // 32)
    def _(i):
        body(pl.ds(pl.multiple_of(first + i * 32, 32), 32))


def scatter_pairs(
    place, wires, value, rc, rd, rx, ry, qbuf, zbuf, make, result, hook=lambda: None, jobs=None, mine=None, theirs=None
):
    p, pair = place, place.pair
    rows, width = rx.shape[1], rx.shape[2]
    count = 4 if pair > 1 else 2
    half, wide = rows // 2, width // count
    top, low = pl.ds(0, half), pl.ds(half, half)
    slots = {"d": p.sd, "x": p.sx, "y": p.sy, "o": p.s}
    order = ["d", "x", "y", "o"]
    planes = [1 - p.q, p.q] if pair > 1 else [p.q]
    jobs = jobs or [(t, c) for t in range(pair) for c in range(count)]
    mine = mine or list(range(count))
    theirs = theirs or mine
    for job in jobs:
        for name in ["c" + k for k in order] + ["da", "db", "xa", "xb", "ya", "yb"]:
            wires.new((job, name))
    if pair > 1:
        for c in range(count):
            wires.new(f"z{c}")
    live = {}

    def go(key, src, dst, device):
        live[key] = wires.go(key, src, dst, device)

    def arrived(*keys):
        for key in keys:
            live[key].wait_recv()

    def span(block):
        return pl.ds(block * wide if isinstance(block, int) else pl.multiple_of(block * wide, wide), wide)

    def at(c):
        return span(mine[c])

    def part(job, slot, rows_):
        return value.at[planes[job[0]], slot, rows_, at(job[1])]

    every = pl.ds(0, rows)

    def begin(job):
        t, c = job

        @pl.loop(0, 2)
        def _(k):
            make(planes[t], k, c, mine[c] * wide)

        for i, k in enumerate(order):
            go((job, "c" + k), part(job, flip(slots[k], 1), every), rc.at[t, i, :, at(c)], p.core)

    def rest(job):
        t, c = job

        def sum_of(i, slot):
            def body(r):
                qbuf[t, i, r, at(c)] = add(value[planes[t], slot, r, at(c)], rc[t, i, r, at(c)])

            return body

        arrived((job, "cd"))
        by_rows(0, rows, sum_of(0, p.sd))
        go((job, "da"), qbuf.at[t, 0, top, at(c)], rd.at[t, top, at(c)], p.x)
        go((job, "db"), qbuf.at[t, 0, low, at(c)], rd.at[t, low, at(c)], p.y)
        arrived((job, "cx"))
        by_rows(0, half, sum_of(1, p.sx))
        go((job, "xa"), qbuf.at[t, 1, top, at(c)], rx.at[t, top, at(c)], p.x)
        arrived((job, "cy"))
        by_rows(half, half, sum_of(2, p.sy))
        go((job, "yb"), qbuf.at[t, 2, low, at(c)], ry.at[t, low, at(c)], p.y)

    def relay(job):
        t, c = job

        def sum_of(i, slot):
            def body(r):
                held = value[planes[t], slot, r, at(c)].astype(F32) + rc[t, i, r, at(c)].astype(F32)
                qbuf[t, i, r, at(c)] = (held + rd[t, r, at(c)].astype(F32)).astype(BF16)

            return body

        arrived((job, "db"))
        by_rows(half, half, sum_of(1, p.sx))
        go((job, "xb"), qbuf.at[t, 1, low, at(c)], rx.at[t, low, at(c)], p.x)
        arrived((job, "da"))
        by_rows(0, half, sum_of(2, p.sy))
        go((job, "ya"), qbuf.at[t, 2, top, at(c)], ry.at[t, top, at(c)], p.y)

    def total(job):
        t, c = job
        arrived((job, "co"), (job, "xa"), (job, "yb"), (job, "xb"), (job, "ya"))

        def body(r):
            held = value[planes[t], p.s, r, at(c)].astype(F32) + rc[t, 3, r, at(c)].astype(F32)
            held = held + rx[t, r, at(c)].astype(F32) + ry[t, r, at(c)].astype(F32)
            if pair > 1 and t == 0:
                zbuf[0, r, at(c)] = held.astype(BF16)
            else:
                result[r, at(c)] = held

        by_rows(0, rows, body)
        if pair > 1 and t == 0:
            go(f"z{c}", zbuf.at[0, :, at(c)], zbuf.at[1, :, at(c)], p.z)

    begin(jobs[0])
    rest(jobs[0])
    if len(jobs) > 1:
        begin(jobs[1])
    for i, job in enumerate(jobs):
        if i + 1 < len(jobs):
            rest(jobs[i + 1])
        hook()
        if i + 2 < len(jobs):
            begin(jobs[i + 2])
        relay(job)
        hook()
        if i > 0:
            total(jobs[i - 1])
    total(jobs[-1])
    if pair > 1:
        for c in range(count):
            here = span(theirs[c])
            arrived(f"z{c}")

            def body(r):
                result[r, here] += zbuf[1, r, here].astype(F32)

            by_rows(0, rows, body)
    return live


def rms_back(value, gain, grad):
    inverse = lax.rsqrt(jnp.mean(value * value, axis=-1, keepdims=True) + EPSILON)
    normal = value * inverse
    u = grad * gain
    return inverse * (u - normal * jnp.mean(u * normal, axis=-1, keepdims=True)), grad * normal


def any_specs(count):
    return [pl.BlockSpec(memory_space=pl.ANY)] * count


def vmem_specs(count):
    return [pl.BlockSpec(memory_space=pltpu.VMEM)] * count


def kernel_params(ident, mib=60):
    return pltpu.CompilerParams(collective_id=ident, has_side_effects=True, vmem_limit_bytes=mib * 2**20)


def shape(dims, kind):
    return jax.ShapeDtypeStruct(dims, kind)


def feed_kernel(
    pair, h, hidden, gains, cotangent, wg, wu, down_w,
    layer_out, gain_term, hs, wu_all, grad_gate, grad_up, gate_t, up_t, down_term,
    hs_v, w_v, d_v, g_v, u_v, i_v, t_v, gt_v, ut_v, acc, grad_low, sum_v, value,
    rc, rd, rx, ry, qbuf, zbuf, ssend, srecv, send, recv, gsend, grecv, zsem, rsem, sems
):
    place = Place(pair)
    place.peers.append((place.s, flip(place.f, 1)))
    moves = Moves(sems)
    deep = wu.shape[1]
    loads = [moves.start(wg, w_v.at[0])]
    far_f, near_f = opposite(place.f), flip(place.f, 1)

    def up_rows(plane):
        return w_v.at[1, pl.ds(pl.multiple_of(plane * deep, deep), deep)]

    loads += [moves.start(wu.at[plane], up_rows(plane)) for plane in (place.f, near_f, far_f)]
    rows, width = h.shape
    block, share = 2 * rows, wg.shape[1]
    up_pass = pltpu.make_async_remote_copy(
        wu.at[far_f], up_rows(far_f), rsem.at[0], rsem.at[1], device_id=(place.s, near_f), device_id_type=MESH
    )
    hs_v[place.q, place.s] = h[...]
    place.barrier()
    stream, view = Stream(place, zsem), half_rows(down_w, share)
    deep_d = down_w.shape[1]

    def columns(plane):
        return d_v.at[:, pl.ds(pl.multiple_of(plane * deep_d, deep_d), deep_d)]

    own_copy = pltpu.make_async_copy(view(stream.half), columns(place.f), zsem.at[0, 3, 0])
    near_copy = stream.remote(0, 1, view(stream.half), columns(place.f), stream.near)
    far_copy = stream.remote(0, 0, view(1 - stream.half), columns(place.f), stream.far)
    relay = stream.remote(0, 2, columns(far_f), columns(far_f), stream.near)

    def pass_up():
        moves.wait(loads)
        up_pass.start()
        near_copy.start()
        own_copy.start()

    def pass_down():
        far_copy.start()

    n = hs.shape[1]
    step = min(256, share)

    def ready(q, chip):
        slots, here = where(q, chip)

        @pl.loop(0, share // step)
        def _(j):
            cols = pl.ds(pl.multiple_of(j * step, step), step)
            g_v[here, cols] = dot(hs_v[q, slots].reshape(block, width), w_v[0, :, cols], NN)

        if whole:
            second(q, slots, here)

    def done(q, chip):
        slots, here = where(q, chip)
        moves.start(hs_v.at[q, slots], hs.at[q, slots])
        if not whole:
            held.append((q, chip))

    whole, held = [], []

    def where(q, chip):
        return pl.ds(2 * chip, 2), pl.ds(pl.multiple_of(q * n * rows + chip * block, block), block)

    def second(q, slots, here):
        @pl.loop(0, share // step)
        def _(j):
            cols = pl.ds(pl.multiple_of(j * step, step), step)
            u = dot(hs_v[q, slots].reshape(block, width), w_v[1, :, cols], NN)
            g = g_v[here, cols]
            u_v[here, cols] = u
            value = g * (1.0 / (1.0 + jnp.exp(-g))) * u
            i_v[here, cols] = value.astype(BF16)
            t_v[cols, here] = value.T.astype(BF16)

    def complete():
        up_pass.wait_recv()
        whole.append(True)

        @pl.loop(0, n // 2)
        def _(chip):
            second(place.q, *where(place.q, chip))

        for q, chip in held[n // 2 :]:
            second(q, *where(q, chip))

    gathered = gather_pairs(place, Wires(send, recv), h, hs_v, ready, Work([pass_up, lambda: None, pass_down, complete]), done)
    moves.start(w_v.at[1], wu_all)
    for copy in gathered.values():
        copy.wait_send()
    moves.finish()
    gain = gains[3:4, :]
    own_copy.wait()
    near_copy.wait_recv()

    def pass_on():
        far_copy.wait_recv()
        relay.start()

    def make(q, chip, c, at):
        here = pl.ds(pl.multiple_of(q * n * rows + chip * 2 * block, 2 * block), 2 * block)
        cols = pl.ds(pl.multiple_of(at, deep_d), deep_d)
        part = dot(i_v[here, :], d_v[:, cols], NN).astype(BF16)
        value[q, pl.ds(4 * chip, 4), :, cols] = part.reshape(4, rows, deep_d)

    f = place.f
    mine = [f, near_f, far_f, opposite(near_f)]
    theirs = [far_f, opposite(near_f), f, near_f]
    jobs = [(0, 0), (0, 1), (1, 0), (0, 2), (1, 1), (0, 3), (1, 2), (1, 3)]
    live = scatter_pairs(
        place, Wires(ssend, srecv), value, rc, rd, rx, ry, qbuf, zbuf, make, sum_v,
        Work([lambda: None] * 2 + [pass_on] + [lambda: None] * 3 + [relay.wait_recv]), jobs, mine, theirs,
    )
    gain_term[...] = jnp.zeros_like(gain_term)

    def last(r):
        feed, grad = sum_v[r], cotangent[r].astype(F32)
        back, term = rms_back(feed, gain, grad)
        inverse = lax.rsqrt(jnp.mean(feed * feed, axis=-1, keepdims=True) + EPSILON)
        layer_out[r] = (hidden[r] + feed * inverse * gain).astype(BF16)
        grad_low[r] = back.astype(BF16)
        gain_term[...] += jnp.sum(term, axis=0, keepdims=True)

    by_rows(0, rows, last)
    def turn_back(q, chip):
        slots = pl.ds(2 * chip, 2)
        here = pl.ds(pl.multiple_of(q * n * rows + chip * block, block), block)

        @pl.loop(0, share // step)
        def _(j):
            cols = pl.ds(pl.multiple_of(j * step, step), step)
            a = hs_v[q, slots].reshape(block, width)
            e = dot(a, d_v[cols, :], NT)
            v, u = g_v[here, cols], u_v[here, cols]
            s = 1.0 / (1.0 + jnp.exp(-v))
            dg = e * u * s * (1.0 + v * (1.0 - s))
            du = e * v * s
            i_v[here, cols] = dg.astype(BF16)
            w_v[1, here, cols] = du.astype(BF16)
            gt_v[cols, here] = dg.T.astype(BF16)
            ut_v[cols, here] = du.T.astype(BF16)

    def keep(q, chip):
        here = pl.ds(pl.multiple_of(q * n * rows + chip * block, block), block)
        moves.start(i_v.at[here], grad_gate.at[here])
        moves.start(w_v.at[1, here], grad_up.at[here])

    def add_term(t):
        q = place.q if t == 0 else 1 - place.q
        tokens = pl.ds(pl.multiple_of(q * n * rows, n * rows), n * rows)

        @pl.loop(0, width // step)
        def _(j):
            cols = pl.ds(pl.multiple_of(j * step, step), step)
            part = dot(t_v[:, tokens], hs_v[q, :, :, cols].reshape(n * rows, step), NN)
            if t == 0:
                acc[:, cols] = part
            else:
                acc[:, cols] += part

    nothing = lambda: None
    hs_v[place.q, place.s] = grad_low[...]
    returned = gather_pairs(
        place, Wires(gsend, grecv), grad_low, hs_v, turn_back,
        Work([nothing, nothing, nothing, lambda: add_term(0)]), keep
    )
    add_term(1)
    for j in range(down_term.shape[0]):
        to = w_v.at[0, pl.ds(j * share, share)]
        to[...] = acc[:, pl.ds(j * deep_d, deep_d)].astype(BF16)
        moves.start(to, down_term.at[j])
    moves.start(gt_v, gate_t)
    moves.start(ut_v, up_t)
    for copy in list(live.values()) + list(returned.values()) + [relay, near_copy, far_copy, up_pass]:
        copy.wait_send()
    moves.finish()


def ffn_feed(h, hidden, gains, cotangent, wg, wu, down_w, n, m, pair, ident):
    rows, width = h.shape
    share, long = wg.shape[1], pair * n * rows
    dma = pltpu.SemaphoreType.DMA
    vmem = pltpu.VMEM
    outs = [
        shape((rows, width), BF16),
        shape((1, width), F32),
        shape((pair, n, rows, width), BF16),
        shape((width, share), BF16),
        shape((long, share), BF16),
        shape((long, share), BF16),
        shape((share, long), BF16),
        shape((share, long), BF16),
        shape((m, share, width // m), BF16),
    ]
    return pl.pallas_call(
        functools.partial(feed_kernel, pair),
        in_specs=vmem_specs(4) + any_specs(3),
        out_specs=vmem_specs(2) + any_specs(7),
        out_shape=outs,
        scratch_shapes=[
            vmem((pair, n, rows, width), BF16),
            vmem((2, width, share), BF16),
            vmem((share, width), BF16),
            vmem((long, share), F32),
            vmem((long, share), F32),
            vmem((long, share), BF16),
            vmem((share, long), BF16),
            vmem((share, long), BF16),
            vmem((share, long), BF16),
            vmem((share, width), F32),
            vmem((rows, width), BF16),
            vmem((rows, width), F32),
            vmem((pair, n, rows, width), BF16),
        ]
        + scatter_scratch(pair, rows, width)
        + [dma((gather_wires(pair),))] * 4
        + [dma((1, 4, 2)), dma((2,)), dma((16 + 4 * pair * n // 2,))],
        compiler_params=kernel_params(ident, 63),
        cost_estimate=pl.CostEstimate(
            flops=10 * long * width * share, bytes_accessed=long * width * 90, transcendentals=0
        ),
        name=f"feed_{ident}",
    )(h, hidden, gains, cotangent, wg, wu, down_w)


def back_kernel(
    pair, gg, gu, wg, wu, gate_t, hs, down_term, branch, gains, cotangent,
    grad_hidden, grad_low, gain_term, down_grad, gate_term,
    a_v, w_v, value, rc, rd, rx, ry, qbuf, zbuf, send, recv,
    gt_v, hs_v, gterm, down_own, down_near, down_total, down_from, dsem, sems
):
    place = Place(pair)
    place.peers.append((place.s, flip(place.f, 1)))
    moves = Moves(sems)
    loads = [moves.start(wg, w_v.at[0]), moves.start(wu, w_v.at[1])]
    loads += [moves.start(gg, a_v.at[0]), moves.start(gu, a_v.at[1])]
    late = []
    down = Settle(place, dsem, down_term, down_own, down_near, down_total, down_from)
    pieces = term_work(gterm, gt_v, hs_v, lambda: moves.wait(late), gate_term, moves)
    idle = [lambda: None]
    work = Work(idle + pieces[:1] + idle + [down.middle] + pieces[1:2] + idle + pieces[2:3] + idle + pieces[3:])
    rows, width = branch.shape
    block = 2 * rows
    n = value.shape[1]
    step = min(256, width)
    place.barrier()
    down.start(True)
    moves.wait(loads)
    late.append(moves.start(gate_t, gt_v))
    for q in range(pair):
        late.append(moves.start(hs.at[q], hs_v.at[q]))

    def make(q, chip, c, at):
        here = pl.ds(pl.multiple_of(q * n * rows + chip * 2 * block, 2 * block), 2 * block)

        @pl.loop(0, width // 4 // step)
        def _(j):
            cols = pl.ds(pl.multiple_of(at + j * step, step), step)
            part = dot(a_v[0, here, :], w_v[0, cols, :], NT) + dot(a_v[1, here, :], w_v[1, cols, :], NT)
            value[q, pl.ds(4 * chip, 4), :, cols] = part.astype(BF16).reshape(4, rows, step)

    live = scatter_pairs(place, Wires(send, recv), value, rc, rd, rx, ry, qbuf, zbuf, make, grad_hidden, work)
    work.rest()
    gain_term[...] = jnp.zeros_like(gain_term)

    def last(r):
        grad = cotangent[r].astype(F32) + grad_hidden[r]
        grad_hidden[r] = grad
        back, term = rms_back(branch[r], gains[2:3, :], grad)
        grad_low[r] = back.astype(BF16)
        gain_term[...] += jnp.sum(term, axis=0, keepdims=True)

    by_rows(0, rows, last)
    share = down_grad.shape[0] // 2

    def store(u, i, value):
        size = value.shape[0]
        down_grad[pl.ds(pl.multiple_of(u * share + i * size, size), size), :] = value

    down.finish(store)
    for copy in live.values():
        copy.wait_send()
    moves.finish()


def ffn_back(gg, gu, wg, wu, gate_t, hs, down_term, branch, gains, cotangent, n, m, pair, ident):
    rows, width = branch.shape
    share, deep = gate_t.shape[0], width // m
    term = down_term.shape
    dma = pltpu.SemaphoreType.DMA
    return pl.pallas_call(
        functools.partial(back_kernel, pair),
        in_specs=any_specs(7) + vmem_specs(3),
        out_specs=vmem_specs(4) + any_specs(1),
        out_shape=[
            shape((rows, width), F32),
            shape((rows, width), BF16),
            shape((1, width), F32),
            shape((2 * share, deep), F32),
            shape(term, BF16),
        ],
        scratch_shapes=[
            pltpu.VMEM((2,) + gg.shape, BF16),
            pltpu.VMEM((2,) + wg.shape, BF16),
            pltpu.VMEM((pair, n, rows, width), BF16),
        ]
        + scatter_scratch(pair, rows, width)
        + [pltpu.VMEM(v.shape, BF16) for v in (gate_t, hs)]
        + [pltpu.VMEM(term, BF16)]
        + settle_scratch(share, deep)
        + [dma((20,))],
        compiler_params=kernel_params(ident, 63),
        cost_estimate=pl.CostEstimate(
            flops=4 * gg.shape[0] * gg.shape[1] * width, bytes_accessed=pair * n * rows * width * 40, transcendentals=0
        ),
        name=f"back_{ident}",
    )(gg, gu, wg, wu, gate_t, hs, down_term, branch, gains, cotangent)


def opposite(f):
    return (f + 2) % 4


class Stream:
    def __init__(self, place, sems):
        self.place, self.sems = place, sems
        f = place.f
        self.half, self.far_f, self.near_f = f // 2, opposite(f), flip(f, 1)
        self.far, self.near = (place.s, self.far_f), (place.s, self.near_f)

    def remote(self, k, step, src, dst, device):
        return pltpu.make_async_remote_copy(
            src, dst, self.sems.at[k, step, 0], self.sems.at[k, step, 1], device_id=device, device_id_type=MESH
        )

    def far_copy(self, k, view, full):
        return self.remote(k, 0, view(1 - self.half), full.at[self.place.f], self.far)

    def near_copy(self, k, view, full):
        return self.remote(k, 1, view(self.half), full.at[self.place.f], self.near)

    def own_copy(self, k, view, full):
        return pltpu.make_async_copy(view(self.half), full.at[self.place.f], self.sems.at[k, 3, 0])

    def relay_copy(self, k, full):
        return self.remote(k, 2, full.at[self.far_f], full.at[self.far_f], self.near)

    def start_far(self, k, view, full):
        self.far_copy(k, view, full).start()

    def start_near(self, k, view, full):
        self.near_copy(k, view, full).start()
        self.own_copy(k, view, full).start()

    def relay(self, k, view, full):
        self.far_copy(k, view, full).wait_recv()
        self.relay_copy(k, full).start()

    def finish(self, k, view, full):
        self.near_copy(k, view, full).wait_recv()
        self.relay_copy(k, full).wait_recv()
        self.own_copy(k, view, full).wait()
        self.far_copy(k, view, full).wait_send()
        self.near_copy(k, view, full).wait_send()
        self.relay_copy(k, full).wait_send()


def half_columns(ref, share):
    return lambda u: ref.at[:, pl.ds(pl.multiple_of(u * share, share), share)]


def half_rows(ref, share):
    return lambda u: ref.at[pl.ds(pl.multiple_of(u * share, share), share), :]


def full_barrier(place, n, near):
    sem = pltpu.get_barrier_semaphore()
    s, f = place.s, place.f
    for d in range(1, n):
        pl.semaphore_signal(sem, inc=1, device_id=((s + d) % n, f), device_id_type=MESH)
    for other in near:
        pl.semaphore_signal(sem, inc=1, device_id=(s, other), device_id_type=MESH)
    pl.semaphore_wait(sem, n - 1 + len(near))


def swap_halves(v):
    return pltpu.roll(v, HD // 2, axis=1)


def to_rows(first, second):
    rows = first.shape[0]
    lane = lax.broadcasted_iota(jnp.int32, (rows, 128), 1)
    wide = jnp.where(lane == 0, first, jnp.where(lane == 1, second, 0.0))
    return wide.T[:8]


def to_columns(v):
    return jnp.concatenate([v, jnp.zeros((120, v.shape[1]), F32)], axis=0).T


def exchange(place, n, own, held, send, recv):
    copies = []
    for d in range(1, n):
        copy = pltpu.make_async_remote_copy(
            own,
            held.at[d - 1],
            send.at[d - 1],
            recv.at[d - 1],
            device_id=((place.s + d) % n, place.f),
            device_id_type=MESH,
        )
        copy.start()
        copies.append(copy)
    total = own[...]
    for d in range(1, n):
        copies[d - 1].wait_recv()
        total = total + held[d - 1]
    return total, copies


def attend(block, q_v, k_v, v_v, out_v, low_v, lt_v, log_v):
    length = q_v.shape[0]
    scale = HD ** (-0.5)

    @pl.loop(0, q_v.shape[1] // HD)
    def _(h):
        cols = pl.ds(pl.multiple_of(h * HD, HD), HD)
        for half in range(2):
            wide = pl.ds(0, (half + 1) * length // 2)

            @pl.loop(half * length // 2 // block, (half + 1) * length // 2 // block)
            def _(i):
                rows = pl.ds(pl.multiple_of(i * block, block), block)
                s = dot(q_v[rows, cols], k_v[wide, cols], NT) * scale
                column = lax.broadcasted_iota(jnp.int32, s.shape, 1)
                row = lax.broadcasted_iota(jnp.int32, s.shape, 0) + i * block
                s = jnp.where(column <= row, s, -jnp.inf)
                top = jnp.max(s, axis=-1, keepdims=True)
                p = jnp.exp(s - top)
                total = jnp.sum(p, axis=-1, keepdims=True)
                out = dot((p * (1.0 / total)).astype(BF16), v_v[wide, cols], NN)
                out_v[rows, cols] = out
                low_v[rows, cols] = out.astype(BF16)
                lt_v[cols, rows] = out.T.astype(BF16)
                log_v[h, rows, :] = top + jnp.log(total)


def opening_kernel(
    n, m, x, wq, wk, wv, own_gains, wo_own, gate_w, up_w, down_w,
    qkv, all_gains, tables, raw, heads, attended, low_t, xs_t, log_total, inverse, branch, hidden, hidden_low, wg, wu, wo,
    full, xs_v, xt_v, lt_v, w_v, wo_v, raw_v, heads_v, out_v, low_v, log_v, small, held, value,
    rc, rd, rx, ry, qbuf, zbuf, send, recv, ssend, srecv, zsem, osem,
    tsend, trecv, asend, arecv, zsend, zrecv, gsend, grecv, sems,
):
    place = Place(1)
    s, f = place.s, place.f
    rows, width = x.shape
    part = wq.shape[0]
    length, cols = raw.shape[1], raw.shape[2]
    share = wg.shape[2]
    block = min(256, length)
    per = block // rows
    weights = (wq, wk, wv)
    moves = Moves(sems)
    kept = []
    for j, w in enumerate(weights):
        own = w.at[:, pl.ds(pl.multiple_of(s * cols, cols), cols)]
        kept.append(moves.start(own, w_v.at[j, s, f]))
    own_out = [moves.start(wo_own, wo_v.at[f])]
    full[f, s] = own_gains[...]
    xs_v[0, s] = x[...]
    line_barrier(n, m)
    sent = []

    def remote(src, dst, a, b, device):
        copy = pltpu.make_async_remote_copy(src, dst, a, b, device_id=device, device_id_type=MESH)
        copy.start()
        sent.append(copy)
        return copy

    second = []
    for j, w in enumerate(weights):
        row = []
        for d in range(1, n):
            t = (s + d) % n
            src = w.at[:, pl.ds(pl.multiple_of(t * cols, cols), cols)]
            row.append(remote(src, w_v.at[j, s, f], asend.at[j, d], arecv.at[j, d], (t, f)))
        second.append(row)
    first = []
    for d in range(1, n):
        first.append(remote(own_gains, full.at[f, s], gsend.at[d], grecv.at[d], ((s + d) % n, f)))

    def piece(j, o):
        return full.at[o] if j == 3 else w_v.at[j, :, o]

    def hop(way, h, j):
        o = f - h if way == 0 else f + h
        there = f + 1 if way == 0 else f - 1
        place_ = piece(j, o)
        return pltpu.make_async_remote_copy(
            place_, place_, zsend.at[way, h, j], zrecv.at[way, h, j], device_id=(s, there), device_id_type=MESH
        )

    def sends(way, h):
        return ((f - h >= 0) & (f < m - 1)) if way == 0 else ((f + h <= m - 1) & (f > 0))

    def receives(way, h):
        return (f - h - 1 >= 0) if way == 0 else (f + h + 1 <= m - 1)

    def start(h, j):
        for way in (0, 1):
            when(sends(way, h), lambda: hop(way, h, j).start())

    def landed(h, j):
        for way in (0, 1):
            o = f - h - 1 if way == 0 else f + h + 1

            def wait():
                there = f - 1 if way == 0 else f + 1
                place_ = piece(j, o)
                pltpu.make_async_remote_copy(
                    place_, place_, zsend.at[way, h, j], zrecv.at[way, h, j], device_id=(s, there), device_id_type=MESH
                ).wait_recv()

            when(receives(way, h), wait)

    def step(h, j):
        landed(h, j)
        if h + 1 < m - 1:
            start(h + 1, j)

    moves.wait(kept)
    for j in range(3):
        for copy in second[j]:
            copy.wait_recv()
        start(0, j)
    for copy in first:
        copy.wait_recv()
    start(0, 3)
    gathered = gather_pairs(
        place, Wires(tsend, trecv), x, xs_v, lambda *_: None, Work([lambda: None, lambda: step(0, 0), lambda: step(0, 1)])
    )
    step(0, 2)
    step(0, 3)
    half = HD // 2
    lane = lax.broadcasted_iota(jnp.int32, (block, HD), 1)
    row = lax.broadcasted_iota(jnp.int32, (block, HD), 0)
    frequency = jnp.exp((lane % half).astype(F32) * (-2.0 * math.log(THETA) / HD))

    @pl.loop(0, length // block)
    def _(i):
        angle = (row + i * block).astype(F32) * frequency
        here = pl.ds(pl.multiple_of(i * block, block), block)
        tables[0, here, :] = jnp.cos(angle)
        sine = jnp.sin(angle)
        tables[1, here, :] = jnp.where(lane < half, -sine, sine)

    for h in range(1, m - 2):
        for j in range(4):
            step(h, j)

    out_copies = []
    for d, plane in enumerate((flip(f, 1), opposite(f), opposite(flip(f, 1)))):
        out_copies.append(
            pltpu.make_async_remote_copy(
                wo_own, wo_v.at[f], osem.at[0, d], osem.at[1, d], device_id=(s, plane), device_id_type=MESH
            )
        )
        out_copies[-1].start()
    stream = Stream(place, zsem)
    views = [half_columns(gate_w, share), half_columns(up_w, share)]
    fulls = [wg, wu]
    for k in range(2):
        stream.start_far(k, views[k], fulls[k])
    for k in range(2):
        stream.start_near(k, views[k], fulls[k])

    @pl.loop(0, length // block)
    def _(i):
        here = pl.ds(pl.multiple_of(i * block, block), block)
        xt_v[:, here] = xs_v[0, pl.ds(i * per, per)].reshape(block, width).T

    def project(j):
        @pl.loop(0, length // block)
        def _(i):
            here = pl.ds(pl.multiple_of(i * block, block), block)
            a = xs_v[0, pl.ds(i * per, per)].reshape(block, width)
            product = dot(a, w_v[j].reshape(width, cols), NN)
            if j == 2:
                heads_v[2, here, :] = product.astype(BF16)
            else:
                raw_v[j, here, :] = product

    moves.start(xt_v, xs_t)
    for j in range(3):
        landed(m - 2, j)
        project(j)
    landed(m - 2, 3)
    for t in range(n):
        for plane in range(m):
            at = (t * m + plane) * part
            all_gains[:, at : at + part] = full[plane, t, :, :part]
    moves.start(w_v, qkv)

    @pl.loop(0, length // block)
    def _(i):
        here = pl.ds(pl.multiple_of(i * block, block), block)
        q, k = raw_v[0, here, :], raw_v[1, here, :]
        small[0, :, here] = to_rows(
            jnp.sum(q * q, axis=1, keepdims=True), jnp.sum(k * k, axis=1, keepdims=True)
        )

    moves.start(raw_v, raw)
    first_col = pl.multiple_of(s * cols, cols)
    total, stat_copies = exchange(place, n, small.at[0], held, ssend, srecv)
    small[1] = lax.rsqrt(total * (1.0 / width) + EPSILON)
    moves.start(small.at[1], inverse)

    @pl.loop(0, length // block)
    def _(i):
        here = pl.ds(pl.multiple_of(i * block, block), block)
        inv = to_columns(small[1, :, here])
        cosine, sine = tables[0, here, :], tables[1, here, :]
        for j in range(2):
            for h in range(cols // HD):
                part = pl.ds(h * HD, HD)
                v = raw_v[j, here, part] * inv[:, j : j + 1] * all_gains[j : j + 1, pl.ds(first_col + h * HD, HD)]
                heads_v[j, here, part] = (v * cosine + swap_halves(v) * sine).astype(BF16)

    moves.start(heads_v, heads)
    attend(block, heads_v.at[0], heads_v.at[1], heads_v.at[2], out_v, low_v, lt_v, log_v)
    moves.start(out_v, attended)
    moves.start(lt_v, low_t)
    moves.start(log_v, log_total)
    moves.wait(own_out)
    for copy in out_copies:
        copy.wait_recv()
    moves.start(wo_v, wo)
    step = min(512, width)

    def make(q, chip, c, first):
        here = pl.ds(pl.multiple_of(chip * 4 * rows, 4 * rows), 4 * rows)

        @pl.loop(0, width // 2 // step)
        def _(j):
            at = pl.ds(pl.multiple_of(first + j * step, step), step)
            part = dot(low_v[here, :], wo_v[:, :, at].reshape(cols, step), NN).astype(BF16)
            value[q, pl.ds(4 * chip, 4), :, at] = part.reshape(4, rows, step)

    live = scatter_pairs(
        place, Wires(send, recv), value, rc, rd, rx, ry, qbuf, zbuf, make, branch,
        Work([lambda: None, lambda: stream.relay(0, views[0], fulls[0])]),
    )

    def last(r):
        total = branch[r]
        inv = lax.rsqrt(jnp.mean(total * total, axis=-1, keepdims=True) + EPSILON)
        h = x[r].astype(F32) + total * inv * all_gains[2:3, :]
        hidden[r] = h
        hidden_low[r] = h.astype(BF16)

    by_rows(0, rows, last)
    for copy in list(live.values()) + list(gathered.values()) + stat_copies + sent:
        copy.wait_send()
    for h in range(m - 1):
        for j in range(4):
            for way in (0, 1):
                when(sends(way, h), lambda: hop(way, h, j).wait_send())
    moves.finish()
    stream.finish(0, views[0], fulls[0])
    for copy in (
        stream.near_copy(1, views[1], fulls[1]),
        stream.far_copy(1, views[1], fulls[1]),
        stream.own_copy(1, views[1], fulls[1]),
    ):
        copy.wait()
    for copy in out_copies:
        copy.wait_send()


def opening(x, wq, wk, wv, gains, wo, gate_w, up_w, down_w, n, m, ident):
    rows, width = x.shape
    part, cols = wq.shape[0], width // n
    length, share = n * rows, gate_w.shape[1] // 2
    dma = pltpu.SemaphoreType.DMA
    heads = cols // HD
    outs = [
        shape((3, n, m, part, cols), BF16),
        shape((gains.shape[0], width), F32),
        shape((2, length, HD), F32),
        shape((2, length, cols), F32),
        shape((3, length, cols), BF16),
        shape((length, cols), F32),
        shape((cols, length), BF16),
        shape((width, length), BF16),
        shape((heads, length, 1), F32),
        shape((8, length), F32),
        shape((rows, width), F32),
        shape((rows, width), F32),
        shape((rows, width), BF16),
        shape((m, gate_w.shape[0], share), BF16),
        shape((m, gate_w.shape[0], share), BF16),
        shape((m,) + wo.shape, BF16),
    ]
    return pl.pallas_call(
        functools.partial(opening_kernel, n, m),
        in_specs=vmem_specs(5) + any_specs(4),
        out_specs=any_specs(1) + vmem_specs(2) + any_specs(7) + vmem_specs(3) + any_specs(3),
        out_shape=outs,
        scratch_shapes=[
            pltpu.VMEM((m, n) + gains.shape, F32),
            pltpu.VMEM((1, n, rows, width), BF16),
            pltpu.VMEM((width, length), BF16),
            pltpu.VMEM((cols, length), BF16),
            pltpu.VMEM((3, n, m, part, cols), BF16),
            pltpu.VMEM((m,) + wo.shape, BF16),
            pltpu.VMEM((2, length, cols), F32),
            pltpu.VMEM((3, length, cols), BF16),
            pltpu.VMEM((length, cols), F32),
            pltpu.VMEM((length, cols), BF16),
            pltpu.VMEM((heads, length, 1), F32),
            pltpu.VMEM((2, 8, length), F32),
            pltpu.VMEM((n - 1, 8, length), F32),
            pltpu.VMEM((1, n, rows, width), BF16),
        ]
        + scatter_scratch(1, rows, width)
        + [dma((n - 1,)), dma((n - 1,)), dma((2, 4, 2)), dma((2, m))]
        + [dma((gather_wires(1),))] * 2
        + [dma((3, n))] * 2
        + [dma((2, m, 4))] * 2
        + [dma((n,))] * 2
        + [dma((16,))],
        compiler_params=kernel_params(ident),
        cost_estimate=pl.CostEstimate(flops=10**10, bytes_accessed=200 * 2**20, transcendentals=0),
        name=f"opening_{ident}",
    )(x, wq, wk, wv, gains, wo, gate_w, up_w, down_w)


class Settle:
    def __init__(self, place, sems, term, own, near, total, far):
        self.place, self.sems, self.term, self.own = place, sems, term, own
        self.near, self.total, self.far = near, total, far
        f = place.f
        self.f = f
        self.odd, self.half = f % 2, f // 2

    def remote(self, step, src, dst, plane):
        return pltpu.make_async_remote_copy(
            src, dst, self.sems.at[step, 0], self.sems.at[step, 1], device_id=(self.place.s, plane), device_id_type=MESH
        )

    def given(self, i):
        return 1 - self.odd + 2 * i

    def kept(self, i):
        return self.odd + 2 * i

    def near_copy(self, step):
        i = 1 - self.half if step == 0 else self.half
        return self.remote(step, self.term.at[self.given(i)], self.near.at[i], flip(self.f, 1))

    def far_copy(self):
        return self.remote(2, self.total.at[0], self.far, opposite(self.f))

    def load(self, i):
        return pltpu.make_async_copy(self.term.at[self.kept(i)], self.own.at[i], self.sems.at[3, i])

    def start(self, both=False):
        self.near_copy(0).start()
        self.both = both
        if both:
            self.near_copy(1).start()
        for i in (0, 1):
            self.load(i).start()

    def mine(self, i):
        return self.term.at[self.kept(i)] if self.own is None else self.own.at[i]

    def chunks(self, body):
        size = 128

        @pl.loop(0, self.far.shape[0] // size)
        def _(i):
            body(i, pl.ds(pl.multiple_of(i * size, size), size))

    def middle(self):
        if self.own is not None:
            for i in (0, 1):
                self.load(i).wait()
        self.near_copy(0).wait_recv()
        other = 1 - self.half
        mine = self.mine(other)

        def body(i, r):
            self.total[0, r] = add(mine[r], self.near[other, r])

        self.chunks(body)
        self.far_copy().start()
        if not self.both:
            self.near_copy(1).start()

    def finish(self, store):
        half = self.half
        self.near_copy(1).wait_recv()
        mine = self.mine(half)
        self.chunks(lambda i, r: store(half, i, mine[r].astype(F32) + self.near[half, r].astype(F32)))
        self.far_copy().wait_recv()
        self.chunks(lambda i, r: store(1 - half, i, self.far[r].astype(F32)))
        for step in (0, 1):
            self.near_copy(step).wait_send()
        self.far_copy().wait_send()


def settle_scratch(share, depth, own=True):
    block = lambda *lead: pltpu.VMEM(lead + (share, depth), BF16)
    return ([block(2)] if own else []) + [block(2), block(1), block(), pltpu.SemaphoreType.DMA((4, 2))]


def term_block(term, left, right, block):
    deep, long = term.shape[2], left.shape[1]
    step = min(256, deep)

    @pl.loop(0, deep // step)
    def _(j):
        at = pl.ds(pl.multiple_of((0 if right.shape[3] == deep else block * deep) + j * step, step), step)
        to = pl.ds(pl.multiple_of(j * step, step), step)
        term[block, :, to] = dot(left[...], right[:, :, :, at].reshape(long, step), NN).astype(BF16)


class Work:
    def __init__(self, pieces):
        self.pieces = list(pieces)

    def __call__(self):
        if self.pieces:
            self.pieces.pop(0)()

    def rest(self):
        while self.pieces:
            self()


def term_work(term, left, right, prepare, out, moves):
    def piece(block):
        def run():
            if block == 0:
                prepare()
            term_block(term, left, right, block)
            moves.start(term.at[block], out.at[block])

        return run

    return [piece(block) for block in range(term.shape[0])]


def turn(v, cosine, sine):
    return v * cosine + swap_halves(v) * sine


def attend_back(block, q_v, k_v, v_v, out_v, log_v, g_v, dq, dk, dv):
    length = q_v.shape[0]
    scale = HD ** (-0.5)
    dk[...] = jnp.zeros_like(dk)
    dv[...] = jnp.zeros_like(dv)

    @pl.loop(0, q_v.shape[1] // HD)
    def _(h):
        cols = pl.ds(pl.multiple_of(h * HD, HD), HD)
        for half in range(2):
            wide = pl.ds(0, (half + 1) * length // 2)

            @pl.loop(half * length // 2 // block, (half + 1) * length // 2 // block)
            def _(i):
                rows = pl.ds(pl.multiple_of(i * block, block), block)
                q, g = q_v[rows, cols], g_v[rows, cols]
                s = dot(q, k_v[wide, cols], NT) * scale
                column = lax.broadcasted_iota(jnp.int32, s.shape, 1)
                row = lax.broadcasted_iota(jnp.int32, s.shape, 0) + i * block
                s = jnp.where(column <= row, s, -jnp.inf)
                weights = jnp.exp(s - log_v[h, rows, :])
                correction = jnp.sum(g.astype(F32) * out_v[rows, cols], axis=-1, keepdims=True)
                gw = dot(g, v_v[wide, cols], NT)
                gs = (weights * (gw - correction)).astype(BF16)
                dq[rows, cols] = dot(gs, k_v[wide, cols], NN) * scale
                dk[wide, cols] += dot(gs, q, TN) * scale
                dv[wide, cols] += dot(weights.astype(BF16), g, TN)


def closing_kernel(
    g, gains, tables, inverse, branch_gain, feed_gain,
    wo, raw, heads, attended, low_t, log_total, xs_t, gate_term, up_t, hs, qkv, grad_hidden_,
    gate_grad, up_grad, tokens_grad, weight_grad, gain_grad,
    bs, wo_v, raw_v, heads_v, out_v, low_v, log_v, ga_v, dq, dk, dv, d_v, xs_v, term_v, small, held, gain_term,
    ut_v, hs_v, up_term, gown, gnear, gtotal, gfar, gsem, unear, utotal, ufar, usem,
    grad_hidden, w_v, rc, rd, rx, ry, qbuf, zbuf, tsend, trecv, line, done, got, gbuf, gplane, gsum, gline,
    send, recv, ssend, srecv, zsend, zrecv, asend, arecv, qsend, qrecv, lsend, lrecv, sems,
):
    place = Place(1)
    n, m = bs.shape[1], wo.shape[0]
    rows, width = g.shape
    length, cols = raw.shape[1], raw.shape[2]
    share = gate_term.shape[1]
    first_col = pl.multiple_of(place.s * cols, cols)
    moves = Moves(sems)
    second = [moves.start(wo, wo_v)]
    fourth = [
        moves.start(heads, heads_v),
        moves.start(attended, out_v),
        moves.start(log_total, log_v),
        moves.start(low_t, low_v),
        moves.start(raw, raw_v),
        moves.start(xs_t, xs_v),
    ]
    moves.start(qkv, w_v)
    moves.start(grad_hidden_, grad_hidden)
    bs[0, place.s] = g[...]
    line_barrier(n, m)
    gate = Settle(place, gsem, gate_term, gown, gnear, gtotal, gfar)
    up = Settle(place, usem, up_term, None, unear, utotal, ufar)
    gate.start()
    late = [moves.start(up_t, ut_v)]
    deep = gate_term.shape[2]
    blocks = (up.given(1 - up.half), up.kept(1 - up.half), up.given(up.half), up.kept(up.half))

    def fetch(i):
        at = pl.ds(pl.multiple_of(blocks[i] * deep, deep), deep)
        late.extend(moves.start(hs.at[q, :, :, at], hs_v.at[q]) for q in range(hs.shape[0]))

    fetch(0)

    up.both = False

    def up_block(i):
        moves.wait(late)
        late.clear()
        term_block(up_term, ut_v, hs_v, blocks[i])
        if i == 0:
            up.near_copy(0).start()
        if i < 3:
            fetch(i + 1)

    block = min(256, length)

    def ready(q, chip):
        here = pl.ds(pl.multiple_of(chip * 2 * rows, 2 * rows), 2 * rows)
        a = bs[0, pl.ds(2 * chip, 2)].reshape(2 * rows, width)
        ga_v[here, :] = dot(a, wo_v[...].reshape(cols, width), NT).astype(BF16)

    moves.wait(second)
    gathered = gather_pairs(place, Wires(send, recv), g, bs, ready, Work([lambda: up_block(0), lambda: up_block(1), gate.middle]))
    up_block(2)
    up.middle()
    moves.wait(fourth)
    up_block(3)
    attend_back(block, heads_v.at[0], heads_v.at[1], heads_v.at[2], out_v, log_v, ga_v, dq, dk, dv)
    @pl.loop(0, length // block)
    def _(i):
        here = pl.ds(pl.multiple_of(i * block, block), block)
        inv = to_columns(inverse[:, here])
        cosine, sine = tables[0, here, :], -tables[1, here, :]
        sums = []
        for j, d in enumerate((dq, dk)):
            total = jnp.zeros((block, 1), F32)
            for h in range(cols // HD):
                part = pl.ds(h * HD, HD)
                normal = raw_v[j, here, part] * inv[:, j : j + 1]
                v = turn(d[here, part].astype(BF16).astype(F32), cosine, sine)
                raw_v[j, here, part] = normal
                gained = v * gains[j : j + 1, pl.ds(first_col + h * HD, HD)]
                total = total + jnp.sum(gained * normal, axis=1, keepdims=True)
                term_sum = jnp.sum(v * normal, axis=0, keepdims=True)
                d[here, part] = gained

                @pl.when(i == 0)
                def _():
                    gain_term[j, :, part] = term_sum

                @pl.when(i > 0)
                def _():
                    gain_term[j, :, part] += term_sum

            sums.append(total)
        small[0, :, here] = to_rows(sums[0], sums[1])
        d_v[2, here, :] = dv[here, :].astype(BF16)

    total, stat_copies = exchange(place, n, small.at[0], held, ssend, srecv)
    small[1] = total * (1.0 / width)

    @pl.loop(0, length // block)
    def _(i):
        here = pl.ds(pl.multiple_of(i * block, block), block)
        inv = to_columns(inverse[:, here])
        mean = to_columns(small[1, :, here])
        for j, d in enumerate((dq, dk)):
            d_v[j, here, :] = (
                inv[:, j : j + 1] * (d[here, :] - raw_v[j, here, :] * mean[:, j : j + 1])
            ).astype(BF16)


    @pl.loop(0, n)
    def _(i):
        at = pl.ds(pl.multiple_of(i * cols, cols), cols)
        part = dot(low_v[...], bs[0, :, :, at].reshape(length, cols), NN)
        term_v[3, i] = part.astype(BF16).reshape(m, cols // m, cols)
        for j in range(3):
            part = dot(xs_v[at, :], d_v[j], NN)
            term_v[j, i] = part.astype(BF16).reshape(m, cols // m, cols)


    def store(ref):
        def put(u, i, value):
            size = value.shape[0]
            ref[:, pl.ds(pl.multiple_of(u * share + i * size, size), size)] = value.T

        return put

    last = m - 1
    s, f, term, d3 = place.s, place.f, term_v, d_v
    for copy in gathered.values():
        copy.wait_send()

    def remote(src, dst, a, b, device):
        return pltpu.make_async_remote_copy(src, dst, a, b, device_id=device, device_id_type=MESH)

    def target(way, r):
        return last - r if way == 0 else r

    def hop(way, r, j, fresh):
        there = f + 1 if way == 0 else f - 1
        src = term.at[j, :, target(way, r)] if fresh else line.at[way, r, j]
        return remote(src, line.at[way, r, j], zsend.at[way, r, j], zrecv.at[way, r, j], (s, there))

    ends = (f == 0, f == last)
    inner = (f > 0, f < last)

    def beyond(way, r):
        return target(way, r) > f if way == 0 else target(way, r) < f

    for group in ((0, 1, 2), (3,)):
        for r in range(last):
            for j in group:
                for way in (0, 1):
                    when(ends[way], lambda: hop(way, r, j, True).start())

    gain_copies = []
    for t in range(n):
        at = pl.ds(t * cols, cols)
        for j in range(2):
            gbuf[t, j : j + 1, :] = jnp.where(s == t, gain_term[j], 0.0)
        gbuf[t, 2:3, :] = branch_gain[:, at]
        gbuf[t, 3:4, :] = feed_gain[:, at]
        gbuf[t, 4:, :] = jnp.zeros((4, cols), F32)
    for d in range(1, n):
        t = (s + d) % n
        copy = remote(gbuf.at[t], gplane.at[d - 1], qsend.at[d], qrecv.at[d], (t, f))
        copy.start()
        gain_copies.append(copy)

    moves.finish()
    block, step = 4 * rows, min(512, width)
    per = step // (m * qkv.shape[3])

    def make(q, chip, c, first):
        here = pl.ds(pl.multiple_of(chip * block, block), block)

        @pl.loop(0, width // 2 // step)
        def _(k):
            i = first // step + k
            at = pl.ds(pl.multiple_of(i * step, step), step)
            total = jnp.zeros((block, step), F32)
            for j in range(3):
                w = w_v[j, pl.ds(i * per, per)].reshape(step, cols)
                total = total + dot(d3[j, here, :], w, NT)
            bs[q, pl.ds(4 * chip, 4), :, at] = total.astype(BF16).reshape(4, rows, step)

    side = f // (m // 2)
    middle = (f > 0) & (f < last)

    def relays(k, j, from_end):
        way = side if from_end else 1 - side
        o = way * k + (1 - way) * (last - k)

        def relay():
            there = f + 1 - 2 * way
            copy = remote(
                line.at[way, k, j], line.at[way, k, j], zsend.at[way, k, j], zrecv.at[way, k, j], (s, there)
            )
            copy.wait_recv()
            line[way, k, j] = add(term[j, :, o], line[way, k, j])
            copy.start()

        when(middle, relay)

    live = scatter_pairs(
        place, Wires(tsend, trecv), bs, rc, rd, rx, ry, qbuf, zbuf, make, tokens_grad,
    )

    def join(r):
        tokens_grad[r] += grad_hidden[r]

    by_rows(0, rows, join)
    gate.finish(store(gate_grad))
    up.finish(store(up_grad))

    total = gbuf[s]
    for d in range(1, n):
        gain_copies[d - 1].wait_recv()
        total = total + gplane[d - 1]
    gsum[...] = total
    line_copies = []
    for d in range(1, m):
        t = (f + d) % m
        copy = remote(gsum, gline.at[d - 1], lsend.at[d], lrecv.at[d], (s, t))
        copy.start()
        line_copies.append(copy)

    copies = []
    plan = [(True, k, j) for k in range(m // 2) for j in range(3)]
    plan += [(False, k, j) for k in range(m // 2 - 1) for j in range(3)] + [(None, 0, j) for j in range(3)]
    plan += [(True, k, 3) for k in range(m // 2)] + [(False, k, 3) for k in range(m // 2 - 1)] + [(None, 0, 3)]
    for from_end, k, j in plan:
        if from_end is not None:
            relays(k, j, from_end)
            continue
        own = term[j, :, f].astype(F32)
        done[...] = own
        for way in (0, 1):
            r = last - f if way == 0 else f

            def take():
                pltpu.make_async_remote_copy(
                    line.at[way, 0, j],
                    line.at[way, r, j],
                    zsend.at[way, r, j],
                    zrecv.at[way, r, j],
                    device_id=(s, f - 1 if way == 0 else f + 1),
                    device_id_type=MESH,
                ).wait_recv()
                done[...] += line[way, r, j].astype(F32)

            when(inner[way], take)
        if j == 3:
            for t in range(n):
                weight_grad[j, :, pl.ds(t * cols, cols)] = done[t]
            continue
        weight_grad[j, :, pl.ds(pl.multiple_of(s * cols, cols), cols)] = done[s]
        got[0, j] = done[...].astype(BF16)
        for d in range(1, n):
            t = (s + d) % n
            copy = remote(got.at[0, j, t], got.at[1, j, s], asend.at[j, d], arecv.at[j, d], (t, f))
            copy.start()
            copies.append(copy)
    total = gsum[...]
    for d in range(1, m):
        line_copies[d - 1].wait_recv()
        total = total + gline[d - 1]
    thin = cols // m
    gain = jnp.zeros((8, thin), F32)
    for plane in range(m):
        gain = gain + jnp.where(f == plane, total[:, plane * thin : (plane + 1) * thin], 0.0)
    gain_grad[...] = gain
    for copy in copies:
        copy.wait_recv()
    for j in range(3):
        for d in range(1, n):
            t = (s + d) % n
            weight_grad[j, :, pl.ds(pl.multiple_of(t * cols, cols), cols)] = got[1, j, t].astype(F32)
    for copy in copies + gain_copies + line_copies + list(live.values()) + stat_copies:
        copy.wait_send()
    for r in range(last):
        for j in range(4):
            for way in (0, 1):
                when(ends[way] | (inner[way] & beyond(way, r)), lambda: hop(way, r, j, False).wait_send())


def closing(
    g, gains, tables, inverse, branch_gain, feed_gain,
    wo, raw, heads, attended, low_t, log_total, xs_t, gate_term, up_t, hs, qkv, grad_hidden, n, ident,
):
    rows, width = g.shape
    m = wo.shape[0]
    length, cols = raw.shape[1], raw.shape[2]
    share, deep, part = gate_term.shape[1], width // m, cols // m
    dma = pltpu.SemaphoreType.DMA
    vmem = pltpu.VMEM
    piece = (n, m, part, cols)
    return pl.pallas_call(
        closing_kernel,
        in_specs=vmem_specs(6) + any_specs(12),
        out_specs=vmem_specs(5),
        out_shape=[
            shape((deep, 2 * share), F32),
            shape((deep, 2 * share), F32),
            shape((rows, width), F32),
            shape((4, part, width), F32),
            shape((8, part), F32),
        ],
        scratch_shapes=[
            vmem((1, n, rows, width), BF16),
            vmem(wo.shape, BF16),
            vmem(raw.shape, F32),
            vmem(heads.shape, BF16),
            vmem(attended.shape, F32),
            vmem(low_t.shape, BF16),
            vmem(log_total.shape, F32),
            vmem((length, cols), BF16),
            vmem((length, cols), F32),
            vmem((length, cols), F32),
            vmem((length, cols), F32),
            vmem((3, length, cols), BF16),
            vmem(xs_t.shape, BF16),
            vmem((4,) + piece, BF16),
            vmem((2, 8, length), F32),
            vmem((n - 1, 8, length), F32),
            vmem((2, 1, cols), F32),
            vmem(up_t.shape, BF16),
            vmem(hs.shape[:3] + (deep,), BF16),
            vmem(gate_term.shape, BF16),
        ]
        + settle_scratch(share, deep)
        + settle_scratch(share, deep, False)
        + [vmem((rows, width), F32), vmem((3,) + piece, BF16)]
        + scatter_scratch(1, rows, width)
        + [
            vmem((2, m - 1, 4, n, part, cols), BF16),
            vmem((n, part, cols), F32),
            vmem((2, 3, n, part, cols), BF16),
            vmem((n, 8, cols), F32),
            vmem((n - 1, 8, cols), F32),
            vmem((8, cols), F32),
            vmem((m - 1, 8, cols), F32),
            dma((gather_wires(1),)),
            dma((gather_wires(1),)),
            dma((n - 1,)),
            dma((n - 1,)),
        ]
        + [dma((2, m, 4))] * 2
        + [dma((3, n))] * 2
        + [dma((n,))] * 2
        + [dma((m,))] * 2
        + [dma((24,))],
        compiler_params=kernel_params(ident, 63),
        cost_estimate=pl.CostEstimate(flops=10**10, bytes_accessed=400 * 2**20, transcendentals=0),
        name=f"closing_{ident}",
    )(
        g, gains, tables, inverse, branch_gain, feed_gain,
        wo, raw, heads, attended, low_t, log_total, xs_t, gate_term, up_t, hs, qkv, grad_hidden,
    )


def attention_forward_kernel(block, q_ref, k_ref, v_ref, out_ref, low_ref, log_ref):
    length = q_ref.shape[0]
    scale = HD ** (-0.5)
    for i in range(length // block):
        rows = pl.ds(i * block, block)
        width = (i + 1) * block
        s = dot(q_ref[rows, :], k_ref[pl.ds(0, width), :], NT) * scale
        column = lax.broadcasted_iota(jnp.int32, (block, width), 1)
        row = lax.broadcasted_iota(jnp.int32, (block, width), 0) + i * block
        s = jnp.where(column <= row, s, -jnp.inf)
        top = jnp.max(s, axis=-1, keepdims=True)
        p = jnp.exp(s - top)
        total = jnp.sum(p, axis=-1, keepdims=True)
        weights = (p * (1.0 / total)).astype(BF16)
        out = dot(weights, v_ref[pl.ds(0, width), :], NN)
        out_ref[rows, :] = out
        low_ref[rows, :] = out.astype(BF16)
        log_ref[0, rows, :] = top + jnp.log(total)


def attention_forward(q, k, v):
    length, width = q.shape
    heads = width // HD
    block = min(256, length)
    column = pl.BlockSpec((length, HD), lambda h: (0, h))
    return pl.pallas_call(
        functools.partial(attention_forward_kernel, block),
        grid=(heads,),
        in_specs=[column] * 3,
        out_specs=[column, column, pl.BlockSpec((1, length, 1), lambda h: (h, 0, 0))],
        out_shape=[
            jax.ShapeDtypeStruct((length, width), F32),
            jax.ShapeDtypeStruct((length, width), BF16),
            jax.ShapeDtypeStruct((heads, length, 1), F32),
        ],
        cost_estimate=pl.CostEstimate(
            flops=2 * heads * length * length * HD, bytes_accessed=10 * length * width, transcendentals=0
        ),
    )(q, k, v)


def attention_backward_kernel(block, q_ref, k_ref, v_ref, out_ref, log_ref, g_ref, dq_ref, dk_ref, dv_ref, dk, dv):
    length = q_ref.shape[0]
    scale = HD ** (-0.5)
    dk[...] = jnp.zeros_like(dk)
    dv[...] = jnp.zeros_like(dv)
    for i in range(length // block):
        rows = pl.ds(i * block, block)
        width = (i + 1) * block
        wide = pl.ds(0, width)
        q = q_ref[rows, :]
        g = g_ref[rows, :]
        s = dot(q, k_ref[wide, :], NT) * scale
        column = lax.broadcasted_iota(jnp.int32, (block, width), 1)
        row = lax.broadcasted_iota(jnp.int32, (block, width), 0) + i * block
        s = jnp.where(column <= row, s, -jnp.inf)
        weights = jnp.exp(s - log_ref[0, rows, :])
        correction = jnp.sum(g.astype(F32) * out_ref[rows, :], axis=-1, keepdims=True)
        gw = dot(g, v_ref[wide, :], NT)
        gs = (weights * (gw - correction)).astype(BF16)
        dq_ref[rows, :] = (dot(gs, k_ref[wide, :], NN) * scale).astype(BF16)
        dk[wide, :] += dot(gs, q, TN)
        dv[wide, :] += dot(weights.astype(BF16), g, TN)
    dk_ref[...] = (dk[...] * scale).astype(BF16)
    dv_ref[...] = dv[...].astype(BF16)


def attention_backward(q, k, v, out, log_total, g):
    length, width = q.shape
    heads = width // HD
    block = min(256, length)
    column = pl.BlockSpec((length, HD), lambda h: (0, h))
    return pl.pallas_call(
        functools.partial(attention_backward_kernel, block),
        grid=(heads,),
        in_specs=[column] * 4 + [pl.BlockSpec((1, length, 1), lambda h: (h, 0, 0)), column],
        out_specs=[column] * 3,
        out_shape=[jax.ShapeDtypeStruct((length, width), BF16)] * 3,
        scratch_shapes=[pltpu.VMEM((length, HD), F32)] * 2,
        cost_estimate=pl.CostEstimate(
            flops=5 * heads * length * length * HD, bytes_accessed=16 * length * width, transcendentals=0
        ),
    )(q, k, v, out, log_total, g)


def on_device(n, m, pair, *args):
    (
        tokens,
        query_weight,
        key_weight,
        value_weight,
        out_weight,
        query_gain,
        key_gain,
        attention_gain,
        gate_weight,
        up_weight,
        down_weight,
        feedforward_gain,
        cotangent,
    ) = args
    rows, width = tokens.shape[1], tokens.shape[2]
    length = rows * n
    part = query_weight.shape[0]
    cols = width // n
    depth, units = gate_weight.shape
    share = units // pair
    x = tokens.reshape(rows, width)
    groups = [[g * pair + u for u in range(pair)] for g in range(m // pair)]

    native = n == 8 and m == 4

    def gather_plane(v, ident):
        if native:
            return plane_gather(v, n, 1, ident)
        return lax.all_gather(v, "seq", axis=0, tiled=True)

    def scatter_plane(v, ident):
        if native:
            return plane_scatter(v, n, 1, ident)
        return lax.psum_scatter(v.astype(BF16), "seq", scatter_dimension=0, tiled=True).astype(F32)

    def gather_pair(v, ident):
        if native:
            return plane_gather(v, n, pair, ident)
        if pair > 1:
            v = lax.all_gather(v, "fsdp", axis=0, axis_index_groups=groups)
        v = lax.all_gather(v.reshape(pair, rows, width), "seq", axis=1, tiled=True)
        return v.reshape(pair * length, width)

    def scatter_pair(v, ident):
        if native:
            return plane_scatter(v, n, pair, ident)
        v = lax.psum_scatter(v.astype(BF16).reshape(pair, length, width), "seq", scatter_dimension=1, tiled=True)
        if pair > 1:
            v = lax.psum_scatter(v, "fsdp", scatter_dimension=0, axis_index_groups=groups)
        return v.reshape(rows, width).astype(F32)

    def total_plane(v, ident):
        return plane_sum(v, n, ident) if native else lax.psum(v, "seq")

    def spread(halves):
        return lax.all_to_all(jnp.tile(halves, (m // pair, 1, 1)), "fsdp", 0, 0, tiled=False)

    def settle(blocks):
        back = lax.all_to_all(blocks.astype(BF16), "fsdp", 0, 0, tiled=False)
        if native:
            return jnp.sum(back.reshape((pair, m // pair) + back.shape[1:]).astype(F32), axis=1)
        return jnp.sum(back.reshape((m // pair, pair) + back.shape[1:]).astype(F32), axis=0)

    gains = jnp.stack([query_gain, key_gain, attention_gain, feedforward_gain]).astype(F32)
    grad_out = cotangent.reshape(rows, width)
    if native:
        (
            qkv, gains, tables, raw, heads, attended, low_t, xs_t, log_total, inverse, branch, hidden, hidden_low,
            gate_cols, up_cols, out_rows,
        ) = opening(
            x, query_weight, key_weight, value_weight, jnp.pad(gains, ((0, 4), (0, 128 - part))),
            out_weight, gate_weight, up_weight, down_weight, n, m, 1
        )
        gate_cols = gate_cols.reshape(width, share)
        layer_out, feed_gain_term, hs, up_cols, grad_gate, grad_up, gate_t, up_t, down_term = ffn_feed(
            hidden_low, hidden, gains, grad_out, gate_cols, up_cols, down_weight, n, m, pair, 5
        )
        grad_hidden, branch_low, branch_gain_term, down_grad, gate_term = ffn_back(
            grad_gate, grad_up, gate_cols, up_cols, gate_t, hs, down_term, branch, gains, grad_out, n, m, pair, 8
        )
        gate_grad, up_grad, tokens_grad, term, gain_grads = closing(
            branch_low, gains, tables, inverse, branch_gain_term, feed_gain_term,
            out_rows, raw, heads, attended, low_t, log_total, xs_t, gate_term, up_t, hs, qkv, grad_hidden, n, 2
        )
        layer_out, tokens_grad, *term, gate_grad, up_grad, down_grad = place_outputs(
            [layer_out, tokens_grad, term, gate_grad, up_grad, down_grad]
        )
        out_grad = term[3]
    else:
        cosine, sine = angles_of(length)
        seq = lax.axis_index("seq")
        stacked = jnp.stack([query_weight, key_weight, value_weight]).reshape(3, part, n, cols)
        mine = lax.all_to_all(stacked.transpose(2, 0, 1, 3), "seq", 0, 0)
        qkv = lax.all_gather(mine, "fsdp", axis=1).transpose(2, 0, 1, 3, 4).reshape(3, width, cols)
        full_gain = lax.all_gather(gains, ("seq", "fsdp"), axis=1).reshape(4, width)
        xs = gather_plane(x, 1)
        out_rows = lax.all_gather(out_weight, "fsdp", axis=0, tiled=True)
        own_gain = lax.dynamic_slice_in_dim(full_gain[:2], seq * cols, cols, 1)
        q_gain, k_gain, branch_gain, feed_gain = own_gain[0], own_gain[1], full_gain[2], full_gain[3]
        q_raw, k_raw, v = dot(xs, qkv[0], NN), dot(xs, qkv[1], NN), dot(xs, qkv[2], NN).astype(BF16)
        squares = jnp.stack([jnp.sum(q_raw * q_raw, axis=1), jnp.sum(k_raw * k_raw, axis=1)])
        inverse = lax.rsqrt(lax.psum(squares, "seq") / width + EPSILON)
        q_inv, k_inv = inverse[0][:, None], inverse[1][:, None]
        q = rotate(q_raw * q_inv * q_gain, cosine, sine, 1.0).astype(BF16)
        k = rotate(k_raw * k_inv * k_gain, cosine, sine, 1.0).astype(BF16)
        attended, attended_low, log_total = attention_forward(q, k, v)
        branch = scatter_plane(dot(attended_low, out_rows, NN), 3)
        branch_inv = lax.rsqrt(jnp.mean(branch * branch, axis=1, keepdims=True) + EPSILON)
        hidden = x.astype(F32) + branch * branch_inv * branch_gain
        hidden_low = hidden.astype(BF16)
        gate_cols = spread(gate_weight.reshape(depth, pair, share).transpose(1, 0, 2)).reshape(width, share)
        up_cols = spread(up_weight.reshape(depth, pair, share).transpose(1, 0, 2)).reshape(width, share)
        down_rows = spread(down_weight.reshape(pair, share, depth)).transpose(1, 0, 2).reshape(share, width)
        grad_out = grad_out.astype(F32)
        hs = gather_pair(hidden_low, 5)
        gate = dot(hs, gate_cols, NN)
        up = dot(hs, up_cols, NN)
        sig = jax.nn.sigmoid(gate)
        inner = (gate * sig * up).astype(BF16)
        feed = scatter_pair(dot(inner, down_rows, NN), 7)
        feed_inv = lax.rsqrt(jnp.mean(feed * feed, axis=1, keepdims=True) + EPSILON)
        layer_out = (hidden + feed * feed_inv * feed_gain).astype(BF16)
        grad_feed, term = rms_back(feed, feed_gain, grad_out)
        feed_gain_term = jnp.sum(term, axis=0)
        gs = gather_pair(grad_feed.astype(BF16), 6)
        grad_inner = dot(gs, down_rows, NT)
        grad_gate = (grad_inner * up * sig * (1.0 + gate * (1.0 - sig))).astype(BF16)
        grad_up = (grad_inner * gate * sig).astype(BF16)
        grad_hidden = grad_out + scatter_pair(dot(grad_gate, gate_cols, NT) + dot(grad_up, up_cols, NT), 8)
        grad_branch, term = rms_back(branch, branch_gain, grad_hidden)
        branch_low = grad_branch.astype(BF16)
        branch_gain_term = jnp.sum(term, axis=0)
        inner_t, gate_t, up_t = inner.T, grad_gate.T, grad_up.T

        def cut(v):
            return v.reshape(share, m, depth).transpose(1, 0, 2)

        down_grad = settle(cut(dot(inner_t, gs, NN))).reshape(units, depth)
        gate_grad = settle(cut(dot(gate_t, hs, NN))).transpose(2, 0, 1).reshape(depth, units)
        up_grad = settle(cut(dot(up_t, hs, NN))).transpose(2, 0, 1).reshape(depth, units)
        bs = gather_plane(branch_low, 2)
        out_grad = lax.psum_scatter(
            dot(attended_low, bs, TN).astype(BF16), "fsdp", scatter_dimension=0, tiled=True
        ).astype(F32)
        grad_attended = dot(bs, out_rows, NT).astype(BF16)
        dq, dk, dv = attention_backward(q, k, v, attended, log_total, grad_attended)
        dq = rotate(dq.astype(F32), cosine, sine, -1.0)
        dk = rotate(dk.astype(F32), cosine, sine, -1.0)
        q_normal, k_normal = q_raw * q_inv, k_raw * k_inv
        q_gain_term = jnp.sum(dq * q_normal, axis=0)
        k_gain_term = jnp.sum(dk * k_normal, axis=0)
        dq, dk = dq * q_gain, dk * k_gain
        means = total_plane(jnp.stack([jnp.sum(dq * q_normal, axis=1), jnp.sum(dk * k_normal, axis=1)]), 10) / width
        dq = (q_inv * (dq - q_normal * means[0][:, None])).astype(BF16)
        dk = (k_inv * (dk - k_normal * means[1][:, None])).astype(BF16)
        value = dot(dq, qkv[0], NT) + dot(dk, qkv[1], NT) + dot(dv, qkv[2], NT)
        term = jnp.stack([dot(xs, d, TN).astype(BF16) for d in (dq, dk, dv)]).reshape(3, n, m, part, cols)
        gain_own = jnp.stack([q_gain_term, k_gain_term])
        gain_own = lax.dynamic_update_slice(jnp.zeros((2, width), F32), gain_own, (0, seq * cols))
        gain_terms = jnp.concatenate([gain_own, jnp.stack([branch_gain_term, feed_gain_term])]).reshape(4, n, m, part)
        tokens_grad = grad_hidden + scatter_plane(value, 4)
        term = lax.psum_scatter(term, "fsdp", scatter_dimension=2)
        term = lax.all_to_all(term, "seq", 1, 1).astype(F32).transpose(0, 2, 1, 3)
        gain_grads = lax.psum_scatter(
            gain_terms.reshape(4, width), ("seq", "fsdp"), scatter_dimension=1, tiled=True
        )
        term = term.reshape(3, part, width)

    return (
        layer_out.reshape(tokens.shape),
        tokens_grad.reshape(tokens.shape),
        term[0],
        term[1],
        term[2],
        out_grad,
        gain_grads[0],
        gain_grads[1],
        gain_grads[2],
        gate_grad,
        up_grad,
        down_grad,
        gain_grads[3],
    )


def solution(mesh):
    n, m = mesh.shape["seq"], mesh.shape["fsdp"]
    tall, flat, act = P(("seq", "fsdp"), None), P(("seq", "fsdp")), P("fsdp", "seq", None)
    wide, deep = P("fsdp", "seq"), P("seq", "fsdp")
    return jax.shard_map(
        functools.partial(on_device, n, m, 2),
        mesh=mesh,
        in_specs=(act, tall, tall, tall, tall, flat, flat, flat, wide, wide, deep, flat, act),
        out_specs=(act, act, tall, tall, tall, tall, flat, flat, flat, wide, wide, deep, flat),
        check_vma=False,
    )
```

```python
import functools
import math

import jax
import jax.numpy as jnp
from jax import lax
from jax.experimental import pallas as pl
from jax.experimental.pallas import tpu as pltpu
from jax.sharding import PartitionSpec as P

EPSILON = 1e-06
THETA = 500000.0
HD = 128
F32 = jnp.float32
BF16 = jnp.bfloat16


def dot(a, b, dims):
    return lax.dot_general(a, b, (dims, ((), ())), preferred_element_type=F32)


NN = ((1,), (0,))
NT = ((1,), (1,))
TN = ((0,), (0,))


def angles_of(length):
    half = HD // 2
    frequency = jnp.exp(jnp.arange(half, dtype=F32) * (-2.0 * math.log(THETA) / HD))
    angle = jnp.arange(length, dtype=F32)[:, None] * frequency[None, :]
    return jnp.cos(angle), jnp.sin(angle)


def rotate(value, cosine, sine, sign):
    length, width = value.shape
    value = value.reshape(length, width // HD, 2, HD // 2)
    first, second = value[:, :, 0], value[:, :, 1]
    c, s = cosine[:, None, :], sign * sine[:, None, :]
    return jnp.stack([first * c - second * s, second * c + first * s], axis=2).reshape(length, width)


MESH = pl.DeviceIdType.MESH


def flip(index, bit):
    return index + bit - 2 * bit * ((index // bit) % 2)


class Place:
    def __init__(self, pair):
        self.s, self.f = lax.axis_index("seq"), lax.axis_index("fsdp")
        self.pair = pair
        s, f = self.s, self.f
        self.sx, self.sy = flip(s, 2), flip(s, 4)
        self.sd, self.sc = flip(self.sx, 4), flip(s, 1)
        self.q = f // 2 if pair > 1 else 0
        self.x, self.y, self.core = (self.sx, f), (self.sy, f), (self.sc, f)
        self.z = (s, opposite(f)) if pair > 1 else None
        self.peers = [self.x, self.y, self.core] + ([self.z] if pair > 1 else [])

    def barrier(self):
        sem = pltpu.get_barrier_semaphore()
        for peer in self.peers:
            pl.semaphore_signal(sem, inc=1, device_id=peer, device_id_type=MESH)
        pl.semaphore_wait(sem, len(self.peers))


class Wires:
    def __init__(self, send, recv):
        self.send, self.recv, self.count, self.open = send, recv, 0, {}

    def new(self, key):
        self.open[key] = self.count
        self.count += 1

    def go(self, key, src, dst, device):
        i = self.open[key]
        copy = pltpu.make_async_remote_copy(
            src, dst, self.send.at[i], self.recv.at[i], device_id=device, device_id_type=MESH
        )
        copy.start()
        return copy


def gather_steps(place, wires, own, out, ready):
    pair, rows = place.pair, own.shape[0]
    half = rows // 2
    top, low = pl.ds(0, half), pl.ds(half, half)
    p = place
    qs = [p.q] + ([1 - p.q] if pair > 1 else [])
    kinds = ["xa", "xb", "ya", "yb", "xd", "yd", "c0", "cxa", "cxb", "cya", "cyb", "cda", "cdb"]
    for t in range(pair):
        for kind in kinds:
            wires.new((t, kind))
    if pair > 1:
        wires.new("z")
    live = {}

    def go(key, src, dst, device):
        live[key] = wires.go(key, src, dst, device)

    def begin(t, src):
        q = qs[t]
        go((t, "xa"), src.at[top], out.at[q, p.s, top], p.x)
        go((t, "yb"), src.at[low], out.at[q, p.s, low], p.y)
        go((t, "xb"), src.at[low], out.at[q, p.s, low], p.x)
        go((t, "ya"), src.at[top], out.at[q, p.s, top], p.y)
        go((t, "c0"), src, out.at[q, p.s], p.core)

    def arrived(key):
        live[key].wait_recv()

    if pair > 1:
        go("z", own, out.at[qs[0], p.s], p.z)
    begin(0, own)
    ready(qs[0], p.s, None)

    def first(t):
        q = qs[t]
        arrived((t, "xa"))
        go((t, "xd"), out.at[q, p.sx, top], out.at[q, p.sx, top], p.y)
        go((t, "cxa"), out.at[q, p.sx, top], out.at[q, p.sx, top], p.core)
        arrived((t, "yb"))
        go((t, "yd"), out.at[q, p.sy, low], out.at[q, p.sy, low], p.x)
        go((t, "cyb"), out.at[q, p.sy, low], out.at[q, p.sy, low], p.core)
        arrived((t, "c0"))
        ready(q, p.sc, None)

    def second(t):
        q = qs[t]
        arrived((t, "xb"))
        go((t, "cxb"), out.at[q, p.sx, low], out.at[q, p.sx, low], p.core)
        ready(q, p.sx, None)
        arrived((t, "ya"))
        go((t, "cya"), out.at[q, p.sy, top], out.at[q, p.sy, top], p.core)
        ready(q, p.sy, None)
        arrived((t, "xd"))
        go((t, "cda"), out.at[q, p.sd, top], out.at[q, p.sd, top], p.core)
        arrived((t, "yd"))
        go((t, "cdb"), out.at[q, p.sd, low], out.at[q, p.sd, low], p.core)

    def third(t):
        q = qs[t]
        arrived((t, "cxa"))
        arrived((t, "cxb"))
        ready(q, flip(p.sx, 1), None)
        arrived((t, "cya"))
        arrived((t, "cyb"))
        ready(q, flip(p.sy, 1), None)
        ready(q, p.sd, None)
        arrived((t, "cda"))
        arrived((t, "cdb"))
        ready(q, flip(p.sd, 1), None)

    first(0)
    if pair > 1:
        arrived("z")
        begin(1, out.at[qs[1], p.s])
        ready(qs[1], p.s, None)
    second(0)
    if pair > 1:
        first(1)
    third(0)
    if pair > 1:
        second(1)
        third(1)
    for copy in live.values():
        copy.wait_send()


def gather_wires(pair):
    return 14 * pair + (2 if pair > 1 else 0)


def gather_kernel(pair, own, out, send, recv, local):
    place = Place(pair)
    keep = pltpu.make_async_copy(own, out.at[place.q, place.s], local)
    keep.start()
    place.barrier()
    gather_steps(place, Wires(send, recv), own, out, lambda q, slot, half: None)
    keep.wait()


def plane_gather(v, n, pair, ident):
    rows, width = v.shape
    return pl.pallas_call(
        functools.partial(gather_kernel, pair),
        in_specs=[pl.BlockSpec(memory_space=pltpu.VMEM)],
        out_specs=pl.BlockSpec(memory_space=pl.ANY),
        out_shape=jax.ShapeDtypeStruct((pair, n, rows, width), v.dtype),
        scratch_shapes=[pltpu.SemaphoreType.DMA((gather_wires(pair),))] * 2 + [pltpu.SemaphoreType.DMA],
        compiler_params=pltpu.CompilerParams(collective_id=ident, has_side_effects=True),
        cost_estimate=pl.CostEstimate(flops=0, bytes_accessed=pair * n * rows * width * 20, transcendentals=0),
        name=f"gather_{ident}",
    )(v).reshape(pair * n * rows, width)


def add(a, b):
    return (a.astype(F32) + b.astype(F32)).astype(BF16)


def scatter_steps(place, wires, part, rc, rd, rx, ry, qbuf, zbuf, make, finish):
    p, pair = place, place.pair
    rows = rx.shape[1]
    half = rows // 2
    top, low = pl.ds(0, half), pl.ds(half, half)
    slots = {"d": p.sd, "x": p.sx, "y": p.sy, "o": p.s}
    order = ["d", "x", "y", "o"]
    names = ["c" + k for k in order] + ["da", "db", "xa", "xb", "ya", "yb"]
    for t in range(pair):
        for name in names:
            wires.new((t, name))
    if pair > 1:
        wires.new("z")
    live = {}

    def go(key, src, dst, device):
        live[key] = wires.go(key, src, dst, device)

    def arrived(key):
        live[key].wait_recv()

    for t in range(pair):
        for i, k in enumerate(order):
            make(t, k, 1)
            go((t, "c" + k), part(t, flip(slots[k], 1)), rc.at[t, i], p.core)

    def start(t):
        make(t, "d", 0)
        arrived((t, "cd"))
        qbuf[t, 0] = add(part(t, p.sd)[...], rc[t, 0])
        go((t, "da"), qbuf.at[t, 0, top], rd.at[t, top], p.x)
        go((t, "db"), qbuf.at[t, 0, low], rd.at[t, low], p.y)
        make(t, "x", 0)
        arrived((t, "cx"))
        qbuf[t, 1, top] = add(part(t, p.sx)[top], rc[t, 1, top])
        go((t, "xa"), qbuf.at[t, 1, top], rx.at[t, top], p.x)
        make(t, "y", 0)
        arrived((t, "cy"))
        qbuf[t, 2, low] = add(part(t, p.sy)[low], rc[t, 2, low])
        go((t, "yb"), qbuf.at[t, 2, low], ry.at[t, low], p.y)

    def relay(t):
        held = part(t, p.sx)[low].astype(F32) + rc[t, 1, low].astype(F32)
        arrived((t, "db"))
        qbuf[t, 1, low] = (held + rd[t, low].astype(F32)).astype(BF16)
        go((t, "xb"), qbuf.at[t, 1, low], rx.at[t, low], p.x)
        held = part(t, p.sy)[top].astype(F32) + rc[t, 2, top].astype(F32)
        arrived((t, "da"))
        qbuf[t, 2, top] = (held + rd[t, top].astype(F32)).astype(BF16)
        go((t, "ya"), qbuf.at[t, 2, top], ry.at[t, top], p.y)

    def total(t):
        make(t, "o", 0)
        arrived((t, "co"))
        value = part(t, p.s)[...].astype(F32) + rc[t, 3].astype(F32)
        for key in ("xa", "yb", "xb", "ya"):
            arrived((t, key))
        return value + rx[t].astype(F32) + ry[t].astype(F32)

    if pair > 1:
        start(0)
        start(1)
        relay(0)
        relay(1)
        zbuf[0] = total(0).astype(BF16)
        go("z", zbuf.at[0], zbuf.at[1], p.z)
        value = total(1)
        arrived("z")
        value = value + zbuf[1].astype(F32)
    else:
        start(0)
        relay(0)
        value = total(0)
    finish(value)
    for copy in live.values():
        copy.wait_send()


def scatter_wires(pair):
    return 84 if pair > 1 else 20


def scatter_scratch(pair, rows, width):
    block = lambda *lead: pltpu.VMEM(lead + (rows, width), BF16)
    return [
        block(pair, 4),
        block(pair),
        block(pair),
        block(pair),
        block(pair, 3),
        block(2) if pair > 1 else pltpu.VMEM((2, 16, 128), BF16),
        pltpu.SemaphoreType.DMA((scatter_wires(pair),)),
        pltpu.SemaphoreType.DMA((scatter_wires(pair),)),
    ]


def scatter_kernel(pair, value, out, rc, rd, rx, ry, qbuf, zbuf, send, recv):
    place = Place(pair)
    place.barrier()
    planes = [1 - place.q, place.q] if pair > 1 else [0]

    def part(t, slot):
        return value.at[planes[t], slot]

    def finish(total):
        out[...] = total

    scatter_steps(
        place, Wires(send, recv), part, rc, rd, rx, ry, qbuf, zbuf, lambda *_: None, finish
    )


def plane_scatter(v, n, pair, ident):
    width = v.shape[1]
    rows = v.shape[0] // (pair * n)
    return pl.pallas_call(
        functools.partial(scatter_kernel, pair),
        in_specs=[pl.BlockSpec(memory_space=pltpu.VMEM)],
        out_specs=pl.BlockSpec(memory_space=pltpu.VMEM),
        out_shape=jax.ShapeDtypeStruct((rows, width), F32),
        scratch_shapes=scatter_scratch(pair, rows, width),
        compiler_params=pltpu.CompilerParams(
            collective_id=ident, has_side_effects=True, vmem_limit_bytes=40 * 2**20
        ),
        cost_estimate=pl.CostEstimate(flops=0, bytes_accessed=pair * n * rows * width * 20, transcendentals=0),
        name=f"scatter_{ident}",
    )(v.astype(BF16).reshape(pair, n, rows, width))


def sum_kernel(n, own, out, held, send, recv):
    s, f = lax.axis_index("seq"), lax.axis_index("fsdp")
    sem = pltpu.get_barrier_semaphore()
    for d in range(1, n):
        pl.semaphore_signal(sem, inc=1, device_id=((s + d) % n, f), device_id_type=MESH)
    pl.semaphore_wait(sem, n - 1)
    copies = []
    for d in range(1, n):
        copy = pltpu.make_async_remote_copy(
            own,
            held.at[d - 1],
            send.at[d - 1],
            recv.at[d - 1],
            device_id=((s + d) % n, f),
            device_id_type=MESH,
        )
        copy.start()
        copies.append(copy)
    total = own[...]
    for d in range(1, n):
        copies[d - 1].wait_recv()
        total = total + held[d - 1]
    out[...] = total
    for copy in copies:
        copy.wait_send()


def plane_sum(v, n, ident):
    return pl.pallas_call(
        functools.partial(sum_kernel, n),
        in_specs=[pl.BlockSpec(memory_space=pltpu.VMEM)],
        out_specs=pl.BlockSpec(memory_space=pltpu.VMEM),
        out_shape=jax.ShapeDtypeStruct(v.shape, v.dtype),
        scratch_shapes=[pltpu.VMEM((n - 1,) + v.shape, v.dtype)]
        + [pltpu.SemaphoreType.DMA((n - 1,))] * 2,
        compiler_params=pltpu.CompilerParams(collective_id=ident, has_side_effects=True),
        name=f"sum_{ident}",
    )(v)


def when(condition, body):
    pl.when(condition)(body)


def line_barrier(n, m):
    s, f = lax.axis_index("seq"), lax.axis_index("fsdp")
    sem = pltpu.get_barrier_semaphore()
    for d in range(1, n):
        pl.semaphore_signal(sem, inc=1, device_id=((s + d) % n, f), device_id_type=MESH)
    for d in range(1, m):
        pl.semaphore_signal(sem, inc=1, device_id=(s, (f + d) % m), device_id_type=MESH)
    pl.semaphore_wait(sem, n + m - 2)


class Moves:
    def __init__(self, sems):
        self.sems, self.count, self.open = sems, 0, []

    def start(self, src, dst):
        copy = pltpu.make_async_copy(src, dst, self.sems.at[self.count])
        self.count += 1
        copy.start()
        self.open.append(copy)
        return copy

    def finish(self):
        for copy in self.open:
            copy.wait()
        self.open = []

    def wait(self, copies):
        for copy in copies:
            copy.wait()
        self.open = [copy for copy in self.open if all(copy is not other for other in copies)]


def place_kernel(parts, count, *refs):
    ins, outs = refs[:count], refs[count : count + len(parts)]
    held, sems = refs[count + len(parts) : -1], refs[-1]
    copies = []
    for i, (source, row) in enumerate(parts):
        src = ins[source] if row is None else ins[source].at[row]
        copies.append(pltpu.make_async_copy(src, held[i], sems.at[0, i]))
        copies[-1].start()
    back = []
    for i in range(len(parts)):
        copies[i].wait()
        back.append(pltpu.make_async_copy(held[i], outs[i], sems.at[1, i]))
        back[-1].start()
    for copy in back:
        copy.wait()


def place_outputs(arrays):
    parts, shapes = [], []
    for source, a in enumerate(arrays):
        for row in range(a.shape[0]) if a.ndim == 3 else [None]:
            parts.append((source, row))
            shapes.append(shape(a.shape[-2:], a.dtype))
    return pl.pallas_call(
        functools.partial(place_kernel, tuple(parts), len(arrays)),
        in_specs=[pl.BlockSpec(memory_space=pltpu.MemorySpace.HBM)] * len(arrays),
        out_specs=[pl.BlockSpec(memory_space=pltpu.MemorySpace.HBM)] * len(parts),
        out_shape=shapes,
        scratch_shapes=[pltpu.VMEM(a.shape, a.dtype) for a in shapes] + [pltpu.SemaphoreType.DMA((2, len(parts)))],
        compiler_params=pltpu.CompilerParams(vmem_limit_bytes=63 * 2**20),
        name="place",
    )(*arrays)


def gather_pairs(place, wires, own, out, work, hook=lambda: None, done=lambda q, chip: None):
    p, pair = place, place.pair
    half = own.shape[0] // 2
    top, low = pl.ds(0, half), pl.ds(half, half)
    qs = [p.q] + ([1 - p.q] if pair > 1 else [])
    for t in range(pair):
        for kind in ["xa", "xb", "ya", "yb", "xd", "yd", "ca", "cb", "cxa", "cxb", "cya", "cyb", "cda", "cdb"]:
            wires.new((t, kind))
    if pair > 1:
        wires.new("za")
        wires.new("zb")
    live = {}

    def go(key, src, dst, device):
        live[key] = wires.go(key, src, dst, device)

    def arrived(*keys):
        for key in keys:
            live[key].wait_recv()

    def begin(t, src, tops):
        q = qs[t]
        rows = top if tops else low
        go((t, "xa" if tops else "xb"), src.at[rows], out.at[q, p.s, rows], p.x)
        go((t, "ya" if tops else "yb"), src.at[rows], out.at[q, p.s, rows], p.y)
        go((t, "ca" if tops else "cb"), src.at[rows], out.at[q, p.s, rows], p.core)

    def pass_on(t, name, slot, rows, device):
        ref = out.at[qs[t], slot, rows]
        go((t, name), ref, ref, device)

    def first(t):
        arrived((t, "xa"))
        pass_on(t, "xd", p.sx, top, p.y)
        pass_on(t, "cxa", p.sx, top, p.core)
        arrived((t, "ya"))
        pass_on(t, "cya", p.sy, top, p.core)

    def second(t):
        arrived((t, "yb"))
        pass_on(t, "yd", p.sy, low, p.x)
        pass_on(t, "cyb", p.sy, low, p.core)
        arrived((t, "xb"))
        pass_on(t, "cxb", p.sx, low, p.core)

    def third(t):
        arrived((t, "xd"))
        pass_on(t, "cda", p.sd, top, p.core)
        arrived((t, "yd"))
        pass_on(t, "cdb", p.sd, low, p.core)

    def chip_at(k):
        chip = p.s // 2
        return (chip % 2 + k % 2) % 2 + 2 * ((chip // 2 + k // 2) % 2)

    def use(t, first, count, *keys):
        arrived(*[(t, key) for key in keys])
        if count == 1:
            work(qs[t], chip_at(first))
        else:

            @pl.loop(first, first + count)
            def _(k):
                work(qs[t], chip_at(k))

        for k in range(first, first + count):
            done(qs[t], chip_at(k))

    if pair > 1:
        go("za", own.at[top], out.at[qs[0], p.s, top], p.z)
        go("zb", own.at[low], out.at[qs[0], p.s, low], p.z)
    begin(0, own, True)
    begin(0, own, False)
    if pair > 1:
        arrived((0, "ca"), (0, "cb"))
        hook()
        first(0)
        second(0)
        use(0, 0, 2, "cxa", "cxb")
        arrived("za")
        begin(1, out.at[qs[1], p.s], True)
        third(0)
        hook()
        use(0, 2, 2, "cya", "cyb", "cda", "cdb")
        arrived("zb")
        begin(1, out.at[qs[1], p.s], False)
        first(1)
        use(1, 0, 1, "ca", "cb")
        hook()
        second(1)
        hook()
        use(1, 1, 2, "cxa", "cxb", "cya", "cyb")
        third(1)
        use(1, 3, 1, "cda", "cdb")
    else:
        use(0, 0, 1, "ca", "cb")
        hook()
        first(0)
        hook()
        second(0)
        use(0, 1, 2, "cxa", "cxb", "cya", "cyb")
        hook()
        third(0)
        use(0, 3, 1, "cda", "cdb")
    return live


def by_rows(first, count, body):
    @pl.loop(0, count // 32)
    def _(i):
        body(pl.ds(pl.multiple_of(first + i * 32, 32), 32))


def scatter_pairs(
    place, wires, value, rc, rd, rx, ry, qbuf, zbuf, make, result, hook=lambda: None, jobs=None, mine=None, theirs=None
):
    p, pair = place, place.pair
    rows, width = rx.shape[1], rx.shape[2]
    count = 4 if pair > 1 else 2
    half, wide = rows // 2, width // count
    top, low = pl.ds(0, half), pl.ds(half, half)
    slots = {"d": p.sd, "x": p.sx, "y": p.sy, "o": p.s}
    order = ["d", "x", "y", "o"]
    planes = [1 - p.q, p.q] if pair > 1 else [p.q]
    jobs = jobs or [(t, c) for t in range(pair) for c in range(count)]
    mine = mine or list(range(count))
    theirs = theirs or mine
    for job in jobs:
        for name in ["c" + k for k in order] + ["da", "db", "xa", "xb", "ya", "yb"]:
            wires.new((job, name))
    if pair > 1:
        for c in range(count):
            wires.new(f"z{c}")
    live = {}

    def go(key, src, dst, device):
        live[key] = wires.go(key, src, dst, device)

    def arrived(*keys):
        for key in keys:
            live[key].wait_recv()

    def span(block):
        return pl.ds(block * wide if isinstance(block, int) else pl.multiple_of(block * wide, wide), wide)

    def at(c):
        return span(mine[c])

    def part(job, slot, rows_):
        return value.at[planes[job[0]], slot, rows_, at(job[1])]

    every = pl.ds(0, rows)

    def begin(job):
        t, c = job

        @pl.loop(0, 2)
        def _(k):
            make(planes[t], k, c, mine[c] * wide)

        for i, k in enumerate(order):
            go((job, "c" + k), part(job, flip(slots[k], 1), every), rc.at[t, i, :, at(c)], p.core)

    def rest(job):
        t, c = job

        def sum_of(i, slot):
            def body(r):
                qbuf[t, i, r, at(c)] = add(value[planes[t], slot, r, at(c)], rc[t, i, r, at(c)])

            return body

        arrived((job, "cd"))
        by_rows(0, rows, sum_of(0, p.sd))
        go((job, "da"), qbuf.at[t, 0, top, at(c)], rd.at[t, top, at(c)], p.x)
        go((job, "db"), qbuf.at[t, 0, low, at(c)], rd.at[t, low, at(c)], p.y)
        arrived((job, "cx"))
        by_rows(0, half, sum_of(1, p.sx))
        go((job, "xa"), qbuf.at[t, 1, top, at(c)], rx.at[t, top, at(c)], p.x)
        arrived((job, "cy"))
        by_rows(half, half, sum_of(2, p.sy))
        go((job, "yb"), qbuf.at[t, 2, low, at(c)], ry.at[t, low, at(c)], p.y)

    def relay(job):
        t, c = job

        def sum_of(i, slot):
            def body(r):
                held = value[planes[t], slot, r, at(c)].astype(F32) + rc[t, i, r, at(c)].astype(F32)
                qbuf[t, i, r, at(c)] = (held + rd[t, r, at(c)].astype(F32)).astype(BF16)

            return body

        arrived((job, "db"))
        by_rows(half, half, sum_of(1, p.sx))
        go((job, "xb"), qbuf.at[t, 1, low, at(c)], rx.at[t, low, at(c)], p.x)
        arrived((job, "da"))
        by_rows(0, half, sum_of(2, p.sy))
        go((job, "ya"), qbuf.at[t, 2, top, at(c)], ry.at[t, top, at(c)], p.y)

    def total(job):
        t, c = job
        arrived((job, "co"), (job, "xa"), (job, "yb"), (job, "xb"), (job, "ya"))

        def body(r):
            held = value[planes[t], p.s, r, at(c)].astype(F32) + rc[t, 3, r, at(c)].astype(F32)
            held = held + rx[t, r, at(c)].astype(F32) + ry[t, r, at(c)].astype(F32)
            if pair > 1 and t == 0:
                zbuf[0, r, at(c)] = held.astype(BF16)
            else:
                result[r, at(c)] = held

        by_rows(0, rows, body)
        if pair > 1 and t == 0:
            go(f"z{c}", zbuf.at[0, :, at(c)], zbuf.at[1, :, at(c)], p.z)

    begin(jobs[0])
    rest(jobs[0])
    if len(jobs) > 1:
        begin(jobs[1])
    for i, job in enumerate(jobs):
        if i + 1 < len(jobs):
            rest(jobs[i + 1])
        hook()
        if i + 2 < len(jobs):
            begin(jobs[i + 2])
        relay(job)
        hook()
        if i > 0:
            total(jobs[i - 1])
    total(jobs[-1])
    if pair > 1:
        for c in range(count):
            here = span(theirs[c])
            arrived(f"z{c}")

            def body(r):
                result[r, here] += zbuf[1, r, here].astype(F32)

            by_rows(0, rows, body)
    return live


def rms_back(value, gain, grad):
    inverse = lax.rsqrt(jnp.mean(value * value, axis=-1, keepdims=True) + EPSILON)
    normal = value * inverse
    u = grad * gain
    return inverse * (u - normal * jnp.mean(u * normal, axis=-1, keepdims=True)), grad * normal


def any_specs(count):
    return [pl.BlockSpec(memory_space=pl.ANY)] * count


def vmem_specs(count):
    return [pl.BlockSpec(memory_space=pltpu.VMEM)] * count


def kernel_params(ident, mib=60):
    return pltpu.CompilerParams(collective_id=ident, has_side_effects=True, vmem_limit_bytes=mib * 2**20)


def shape(dims, kind):
    return jax.ShapeDtypeStruct(dims, kind)


def feed_kernel(
    pair, h, hidden, gains, cotangent, wg, wu, down_w,
    layer_out, gain_term, hs, wu_all, grad_gate, grad_up, gate_t, up_t, down_term,
    hs_v, w_v, d_v, g_v, u_v, i_v, t_v, gt_v, ut_v, acc, grad_low, sum_v, value,
    rc, rd, rx, ry, qbuf, zbuf, ssend, srecv, send, recv, gsend, grecv, zsem, rsem, sems
):
    place = Place(pair)
    place.peers.append((place.s, flip(place.f, 1)))
    moves = Moves(sems)
    deep = wu.shape[1]
    loads = [moves.start(wg, w_v.at[0])]
    far_f, near_f = opposite(place.f), flip(place.f, 1)

    def up_rows(plane):
        return w_v.at[1, pl.ds(pl.multiple_of(plane * deep, deep), deep)]

    loads += [moves.start(wu.at[plane], up_rows(plane)) for plane in (place.f, near_f, far_f)]
    rows, width = h.shape
    block, share = 2 * rows, wg.shape[1]
    up_pass = pltpu.make_async_remote_copy(
        wu.at[far_f], up_rows(far_f), rsem.at[0], rsem.at[1], device_id=(place.s, near_f), device_id_type=MESH
    )
    hs_v[place.q, place.s] = h[...]
    place.barrier()
    stream, view = Stream(place, zsem), half_rows(down_w, share)
    deep_d = down_w.shape[1]

    def columns(plane):
        return d_v.at[:, pl.ds(pl.multiple_of(plane * deep_d, deep_d), deep_d)]

    own_copy = pltpu.make_async_copy(view(stream.half), columns(place.f), zsem.at[0, 3, 0])
    near_copy = stream.remote(0, 1, view(stream.half), columns(place.f), stream.near)
    far_copy = stream.remote(0, 0, view(1 - stream.half), columns(place.f), stream.far)
    relay = stream.remote(0, 2, columns(far_f), columns(far_f), stream.near)

    def pass_up():
        moves.wait(loads)
        up_pass.start()
        near_copy.start()
        own_copy.start()

    def pass_down():
        far_copy.start()

    n = hs.shape[1]
    step = min(256, share)

    def ready(q, chip):
        slots, here = where(q, chip)

        @pl.loop(0, share // step)
        def _(j):
            cols = pl.ds(pl.multiple_of(j * step, step), step)
            g_v[here, cols] = dot(hs_v[q, slots].reshape(block, width), w_v[0, :, cols], NN)

        if whole:
            second(q, slots, here)

    def done(q, chip):
        slots, here = where(q, chip)
        moves.start(hs_v.at[q, slots], hs.at[q, slots])
        if not whole:
            held.append((q, chip))

    whole, held = [], []

    def where(q, chip):
        return pl.ds(2 * chip, 2), pl.ds(pl.multiple_of(q * n * rows + chip * block, block), block)

    def second(q, slots, here):
        @pl.loop(0, share // step)
        def _(j):
            cols = pl.ds(pl.multiple_of(j * step, step), step)
            u = dot(hs_v[q, slots].reshape(block, width), w_v[1, :, cols], NN)
            g = g_v[here, cols]
            u_v[here, cols] = u
            value = g * (1.0 / (1.0 + jnp.exp(-g))) * u
            i_v[here, cols] = value.astype(BF16)
            t_v[cols, here] = value.astype(BF16).T

    def complete():
        up_pass.wait_recv()
        whole.append(True)

        @pl.loop(0, n // 2)
        def _(chip):
            second(place.q, *where(place.q, chip))

        for q, chip in held[n // 2 :]:
            second(q, *where(q, chip))

    gathered = gather_pairs(place, Wires(send, recv), h, hs_v, ready, Work([pass_up, lambda: None, pass_down, complete]), done)
    moves.start(w_v.at[1], wu_all)
    for copy in gathered.values():
        copy.wait_send()
    moves.finish()
    gain = gains[3:4, :]
    own_copy.wait()
    near_copy.wait_recv()

    def pass_on():
        far_copy.wait_recv()
        relay.start()

    def make(q, chip, c, at):
        here = pl.ds(pl.multiple_of(q * n * rows + chip * 2 * block, 2 * block), 2 * block)
        cols = pl.ds(pl.multiple_of(at, deep_d), deep_d)
        part = dot(i_v[here, :], d_v[:, cols], NN).astype(BF16)
        value[q, pl.ds(4 * chip, 4), :, cols] = part.reshape(4, rows, deep_d)

    f = place.f
    mine = [f, near_f, far_f, opposite(near_f)]
    theirs = [far_f, opposite(near_f), f, near_f]
    jobs = [(0, 0), (0, 1), (1, 0), (0, 2), (1, 1), (0, 3), (1, 2), (1, 3)]
    live = scatter_pairs(
        place, Wires(ssend, srecv), value, rc, rd, rx, ry, qbuf, zbuf, make, sum_v,
        Work([lambda: None] * 2 + [pass_on] + [lambda: None] * 3 + [relay.wait_recv]), jobs, mine, theirs,
    )
    gain_term[...] = jnp.zeros_like(gain_term)

    def last(r):
        feed, grad = sum_v[r], cotangent[r].astype(F32)
        back, term = rms_back(feed, gain, grad)
        inverse = lax.rsqrt(jnp.mean(feed * feed, axis=-1, keepdims=True) + EPSILON)
        layer_out[r] = (hidden[r] + feed * inverse * gain).astype(BF16)
        grad_low[r] = back.astype(BF16)
        gain_term[...] += jnp.sum(term, axis=0, keepdims=True)

    by_rows(0, rows, last)
    def turn_back(q, chip):
        slots = pl.ds(2 * chip, 2)
        here = pl.ds(pl.multiple_of(q * n * rows + chip * block, block), block)

        @pl.loop(0, share // step)
        def _(j):
            cols = pl.ds(pl.multiple_of(j * step, step), step)
            a = hs_v[q, slots].reshape(block, width)
            e = dot(a, d_v[cols, :], NT)
            v, u = g_v[here, cols], u_v[here, cols]
            s = 1.0 / (1.0 + jnp.exp(-v))
            dg = e * u * s * (1.0 + v * (1.0 - s))
            du = e * v * s
            i_v[here, cols] = dg.astype(BF16)
            w_v[1, here, cols] = du.astype(BF16)
            gt_v[cols, here] = dg.astype(BF16).T
            ut_v[cols, here] = du.astype(BF16).T

    def keep(q, chip):
        here = pl.ds(pl.multiple_of(q * n * rows + chip * block, block), block)
        moves.start(i_v.at[here], grad_gate.at[here])
        moves.start(w_v.at[1, here], grad_up.at[here])

    def add_term(t):
        q = place.q if t == 0 else 1 - place.q
        tokens = pl.ds(pl.multiple_of(q * n * rows, n * rows), n * rows)

        @pl.loop(0, width // step)
        def _(j):
            cols = pl.ds(pl.multiple_of(j * step, step), step)
            part = dot(t_v[:, tokens], hs_v[q, :, :, cols].reshape(n * rows, step), NN)
            if t == 0:
                acc[:, cols] = part
            else:
                acc[:, cols] += part

    nothing = lambda: None
    hs_v[place.q, place.s] = grad_low[...]
    returned = gather_pairs(
        place, Wires(gsend, grecv), grad_low, hs_v, turn_back,
        Work([nothing, nothing, nothing, lambda: add_term(0)]), keep
    )
    add_term(1)
    for j in range(down_term.shape[0]):
        to = w_v.at[0, pl.ds(j * share, share)]
        to[...] = acc[:, pl.ds(j * deep_d, deep_d)].astype(BF16)
        moves.start(to, down_term.at[j])
    moves.start(gt_v, gate_t)
    moves.start(ut_v, up_t)
    for copy in list(live.values()) + list(returned.values()) + [relay, near_copy, far_copy, up_pass]:
        copy.wait_send()
    moves.finish()


def ffn_feed(h, hidden, gains, cotangent, wg, wu, down_w, n, m, pair, ident):
    rows, width = h.shape
    share, long = wg.shape[1], pair * n * rows
    dma = pltpu.SemaphoreType.DMA
    vmem = pltpu.VMEM
    outs = [
        shape((rows, width), BF16),
        shape((1, width), F32),
        shape((pair, n, rows, width), BF16),
        shape((width, share), BF16),
        shape((long, share), BF16),
        shape((long, share), BF16),
        shape((share, long), BF16),
        shape((share, long), BF16),
        shape((m, share, width // m), BF16),
    ]
    return pl.pallas_call(
        functools.partial(feed_kernel, pair),
        in_specs=vmem_specs(4) + any_specs(3),
        out_specs=vmem_specs(2) + any_specs(7),
        out_shape=outs,
        scratch_shapes=[
            vmem((pair, n, rows, width), BF16),
            vmem((2, width, share), BF16),
            vmem((share, width), BF16),
            vmem((long, share), F32),
            vmem((long, share), F32),
            vmem((long, share), BF16),
            vmem((share, long), BF16),
            vmem((share, long), BF16),
            vmem((share, long), BF16),
            vmem((share, width), F32),
            vmem((rows, width), BF16),
            vmem((rows, width), F32),
            vmem((pair, n, rows, width), BF16),
        ]
        + scatter_scratch(pair, rows, width)
        + [dma((gather_wires(pair),))] * 4
        + [dma((1, 4, 2)), dma((2,)), dma((16 + 4 * pair * n // 2,))],
        compiler_params=kernel_params(ident, 63),
        cost_estimate=pl.CostEstimate(
            flops=10 * long * width * share, bytes_accessed=long * width * 90, transcendentals=0
        ),
        name=f"feed_{ident}",
    )(h, hidden, gains, cotangent, wg, wu, down_w)


def back_kernel(
    pair, gg, gu, wg, wu, gate_t, hs, down_term, branch, gains, cotangent,
    grad_hidden, grad_low, gain_term, down_grad, gate_term,
    a_v, w_v, value, rc, rd, rx, ry, qbuf, zbuf, send, recv,
    gt_v, hs_v, gterm, down_own, down_near, down_total, down_from, dsem, sems
):
    place = Place(pair)
    place.peers.append((place.s, flip(place.f, 1)))
    moves = Moves(sems)
    loads = [moves.start(wg, w_v.at[0]), moves.start(wu, w_v.at[1])]
    loads += [moves.start(gg, a_v.at[0]), moves.start(gu, a_v.at[1])]
    late = []
    down = Settle(place, dsem, down_term, down_own, down_near, down_total, down_from)
    pieces = term_work(gterm, gt_v, hs_v, lambda: moves.wait(late), gate_term, moves)
    idle = [lambda: None]
    work = Work(idle + pieces[:1] + idle + [down.middle] + pieces[1:2] + idle + pieces[2:3] + idle + pieces[3:])
    rows, width = branch.shape
    block = 2 * rows
    n = value.shape[1]
    step = min(256, width)
    place.barrier()
    down.start(True)
    moves.wait(loads)
    late.append(moves.start(gate_t, gt_v))
    for q in range(pair):
        late.append(moves.start(hs.at[q], hs_v.at[q]))

    def make(q, chip, c, at):
        here = pl.ds(pl.multiple_of(q * n * rows + chip * 2 * block, 2 * block), 2 * block)

        @pl.loop(0, width // 4 // step)
        def _(j):
            cols = pl.ds(pl.multiple_of(at + j * step, step), step)
            part = dot(a_v[0, here, :], w_v[0, cols, :], NT) + dot(a_v[1, here, :], w_v[1, cols, :], NT)
            value[q, pl.ds(4 * chip, 4), :, cols] = part.astype(BF16).reshape(4, rows, step)

    live = scatter_pairs(place, Wires(send, recv), value, rc, rd, rx, ry, qbuf, zbuf, make, grad_hidden, work)
    work.rest()
    gain_term[...] = jnp.zeros_like(gain_term)

    def last(r):
        grad = cotangent[r].astype(F32) + grad_hidden[r]
        grad_hidden[r] = grad
        back, term = rms_back(branch[r], gains[2:3, :], grad)
        grad_low[r] = back.astype(BF16)
        gain_term[...] += jnp.sum(term, axis=0, keepdims=True)

    by_rows(0, rows, last)
    share = down_grad.shape[0] // 2

    def store(u, i, value):
        size = value.shape[0]
        down_grad[pl.ds(pl.multiple_of(u * share + i * size, size), size), :] = value

    down.finish(store)
    for copy in live.values():
        copy.wait_send()
    moves.finish()


def ffn_back(gg, gu, wg, wu, gate_t, hs, down_term, branch, gains, cotangent, n, m, pair, ident):
    rows, width = branch.shape
    share, deep = gate_t.shape[0], width // m
    term = down_term.shape
    dma = pltpu.SemaphoreType.DMA
    return pl.pallas_call(
        functools.partial(back_kernel, pair),
        in_specs=any_specs(7) + vmem_specs(3),
        out_specs=vmem_specs(4) + any_specs(1),
        out_shape=[
            shape((rows, width), F32),
            shape((rows, width), BF16),
            shape((1, width), F32),
            shape((2 * share, deep), F32),
            shape(term, BF16),
        ],
        scratch_shapes=[
            pltpu.VMEM((2,) + gg.shape, BF16),
            pltpu.VMEM((2,) + wg.shape, BF16),
            pltpu.VMEM((pair, n, rows, width), BF16),
        ]
        + scatter_scratch(pair, rows, width)
        + [pltpu.VMEM(v.shape, BF16) for v in (gate_t, hs)]
        + [pltpu.VMEM(term, BF16)]
        + settle_scratch(share, deep)
        + [dma((20,))],
        compiler_params=kernel_params(ident, 63),
        cost_estimate=pl.CostEstimate(
            flops=4 * gg.shape[0] * gg.shape[1] * width, bytes_accessed=pair * n * rows * width * 40, transcendentals=0
        ),
        name=f"back_{ident}",
    )(gg, gu, wg, wu, gate_t, hs, down_term, branch, gains, cotangent)


def opposite(f):
    return (f + 2) % 4


class Stream:
    def __init__(self, place, sems):
        self.place, self.sems = place, sems
        f = place.f
        self.half, self.far_f, self.near_f = f // 2, opposite(f), flip(f, 1)
        self.far, self.near = (place.s, self.far_f), (place.s, self.near_f)

    def remote(self, k, step, src, dst, device):
        return pltpu.make_async_remote_copy(
            src, dst, self.sems.at[k, step, 0], self.sems.at[k, step, 1], device_id=device, device_id_type=MESH
        )

    def far_copy(self, k, view, full):
        return self.remote(k, 0, view(1 - self.half), full.at[self.place.f], self.far)

    def near_copy(self, k, view, full):
        return self.remote(k, 1, view(self.half), full.at[self.place.f], self.near)

    def own_copy(self, k, view, full):
        return pltpu.make_async_copy(view(self.half), full.at[self.place.f], self.sems.at[k, 3, 0])

    def relay_copy(self, k, full):
        return self.remote(k, 2, full.at[self.far_f], full.at[self.far_f], self.near)

    def start_far(self, k, view, full):
        self.far_copy(k, view, full).start()

    def start_near(self, k, view, full):
        self.near_copy(k, view, full).start()
        self.own_copy(k, view, full).start()

    def relay(self, k, view, full):
        self.far_copy(k, view, full).wait_recv()
        self.relay_copy(k, full).start()

    def finish(self, k, view, full):
        self.near_copy(k, view, full).wait_recv()
        self.relay_copy(k, full).wait_recv()
        self.own_copy(k, view, full).wait()
        self.far_copy(k, view, full).wait_send()
        self.near_copy(k, view, full).wait_send()
        self.relay_copy(k, full).wait_send()


def half_columns(ref, share):
    return lambda u: ref.at[:, pl.ds(pl.multiple_of(u * share, share), share)]


def half_rows(ref, share):
    return lambda u: ref.at[pl.ds(pl.multiple_of(u * share, share), share), :]


def full_barrier(place, n, near):
    sem = pltpu.get_barrier_semaphore()
    s, f = place.s, place.f
    for d in range(1, n):
        pl.semaphore_signal(sem, inc=1, device_id=((s + d) % n, f), device_id_type=MESH)
    for other in near:
        pl.semaphore_signal(sem, inc=1, device_id=(s, other), device_id_type=MESH)
    pl.semaphore_wait(sem, n - 1 + len(near))


def swap_halves(v):
    return pltpu.roll(v, HD // 2, axis=1)


def to_rows(first, second):
    rows = first.shape[0]
    lane = lax.broadcasted_iota(jnp.int32, (rows, 128), 1)
    wide = jnp.where(lane == 0, first, jnp.where(lane == 1, second, 0.0))
    return wide.T[:8]


def to_columns(v):
    return jnp.concatenate([v, jnp.zeros((120, v.shape[1]), F32)], axis=0).T


def exchange(place, n, own, held, send, recv):
    copies = []
    for d in range(1, n):
        copy = pltpu.make_async_remote_copy(
            own,
            held.at[d - 1],
            send.at[d - 1],
            recv.at[d - 1],
            device_id=((place.s + d) % n, place.f),
            device_id_type=MESH,
        )
        copy.start()
        copies.append(copy)
    total = own[...]
    for d in range(1, n):
        copies[d - 1].wait_recv()
        total = total + held[d - 1]
    return total, copies


def attend(block, q_v, k_v, v_v, out_v, low_v, lt_v, log_v):
    length = q_v.shape[0]
    scale = HD ** (-0.5)

    @pl.loop(0, q_v.shape[1] // HD)
    def _(h):
        cols = pl.ds(pl.multiple_of(h * HD, HD), HD)
        for half in range(2):
            wide = pl.ds(0, (half + 1) * length // 2)

            @pl.loop(half * length // 2 // block, (half + 1) * length // 2 // block)
            def _(i):
                rows = pl.ds(pl.multiple_of(i * block, block), block)
                s = dot(q_v[rows, cols], k_v[wide, cols], NT) * scale
                column = lax.broadcasted_iota(jnp.int32, s.shape, 1)
                row = lax.broadcasted_iota(jnp.int32, s.shape, 0) + i * block
                s = jnp.where(column <= row, s, -jnp.inf)
                top = jnp.max(s, axis=-1, keepdims=True)
                p = jnp.exp(s - top)
                total = jnp.sum(p, axis=-1, keepdims=True)
                out = dot((p * (1.0 / total)).astype(BF16), v_v[wide, cols], NN)
                out_v[rows, cols] = out
                low_v[rows, cols] = out.astype(BF16)
                lt_v[cols, rows] = out.astype(BF16).T
                log_v[h, rows, :] = top + jnp.log(total)


def opening_kernel(
    n, m, x, wq, wk, wv, own_gains, wo_own, gate_w, up_w, down_w,
    qkv, all_gains, tables_out, raw, heads, attended, low_t, xs_t, log_total, inverse, branch_out, hidden_out, low_out, wg, wu, wo,
    tables, branch, hidden, hidden_low, full, xs_v, xt_v, lt_v, w_v, wo_v, raw_v, heads_v, out_v, low_v, log_v, small, held, value,
    rc, rd, rx, ry, qbuf, zbuf, send, recv, ssend, srecv, zsem, osem,
    tsend, trecv, asend, arecv, zsend, zrecv, gsend, grecv, sems,
):
    place = Place(1)
    s, f = place.s, place.f
    rows, width = x.shape
    part = wq.shape[0]
    length, cols = raw.shape[1], raw.shape[2]
    share = wg.shape[2]
    block = min(256, length)
    per = block // rows
    weights = (wq, wk, wv)
    moves = Moves(sems)
    kept = []
    for j, w in enumerate(weights):
        own = w.at[:, pl.ds(pl.multiple_of(s * cols, cols), cols)]
        kept.append(moves.start(own, w_v.at[j, s, f]))
    own_out = [moves.start(wo_own, wo_v.at[f])]
    full[f, s] = own_gains[...]
    xs_v[0, s] = x[...]
    line_barrier(n, m)
    sent = []

    def remote(src, dst, a, b, device):
        copy = pltpu.make_async_remote_copy(src, dst, a, b, device_id=device, device_id_type=MESH)
        copy.start()
        sent.append(copy)
        return copy

    second = []
    for j, w in enumerate(weights):
        row = []
        for d in range(1, n):
            t = (s + d) % n
            src = w.at[:, pl.ds(pl.multiple_of(t * cols, cols), cols)]
            row.append(remote(src, w_v.at[j, s, f], asend.at[j, d], arecv.at[j, d], (t, f)))
        second.append(row)
    first = []
    for d in range(1, n):
        first.append(remote(own_gains, full.at[f, s], gsend.at[d], grecv.at[d], ((s + d) % n, f)))

    def piece(j, o):
        return full.at[o] if j == 3 else w_v.at[j, :, o]

    def hop(way, h, j):
        o = f - h if way == 0 else f + h
        there = f + 1 if way == 0 else f - 1
        place_ = piece(j, o)
        return pltpu.make_async_remote_copy(
            place_, place_, zsend.at[way, h, j], zrecv.at[way, h, j], device_id=(s, there), device_id_type=MESH
        )

    def sends(way, h):
        return ((f - h >= 0) & (f < m - 1)) if way == 0 else ((f + h <= m - 1) & (f > 0))

    def receives(way, h):
        return (f - h - 1 >= 0) if way == 0 else (f + h + 1 <= m - 1)

    def start(h, j):
        for way in (0, 1):
            when(sends(way, h), lambda: hop(way, h, j).start())

    def landed(h, j):
        for way in (0, 1):
            o = f - h - 1 if way == 0 else f + h + 1

            def wait():
                there = f - 1 if way == 0 else f + 1
                place_ = piece(j, o)
                pltpu.make_async_remote_copy(
                    place_, place_, zsend.at[way, h, j], zrecv.at[way, h, j], device_id=(s, there), device_id_type=MESH
                ).wait_recv()

            when(receives(way, h), wait)

    def step(h, j):
        landed(h, j)
        if h + 1 < m - 1:
            start(h + 1, j)

    moves.wait(kept)
    for j in range(3):
        for copy in second[j]:
            copy.wait_recv()
        start(0, j)
    for copy in first:
        copy.wait_recv()
    start(0, 3)
    gathered = gather_pairs(
        place, Wires(tsend, trecv), x, xs_v, lambda *_: None, Work([lambda: None, lambda: step(0, 0), lambda: step(0, 1)])
    )
    step(0, 2)
    step(0, 3)
    half = HD // 2
    lane = lax.broadcasted_iota(jnp.int32, (block, HD), 1)
    row = lax.broadcasted_iota(jnp.int32, (block, HD), 0)
    frequency = jnp.exp((lane % half).astype(F32) * (-2.0 * math.log(THETA) / HD))

    @pl.loop(0, length // block)
    def _(i):
        angle = (row + i * block).astype(F32) * frequency
        here = pl.ds(pl.multiple_of(i * block, block), block)
        tables[0, here, :] = jnp.cos(angle)
        sine = jnp.sin(angle)
        tables[1, here, :] = jnp.where(lane < half, -sine, sine)

    for h in range(1, m - 2):
        for j in range(4):
            step(h, j)

    out_copies = []
    for d, plane in enumerate((flip(f, 1), opposite(f), opposite(flip(f, 1)))):
        out_copies.append(
            pltpu.make_async_remote_copy(
                wo_own, wo_v.at[f], osem.at[0, d], osem.at[1, d], device_id=(s, plane), device_id_type=MESH
            )
        )
        out_copies[-1].start()
    stream = Stream(place, zsem)
    views = [half_columns(gate_w, share), half_columns(up_w, share)]
    fulls = [wg, wu]
    for k in range(2):
        stream.start_far(k, views[k], fulls[k])
    for k in range(2):
        stream.start_near(k, views[k], fulls[k])

    @pl.loop(0, length // block)
    def _(i):
        here = pl.ds(pl.multiple_of(i * block, block), block)
        xt_v[:, here] = xs_v[0, pl.ds(i * per, per)].reshape(block, width).T

    def project(j):
        @pl.loop(0, length // block)
        def _(i):
            here = pl.ds(pl.multiple_of(i * block, block), block)
            a = xs_v[0, pl.ds(i * per, per)].reshape(block, width)
            product = dot(a, w_v[j].reshape(width, cols), NN)
            if j == 2:
                heads_v[2, here, :] = product.astype(BF16)
            else:
                raw_v[j, here, :] = product

    moves.start(xt_v, xs_t)
    for j in range(3):
        landed(m - 2, j)
        project(j)
    landed(m - 2, 3)
    for t in range(n):
        for plane in range(m):
            at = (t * m + plane) * part
            all_gains[:, at : at + part] = full[plane, t, :, :part]
    moves.start(w_v, qkv)

    @pl.loop(0, length // block)
    def _(i):
        here = pl.ds(pl.multiple_of(i * block, block), block)
        q, k = raw_v[0, here, :], raw_v[1, here, :]
        small[0, :, here] = to_rows(
            jnp.sum(q * q, axis=1, keepdims=True), jnp.sum(k * k, axis=1, keepdims=True)
        )

    moves.start(raw_v, raw)
    first_col = pl.multiple_of(s * cols, cols)
    total, stat_copies = exchange(place, n, small.at[0], held, ssend, srecv)
    small[1] = lax.rsqrt(total * (1.0 / width) + EPSILON)
    moves.start(small.at[1], inverse)

    @pl.loop(0, length // block)
    def _(i):
        here = pl.ds(pl.multiple_of(i * block, block), block)
        inv = to_columns(small[1, :, here])
        cosine, sine = tables[0, here, :], tables[1, here, :]
        for j in range(2):
            for h in range(cols // HD):
                part = pl.ds(h * HD, HD)
                v = raw_v[j, here, part] * inv[:, j : j + 1] * all_gains[j : j + 1, pl.ds(first_col + h * HD, HD)]
                heads_v[j, here, part] = (v * cosine + swap_halves(v) * sine).astype(BF16)

    moves.start(heads_v, heads)
    attend(block, heads_v.at[0], heads_v.at[1], heads_v.at[2], out_v, low_v, lt_v, log_v)
    moves.start(out_v, attended)
    moves.start(lt_v, low_t)
    moves.start(log_v, log_total)
    moves.wait(own_out)
    for copy in out_copies:
        copy.wait_recv()
    moves.start(wo_v, wo)
    step = min(512, width)

    def make(q, chip, c, first):
        here = pl.ds(pl.multiple_of(chip * 4 * rows, 4 * rows), 4 * rows)

        @pl.loop(0, width // 2 // step)
        def _(j):
            at = pl.ds(pl.multiple_of(first + j * step, step), step)
            part = dot(low_v[here, :], wo_v[:, :, at].reshape(cols, step), NN).astype(BF16)
            value[q, pl.ds(4 * chip, 4), :, at] = part.reshape(4, rows, step)

    live = scatter_pairs(
        place, Wires(send, recv), value, rc, rd, rx, ry, qbuf, zbuf, make, branch,
        Work([lambda: None, lambda: stream.relay(0, views[0], fulls[0])]),
    )

    def last(r):
        total = branch[r]
        inv = lax.rsqrt(jnp.mean(total * total, axis=-1, keepdims=True) + EPSILON)
        h = x[r].astype(F32) + total * inv * all_gains[2:3, :]
        hidden[r] = h
        hidden_low[r] = h.astype(BF16)

    by_rows(0, rows, last)
    for held_, out_ in ((tables, tables_out), (branch, branch_out), (hidden, hidden_out), (hidden_low, low_out)):
        moves.start(held_, out_)
    for copy in list(live.values()) + list(gathered.values()) + stat_copies + sent:
        copy.wait_send()
    for h in range(m - 1):
        for j in range(4):
            for way in (0, 1):
                when(sends(way, h), lambda: hop(way, h, j).wait_send())
    moves.finish()
    stream.finish(0, views[0], fulls[0])
    for copy in (
        stream.near_copy(1, views[1], fulls[1]),
        stream.far_copy(1, views[1], fulls[1]),
        stream.own_copy(1, views[1], fulls[1]),
    ):
        copy.wait()
    for copy in out_copies:
        copy.wait_send()


def opening(x, wq, wk, wv, gains, wo, gate_w, up_w, down_w, n, m, ident):
    rows, width = x.shape
    part, cols = wq.shape[0], width // n
    length, share = n * rows, gate_w.shape[1] // 2
    dma = pltpu.SemaphoreType.DMA
    heads = cols // HD
    outs = [
        shape((3, n, m, part, cols), BF16),
        shape((gains.shape[0], width), F32),
        shape((2, length, HD), F32),
        shape((2, length, cols), F32),
        shape((3, length, cols), BF16),
        shape((length, cols), F32),
        shape((cols, length), BF16),
        shape((width, length), BF16),
        shape((heads, length, 1), F32),
        shape((8, length), F32),
        shape((rows, width), F32),
        shape((rows, width), F32),
        shape((rows, width), BF16),
        shape((m, gate_w.shape[0], share), BF16),
        shape((m, gate_w.shape[0], share), BF16),
        shape((m,) + wo.shape, BF16),
    ]
    return pl.pallas_call(
        functools.partial(opening_kernel, n, m),
        in_specs=vmem_specs(5) + any_specs(4),
        out_specs=any_specs(1) + vmem_specs(1) + any_specs(14),
        out_shape=outs,
        scratch_shapes=[
            pltpu.VMEM((2, length, HD), F32),
            pltpu.VMEM((rows, width), F32),
            pltpu.VMEM((rows, width), F32),
            pltpu.VMEM((rows, width), BF16),
            pltpu.VMEM((m, n) + gains.shape, F32),
            pltpu.VMEM((1, n, rows, width), BF16),
            pltpu.VMEM((width, length), BF16),
            pltpu.VMEM((cols, length), BF16),
            pltpu.VMEM((3, n, m, part, cols), BF16),
            pltpu.VMEM((m,) + wo.shape, BF16),
            pltpu.VMEM((2, length, cols), F32),
            pltpu.VMEM((3, length, cols), BF16),
            pltpu.VMEM((length, cols), F32),
            pltpu.VMEM((length, cols), BF16),
            pltpu.VMEM((heads, length, 1), F32),
            pltpu.VMEM((2, 8, length), F32),
            pltpu.VMEM((n - 1, 8, length), F32),
            pltpu.VMEM((1, n, rows, width), BF16),
        ]
        + scatter_scratch(1, rows, width)
        + [dma((n - 1,)), dma((n - 1,)), dma((2, 4, 2)), dma((2, m))]
        + [dma((gather_wires(1),))] * 2
        + [dma((3, n))] * 2
        + [dma((2, m, 4))] * 2
        + [dma((n,))] * 2
        + [dma((24,))],
        compiler_params=kernel_params(ident),
        cost_estimate=pl.CostEstimate(flops=10**10, bytes_accessed=200 * 2**20, transcendentals=0),
        name=f"opening_{ident}",
    )(x, wq, wk, wv, gains, wo, gate_w, up_w, down_w)


class Settle:
    def __init__(self, place, sems, term, own, near, total, far):
        self.place, self.sems, self.term, self.own = place, sems, term, own
        self.near, self.total, self.far = near, total, far
        f = place.f
        self.f = f
        self.odd, self.half = f % 2, f // 2

    def remote(self, step, src, dst, plane):
        return pltpu.make_async_remote_copy(
            src, dst, self.sems.at[step, 0], self.sems.at[step, 1], device_id=(self.place.s, plane), device_id_type=MESH
        )

    def given(self, i):
        return 1 - self.odd + 2 * i

    def kept(self, i):
        return self.odd + 2 * i

    def near_copy(self, step):
        i = 1 - self.half if step == 0 else self.half
        return self.remote(step, self.term.at[self.given(i)], self.near.at[i], flip(self.f, 1))

    def far_copy(self):
        return self.remote(2, self.total.at[0], self.far, opposite(self.f))

    def load(self, i):
        return pltpu.make_async_copy(self.term.at[self.kept(i)], self.own.at[i], self.sems.at[3, i])

    def start(self, both=False):
        self.near_copy(0).start()
        self.both = both
        if both:
            self.near_copy(1).start()
        for i in (0, 1):
            self.load(i).start()

    def mine(self, i):
        return self.term.at[self.kept(i)] if self.own is None else self.own.at[i]

    def chunks(self, body):
        size = 128

        @pl.loop(0, self.far.shape[0] // size)
        def _(i):
            body(i, pl.ds(pl.multiple_of(i * size, size), size))

    def middle(self):
        if self.own is not None:
            for i in (0, 1):
                self.load(i).wait()
        self.near_copy(0).wait_recv()
        other = 1 - self.half
        mine = self.mine(other)

        def body(i, r):
            self.total[0, r] = add(mine[r], self.near[other, r])

        self.chunks(body)
        self.far_copy().start()
        if not self.both:
            self.near_copy(1).start()

    def finish(self, store):
        half = self.half
        self.near_copy(1).wait_recv()
        mine = self.mine(half)
        self.chunks(lambda i, r: store(half, i, mine[r].astype(F32) + self.near[half, r].astype(F32)))
        self.far_copy().wait_recv()
        self.chunks(lambda i, r: store(1 - half, i, self.far[r].astype(F32)))
        for step in (0, 1):
            self.near_copy(step).wait_send()
        self.far_copy().wait_send()


def settle_scratch(share, depth, own=True):
    block = lambda *lead: pltpu.VMEM(lead + (share, depth), BF16)
    return ([block(2)] if own else []) + [block(2), block(1), block(), pltpu.SemaphoreType.DMA((4, 2))]


def term_block(term, left, right, block):
    deep, long = term.shape[2], left.shape[1]
    step = min(256, deep)

    @pl.loop(0, deep // step)
    def _(j):
        at = pl.ds(pl.multiple_of((0 if right.shape[3] == deep else block * deep) + j * step, step), step)
        to = pl.ds(pl.multiple_of(j * step, step), step)
        term[block, :, to] = dot(left[...], right[:, :, :, at].reshape(long, step), NN).astype(BF16)


class Work:
    def __init__(self, pieces):
        self.pieces = list(pieces)

    def __call__(self):
        if self.pieces:
            self.pieces.pop(0)()

    def rest(self):
        while self.pieces:
            self()


def term_work(term, left, right, prepare, out, moves):
    def piece(block):
        def run():
            if block == 0:
                prepare()
            term_block(term, left, right, block)
            moves.start(term.at[block], out.at[block])

        return run

    return [piece(block) for block in range(term.shape[0])]


def turn(v, cosine, sine):
    return v * cosine + swap_halves(v) * sine


def attend_back(block, q_v, k_v, v_v, out_v, log_v, g_v, dq, dk, dv):
    length = q_v.shape[0]
    scale = HD ** (-0.5)
    dk[...] = jnp.zeros_like(dk)
    dv[...] = jnp.zeros_like(dv)

    @pl.loop(0, q_v.shape[1] // HD)
    def _(h):
        cols = pl.ds(pl.multiple_of(h * HD, HD), HD)
        for half in range(2):
            wide = pl.ds(0, (half + 1) * length // 2)

            @pl.loop(half * length // 2 // block, (half + 1) * length // 2 // block)
            def _(i):
                rows = pl.ds(pl.multiple_of(i * block, block), block)
                q, g = q_v[rows, cols], g_v[rows, cols]
                s = dot(q, k_v[wide, cols], NT) * scale
                column = lax.broadcasted_iota(jnp.int32, s.shape, 1)
                row = lax.broadcasted_iota(jnp.int32, s.shape, 0) + i * block
                s = jnp.where(column <= row, s, -jnp.inf)
                weights = jnp.exp(s - log_v[h, rows, :])
                correction = jnp.sum(g.astype(F32) * out_v[rows, cols], axis=-1, keepdims=True)
                gw = dot(g, v_v[wide, cols], NT)
                gs = (weights * (gw - correction)).astype(BF16)
                dq[rows, cols] = dot(gs, k_v[wide, cols], NN) * scale
                dk[wide, cols] += dot(gs, q, TN) * scale
                dv[wide, cols] += dot(weights.astype(BF16), g, TN)


def closing_kernel(
    g, gains, tables, inverse, branch_gain, feed_gain,
    wo, raw, heads, attended, low_t, log_total, xs_t, gate_term, up_t, hs, qkv, grad_hidden_,
    gate_out, up_out, tokens_out, weight_grad, gain_grad,
    gate_grad, up_grad, tokens_grad, bs, wo_v, raw_v, heads_v, out_v, low_v, log_v, ga_v, dq, dk, dv, d_v, xs_v, term_v, small, held, gain_term,
    ut_v, hs_v, up_term, gown, gnear, gtotal, gfar, gsem, unear, utotal, ufar, usem,
    grad_hidden, w_v, rc, rd, rx, ry, qbuf, zbuf, tsend, trecv, line, done, got, gbuf, gplane, gsum, gline,
    send, recv, ssend, srecv, zsend, zrecv, asend, arecv, qsend, qrecv, lsend, lrecv, sems,
):
    place = Place(1)
    n, m = bs.shape[1], wo.shape[0]
    rows, width = g.shape
    length, cols = raw.shape[1], raw.shape[2]
    share = gate_term.shape[1]
    first_col = pl.multiple_of(place.s * cols, cols)
    moves = Moves(sems)
    second = [moves.start(wo, wo_v)]
    fourth = [
        moves.start(heads, heads_v),
        moves.start(attended, out_v),
        moves.start(log_total, log_v),
        moves.start(low_t, low_v),
        moves.start(raw, raw_v),
        moves.start(xs_t, xs_v),
    ]
    moves.start(qkv, w_v)
    moves.start(grad_hidden_, grad_hidden)
    bs[0, place.s] = g[...]
    line_barrier(n, m)
    gate = Settle(place, gsem, gate_term, gown, gnear, gtotal, gfar)
    up = Settle(place, usem, up_term, None, unear, utotal, ufar)
    gate.start()
    late = [moves.start(up_t, ut_v)]
    deep = gate_term.shape[2]
    blocks = (up.given(1 - up.half), up.kept(1 - up.half), up.given(up.half), up.kept(up.half))

    def fetch(i):
        at = pl.ds(pl.multiple_of(blocks[i] * deep, deep), deep)
        late.extend(moves.start(hs.at[q, :, :, at], hs_v.at[q]) for q in range(hs.shape[0]))

    fetch(0)

    up.both = False

    def up_block(i):
        moves.wait(late)
        late.clear()
        term_block(up_term, ut_v, hs_v, blocks[i])
        if i == 0:
            up.near_copy(0).start()
        if i < 3:
            fetch(i + 1)

    block = min(256, length)

    def ready(q, chip):
        here = pl.ds(pl.multiple_of(chip * 2 * rows, 2 * rows), 2 * rows)
        a = bs[0, pl.ds(2 * chip, 2)].reshape(2 * rows, width)
        ga_v[here, :] = dot(a, wo_v[...].reshape(cols, width), NT).astype(BF16)

    moves.wait(second)
    gathered = gather_pairs(place, Wires(send, recv), g, bs, ready, Work([lambda: up_block(0), lambda: up_block(1), gate.middle]))
    up_block(2)
    up.middle()
    moves.wait(fourth)
    up_block(3)
    attend_back(block, heads_v.at[0], heads_v.at[1], heads_v.at[2], out_v, log_v, ga_v, dq, dk, dv)
    @pl.loop(0, length // block)
    def _(i):
        here = pl.ds(pl.multiple_of(i * block, block), block)
        inv = to_columns(inverse[:, here])
        cosine, sine = tables[0, here, :], -tables[1, here, :]
        sums = []
        for j, d in enumerate((dq, dk)):
            total = jnp.zeros((block, 1), F32)
            for h in range(cols // HD):
                part = pl.ds(h * HD, HD)
                normal = raw_v[j, here, part] * inv[:, j : j + 1]
                v = turn(d[here, part].astype(BF16).astype(F32), cosine, sine)
                raw_v[j, here, part] = normal
                gained = v * gains[j : j + 1, pl.ds(first_col + h * HD, HD)]
                total = total + jnp.sum(gained * normal, axis=1, keepdims=True)
                term_sum = jnp.sum(v * normal, axis=0, keepdims=True)
                d[here, part] = gained

                @pl.when(i == 0)
                def _():
                    gain_term[j, :, part] = term_sum

                @pl.when(i > 0)
                def _():
                    gain_term[j, :, part] += term_sum

            sums.append(total)
        small[0, :, here] = to_rows(sums[0], sums[1])
        d_v[2, here, :] = dv[here, :].astype(BF16)

    total, stat_copies = exchange(place, n, small.at[0], held, ssend, srecv)
    small[1] = total * (1.0 / width)

    @pl.loop(0, length // block)
    def _(i):
        here = pl.ds(pl.multiple_of(i * block, block), block)
        inv = to_columns(inverse[:, here])
        mean = to_columns(small[1, :, here])
        for j, d in enumerate((dq, dk)):
            d_v[j, here, :] = (
                inv[:, j : j + 1] * (d[here, :] - raw_v[j, here, :] * mean[:, j : j + 1])
            ).astype(BF16)


    @pl.loop(0, n)
    def _(i):
        at = pl.ds(pl.multiple_of(i * cols, cols), cols)
        part = dot(low_v[...], bs[0, :, :, at].reshape(length, cols), NN)
        term_v[3, i] = part.astype(BF16).reshape(m, cols // m, cols)
        for j in range(3):
            part = dot(xs_v[at, :], d_v[j], NN)
            term_v[j, i] = part.astype(BF16).reshape(m, cols // m, cols)


    def store(ref):
        def put(u, i, value):
            size = value.shape[0]
            ref[:, pl.ds(pl.multiple_of(u * share + i * size, size), size)] = value.T

        return put

    last = m - 1
    s, f, term, d3 = place.s, place.f, term_v, d_v
    for copy in gathered.values():
        copy.wait_send()

    def remote(src, dst, a, b, device):
        return pltpu.make_async_remote_copy(src, dst, a, b, device_id=device, device_id_type=MESH)

    def target(way, r):
        return last - r if way == 0 else r

    def hop(way, r, j, fresh):
        there = f + 1 if way == 0 else f - 1
        src = term.at[j, :, target(way, r)] if fresh else line.at[way, r, j]
        return remote(src, line.at[way, r, j], zsend.at[way, r, j], zrecv.at[way, r, j], (s, there))

    ends = (f == 0, f == last)
    inner = (f > 0, f < last)

    def beyond(way, r):
        return target(way, r) > f if way == 0 else target(way, r) < f

    for group in ((0, 1, 2), (3,)):
        for r in range(last):
            for j in group:
                for way in (0, 1):
                    when(ends[way], lambda: hop(way, r, j, True).start())

    gain_copies = []
    for t in range(n):
        at = pl.ds(t * cols, cols)
        for j in range(2):
            gbuf[t, j : j + 1, :] = jnp.where(s == t, gain_term[j], 0.0)
        gbuf[t, 2:3, :] = branch_gain[:, at]
        gbuf[t, 3:4, :] = feed_gain[:, at]
        gbuf[t, 4:, :] = jnp.zeros((4, cols), F32)
    for d in range(1, n):
        t = (s + d) % n
        copy = remote(gbuf.at[t], gplane.at[d - 1], qsend.at[d], qrecv.at[d], (t, f))
        copy.start()
        gain_copies.append(copy)

    moves.finish()
    block, step = 4 * rows, min(512, width)
    per = step // (m * qkv.shape[3])

    def make(q, chip, c, first):
        here = pl.ds(pl.multiple_of(chip * block, block), block)

        @pl.loop(0, width // 2 // step)
        def _(k):
            i = first // step + k
            at = pl.ds(pl.multiple_of(i * step, step), step)
            total = jnp.zeros((block, step), F32)
            for j in range(3):
                w = w_v[j, pl.ds(i * per, per)].reshape(step, cols)
                total = total + dot(d3[j, here, :], w, NT)
            bs[q, pl.ds(4 * chip, 4), :, at] = total.astype(BF16).reshape(4, rows, step)

    side = f // (m // 2)
    middle = (f > 0) & (f < last)

    def relays(k, j, from_end):
        way = side if from_end else 1 - side
        o = way * k + (1 - way) * (last - k)

        def relay():
            there = f + 1 - 2 * way
            copy = remote(
                line.at[way, k, j], line.at[way, k, j], zsend.at[way, k, j], zrecv.at[way, k, j], (s, there)
            )
            copy.wait_recv()
            line[way, k, j] = add(term[j, :, o], line[way, k, j])
            copy.start()

        when(middle, relay)

    live = scatter_pairs(
        place, Wires(tsend, trecv), bs, rc, rd, rx, ry, qbuf, zbuf, make, tokens_grad,
    )

    def join(r):
        tokens_grad[r] += grad_hidden[r]

    by_rows(0, rows, join)
    moves.start(tokens_grad, tokens_out)
    gate.finish(store(gate_grad))
    moves.start(gate_grad, gate_out)
    up.finish(store(up_grad))
    moves.start(up_grad, up_out)

    total = gbuf[s]
    for d in range(1, n):
        gain_copies[d - 1].wait_recv()
        total = total + gplane[d - 1]
    gsum[...] = total
    line_copies = []
    for d in range(1, m):
        t = (f + d) % m
        copy = remote(gsum, gline.at[d - 1], lsend.at[d], lrecv.at[d], (s, t))
        copy.start()
        line_copies.append(copy)

    copies = []
    plan = [(True, k, j) for k in range(m // 2) for j in range(3)]
    plan += [(False, k, j) for k in range(m // 2 - 1) for j in range(3)] + [(None, 0, j) for j in range(3)]
    plan += [(True, k, 3) for k in range(m // 2)] + [(False, k, 3) for k in range(m // 2 - 1)] + [(None, 0, 3)]
    for from_end, k, j in plan:
        if from_end is not None:
            relays(k, j, from_end)
            continue
        own = term[j, :, f].astype(F32)
        done[...] = own
        for way in (0, 1):
            r = last - f if way == 0 else f

            def take():
                pltpu.make_async_remote_copy(
                    line.at[way, 0, j],
                    line.at[way, r, j],
                    zsend.at[way, r, j],
                    zrecv.at[way, r, j],
                    device_id=(s, f - 1 if way == 0 else f + 1),
                    device_id_type=MESH,
                ).wait_recv()
                done[...] += line[way, r, j].astype(F32)

            when(inner[way], take)
        if j == 3:
            for t in range(n):
                weight_grad[j, :, pl.ds(t * cols, cols)] = done[t]
            continue
        weight_grad[j, :, pl.ds(pl.multiple_of(s * cols, cols), cols)] = done[s]
        got[0, j] = done[...].astype(BF16)
        for d in range(1, n):
            t = (s + d) % n
            copy = remote(got.at[0, j, t], got.at[1, j, s], asend.at[j, d], arecv.at[j, d], (t, f))
            copy.start()
            copies.append(copy)
    total = gsum[...]
    for d in range(1, m):
        line_copies[d - 1].wait_recv()
        total = total + gline[d - 1]
    thin = cols // m
    gain = jnp.zeros((8, thin), F32)
    for plane in range(m):
        gain = gain + jnp.where(f == plane, total[:, plane * thin : (plane + 1) * thin], 0.0)
    gain_grad[...] = gain
    for copy in copies:
        copy.wait_recv()
    for j in range(3):
        for d in range(1, n):
            t = (s + d) % n
            weight_grad[j, :, pl.ds(pl.multiple_of(t * cols, cols), cols)] = got[1, j, t].astype(F32)
    for copy in copies + gain_copies + line_copies + list(live.values()) + stat_copies:
        copy.wait_send()
    for r in range(last):
        for j in range(4):
            for way in (0, 1):
                when(ends[way] | (inner[way] & beyond(way, r)), lambda: hop(way, r, j, False).wait_send())
    moves.finish()


def closing(
    g, gains, tables, inverse, branch_gain, feed_gain,
    wo, raw, heads, attended, low_t, log_total, xs_t, gate_term, up_t, hs, qkv, grad_hidden, n, ident,
):
    rows, width = g.shape
    m = wo.shape[0]
    length, cols = raw.shape[1], raw.shape[2]
    share, deep, part = gate_term.shape[1], width // m, cols // m
    dma = pltpu.SemaphoreType.DMA
    vmem = pltpu.VMEM
    piece = (n, m, part, cols)
    return pl.pallas_call(
        closing_kernel,
        in_specs=vmem_specs(6) + any_specs(12),
        out_specs=any_specs(3) + vmem_specs(2),
        out_shape=[
            shape((deep, 2 * share), F32),
            shape((deep, 2 * share), F32),
            shape((rows, width), F32),
            shape((4, part, width), F32),
            shape((8, part), F32),
        ],
        scratch_shapes=[
            vmem((deep, 2 * share), F32),
            vmem((deep, 2 * share), F32),
            vmem((rows, width), F32),
            vmem((1, n, rows, width), BF16),
            vmem(wo.shape, BF16),
            vmem(raw.shape, F32),
            vmem(heads.shape, BF16),
            vmem(attended.shape, F32),
            vmem(low_t.shape, BF16),
            vmem(log_total.shape, F32),
            vmem((length, cols), BF16),
            vmem((length, cols), F32),
            vmem((length, cols), F32),
            vmem((length, cols), F32),
            vmem((3, length, cols), BF16),
            vmem(xs_t.shape, BF16),
            vmem((4,) + piece, BF16),
            vmem((2, 8, length), F32),
            vmem((n - 1, 8, length), F32),
            vmem((2, 1, cols), F32),
            vmem(up_t.shape, BF16),
            vmem(hs.shape[:3] + (deep,), BF16),
            vmem(gate_term.shape, BF16),
        ]
        + settle_scratch(share, deep)
        + settle_scratch(share, deep, False)
        + [vmem((rows, width), F32), vmem((3,) + piece, BF16)]
        + scatter_scratch(1, rows, width)
        + [
            vmem((2, m - 1, 4, n, part, cols), BF16),
            vmem((n, part, cols), F32),
            vmem((2, 3, n, part, cols), BF16),
            vmem((n, 8, cols), F32),
            vmem((n - 1, 8, cols), F32),
            vmem((8, cols), F32),
            vmem((m - 1, 8, cols), F32),
            dma((gather_wires(1),)),
            dma((gather_wires(1),)),
            dma((n - 1,)),
            dma((n - 1,)),
        ]
        + [dma((2, m, 4))] * 2
        + [dma((3, n))] * 2
        + [dma((n,))] * 2
        + [dma((m,))] * 2
        + [dma((24,))],
        compiler_params=kernel_params(ident, 63),
        cost_estimate=pl.CostEstimate(flops=10**10, bytes_accessed=400 * 2**20, transcendentals=0),
        name=f"closing_{ident}",
    )(
        g, gains, tables, inverse, branch_gain, feed_gain,
        wo, raw, heads, attended, low_t, log_total, xs_t, gate_term, up_t, hs, qkv, grad_hidden,
    )


def attention_forward_kernel(block, q_ref, k_ref, v_ref, out_ref, low_ref, log_ref):
    length = q_ref.shape[0]
    scale = HD ** (-0.5)
    for i in range(length // block):
        rows = pl.ds(i * block, block)
        width = (i + 1) * block
        s = dot(q_ref[rows, :], k_ref[pl.ds(0, width), :], NT) * scale
        column = lax.broadcasted_iota(jnp.int32, (block, width), 1)
        row = lax.broadcasted_iota(jnp.int32, (block, width), 0) + i * block
        s = jnp.where(column <= row, s, -jnp.inf)
        top = jnp.max(s, axis=-1, keepdims=True)
        p = jnp.exp(s - top)
        total = jnp.sum(p, axis=-1, keepdims=True)
        weights = (p * (1.0 / total)).astype(BF16)
        out = dot(weights, v_ref[pl.ds(0, width), :], NN)
        out_ref[rows, :] = out
        low_ref[rows, :] = out.astype(BF16)
        log_ref[0, rows, :] = top + jnp.log(total)


def attention_forward(q, k, v):
    length, width = q.shape
    heads = width // HD
    block = min(256, length)
    column = pl.BlockSpec((length, HD), lambda h: (0, h))
    return pl.pallas_call(
        functools.partial(attention_forward_kernel, block),
        grid=(heads,),
        in_specs=[column] * 3,
        out_specs=[column, column, pl.BlockSpec((1, length, 1), lambda h: (h, 0, 0))],
        out_shape=[
            jax.ShapeDtypeStruct((length, width), F32),
            jax.ShapeDtypeStruct((length, width), BF16),
            jax.ShapeDtypeStruct((heads, length, 1), F32),
        ],
        cost_estimate=pl.CostEstimate(
            flops=2 * heads * length * length * HD, bytes_accessed=10 * length * width, transcendentals=0
        ),
    )(q, k, v)


def attention_backward_kernel(block, q_ref, k_ref, v_ref, out_ref, log_ref, g_ref, dq_ref, dk_ref, dv_ref, dk, dv):
    length = q_ref.shape[0]
    scale = HD ** (-0.5)
    dk[...] = jnp.zeros_like(dk)
    dv[...] = jnp.zeros_like(dv)
    for i in range(length // block):
        rows = pl.ds(i * block, block)
        width = (i + 1) * block
        wide = pl.ds(0, width)
        q = q_ref[rows, :]
        g = g_ref[rows, :]
        s = dot(q, k_ref[wide, :], NT) * scale
        column = lax.broadcasted_iota(jnp.int32, (block, width), 1)
        row = lax.broadcasted_iota(jnp.int32, (block, width), 0) + i * block
        s = jnp.where(column <= row, s, -jnp.inf)
        weights = jnp.exp(s - log_ref[0, rows, :])
        correction = jnp.sum(g.astype(F32) * out_ref[rows, :], axis=-1, keepdims=True)
        gw = dot(g, v_ref[wide, :], NT)
        gs = (weights * (gw - correction)).astype(BF16)
        dq_ref[rows, :] = (dot(gs, k_ref[wide, :], NN) * scale).astype(BF16)
        dk[wide, :] += dot(gs, q, TN)
        dv[wide, :] += dot(weights.astype(BF16), g, TN)
    dk_ref[...] = (dk[...] * scale).astype(BF16)
    dv_ref[...] = dv[...].astype(BF16)


def attention_backward(q, k, v, out, log_total, g):
    length, width = q.shape
    heads = width // HD
    block = min(256, length)
    column = pl.BlockSpec((length, HD), lambda h: (0, h))
    return pl.pallas_call(
        functools.partial(attention_backward_kernel, block),
        grid=(heads,),
        in_specs=[column] * 4 + [pl.BlockSpec((1, length, 1), lambda h: (h, 0, 0)), column],
        out_specs=[column] * 3,
        out_shape=[jax.ShapeDtypeStruct((length, width), BF16)] * 3,
        scratch_shapes=[pltpu.VMEM((length, HD), F32)] * 2,
        cost_estimate=pl.CostEstimate(
            flops=5 * heads * length * length * HD, bytes_accessed=16 * length * width, transcendentals=0
        ),
    )(q, k, v, out, log_total, g)


def on_device(n, m, pair, *args):
    (
        tokens,
        query_weight,
        key_weight,
        value_weight,
        out_weight,
        query_gain,
        key_gain,
        attention_gain,
        gate_weight,
        up_weight,
        down_weight,
        feedforward_gain,
        cotangent,
    ) = args
    rows, width = tokens.shape[1], tokens.shape[2]
    length = rows * n
    part = query_weight.shape[0]
    cols = width // n
    depth, units = gate_weight.shape
    share = units // pair
    x = tokens.reshape(rows, width)
    groups = [[g * pair + u for u in range(pair)] for g in range(m // pair)]

    native = n == 8 and m == 4

    def gather_plane(v, ident):
        if native:
            return plane_gather(v, n, 1, ident)
        return lax.all_gather(v, "seq", axis=0, tiled=True)

    def scatter_plane(v, ident):
        if native:
            return plane_scatter(v, n, 1, ident)
        return lax.psum_scatter(v.astype(BF16), "seq", scatter_dimension=0, tiled=True).astype(F32)

    def gather_pair(v, ident):
        if native:
            return plane_gather(v, n, pair, ident)
        if pair > 1:
            v = lax.all_gather(v, "fsdp", axis=0, axis_index_groups=groups)
        v = lax.all_gather(v.reshape(pair, rows, width), "seq", axis=1, tiled=True)
        return v.reshape(pair * length, width)

    def scatter_pair(v, ident):
        if native:
            return plane_scatter(v, n, pair, ident)
        v = lax.psum_scatter(v.astype(BF16).reshape(pair, length, width), "seq", scatter_dimension=1, tiled=True)
        if pair > 1:
            v = lax.psum_scatter(v, "fsdp", scatter_dimension=0, axis_index_groups=groups)
        return v.reshape(rows, width).astype(F32)

    def total_plane(v, ident):
        return plane_sum(v, n, ident) if native else lax.psum(v, "seq")

    def spread(halves):
        return lax.all_to_all(jnp.tile(halves, (m // pair, 1, 1)), "fsdp", 0, 0, tiled=False)

    def settle(blocks):
        back = lax.all_to_all(blocks.astype(BF16), "fsdp", 0, 0, tiled=False)
        if native:
            return jnp.sum(back.reshape((pair, m // pair) + back.shape[1:]).astype(F32), axis=1)
        return jnp.sum(back.reshape((m // pair, pair) + back.shape[1:]).astype(F32), axis=0)

    gains = jnp.stack([query_gain, key_gain, attention_gain, feedforward_gain]).astype(F32)
    grad_out = cotangent.reshape(rows, width)
    if native:
        (
            qkv, gains, tables, raw, heads, attended, low_t, xs_t, log_total, inverse, branch, hidden, hidden_low,
            gate_cols, up_cols, out_rows,
        ) = opening(
            x, query_weight, key_weight, value_weight, jnp.pad(gains, ((0, 4), (0, 128 - part))),
            out_weight, gate_weight, up_weight, down_weight, n, m, 1
        )
        gate_cols = gate_cols.reshape(width, share)
        layer_out, feed_gain_term, hs, up_cols, grad_gate, grad_up, gate_t, up_t, down_term = ffn_feed(
            hidden_low, hidden, gains, grad_out, gate_cols, up_cols, down_weight, n, m, pair, 5
        )
        grad_hidden, branch_low, branch_gain_term, down_grad, gate_term = ffn_back(
            grad_gate, grad_up, gate_cols, up_cols, gate_t, hs, down_term, branch, gains, grad_out, n, m, pair, 8
        )
        gate_grad, up_grad, tokens_grad, term, gain_grads = closing(
            branch_low, gains, tables, inverse, branch_gain_term, feed_gain_term,
            out_rows, raw, heads, attended, low_t, log_total, xs_t, gate_term, up_t, hs, qkv, grad_hidden, n, 2
        )
        layer_out, tokens_grad, *term, gate_grad, up_grad, down_grad = place_outputs(
            [layer_out, tokens_grad, term, gate_grad, up_grad, down_grad]
        )
        out_grad = term[3]
    else:
        cosine, sine = angles_of(length)
        seq = lax.axis_index("seq")
        stacked = jnp.stack([query_weight, key_weight, value_weight]).reshape(3, part, n, cols)
        mine = lax.all_to_all(stacked.transpose(2, 0, 1, 3), "seq", 0, 0)
        qkv = lax.all_gather(mine, "fsdp", axis=1).transpose(2, 0, 1, 3, 4).reshape(3, width, cols)
        full_gain = lax.all_gather(gains, ("seq", "fsdp"), axis=1).reshape(4, width)
        xs = gather_plane(x, 1)
        out_rows = lax.all_gather(out_weight, "fsdp", axis=0, tiled=True)
        own_gain = lax.dynamic_slice_in_dim(full_gain[:2], seq * cols, cols, 1)
        q_gain, k_gain, branch_gain, feed_gain = own_gain[0], own_gain[1], full_gain[2], full_gain[3]
        q_raw, k_raw, v = dot(xs, qkv[0], NN), dot(xs, qkv[1], NN), dot(xs, qkv[2], NN).astype(BF16)
        squares = jnp.stack([jnp.sum(q_raw * q_raw, axis=1), jnp.sum(k_raw * k_raw, axis=1)])
        inverse = lax.rsqrt(lax.psum(squares, "seq") / width + EPSILON)
        q_inv, k_inv = inverse[0][:, None], inverse[1][:, None]
        q = rotate(q_raw * q_inv * q_gain, cosine, sine, 1.0).astype(BF16)
        k = rotate(k_raw * k_inv * k_gain, cosine, sine, 1.0).astype(BF16)
        attended, attended_low, log_total = attention_forward(q, k, v)
        branch = scatter_plane(dot(attended_low, out_rows, NN), 3)
        branch_inv = lax.rsqrt(jnp.mean(branch * branch, axis=1, keepdims=True) + EPSILON)
        hidden = x.astype(F32) + branch * branch_inv * branch_gain
        hidden_low = hidden.astype(BF16)
        gate_cols = spread(gate_weight.reshape(depth, pair, share).transpose(1, 0, 2)).reshape(width, share)
        up_cols = spread(up_weight.reshape(depth, pair, share).transpose(1, 0, 2)).reshape(width, share)
        down_rows = spread(down_weight.reshape(pair, share, depth)).transpose(1, 0, 2).reshape(share, width)
        grad_out = grad_out.astype(F32)
        hs = gather_pair(hidden_low, 5)
        gate = dot(hs, gate_cols, NN)
        up = dot(hs, up_cols, NN)
        sig = jax.nn.sigmoid(gate)
        inner = (gate * sig * up).astype(BF16)
        feed = scatter_pair(dot(inner, down_rows, NN), 7)
        feed_inv = lax.rsqrt(jnp.mean(feed * feed, axis=1, keepdims=True) + EPSILON)
        layer_out = (hidden + feed * feed_inv * feed_gain).astype(BF16)
        grad_feed, term = rms_back(feed, feed_gain, grad_out)
        feed_gain_term = jnp.sum(term, axis=0)
        gs = gather_pair(grad_feed.astype(BF16), 6)
        grad_inner = dot(gs, down_rows, NT)
        grad_gate = (grad_inner * up * sig * (1.0 + gate * (1.0 - sig))).astype(BF16)
        grad_up = (grad_inner * gate * sig).astype(BF16)
        grad_hidden = grad_out + scatter_pair(dot(grad_gate, gate_cols, NT) + dot(grad_up, up_cols, NT), 8)
        grad_branch, term = rms_back(branch, branch_gain, grad_hidden)
        branch_low = grad_branch.astype(BF16)
        branch_gain_term = jnp.sum(term, axis=0)
        inner_t, gate_t, up_t = inner.T, grad_gate.T, grad_up.T

        def cut(v):
            return v.reshape(share, m, depth).transpose(1, 0, 2)

        down_grad = settle(cut(dot(inner_t, gs, NN))).reshape(units, depth)
        gate_grad = settle(cut(dot(gate_t, hs, NN))).transpose(2, 0, 1).reshape(depth, units)
        up_grad = settle(cut(dot(up_t, hs, NN))).transpose(2, 0, 1).reshape(depth, units)
        bs = gather_plane(branch_low, 2)
        out_grad = lax.psum_scatter(
            dot(attended_low, bs, TN).astype(BF16), "fsdp", scatter_dimension=0, tiled=True
        ).astype(F32)
        grad_attended = dot(bs, out_rows, NT).astype(BF16)
        dq, dk, dv = attention_backward(q, k, v, attended, log_total, grad_attended)
        dq = rotate(dq.astype(F32), cosine, sine, -1.0)
        dk = rotate(dk.astype(F32), cosine, sine, -1.0)
        q_normal, k_normal = q_raw * q_inv, k_raw * k_inv
        q_gain_term = jnp.sum(dq * q_normal, axis=0)
        k_gain_term = jnp.sum(dk * k_normal, axis=0)
        dq, dk = dq * q_gain, dk * k_gain
        means = total_plane(jnp.stack([jnp.sum(dq * q_normal, axis=1), jnp.sum(dk * k_normal, axis=1)]), 10) / width
        dq = (q_inv * (dq - q_normal * means[0][:, None])).astype(BF16)
        dk = (k_inv * (dk - k_normal * means[1][:, None])).astype(BF16)
        value = dot(dq, qkv[0], NT) + dot(dk, qkv[1], NT) + dot(dv, qkv[2], NT)
        term = jnp.stack([dot(xs, d, TN).astype(BF16) for d in (dq, dk, dv)]).reshape(3, n, m, part, cols)
        gain_own = jnp.stack([q_gain_term, k_gain_term])
        gain_own = lax.dynamic_update_slice(jnp.zeros((2, width), F32), gain_own, (0, seq * cols))
        gain_terms = jnp.concatenate([gain_own, jnp.stack([branch_gain_term, feed_gain_term])]).reshape(4, n, m, part)
        tokens_grad = grad_hidden + scatter_plane(value, 4)
        term = lax.psum_scatter(term, "fsdp", scatter_dimension=2)
        term = lax.all_to_all(term, "seq", 1, 1).astype(F32).transpose(0, 2, 1, 3)
        gain_grads = lax.psum_scatter(
            gain_terms.reshape(4, width), ("seq", "fsdp"), scatter_dimension=1, tiled=True
        )
        term = term.reshape(3, part, width)

    return (
        layer_out.reshape(tokens.shape),
        tokens_grad.reshape(tokens.shape),
        term[0],
        term[1],
        term[2],
        out_grad,
        gain_grads[0],
        gain_grads[1],
        gain_grads[2],
        gate_grad,
        up_grad,
        down_grad,
        gain_grads[3],
    )


def solution(mesh):
    n, m = mesh.shape["seq"], mesh.shape["fsdp"]
    tall, flat, act = P(("seq", "fsdp"), None), P(("seq", "fsdp")), P("fsdp", "seq", None)
    wide, deep = P("fsdp", "seq"), P("seq", "fsdp")
    return jax.shard_map(
        functools.partial(on_device, n, m, 2),
        mesh=mesh,
        in_specs=(act, tall, tall, tall, tall, flat, flat, flat, wide, wide, deep, flat, act),
        out_specs=(act, act, tall, tall, tall, tall, flat, flat, flat, wide, wide, deep, flat),
        check_vma=False,
    )
```
